128 devices in a mesh: tp: 4 (over x), fsdp: 32 (over z, y, core).
Axes of the slice: x: 4, y: 4, z: 4, core: 2. Of those that a mesh axis runs over, the one named last changes fastest.
Arguments:
- emb_table: float32 [16384, 2304], P('tp', 'fsdp')
- tok_ids: int32 [32, 1024], P('fsdp')
- lab_ids: int32 [32, 1024], P('fsdp')
- h_last: bfloat16 [32, 1024, 2304], P('fsdp')
- g_embed: bfloat16 [32, 1024, 2304], P('fsdp')
- norm_w: float32 [2304], P('fsdp')
Outputs:
- output 1: bfloat16 [32, 1024, 2304], P('fsdp')
- output 2: float32 [], replicated
- output 3: bfloat16 [32, 1024, 2304], P('fsdp')
- output 4: float32 [2304], P('fsdp')
- output 5: float32 [16384, 2304], P('tp', 'fsdp')
All inputs are finite; a program needn't handle non-finite values.
Results may differ from the reference program's by a relative error of at most 0.001.
Values are sent between devices in bfloat16 or wider.
A program may use at most 1 GiB of HBM per device.

```python
import math
import jax
import jax.numpy as jnp
from jax import lax

D = 2304
VOCAB = 16384
BATCH = 32
SEQ = 1024

SOFT_CAP = 30.0
NORM_EPS = 1e-6
TOKENS = BATCH * SEQ
LEVELS = VOCAB.bit_length()
GRAD_STD = 12.0 / (TOKENS * math.sqrt(D))


def setup_inputs(seed: int = 0) -> dict:
    key_list = jax.random.split(jax.random.key(seed), 7)
    emb_table = jax.random.normal(key_list[0], (VOCAB, D), jnp.float32) * D ** -0.5
    tok_level = jax.random.randint(key_list[1], (BATCH, SEQ), 0, LEVELS)
    tok_upper = jnp.minimum(jnp.left_shift(jnp.full((BATCH, SEQ), 2, jnp.int32), tok_level), VOCAB)
    tok_ids = jax.random.randint(key_list[2], (BATCH, SEQ), 0, tok_upper)
    tok_ids = tok_ids.at[0, 0].set(VOCAB - 1).at[0, 1].set(0)
    lab_ids = jax.random.randint(key_list[3], (BATCH, SEQ), 0, VOCAB)
    lab_ids = lab_ids.at[BATCH - 1, SEQ - 1].set(VOCAB - 1).at[BATCH - 1, SEQ - 2].set(0)
    h_last = jax.random.normal(key_list[4], (BATCH, SEQ, D), jnp.float32).astype(jnp.bfloat16)
    g_embed = (jax.random.normal(key_list[5], (BATCH, SEQ, D), jnp.float32) * GRAD_STD).astype(jnp.bfloat16)
    norm_w = 15.0 + 5.0 * jax.random.normal(key_list[6], (D,), jnp.float32)
    return {"emb_table": emb_table, "tok_ids": tok_ids, "lab_ids": lab_ids, "h_last": h_last, "g_embed": g_embed, "norm_w": norm_w}


def reference(emb_table, tok_ids, lab_ids, h_last, g_embed, norm_w):
    table_bf = emb_table.astype(jnp.bfloat16)
    emb_scale = jnp.asarray(math.sqrt(D), jnp.bfloat16).astype(jnp.float32)
    x_emb = (jnp.take(table_bf, tok_ids, axis=0).astype(jnp.float32) * emb_scale).astype(jnp.bfloat16)
    norm_gain = 1.0 + norm_w
    vocab_ids = jnp.arange(VOCAB, dtype=jnp.int32)

    def row_step(d_acc, row_in):
        h_row, lab_row = row_in
        h_wide = h_row.astype(jnp.float32)
        inv_rms = lax.rsqrt(jnp.mean(h_wide * h_wide, axis=1, keepdims=True) + NORM_EPS)
        h_norm = h_wide * inv_rms
        x_norm = (h_norm * norm_gain).astype(jnp.bfloat16)
        logits = jnp.dot(x_norm, table_bf.T, preferred_element_type=jnp.float32)
        tanh_z = jnp.tanh(logits / SOFT_CAP)
        capped = SOFT_CAP * tanh_z
        log_norm = jax.nn.logsumexp(capped, axis=1)
        lab_hit = lab_row[:, None] == vocab_ids[None, :]
        lab_logit = jnp.sum(jnp.where(lab_hit, capped, 0.0), axis=1)
        soft_prob = jnp.exp(capped - log_norm[:, None])
        d_logits = ((soft_prob - lab_hit.astype(jnp.float32)) * (1.0 - tanh_z * tanh_z) / TOKENS).astype(jnp.bfloat16)
        d_xnorm = jnp.dot(d_logits, table_bf, preferred_element_type=jnp.float32)
        g_dir = d_xnorm * norm_gain
        d_hid = (inv_rms * (g_dir - h_norm * jnp.mean(g_dir * h_norm, axis=1, keepdims=True))).astype(jnp.bfloat16)
        d_gain = jnp.sum(d_xnorm * h_norm, axis=0)
        d_acc = d_acc + jnp.dot(d_logits.T, x_norm, preferred_element_type=jnp.float32)
        return d_acc, (jnp.sum(log_norm - lab_logit), d_hid, d_gain)

    d_head, (loss_rows, d_hidden, gain_rows) = lax.scan(row_step, jnp.zeros((VOCAB, D), jnp.float32), (h_last, lab_ids))
    loss_val = jnp.sum(loss_rows) / TOKENS
    d_norm_w = jnp.sum(gain_rows, axis=0)
    scaled_grad = (g_embed.astype(jnp.float32) * emb_scale).reshape(TOKENS, D)
    d_look = jax.ops.segment_sum(scaled_grad, tok_ids.reshape(TOKENS), num_segments=VOCAB)
    d_table = d_head + d_look
    return (x_emb, loss_val, d_hidden, d_norm_w, d_table)
```

```python
import math
import jax
import jax.numpy as jnp
from jax import lax
from jax.sharding import PartitionSpec as P

SOFT_CAP = 30.0
NORM_EPS = 1e-6


def solution(mesh):
    fsdp_size = mesh.shape["fsdp"]
    tp_size = mesh.shape["tp"]
    up = [(i, (i + 1) % tp_size) for i in range(tp_size)]
    down = [(i, (i - 1) % tp_size) for i in range(tp_size)]

    def ring_reduce_scatter(part):
        me = lax.axis_index("tp")
        rows = part.shape[0] // tp_size
        half = rows // 2

        def rel(k, lo, n):
            return lax.dynamic_slice_in_dim(part, ((me + k) % tp_size) * rows + lo, n, 0)

        far_up = lax.ppermute(rel(2, 0, half), "tp", up)
        far_down = lax.ppermute(rel(2, half, half), "tp", down)
        to_up = jnp.concatenate([rel(1, 0, half) + far_up, rel(1, half, half)])
        to_down = jnp.concatenate([rel(3, 0, half), rel(3, half, half) + far_down])
        return rel(0, 0, rows) + lax.ppermute(to_up, "tp", up) + lax.ppermute(to_down, "tp", down)

    def ring_all_gather(block):
        me = lax.axis_index("tp")
        rows, width = block.shape
        half = rows // 2
        from_below = lax.ppermute(block, "tp", up)
        from_above = lax.ppermute(block, "tp", down)
        far_lo = lax.ppermute(from_below[:half], "tp", up)
        far_hi = lax.ppermute(from_above[half:], "tp", down)
        out = jnp.zeros((tp_size * rows, width), block.dtype)
        for k, piece, lo in ((0, block, 0), (3, from_below, 0), (1, from_above, 0), (2, far_lo, 0), (2, far_hi, half)):
            out = lax.dynamic_update_slice_in_dim(out, piece, ((me + k) % tp_size) * rows + lo, 0)
        return out

    def device_step(emb_shard, tok_ids, lab_ids, h_last, g_embed, norm_w):
        vocab_rows, cols = emb_shard.shape
        batch_loc, seq_len, width = h_last.shape
        tok_count = batch_loc * seq_len
        total_tokens = tok_count * fsdp_size
        quarter = tok_count // tp_size
        tp_id = lax.axis_index("tp")
        fsdp_id = lax.axis_index("fsdp")
        row_start = tp_id * vocab_rows
        vocab_iota = jnp.arange(vocab_rows, dtype=jnp.int32)
        emb_scale = jnp.asarray(math.sqrt(width), jnp.bfloat16).astype(jnp.float32)
        shard_bf = emb_shard.astype(jnp.bfloat16)

        table = lax.all_gather(shard_bf, "fsdp", axis=1, tiled=True)
        own_w = jnp.where(tp_id == 0, norm_w, 0.0)
        full_w = lax.psum(lax.dynamic_update_slice(jnp.zeros((width,), jnp.float32), own_w, (fsdp_id * cols,)), ("tp", "fsdp"))
        norm_gain = 1.0 + full_w

        tok_local = tok_ids.reshape(tok_count) - row_start
        in_block = (tok_local >= 0) & (tok_local < vocab_rows)
        row_vals = jnp.take(table, jnp.clip(tok_local, 0, vocab_rows - 1), axis=0)
        row_vals = jnp.where(in_block[:, None], row_vals, jnp.zeros_like(row_vals))
        row_vals = ring_all_gather(ring_reduce_scatter(row_vals))
        x_emb = (row_vals.astype(jnp.float32) * emb_scale).astype(jnp.bfloat16)

        h_wide = h_last.reshape(tok_count, width).astype(jnp.float32)
        inv_rms = lax.rsqrt(jnp.mean(h_wide * h_wide, axis=1, keepdims=True) + NORM_EPS)
        h_norm = h_wide * inv_rms
        x_norm = (h_norm * norm_gain).astype(jnp.bfloat16)

        logits = jnp.einsum("td,vd->tv", x_norm, table, preferred_element_type=jnp.float32)
        tanh_z = jnp.tanh(logits / SOFT_CAP)
        capped = SOFT_CAP * tanh_z
        exp_shift = jnp.exp(capped - SOFT_CAP)
        lab_hit = (lab_ids.reshape(tok_count) - row_start)[:, None] == vocab_iota[None, :]
        tok_stats = jnp.stack([jnp.sum(exp_shift, axis=1), jnp.sum(jnp.where(lab_hit, capped, 0.0), axis=1)])
        tok_stats = lax.psum(tok_stats, "tp")
        sum_exp = tok_stats[0]
        loss_rows = jnp.log(sum_exp) + SOFT_CAP - tok_stats[1]

        soft_prob = exp_shift / sum_exp[:, None]
        d_logits = ((soft_prob - lab_hit.astype(jnp.float32)) * (1.0 - tanh_z * tanh_z) / total_tokens).astype(jnp.bfloat16)

        head_part = jnp.einsum("tv,td->vd", d_logits, x_norm, preferred_element_type=jnp.float32)
        tok_hit = (tok_local[:, None] == vocab_iota[None, :]).astype(jnp.bfloat16)
        look_part = jnp.einsum("tv,td->vd", tok_hit, g_embed.reshape(tok_count, width), preferred_element_type=jnp.float32)
        d_table = lax.psum_scatter(head_part + emb_scale * look_part, "fsdp", scatter_dimension=1, tiled=True)

        d_xnorm = ring_reduce_scatter(jnp.dot(d_logits, table, preferred_element_type=jnp.float32))
        h_own = lax.dynamic_slice_in_dim(h_last.reshape(tok_count, width), tp_id * quarter, quarter, 0).astype(jnp.float32)
        r_own = lax.rsqrt(jnp.mean(h_own * h_own, axis=1, keepdims=True) + NORM_EPS)
        hn_own = h_own * r_own
        g_dir = d_xnorm * norm_gain
        d_own = (r_own * (g_dir - hn_own * jnp.mean(g_dir * hn_own, axis=1, keepdims=True))).astype(jnp.bfloat16)
        d_hidden = ring_all_gather(d_own)

        loss_own = jnp.sum(lax.dynamic_slice_in_dim(loss_rows, tp_id * quarter, quarter, 0))
        tail = jnp.concatenate([jnp.sum(d_xnorm * hn_own, axis=0), jnp.full((128,), loss_own)])
        tail = lax.psum(tail, ("tp", "fsdp"))
        loss_val = tail[width] / total_tokens
        d_norm_w = lax.dynamic_slice(tail, (fsdp_id * cols,), (cols,))
        return (x_emb.reshape(batch_loc, seq_len, width), loss_val, d_hidden.reshape(batch_loc, seq_len, width), d_norm_w, d_table)

    spec_tok = P("fsdp", None)
    spec_act = P("fsdp", None, None)
    return jax.shard_map(device_step, mesh=mesh, in_specs=(P("tp", "fsdp"), spec_tok, spec_tok, spec_act, spec_act, P("fsdp")), out_specs=(spec_act, P(), spec_act, P("fsdp"), P("tp", "fsdp")), check_vma=False)
```

```python
import functools
import math
import jax
import jax.numpy as jnp
from jax import lax
from jax.experimental import pallas as pl
from jax.experimental.pallas import tpu as pltpu
from jax.sharding import PartitionSpec as P

SOFT_CAP = 30.0
NORM_EPS = 1e-6
MESH = pl.DeviceIdType.MESH
F32, BF16 = jnp.float32, jnp.bfloat16


class Place:
    def __init__(self, sizes):
        self.nx, self.nz, self.ny, self.nc = sizes
        self.x = lax.axis_index("tp")
        self.f = lax.axis_index("fsdp")
        self.c = self.f % self.nc
        chip = self.f // self.nc
        self.y = chip % self.ny
        self.z = chip // self.ny

    def at(self, dx=0, dz=0, dy=0, dc=0):
        z, y, c = (self.z + dz) % self.nz, (self.y + dy) % self.ny, (self.c + dc) % self.nc
        return ((self.x + dx) % self.nx, (z * self.ny + y) * self.nc + c)

    def peers(self, dims):
        size = {"dx": self.nx, "dz": self.nz, "dy": self.ny, "dc": self.nc}
        return [self.at(**{d: k}) for d in dims for k in range(1, size[d])]


def enter(place, dims):
    barrier = pltpu.get_barrier_semaphore()
    peers = place.peers(dims)
    for peer in peers:
        pl.semaphore_signal(barrier, inc=1, device_id=peer, device_id_type=MESH)
    pl.semaphore_wait(barrier, len(peers))


class SmallSum:
    def __init__(self, place, dims, slots, send_sems, recv_sems):
        self.place, self.dims, self.slots, self.send_sems, self.recv_sems = place, dims, slots, send_sems, recv_sems
        self.size = {"dx": place.nx, "dz": place.nz, "dy": place.ny, "dc": place.nc}
        self.me = {"dx": place.x, "dz": place.z, "dy": place.y, "dc": place.c}
        self.base, count = {}, 0
        for d in dims:
            self.base[d] = count
            count += self.size[d]

    def copies(self, d):
        slot = self.slots.at[self.base[d] + self.me[d]]
        for k in range(1, self.size[d]):
            yield pltpu.make_async_remote_copy(
                slot, slot, self.send_sems.at[self.base[d] + k], self.recv_sems.at[self.base[d] + k],
                device_id=self.place.at(**{d: k}), device_id_type=MESH)

    def start(self, d, value):
        self.slots[self.base[d] + self.me[d]] = value
        for copy in self.copies(d):
            copy.start()

    def finish(self, d):
        for copy in self.copies(d):
            copy.wait()
        total = self.slots[self.base[d]]
        for k in range(1, self.size[d]):
            total = total + self.slots[self.base[d] + k]
        return total


def gain_kernel(sizes, w_ref, o_ref, slots, send_sems, recv_sems):
    place = Place(sizes)
    dims = ("dc", "dy", "dz")
    enter(place, dims)
    ring = SmallSum(place, dims, slots, send_sems, recv_sems)
    value = w_ref[...]
    for d in dims:
        ring.start(d, value)
        value = ring.finish(d)
    o_ref[...] = value


def gather_gain(sizes, placed):
    _, nz, ny, nc = sizes
    n = nz + ny + nc
    return pl.pallas_call(
        functools.partial(gain_kernel, sizes),
        name="gain_sum",
        out_shape=jax.ShapeDtypeStruct(placed.shape, F32),
        in_specs=[pl.BlockSpec(memory_space=pltpu.VMEM)],
        out_specs=pl.BlockSpec(memory_space=pltpu.VMEM),
        scratch_shapes=[
            pltpu.VMEM((n,) + placed.shape, F32),
            pltpu.SemaphoreType.DMA((n,)),
            pltpu.SemaphoreType.DMA((n,)),
        ],
        compiler_params=pltpu.CompilerParams(collective_id=0, has_side_effects=True),
    )(placed)


def back_kernel(
    sizes, dims,
    dz_hbm, et_hbm, xnt_hbm, look_hbm, h_hbm, gain_ref, loss_ref,
    dh_out, de_out, tail_out, ra_hbm, rx_hbm, xpar_hbm,
    dz_own, dz_par, et_buf, part, fx, acc, fa, f2, r2, xb, h_buf, dh_buf, dg_acc, slots,
    x_send, x_recv, a_send, a_recv, p_send, p_recv, h_send, h_recv, s_send, s_recv,
    et_sem, look_sem, xb_sem, misc_sem, stage_sem,
):
    nx, nz, ny, nc = sizes
    tok, vocab, width, tile, per_chunk = dims["tok"], dims["vocab"], dims["width"], dims["tile"], dims["per_chunk"]
    place = Place(sizes)
    x, z, y, c = place.x, place.z, place.y, place.c
    half_v = vocab // nc
    lanes = half_v // 2
    rows = width // (nz * ny)
    quarter = tok // nx
    hq = quarter // 2
    chunks = width // (tile * per_chunk)
    chunk_w = tile * per_chunk
    n_step = min(256, lanes)
    up, down = place.at(dx=1), place.at(dx=nx - 1)
    partner = place.at(dc=1)

    def rcopy(src, dst, sends, recvs, i, dev):
        return pltpu.make_async_remote_copy(src, dst, sends.at[i], recvs.at[i], device_id=dev, device_id_type=MESH)

    enter(place, ("dx", "dz", "dy", "dc"))

    if nc == 2:
        other = pl.multiple_of((1 - c) * half_v, 128)
        give_dz = rcopy(dz_hbm.at[:, pl.ds(other, half_v)], dz_par, p_send, p_recv, 0, partner)
        give_xn = rcopy(xnt_hbm, xpar_hbm, p_send, p_recv, 1, partner)
        give_dz.start()
        give_xn.start()
    load_dz = pltpu.make_async_copy(dz_hbm, dz_own, misc_sem.at[0])
    load_dz.start()
    load_h = pltpu.make_async_copy(h_hbm.at[pl.ds(pl.multiple_of(x * quarter, 16), quarter)], h_buf, misc_sem.at[1])
    load_h.start()

    def load_et(t, slot):
        return pltpu.make_async_copy(et_hbm.at[pl.ds(pl.multiple_of(t * tile, tile), tile)], et_buf.at[slot], et_sem.at[slot])

    load_et(0, 0).start()

    slot_of = {2: 0, 1: 1, 3: 2, 0: 0}
    order = (2, 1, 3, 0)

    def block_of(ref, half, k):
        if half == 0:
            return ref.at[(z + k) % nz]
        return ref.at[:, (y + k) % ny]

    def load_look(half, k):
        if half == 0:
            src = look_hbm.at[(z + k) % nz, :, :, pl.ds(0, lanes)]
        else:
            src = look_hbm.at[:, (y + k) % ny, :, pl.ds(lanes, lanes)]
        return pltpu.make_async_copy(src, acc.at[half, slot_of[k]], look_sem.at[half, slot_of[k]])

    def load_xn(half, k, i):
        return pltpu.make_async_copy(block_of((xnt_hbm, xpar_hbm)[i], half, k), xb.at[half, i], xb_sem.at[half, i])

    def load_xns(half, k):
        for i in range(nc):
            load_xn(half, k, i).start()

    for k in order[:3]:
        for half in (0, 1):
            load_look(half, k).start()
    for half in (0, 1):
        load_xn(half, 2, 0).start()

    load_dz.wait()

    def dxn_chunk(d):
        def body(i, carry):
            t = d * per_chunk + i
            slot = t % 2

            @pl.when(t + 1 < chunks * per_chunk)
            def _():
                load_et(t + 1, (t + 1) % 2).start()

            load_et(t, slot).wait()
            part[d, :, pl.ds(pl.multiple_of(i * tile, tile), tile)] = lax.dot_general(
                dz_own[...], et_buf[slot], (((1,), (1,)), ((), ())), preferred_element_type=F32)
            return carry

        lax.fori_loop(0, per_chunk, body, 0)

    def qrow(k, lo=0):
        return pl.multiple_of(((x + k) % nx) * quarter + lo, 8)

    both = (0, 1)
    ways_x = (up, down)

    def x_far(d, i):
        return rcopy(part.at[d, pl.ds(qrow(2, i * hq), hq)], fx.at[d, i], x_send, x_recv, 4 * d + i, ways_x[i])

    def x_near(d, i):
        return rcopy(part.at[d, pl.ds(qrow((1, 3)[i]), quarter)], rx_hbm.at[d, i], x_send, x_recv, 4 * d + 2 + i, ways_x[i])

    def x_first(d):
        for i in both:
            x_far(d, i).start()

    def x_second(d):
        for i, (k, lo) in enumerate(((1, 0), (3, hq))):
            x_far(d, i).wait_recv()
            sel = pl.ds(qrow(k, lo), hq)
            part[d, sel] = part[d, sel] + fx[d, i]
            x_near(d, i).start()

    def stage_x(d, j):
        return [pltpu.make_async_copy(rx_hbm.at[d, i, pl.ds(j * hq, hq)], fx.at[d, i], stage_sem.at[i]) for i in (0, 1)]

    def x_third(d):
        for i in both:
            x_near(d, i).wait_recv()
        for j in (0, 1):
            for copy in stage_x(d, j):
                copy.start()
            for copy in stage_x(d, j):
                copy.wait()
            sel = pl.ds(qrow(0, j * hq), hq)
            part[d, sel] = part[d, sel] + fx[d, 0] + fx[d, 1]

    def de_unit(half, k):
        slot = slot_of[k]
        load_look(half, k).wait()
        for i in range(nc):
            load_xn(half, k, i).wait()

        def body(n, carry):
            off = half * lanes + n * n_step
            own = dz_own[:, pl.ds(pl.multiple_of(c * half_v + off, 128), n_step)]
            total = jnp.dot(xb[half, 0].reshape(4 * rows, tok), own, preferred_element_type=F32)
            if nc == 2:
                theirs = dz_par[:, pl.ds(pl.multiple_of(off, 128), n_step)]
                total = total + jnp.dot(xb[half, 1].reshape(4 * rows, tok), theirs, preferred_element_type=F32)
            sel = pl.ds(pl.multiple_of(n * n_step, 128), n_step)
            acc[half, slot, :, :, sel] = acc[half, slot, :, :, sel] + total.reshape(4, rows, n_step)
            return carry

        lax.fori_loop(0, lanes // n_step, body, 0)

    def ring(half, step):
        return place.at(dz=step) if half == 0 else place.at(dy=step)

    def cross(half, step):
        return place.at(dy=step) if half == 0 else place.at(dz=step)

    def a_far(half, i):
        return rcopy(acc.at[half, 0, pl.ds(2 * i, 2)], fa.at[half, i], a_send, a_recv, 8 * half + i, ring(half, (1, 3)[i]))

    def a_near(half, i):
        return rcopy(acc.at[half, 1 + i], ra_hbm.at[half, i], a_send, a_recv, 8 * half + 2 + i, ring(half, (1, 3)[i]))

    def a_second(i):
        for half in (0, 1):
            a_far(half, i).wait_recv()
            sel = pl.ds(2 * i, 2)
            acc[half, 1 + i, sel] = acc[half, 1 + i, sel] + fa[half, i]
            a_near(half, i).start()

    def stage_a(half, j):
        return [pltpu.make_async_copy(ra_hbm.at[half, i, pl.ds(2 * j, 2)], fa.at[half, i], stage_sem.at[2 + 2 * half + i]) for i in (0, 1)]

    def cross_of(half, k):
        return ((y if half == 0 else z) + k) % 4

    half_rows = rows // 2

    def c_far(half, i):
        src = acc.at[half, 0, cross_of(half, 2), pl.ds(i * half_rows, half_rows)]
        return rcopy(src, f2.at[half, i], a_send, a_recv, 8 * half + 4 + i, cross(half, (1, 3)[i]))

    def c_near(half, i):
        return rcopy(acc.at[half, 0, cross_of(half, (1, 3)[i])], r2.at[half, i], a_send, a_recv, 8 * half + 6 + i, cross(half, (1, 3)[i]))

    def a_third(half):
        for i in both:
            a_near(half, i).wait_recv()
        for j in (0, 1):
            for copy in stage_a(half, j):
                copy.start()
            for copy in stage_a(half, j):
                copy.wait()
            sel = pl.ds(2 * j, 2)
            acc[half, 0, sel] = acc[half, 0, sel] + fa[half, 0] + fa[half, 1]
        for i in both:
            c_far(half, i).start()

    def c_second(half):
        for i, k in enumerate((1, 3)):
            c_far(half, i).wait_recv()
            piece = cross_of(half, k)
            sel = pl.ds(i * half_rows, half_rows)
            acc[half, 0, piece, sel] = acc[half, 0, piece, sel] + f2[half, i]
            c_near(half, i).start()

    def out_copies(half):
        mine = cross_of(half, 0)
        sel = pl.ds(pl.multiple_of(c * half_v + half * lanes, 128), lanes)
        if nc == 1:
            return [pltpu.make_async_copy(acc.at[half, 0, mine], de_out.at[:, sel], misc_sem.at[2 + half])], []
        local = pltpu.make_async_copy(acc.at[half, 0, mine, pl.ds(pl.multiple_of(c * half_rows, 8), half_rows)], de_out.at[:, sel], misc_sem.at[2 + half])
        remote = rcopy(acc.at[half, 0, mine, pl.ds(pl.multiple_of((1 - c) * half_rows, 8), half_rows)], de_out.at[:, sel], p_send, p_recv, 2 + half, partner)
        return [local], [remote]

    def c_third(half):
        for i in both:
            c_near(half, i).wait_recv()
        mine = cross_of(half, 0)
        acc[half, 0, mine] = acc[half, 0, mine] + r2[half, 0] + r2[half, 1]
        for copies in out_copies(half):
            for copy in copies:
                copy.start()

    ring_x, ring_a = nx == 4, nz == 4

    def at_x(fn, *args):
        if ring_x:
            fn(*args)

    def at_a(fn, *args):
        if ring_a:
            fn(*args)

    dxn_chunk(0)
    at_x(x_first, 0)
    if chunks > 1:
        dxn_chunk(1)
        at_x(x_first, 1)
    if nc == 2:
        give_dz.wait_recv()
        give_xn.wait_recv()
        for half in (0, 1):
            load_xn(half, 2, 1).start()
    for half in (0, 1):
        de_unit(half, 2)
        load_xns(half, 1)
        if ring_a:
            for i in both:
                a_far(half, i).start()
    at_x(x_second, 0)
    for d in range(2, chunks):
        dxn_chunk(d)
        at_x(x_first, d)
        at_x(x_second, d - 1)
    for half in (0, 1):
        de_unit(half, 1)
        load_xns(half, 3)
    at_a(a_second, 0)
    at_x(x_second, chunks - 1)
    for half in (0, 1):
        de_unit(half, 3)
        load_xns(half, 0)
    at_a(a_second, 1)
    for half in (0, 1):
        if ring_a:
            for i in both:
                a_far(half, i).wait_send()
        load_look(half, 0).start()
    for half in (0, 1):
        de_unit(half, 0)
    for d in range(chunks):
        at_x(x_third, d)

    load_h.wait()
    dg_acc[...] = jnp.zeros_like(dg_acc)
    step = min(32, quarter)

    def dh_body(i, carry):
        sel = pl.ds(pl.multiple_of(i * step, step), step)
        row = pl.ds(pl.multiple_of((x * quarter) + i * step, step), step)
        d_x = jnp.concatenate([part[d, row] for d in range(chunks)], axis=1)
        h_wide = h_buf[sel].astype(F32)
        inv_rms = lax.rsqrt(jnp.sum(h_wide * h_wide, axis=1, keepdims=True) * (1.0 / width) + NORM_EPS)
        h_norm = h_wide * inv_rms
        g_dir = d_x * gain_ref[...]
        mean = jnp.sum(g_dir * h_norm, axis=1, keepdims=True) * (1.0 / width)
        dh_buf[sel] = (inv_rms * (g_dir - h_norm * mean)).astype(BF16)
        prod = d_x * h_norm
        total = prod[0:8]
        for j in range(8, step, 8):
            total = total + prod[j:j + 8]
        dg_acc[...] = dg_acc[...] + total
        return carry

    lax.fori_loop(0, quarter // step, dh_body, 0)

    def h_first(i):
        return rcopy(dh_buf, dh_out.at[pl.ds(qrow(0), quarter)], h_send, h_recv, i, ways_x[i])

    def h_second(i):
        ref = dh_out.at[pl.ds(qrow((3, 1)[i], i * hq), hq)]
        return rcopy(ref, ref, h_send, h_recv, 2 + i, ways_x[i])

    keep_dh = pltpu.make_async_copy(dh_buf, dh_out.at[pl.ds(qrow(0), quarter)], misc_sem.at[4])
    keep_dh.start()
    if ring_x:
        for i in both:
            h_first(i).start()

    small = SmallSum(place, ("dc", "dx", "dy", "dz"), slots, s_send, s_recv)
    small.start("dc", jnp.concatenate([dg_acc[...], loss_ref[...]], axis=1))
    at_a(a_third, 0)
    at_a(a_third, 1)
    small.start("dx", small.finish("dc"))
    at_a(c_second, 0)
    at_a(c_second, 1)
    small.start("dy", small.finish("dx"))
    if ring_x:
        for i in (0, 1):
            h_first(i).wait_recv()
            h_second(i).start()
    small.start("dz", small.finish("dy"))
    if ring_a:
        c_third(0)
        c_third(1)
    else:
        for half in (0, 1):
            for copies in out_copies(half):
                for copy in copies:
                    copy.start()
    tail_out[...] = small.finish("dz")

    keep_dh.wait()
    if ring_x:
        for i in both:
            for d in range(chunks):
                x_far(d, i).wait_send()
                x_near(d, i).wait_send()
            h_first(i).wait_send()
            h_second(i).wait()
    if ring_a:
        for half in (0, 1):
            for i in both:
                a_near(half, i).wait_send()
                c_far(half, i).wait_send()
                c_near(half, i).wait_send()
    if nc == 2:
        give_dz.wait_send()
        give_xn.wait_send()
    for half in (0, 1):
        local, remote = out_copies(half)
        for copy in local + remote:
            copy.wait()


def back(sizes, dz, et, xnt, look, h, gain, loss, tile, per_chunk, limit):
    nx, nz, ny, nc = sizes
    tok, vocab = dz.shape
    width = et.shape[0]
    rows = width // (nz * ny)
    half_v = vocab // nc
    lanes = half_v // 2
    quarter = tok // nx
    hq = quarter // 2
    chunk_w = tile * per_chunk
    chunks = width // chunk_w
    tail_w = width + loss.shape[1]
    dims = {"tok": tok, "vocab": vocab, "width": width, "tile": tile, "per_chunk": per_chunk}
    xnt = xnt.reshape(nz, ny, rows, tok)
    look = look.reshape(nz, ny, rows, half_v)
    anyspace = pl.BlockSpec(memory_space=pl.ANY)
    vmem = pl.BlockSpec(memory_space=pltpu.VMEM)
    n_small = nx + nz + ny + nc
    dma = pltpu.SemaphoreType.DMA
    out = pl.pallas_call(
        functools.partial(back_kernel, sizes, dims),
        name="back",
        out_shape=(
            jax.ShapeDtypeStruct((tok, width), BF16),
            jax.ShapeDtypeStruct((rows // nc, vocab), F32),
            jax.ShapeDtypeStruct((8, tail_w), F32),
            jax.ShapeDtypeStruct((2, 2, 4, rows, lanes), F32),
            jax.ShapeDtypeStruct((chunks, 2, quarter, chunk_w), F32),
            jax.ShapeDtypeStruct((nz, ny, rows, tok), BF16),
        ),
        in_specs=[anyspace] * 5 + [vmem] * 2,
        out_specs=(anyspace, anyspace, vmem, anyspace, anyspace, anyspace),
        scratch_shapes=[
            pltpu.VMEM((tok, vocab), BF16),
            pltpu.VMEM((tok, half_v), BF16),
            pltpu.VMEM((2, tile, vocab), BF16),
            pltpu.VMEM((chunks, tok, chunk_w), F32),
            pltpu.VMEM((chunks, 2, hq, chunk_w), F32),
            pltpu.VMEM((2, 3, 4, rows, lanes), F32),
            pltpu.VMEM((2, 2, 2, rows, lanes), F32),
            pltpu.VMEM((2, 2, rows // 2, lanes), F32),
            pltpu.VMEM((2, 2, rows, lanes), F32),
            pltpu.VMEM((2, nc, 4, rows, tok), BF16),
            pltpu.VMEM((quarter, width), BF16),
            pltpu.VMEM((quarter, width), BF16),
            pltpu.VMEM((8, width), F32),
            pltpu.VMEM((n_small, 8, tail_w), F32),
            dma((4 * chunks,)), dma((4 * chunks,)),
            dma((16,)), dma((16,)),
            dma((4,)), dma((4,)),
            dma((4,)), dma((4,)),
            dma((n_small,)), dma((n_small,)),
            dma((2,)), dma((2, 3)), dma((2, nc)), dma((5,)), dma((6,)),
        ],
        compiler_params=pltpu.CompilerParams(collective_id=1, has_side_effects=True, vmem_limit_bytes=limit),
        cost_estimate=pl.CostEstimate(flops=4 * tok * vocab * width, bytes_accessed=200_000_000, transcendentals=0),
    )(dz, et, xnt, look, h, gain, loss)
    return out[:3]


def solution(mesh):
    tp_size, fsdp_size = mesh.shape["tp"], mesh.shape["fsdp"]
    return build(mesh, (tp_size, 4, fsdp_size // 8, 2), 256, 3, 62 * 2**20)


def build(mesh, sizes, tile, per_chunk, limit):
    fsdp_size = mesh.shape["fsdp"]
    nc = sizes[3]
    flip = [(i, i ^ 1) for i in range(fsdp_size)]

    def device_step(emb_shard, tok_ids, lab_ids, h_last, g_embed, norm_w):
        vocab_rows, cols = emb_shard.shape
        batch_loc, seq_len, width = h_last.shape
        tok_count = batch_loc * seq_len
        total_tokens = tok_count * fsdp_size
        quarter = tok_count // mesh.shape["tp"]
        half_v = vocab_rows // nc
        tp_id = lax.axis_index("tp")
        fsdp_id = lax.axis_index("fsdp")
        core = fsdp_id % nc
        row_start = tp_id * vocab_rows
        emb_scale = jnp.asarray(math.sqrt(width), BF16).astype(F32)
        vocab_iota = jnp.arange(vocab_rows, dtype=jnp.int32)

        table = lax.all_gather(emb_shard.T.astype(BF16), "fsdp", axis=0, tiled=True)
        placed = lax.dynamic_update_slice(jnp.zeros((8, width), F32), jnp.broadcast_to(norm_w, (8, cols)), (0, fsdp_id * cols))
        norm_gain = 1.0 + gather_gain(sizes, placed)[0:1]

        h_flat = h_last.reshape(tok_count, width)
        g_flat = g_embed.reshape(tok_count, width)
        tok_flat = tok_ids.reshape(tok_count)
        h_wide = h_flat.astype(F32)
        inv_rms = lax.rsqrt(jnp.mean(h_wide * h_wide, axis=1, keepdims=True) + NORM_EPS)
        x_norm = (h_wide * inv_rms * norm_gain).astype(BF16)

        half_iota = jnp.arange(half_v, dtype=jnp.int32) + row_start + core * half_v

        def look_of(tok, g):
            hit = (tok[:, None] == half_iota[None, :]).astype(BF16)
            return lax.dot_general(g, hit, (((0,), (0,)), ((), ())), preferred_element_type=F32)

        look = look_of(tok_flat, g_flat)
        if nc == 2:
            look = look + look_of(lax.ppermute(tok_flat, "fsdp", flip), lax.ppermute(g_flat, "fsdp", flip))
        look = emb_scale * look

        logits = lax.dot_general(x_norm, table, (((1,), (0,)), ((), ())), preferred_element_type=F32)
        tanh_z = jnp.tanh(logits / SOFT_CAP)
        capped = SOFT_CAP * tanh_z
        exp_shift = jnp.exp(capped - SOFT_CAP)
        lab_hit = (lab_ids.reshape(tok_count) - row_start)[:, None] == vocab_iota[None, :]
        tok_stats = jnp.stack([jnp.sum(exp_shift, axis=1), jnp.sum(jnp.where(lab_hit, capped, 0.0), axis=1)])
        tok_stats = lax.psum(tok_stats, "tp")
        sum_exp = tok_stats[0]
        loss_rows = jnp.log(sum_exp) + SOFT_CAP - tok_stats[1]
        soft_prob = exp_shift / sum_exp[:, None]
        d_logits = ((soft_prob - lab_hit.astype(F32)) * (1.0 - tanh_z * tanh_z) / total_tokens).astype(BF16)

        tok_hit = ((tok_flat - row_start)[:, None] == vocab_iota[None, :]).astype(BF16)
        row_vals = lax.dot_general(tok_hit, table, (((1,), (1,)), ((), ())), preferred_element_type=F32).astype(BF16)
        row_vals = lax.psum(row_vals, "tp")
        x_emb = (row_vals.astype(F32) * emb_scale).astype(BF16)

        loss_own = lax.dynamic_slice_in_dim(loss_rows, tp_id * quarter, quarter, 0)
        loss_part = jnp.sum(loss_own.reshape(8, quarter // 8), axis=1, keepdims=True)
        loss_part = jnp.broadcast_to(loss_part, (8, 128))
        d_hidden, d_cols, tail = back(sizes, d_logits, table, x_norm.T, look, h_flat, norm_gain, loss_part, tile, per_chunk, limit)
        tail = jnp.sum(tail, axis=0)
        loss_val = tail[width] / total_tokens
        d_norm_w = lax.dynamic_slice(tail, (fsdp_id * cols,), (cols,))
        return (x_emb.reshape(batch_loc, seq_len, width), loss_val, d_hidden.reshape(batch_loc, seq_len, width), d_norm_w, d_cols.T)

    spec_tok = P("fsdp", None)
    spec_act = P("fsdp", None, None)
    return jax.shard_map(device_step, mesh=mesh, in_specs=(P("tp", "fsdp"), spec_tok, spec_tok, spec_act, spec_act, P("fsdp")), out_specs=(spec_act, P(), spec_act, P("fsdp"), P("tp", "fsdp")), check_vma=False)
```

```python
import functools
import math
import jax
import numpy as np
import jax.numpy as jnp
from jax import lax
from jax.experimental import pallas as pl
from jax.experimental.pallas import tpu as pltpu
from jax.sharding import PartitionSpec as P

SOFT_CAP = 30.0
NORM_EPS = 1e-6
F32, BF16, I32 = jnp.float32, jnp.bfloat16, jnp.int32
LANE, SUB = 128, 8
BOTH = (0, 1)
FOUR = range(4)
WAYS = (1, 3)
FROM = (3, 1)
FAR = 2
CORES = 2


def span(start, size, unit=LANE):
    return pl.ds(pl.multiple_of(start, unit), size)


class Place:
    def __init__(self, n, sends, recvs, local_sems):
        self.n, self.sends, self.recvs, self.local_sems = n, sends, recvs, local_sems
        self.x = lax.axis_index("tp")
        f = lax.axis_index("fsdp")
        self.f = f
        self.c = f % CORES
        self.y = f // CORES % n
        self.z = f // CORES // n
        self.link_of, self.local_of, self.n_link, self.n_local = {}, {}, 0, 0
        self.size = {"dx": n, "dz": n, "dy": n, "dc": CORES}
        self.me = {"dx": self.x, "dz": self.z, "dy": self.y, "dc": self.c}

    def at(self, dx=0, dz=0, dy=0, dc=0):
        n = self.n
        z, y, c = (self.z + dz) % n, (self.y + dy) % n, (self.c + dc) % CORES
        return ((self.x + dx) % n, (z * n + y) * CORES + c)

    def enter(self):
        barrier = pltpu.get_barrier_semaphore()
        peers = [self.at(**{d: k}) for d in self.size for k in range(1, self.size[d])]
        for peer in peers:
            pl.semaphore_signal(barrier, inc=1, device_id=peer, device_id_type=pl.DeviceIdType.MESH)
        pl.semaphore_wait(barrier, len(peers))

    def link(self, key, count=1):
        if key not in self.link_of:
            self.link_of[key] = self.n_link
            self.n_link += count
        return self.link_of[key]

    def send(self, key, src, dst, **step):
        i = self.link(key)
        return pltpu.make_async_remote_copy(
            src, dst, self.sends.at[i], self.recvs.at[i], device_id=self.at(**step), device_id_type=pl.DeviceIdType.MESH)

    def local(self, key, src, dst, slot=0, count=2):
        if key not in self.local_of:
            self.local_of[key] = self.n_local
            self.n_local += count
        return pltpu.make_async_copy(src, dst, self.local_sems.at[self.local_of[key] + slot])


class SmallSum:
    def __init__(self, place, dims, slots):
        self.place, self.slots, self.dims, self.base = place, slots, dims, {}
        count = 0
        for d in dims:
            self.base[d] = count
            count += place.size[d]

    def copies(self, d):
        slot = self.slots.at[self.base[d] + self.place.me[d]]
        for k in range(1, self.place.size[d]):
            yield self.place.send((self.dims, d, k), slot, slot, **{d: k})

    def start(self, d, value):
        self.slots[self.base[d] + self.place.me[d]] = value
        for copy in self.copies(d):
            copy.start()

    def finish(self, d):
        for copy in self.copies(d):
            copy.wait()
        total = self.slots[self.base[d]]
        for k in range(1, self.place.size[d]):
            total = total + self.slots[self.base[d] + k]
        return total


def scope(name):
    return jax.named_scope(name)


def start_all(copies):
    for copy in copies:
        copy.start()


def digits(text):
    return tuple(tuple(int(d) for d in word) for word in text.split())


UNITS = [digits(u) for u in ("00 10 30", "01 03 20", "02 11 31", "13 33 21 23", "12 32 22")]
PAIR, ALL = 1, "all"
PIECES = [2 * len(u) for u in UNITS]
BASE = [sum(PIECES[:i]) for i in range(len(UNITS))]


def front_kernel(
    dims,
    shard_ref, tok_ref, labc, w_ref, h_hbm, g_hbm,
    et_out, xnt_out, xpar_out, dz_out, dzpar_out, lt_out, x0_out, u_hbm, gain_out, loss_out,
    shard_t, chunk, tokr, hit_t, lhs, xp, xo, xr, xf, xg, xq, etb, xn, gl, lts, z_even, z_odd, dzb,
    acc_e, acc_l, inv_s, w_slots, s_slots, sends, recvs, local_sems,
):
    n, tok, vocab, width, vt = dims["n"], dims["tok"], dims["vocab"], dims["width"], dims["vt"]
    place = Place(n, sends, recvs, local_sems)
    x, z, y, c = place.x, place.z, place.y, place.c
    half_v = vocab // CORES
    n_tile = vocab // vt
    n_half = n_tile // CORES
    hh = n_half // 2
    cols = width // (n * n * CORES)
    quarter = tok // n
    row_start = x * vocab

    def ring1(h, k):
        return {"dy": k} if h == 0 else {"dz": k}

    def ring2(h, k):
        return {"dz": k} if h == 0 else {"dy": k}

    def coord(base, k, paired):
        every = slice(None)
        if k == ALL:
            return every, every
        return every if paired else (base + k) % n // 2, (base + k) % 2

    def loc(h, k1, k2, lo=0, size=n_half, pair1=False, pair2=False):
        first, second = coord((y, z)[h], k1, pair1), coord((z, y)[h], k2, pair2)
        return et_out.at[(pl.ds(c * n_half + lo, size), *((second, first)[h]), *((first, second)[h]), h)]

    with scope("f_enter"):
        place.enter()

    load_g = place.local("g", g_hbm, xn)
    load_g.start()
    with scope("f_cast"):
        for t in range(n_tile):
            shard_t[t] = shard_ref[:, pl.ds(t * vt, vt)].astype(BF16)
        tokr[c] = jnp.broadcast_to(tok_ref[...], (SUB, tok))
        give_tok = place.send("tok", tokr.at[c], tokr.at[c], dc=1)
        give_chunk = place.send("chunk", shard_t.at[pl.ds((1 - c) * n_half, n_half)], chunk.at[c], dc=1)
        give_chunk.start()
        give_tok.start()
        chunk[c] = shard_t[pl.ds(c * n_half, n_half)]
        gain_sum = SmallSum(place, ("dc", "dy", "dz"), w_slots)
        gain_sum.start("dc", w_ref[...])

    def p1_send(h, i):
        return place.send(("p1", h, i), chunk.at[h], loc(h, 0, 0), **ring1(h, WAYS[i]))

    def p1_fwd(h, i):
        ref = loc(h, FROM[i], 0, i * hh, hh)
        return place.send(("p1f", h, i), ref, ref, **ring1(h, WAYS[i]))

    def p2_send(h, k1, i):
        ref = loc(h, k1, 0, pair1=k1 == PAIR)
        return place.send(("p2", h, k1, i), chunk.at[h] if k1 == 0 else ref, ref, **ring2(h, WAYS[i]))

    def p2_fwd(h, k1, i):
        ref = loc(h, k1, FROM[i], i * hh, hh, pair1=k1 == PAIR)
        return place.send(("p2f", h, k1, i), ref, ref, **ring2(h, WAYS[i]))

    def keep(h):
        return place.local("keep", chunk.at[h], loc(h, 0, 0), h)

    def share(h, k2):
        ref = loc(h, ALL, k2, pair2=k2 == PAIR)
        return place.send(("share", h, k2), ref, ref, dc=1)

    def pass_first():
        with scope("f_p1"):
            for h in BOTH:
                for i in BOTH:
                    p1_send(h, i).wait_recv()
                    p1_fwd(h, i).start()
                start_all(p2_send(h, PAIR, i) for i in BOTH)

    def pass_first_far():
        with scope("f_p1f"):
            for h in BOTH:
                for i in BOTH:
                    p1_fwd(h, i).wait_recv()
                start_all(p2_send(h, FAR, j) for j in BOTH)

    def pass_second(k1):
        with scope("f_p2"):
            for h in BOTH:
                for i in BOTH:
                    p2_send(h, k1, i).wait_recv()
                    p2_fwd(h, k1, i).start()

    def end_second(k1):
        with scope("f_p2f"):
            for h in BOTH:
                for i in BOTH:
                    p2_fwd(h, k1, i).wait_recv()

    def share_group(k2):
        start_all(share(h, k2) for h in BOTH)

    with scope("f_chunk"):
        give_chunk.wait_recv()
        for h in BOTH:
            start_all(p1_send(h, i) for i in BOTH)
        for h in BOTH:
            start_all(p2_send(h, 0, i) for i in BOTH)
            keep(h).start()

    v_step = min(64, half_v)

    def hit_body(j, carry):
        off = j * v_step
        ids = lax.broadcasted_iota(I32, (v_step, tok), 0) + (row_start + c * half_v + off)
        for i, core in enumerate((c, 1 - c)):
            hit_t[span(off, v_step, v_step), pl.ds(i * tok, tok)] = jnp.where(ids == tokr[core, 0:1, :], 1.0, 0.0).astype(BF16)
        return carry

    with scope("f_hit"):
        give_tok.wait_recv()
        lax.fori_loop(0, half_v // v_step, hit_body, 0)

    n_step = min(256, tok)
    most = max(PIECES)

    def whole(u):
        return pl.ds(BASE[u], PIECES[u])

    def unit_copies(u):
        slot = u % 2
        for p, (h, (k1, k2)) in enumerate((h, k) for h in BOTH for k in UNITS[u]):
            yield place.local("lhs", loc(h, k1, k2), lhs.at[slot, p], slot * most + p, 2 * most)

    def load_unit(u):
        start_all(unit_copies(u))

    def look(u):
        pieces = PIECES[u]
        with scope("f_look"):
            if u > 1:
                x_swap(u - 2).wait_send()
            left = lhs.at[u % 2]
            for copy in unit_copies(u):
                copy.wait()
            for i, dst in enumerate((xp.at[whole(u)], xo.at[u % 2])):
                def body(j, carry):
                    off = j * n_step
                    value = jnp.concatenate([left[pl.ds(0, pieces), t].reshape(pieces * cols, vt) for t in range(n_half)], axis=1)
                    rows = jnp.dot(value, hit_t[:, span(i * tok + off, n_step)], preferred_element_type=F32)
                    dst[pl.ds(0, pieces), :, span(off, n_step)] = rows.reshape(pieces, cols, n_step).astype(BF16)
                    return carry

                lax.fori_loop(0, tok // n_step, body, 0)
            x_swap(u).start()

    def x_swap(u):
        return place.send(("swap", u), xo.at[u % 2, pl.ds(0, PIECES[u])], xr.at[whole(u)], dc=1)

    def lanes_of(k):
        return span((x + k) % n * quarter, quarter, quarter)

    def side(u, i):
        return pl.ds(BASE[u] + i * len(UNITS[u]), len(UNITS[u]))

    def x_far(u, i):
        return place.send(("xf", u, i), xp.at[side(u, i), :, lanes_of(FAR)], xf.at[side(u, i)], dx=WAYS[i])

    def x_near(u, i):
        return place.send(("xn", u, i), xp.at[whole(u), :, lanes_of(WAYS[i])], xg.at[i, whole(u)], dx=WAYS[i])

    def x_goal(k, sel):
        return x0_out.at[(x + k) % n, sel]

    def x_put(u, i):
        return place.send(("xp", u, i), xq.at[whole(u)], x_goal(0, whole(u)), dx=WAYS[i])

    def x_keep(u):
        return place.local("x0", xq.at[whole(u)], x_goal(0, whole(u)), u, len(UNITS))

    def x_pass(u, i):
        ref = x_goal(FROM[i], side(u, i))
        return place.send(("xs", u, i), ref, ref, dx=WAYS[i])

    def x_first(u):
        with scope("f_x1"):
            x_swap(u).wait_recv()
            for p in range(BASE[u], BASE[u] + PIECES[u]):
                xp[p] = xp[p] + xr[p]
            start_all(x_far(u, i) for i in BOTH)

    def x_second(u):
        with scope("f_x2"):
            for i in BOTH:
                x_far(u, i).wait_recv()
                sel, lanes = side(u, i), lanes_of(WAYS[i])
                xp[sel, :, lanes] = xp[sel, :, lanes] + xf[sel]
                x_near(u, i).start()

    def x_third(u):
        with scope("f_x3"):
            for i in BOTH:
                x_near(u, i).wait_recv()
            sel = whole(u)
            xq[sel] = xp[sel, :, lanes_of(0)] + xg[0, sel] + xg[1, sel]
            start_all(x_put(u, i) for i in BOTH)
            x_keep(u).start()

    def x_fourth(u):
        with scope("f_x4"):
            for i in BOTH:
                x_put(u, i).wait_recv()
                x_pass(u, i).start()

    block = width // dims["n_block"]

    def transpose_block(j):
        return xn[:, pl.ds(j * block, block)].T

    n_block = dims["n_block"]
    early = n_block // 2

    def give_g(part):
        sel = pl.ds(part * early, early)
        return place.send(("g", part), gl.at[sel, 0], gl.at[sel, 1], dc=1)

    def put_xn(j):
        return place.local("xt", gl.at[j, 0], xnt_out.at[pl.ds(j * block, block)], j, dims["n_block"])

    def give_xn(part):
        sel = pl.ds(part * early * block, early * block)
        return place.send(("xt", part), xnt_out.at[sel], xpar_out.at[sel], dc=1)

    def put_lt(m):
        j, t = m // n_half, m % n_half
        return place.local("lt", lts.at[m % 2], lt_out.at[span(j * block, block, SUB), span(t * vt, vt)], m % 2)

    def lt_body(m, carry):
        j, t = m // n_half, m % n_half

        @pl.when(m > 1)
        def _():
            put_lt(m - 2).wait()

        value = jnp.concatenate([gl[j, i] for i in BOTH], axis=1)
        part = lax.dot_general(value, hit_t[span(t * vt, vt)], (((1,), (1,)), ((), ())), preferred_element_type=F32)
        lts[m % 2] = part * dims["scale"]
        put_lt(m).start()
        return carry

    def lt_run(lo, hi):
        with scope("f_lt"):
            lax.fori_loop(lo, hi, lt_body, 0)

    r_step = min(64, tok)

    def xn_body(j, carry):
        sel = span(j * r_step, r_step, r_step)
        h_wide = xn[sel].astype(F32)
        inv_rms = lax.rsqrt(jnp.sum(h_wide * h_wide, axis=1, keepdims=True) * (1.0 / width) + NORM_EPS)
        xn[sel] = (h_wide * inv_rms * gain_out[0:1]).astype(BF16)
        return carry

    def xt(part):
        with scope("f_xt"):
            give_g(part).wait_send()
            for j in range(part * early, (part + 1) * early):
                gl[j, 0] = transpose_block(j)
                put_xn(j).start()

    def lt(j):
        lt_run(j * n_half, (j + 1) * n_half)

    x_steps = (x_first, x_second, x_third, x_fourth)

    def x_run(work):
        for step, u in digits(work):
            x_steps[step](u)

    with scope("f_gt"):
        load_g.wait()
        for j in range(n_block):
            gl[j, 0] = transpose_block(j)
            if (j + 1) % early == 0:
                give_g(j // early).start()
    load_h = place.local("h", h_hbm, xn)
    load_h.start()
    with scope("f_keep"):
        for h in BOTH:
            keep(h).wait()
    pass_first()
    load_unit(0)
    with scope("f_gain1"):
        gain_sum.start("dy", gain_sum.finish("dc"))
    look(0)
    pass_second(0)
    with scope("f_gain2"):
        gain_sum.start("dz", gain_sum.finish("dy"))
    pass_first_far()
    load_unit(1)
    share_group(0)
    x_run("00")
    with scope("f_giveg"):
        for part in BOTH:
            give_g(part).wait_recv()
    lt(0)
    look(1)
    x_run("10 01")
    with scope("f_xn"):
        gain_out[...] = 1.0 + gain_sum.finish("dz")
        load_h.wait()
        lax.fori_loop(0, tok // r_step, xn_body, 0)
    x_run("20 11")
    if early > 1:
        lt(1)
    pass_second(PAIR)
    end_second(0)
    load_unit(FAR)
    x_run("30 21")
    look(FAR)
    x_run("31 02")
    pass_second(FAR)
    load_unit(3)
    share_group(PAIR)
    if early > 2:
        lt(2)
    x_run("12")
    look(3)
    x_run("22 03")
    end_second(PAIR)
    end_second(FAR)
    load_unit(4)
    share_group(FAR)
    xt(0)
    x_run("32 13")
    look(4)
    with scope("f_putx"):
        for j in range(early):
            put_xn(j).wait()
        give_xn(0).start()
    x_run("23 04")

    e_step = min(64, tok)

    def tile_of(j):
        return (c * n_half + j) % n_tile

    def load_tile(j):
        return place.local(("et", 0), et_out.at[tile_of(j)], etb.at[j % 2], j % 2)

    def save_u(i, odd):
        return place.local(("u", odd), (z_even, z_odd)[odd].at[i % 2], u_hbm.at[tile_of(2 * i + odd)], i % 2)

    def lane_blocks():
        return [(b, pl.ds(b, LANE)) for b in range(0, vt, LANE)]

    def post_tile(i, odd):
        base = tile_of(2 * i + odd) * vt
        buf, slot = (z_even, z_odd)[odd], i % 2
        for e in range(0, tok, e_step):
            sel = pl.ds(e, e_step)
            ids = lax.broadcasted_iota(I32, (e_step, LANE), 1) + base
            for b, lanes in lane_blocks():
                tanh_z = jnp.tanh(buf[slot, sel, lanes] * (1.0 / SOFT_CAP))
                buf[slot, sel, lanes] = tanh_z
                acc_e[sel] = acc_e[sel] + jnp.exp(SOFT_CAP * tanh_z - SOFT_CAP)
                acc_l[sel] = acc_l[sel] + jnp.where(ids + b == labc[sel], tanh_z, 0.0)

    def pair(i, carry):
        @pl.when(i > 1)
        def _():
            for odd in BOTH:
                save_u(i - 2, odd).wait()

        for odd in BOTH:
            load_tile(2 * i + odd).wait()
            (z_even, z_odd)[odd][i % 2] = jnp.dot(xn[...], etb[odd].reshape(width, vt), preferred_element_type=F32)
            if odd:
                post_tile(i, 0)

            @pl.when(i + 1 < n_tile // 2)
            def _():
                load_tile(2 * i + odd + 2).start()

        save_u(i, 0).start()
        post_tile(i, 1)
        save_u(i, 1).start()

        for k, work in enumerate(during):
            @pl.when(i == k)
            def _():
                x_run(work)
                if k == share_at:
                    wait_shares()
        return carry

    def wait_shares():
        with scope("f_share"):
            for h in BOTH:
                for k2 in (0, PAIR, FAR):
                    share(h, k2).wait_recv()

    share_at = n_half // 2 - 2
    during = ("14", "33", "24", "", "34")
    if share_at < 0:
        wait_shares()
        for work in during:
            x_run(work)
        during = ()

    acc_e[...] = jnp.zeros_like(acc_e)
    acc_l[...] = jnp.zeros_like(acc_l)
    start_all(load_tile(j) for j in BOTH)
    with scope("f_logits"):
        lax.fori_loop(0, n_tile // 2, pair, 0)

    with scope("f_stats"):
        row = lax.broadcasted_iota(I32, (SUB, tok), 0)
        sum_e = jnp.sum(acc_e[...].T, axis=0, keepdims=True)
        sum_l = SOFT_CAP * jnp.sum(acc_l[...].T, axis=0, keepdims=True)
        stats = SmallSum(place, ("dx",), s_slots)
        stats.start("dx", jnp.where(row == 0, sum_e, sum_l))
    for j in range(early, n_block):
        lt(j)
    xt(1)
    with scope("f_lt_end"):
        for m in range(n_block * n_half - 2, n_block * n_half):
            put_lt(m).wait()
    with scope("f_stats2"):
        stat = stats.finish("dx")
        all_e, all_l = stat[0:1], stat[1:2]
        inv_s[...] = jnp.broadcast_to((1.0 / dims["total"]) / all_e, (LANE, tok)).T
        s_slots[0, 0:1, :] = jnp.log(all_e) + SOFT_CAP - all_l
        own = s_slots[0, 0:1, lanes_of(0)]
        part_w = min(LANE, quarter)
        folded = own[:, 0:part_w]
        for j in range(part_w, quarter, part_w):
            folded = folded + own[:, j:j + part_w]
        loss_out[...] = jnp.where(lax.broadcasted_iota(I32, (SUB, part_w), 0) == 0, folded, 0.0)

    def dz_tile(j):
        return ((1 - c) * n_half + j) % n_tile

    def load_u(i, odd):
        return place.local(("u", odd), u_hbm.at[dz_tile(2 * i + odd)], (z_even, z_odd)[odd].at[i % 2], i % 2)

    def put_dz(i, odd):
        return place.local(("dz", odd), dzb.at[odd, i % 2], dz_out.at[dz_tile(2 * i + odd)], i % 2)

    def give_dz():
        return place.send("dz", dz_out.at[pl.ds((1 - c) * n_half, n_half)], dzpar_out, dc=1)

    d_step = min(LANE, tok)

    def dz_rows(i, odd):
        base = dz_tile(2 * i + odd) * vt
        buf, slot = (z_even, z_odd)[odd], i % 2

        def body(e, carry):
            sel = span(e * d_step, d_step, d_step)
            ids = lax.broadcasted_iota(I32, (d_step, LANE), 1) + base
            for b, lanes in lane_blocks():
                tanh_z = buf[slot, sel, lanes]
                prob = jnp.exp(SOFT_CAP * tanh_z - SOFT_CAP) * inv_s[sel]
                prob = jnp.where(ids + b == labc[sel], prob - 1.0 / dims["total"], prob)
                dzb[odd, slot, sel, lanes] = (prob * (1.0 - tanh_z * tanh_z)).astype(BF16)
            return carry

        lax.fori_loop(0, tok // d_step, body, 0)

    def dz_pair(i, carry):
        for odd in BOTH:
            load_u(i, odd).wait()

            @pl.when(i % (n_half // 2) > 1)
            def _():
                put_dz(i - 2, odd).wait()

            dz_rows(i, odd)
            put_dz(i, odd).start()

            @pl.when(i + 2 < n_tile // 2)
            def _():
                load_u(i + 2, odd).start()

        return carry

    with scope("f_dz"):
        for i in range(n_tile // 2 - 2, n_tile // 2):
            for odd in BOTH:
                save_u(i, odd).wait()
        for i in BOTH:
            start_all(load_u(i, odd) for odd in BOTH)
        lax.fori_loop(0, n_half // 2, dz_pair, 0)
        for i in range(n_half // 2 - 2, n_half // 2):
            for odd in BOTH:
                put_dz(i, odd).wait()
        give_dz().start()
        for j in range(early, n_block):
            put_xn(j).wait()
        give_xn(1).start()
        lax.fori_loop(n_half // 2, n_tile // 2, dz_pair, 0)

    with scope("f_end"):
        give_dz().wait()
        for i in range(n_tile // 2 - 2, n_tile // 2):
            for odd in BOTH:
                put_dz(i, odd).wait()
        give_tok.wait_send()
        give_chunk.wait_send()
        for h in BOTH:
            for i in BOTH:
                p1_send(h, i).wait_send()
                p1_fwd(h, i).wait_send()
                for k in (0, PAIR, FAR):
                    p2_send(h, k, i).wait_send()
                    p2_fwd(h, k, i).wait_send()
            for k in (0, PAIR, FAR):
                share(h, k).wait_send()
        for part in BOTH:
            give_xn(part).wait()
        for u in range(len(UNITS)):
            if u > len(UNITS) - 3:
                x_swap(u).wait_send()
            x_keep(u).wait()
            for i in BOTH:
                x_far(u, i).wait_send()
                x_near(u, i).wait_send()
                x_put(u, i).wait_send()
                x_pass(u, i).wait()
    assert (place.n_link, place.n_local) <= dims["front_sems"], (place.n_link, place.n_local)


def specs(n_vmem, n_any):
    return [pl.BlockSpec(memory_space=pltpu.VMEM)] * n_vmem + [pl.BlockSpec(memory_space=pl.ANY)] * n_any


def shapes(items):
    return tuple(jax.ShapeDtypeStruct(*item) for item in items)


def scratch(items, n_link, n_local):
    dma = pltpu.SemaphoreType.DMA
    return [pltpu.VMEM(*item) for item in items] + [dma((n_link,)), dma((n_link,)), dma((n_local,))]


def params(collective_id, limit):
    return pltpu.CompilerParams(collective_id=collective_id, has_side_effects=True, vmem_limit_bytes=limit)


def front(dims, limit, shard, tok_row, lab_row, w, h, g):
    n, tok, vocab, width, vt = dims["n"], dims["tok"], dims["vocab"], dims["width"], dims["vt"]
    cols = shard.shape[0]
    half_v = vocab // CORES
    quarter = tok // n
    n_tile, n_half, n_block, most = vocab // vt, half_v // vt, dims["n_block"], max(PIECES)
    block = width // n_block
    pieces = n * n * CORES
    grid = (n // 2, 2, n // 2, 2)
    return pl.pallas_call(
        functools.partial(front_kernel, dims),
        name="front",
        out_shape=shapes([
            ((n_tile, *grid, CORES, cols, vt), BF16), ((width, tok), BF16), ((width, tok), BF16), ((n_tile, tok, vt), BF16),
            ((n_half, tok, vt), BF16), ((width, half_v), F32), ((n, pieces, cols, quarter), BF16), ((n_tile, tok, vt), F32),
            ((SUB, width), F32), ((SUB, min(LANE, quarter)), F32),
        ]),
        in_specs=specs(4, 2),
        out_specs=tuple(specs(0, 8) + specs(2, 0)),
        scratch_shapes=scratch([
            ((n_tile, cols, vt), BF16), ((CORES, n_half, cols, vt), BF16), ((CORES, SUB, tok), I32), ((half_v, CORES * tok), BF16),
            ((2, most, n_half, cols, vt), BF16), ((pieces, cols, tok), BF16), ((2, most, cols, tok), BF16), ((pieces, cols, tok), BF16),
            ((pieces, cols, quarter), BF16), ((2, pieces, cols, quarter), BF16), ((pieces, cols, quarter), BF16),
            ((2, *grid, CORES, cols, vt), BF16), ((tok, width), BF16), ((n_block, CORES, block, tok), BF16), ((2, block, vt), F32),
            ((2, tok, vt), F32), ((2, tok, vt), F32), ((2, 2, tok, vt), BF16), ((tok, LANE), F32), ((tok, LANE), F32), ((tok, LANE), F32),
            ((2 * n + CORES, SUB, width), F32), ((n, SUB, tok), F32),
        ], dims["front_sems"][0], dims["front_sems"][1]),
        compiler_params=params(0, limit),
    )(shard, tok_row, lab_row, w, h, g)


def back_kernel(
    dims,
    gain_ref, loss_ref, dz_hbm, dzp_hbm, et_hbm, xnt_hbm, xpar_hbm, look_hbm, h_hbm,
    tail_out, dh_out, de_out, ra_hbm, rx_hbm,
    dz_own, dz_par, et_buf, part, fx, acc, fa, f2, r2, xb, h_buf, dh_buf, dg_acc, slots,
    sends, recvs, local_sems,
):
    n, tok, vocab, width, tile, per_chunk, vt = (dims[k] for k in ("n", "tok", "vocab", "width", "tile", "per_chunk", "vt"))
    place = Place(n, sends, recvs, local_sems)
    x, z, y, c = place.x, place.z, place.y, place.c
    half_v = vocab // CORES
    n_tile, n_half = vocab // vt, half_v // vt
    lanes = half_v // 2
    rows = width // (n * n)
    half_rows = rows // 2
    quarter = tok // n
    hq = quarter // 2
    chunks = width // (tile * per_chunk)
    per_half = n_half // 2

    with scope("b_enter"):
        place.enter()

    loads = [place.local("dz", dz_hbm, dz_own), place.local("dzp", dzp_hbm, dz_par)]
    start_all(loads)
    load_h = place.local("h", h_hbm.at[span(x * quarter, quarter, quarter)], h_buf)

    def load_et(t, slot):
        return place.local("et", et_hbm.at[:, span(t * tile, tile, tile)], et_buf.at[slot], slot)

    load_et(0, 0).start()
    load_h.start()

    slot_of = {FAR: 0, 1: 1, 3: 2, 0: 0}
    units = dims["units"]

    def load_xn(m, i):
        half, k = units[m]
        src = (xnt_hbm, xpar_hbm)[i]
        src = src.at[(z + k) % n] if half == 0 else src.at[:, (y + k) % n]
        return place.local(("xb", i), src, xb.at[m % 2, i], m % 2)

    def load_look(m):
        half, k = units[m]
        sel = pl.ds(half * lanes, lanes)
        src = look_hbm.at[(z + k) % n, :, :, sel] if half == 0 else look_hbm.at[:, (y + k) % n, :, sel]
        return place.local(("look", half), src, acc.at[half, slot_of[k]], slot_of[k], 3)

    def start_unit(m):
        if m < len(units):
            start_all(load_xn(m, i) for i in BOTH)

    for m, (half, k) in enumerate(units):
        if k:
            load_look(m).start()
    for m in BOTH:
        start_unit(m)

    def dxn_chunk(d):
        def body(i, carry):
            t = d * per_chunk + i
            slot = t % 2

            @pl.when(t + 1 < chunks * per_chunk)
            def _():
                load_et(t + 1, 1 - slot).start()

            load_et(t, slot).wait()
            left = jnp.concatenate([dz_own[j] for j in range(n_tile)], axis=1)
            right = jnp.concatenate([et_buf[slot, j] for j in range(n_tile)], axis=1)
            part[d, :, span(i * tile, tile, tile)] = lax.dot_general(
                left, right, (((1,), (1,)), ((), ())), preferred_element_type=F32)
            return carry

        with scope("b_dxn"):
            lax.fori_loop(0, per_chunk, body, 0)

    def qrow(k, lo=0, size=hq):
        return span((x + k) % n * quarter + lo, size, SUB)

    def x_far(d, i):
        return place.send(("xf", d, i), part.at[d, qrow(FAR, i * hq)], fx.at[d, i], dx=WAYS[i])

    def x_near(d, i):
        return place.send(("xn", d, i), part.at[d, qrow(WAYS[i], 0, quarter)], rx_hbm.at[d, i], dx=WAYS[i])

    def x_first(d):
        start_all(x_far(d, i) for i in BOTH)

    def x_second(d):
        with scope("b_x2"):
            for i in BOTH:
                x_far(d, i).wait_recv()
                sel = qrow(WAYS[i], i * hq)
                part[d, sel] = part[d, sel] + fx[d, i]
                x_near(d, i).start()

    def stage_x(d, j, i):
        return place.local("sx", rx_hbm.at[d, i, pl.ds(j * hq, hq)], fx.at[d, i], i)

    def x_third(d):
        with scope("b_x3"):
            for i in BOTH:
                x_near(d, i).wait_recv()
            for j in BOTH:
                start_all(stage_x(d, j, i) for i in BOTH)
                for i in BOTH:
                    stage_x(d, j, i).wait()
                sel = qrow(0, j * hq)
                part[d, sel] = part[d, sel] + fx[d, 0] + fx[d, 1]

    def de_unit(half, k):
        m = units.index((half, k))
        slot = slot_of[k]

        def body(j, carry):
            t = half * per_half + j
            sel = span(j * vt, vt)
            total = jnp.dot(xb[m % 2, 0].reshape(n * rows, tok), dz_own[c * n_half + t], preferred_element_type=F32)
            total = total + jnp.dot(xb[m % 2, 1].reshape(n * rows, tok), dz_par[t], preferred_element_type=F32)
            acc[half, slot, :, :, sel] = acc[half, slot, :, :, sel] + total.reshape(n, rows, vt)
            return carry

        with scope("b_de"):
            load_look(m).wait()
            for i in BOTH:
                load_xn(m, i).wait()
            lax.fori_loop(0, per_half, body, 0)
            start_unit(m + 2)

    def ring(half, k):
        return {"dz": k} if half == 0 else {"dy": k}

    def cross(half, k):
        return {"dy": k} if half == 0 else {"dz": k}

    def a_far(half, i):
        return place.send(("af", half, i), acc.at[half, 0, pl.ds(2 * i, 2)], fa.at[half, i], **ring(half, WAYS[i]))

    def a_near(half, i):
        return place.send(("an", half, i), acc.at[half, 1 + i], ra_hbm.at[half, i], **ring(half, WAYS[i]))

    def a_first(half):
        start_all(a_far(half, i) for i in BOTH)

    def a_second(half, i):
        with scope("b_a2"):
            a_far(half, i).wait_recv()
            sel = pl.ds(2 * i, 2)
            acc[half, 1 + i, sel] = acc[half, 1 + i, sel] + fa[half, i]
            a_near(half, i).start()

    def stage_a(half, j, i):
        return place.local(("sa", half), ra_hbm.at[half, i, pl.ds(2 * j, 2)], fa.at[half, i], i)

    def piece(half, k):
        return ((y if half == 0 else z) + k) % n

    def c_far(half, i):
        src = acc.at[half, 0, piece(half, FAR), pl.ds(i * half_rows, half_rows)]
        return place.send(("cf", half, i), src, f2.at[half, i], **cross(half, WAYS[i]))

    def c_near(half, i):
        return place.send(("cn", half, i), acc.at[half, 0, piece(half, WAYS[i])], r2.at[half, i], **cross(half, WAYS[i]))

    def a_third(half):
        with scope("b_a3"):
            for i in BOTH:
                a_near(half, i).wait_recv()
            for j in BOTH:
                start_all(stage_a(half, j, i) for i in BOTH)
                for i in BOTH:
                    stage_a(half, j, i).wait()
                sel = pl.ds(2 * j, 2)
                acc[half, 0, sel] = acc[half, 0, sel] + fa[half, 0] + fa[half, 1]
            start_all(c_far(half, i) for i in BOTH)

    def c_second(half):
        with scope("b_c2"):
            for i in BOTH:
                c_far(half, i).wait_recv()
                at = piece(half, WAYS[i])
                sel = pl.ds(i * half_rows, half_rows)
                acc[half, 0, at, sel] = acc[half, 0, at, sel] + f2[half, i]
                c_near(half, i).start()

    def out_copies(half):
        sel = span(c * half_v + half * lanes, lanes)
        mine = acc.at[half, 0, piece(half, 0)]
        yield place.local("de", mine.at[span(c * half_rows, half_rows, SUB)], de_out.at[:, sel], half)
        yield place.send(("de", half), mine.at[span((1 - c) * half_rows, half_rows, SUB)], de_out.at[:, sel], dc=1)

    def c_third(half):
        with scope("b_c3"):
            for i in BOTH:
                c_near(half, i).wait_recv()
            at = piece(half, 0)
            acc[half, 0, at] = acc[half, 0, at] + r2[half, 0] + r2[half, 1]
            start_all(out_copies(half))

    with scope("b_load"):
        for copy in loads:
            copy.wait()
    dxn_chunk(0)
    x_first(0)
    de_unit(0, FAR)
    a_first(0)
    if chunks > 1:
        dxn_chunk(1)
        x_first(1)
    de_unit(1, FAR)
    a_first(1)
    x_second(0)
    for d in range(2, chunks):
        dxn_chunk(d)
        x_first(d)
    if chunks > 1:
        x_second(1)
    for half in BOTH:
        for k in WAYS:
            de_unit(half, k)
    for i in BOTH:
        a_second(0, i)
    for d in range(2, chunks):
        x_second(d)
    with scope("b_wait_far"):
        for half in BOTH:
            for i in BOTH:
                a_far(half, i).wait_send()
            load_look(units.index((half, 0))).start()
    de_unit(0, 0)
    for i in BOTH:
        a_second(1, i)
    de_unit(1, 0)
    for d in range(chunks):
        x_third(d)

    step = min(32, quarter)

    def dh_body(i, carry):
        sel = span(i * step, step, step)
        row = span(x * quarter + i * step, step, step)
        d_x = jnp.concatenate([part[d, row] for d in range(chunks)], axis=1)
        h_wide = h_buf[sel].astype(F32)
        inv_rms = lax.rsqrt(jnp.sum(h_wide * h_wide, axis=1, keepdims=True) * (1.0 / width) + NORM_EPS)
        h_norm = h_wide * inv_rms
        g_dir = d_x * gain_ref[0:1]
        mean = jnp.sum(g_dir * h_norm, axis=1, keepdims=True) * (1.0 / width)
        dh_buf[sel] = (inv_rms * (g_dir - h_norm * mean)).astype(BF16)
        prod = d_x * h_norm
        total = prod[0:SUB]
        for j in range(SUB, step, SUB):
            total = total + prod[j:j + SUB]
        dg_acc[...] = dg_acc[...] + total
        return carry

    with scope("b_dh"):
        load_h.wait()
        dg_acc[...] = jnp.zeros_like(dg_acc)
        lax.fori_loop(0, quarter // step, dh_body, 0)

    def h_first(i, part_of):
        lo = ((i + part_of) % 2) * hq
        return place.send(("hf", i, part_of), dh_buf.at[pl.ds(lo, hq)], dh_out.at[qrow(0, lo)], dx=WAYS[i])

    def h_second(i):
        ref = dh_out.at[qrow(FROM[i], i * hq)]
        return place.send(("hs", i), ref, ref, dx=WAYS[i])

    keep_dh = place.local("dh", dh_buf, dh_out.at[qrow(0, 0, quarter)])
    small = SmallSum(place, ("dc", "dx", "dy", "dz"), slots)
    small.start("dc", jnp.concatenate([dg_acc[...], loss_ref[...]], axis=1))
    start_all(h_first(i, 0) for i in BOTH)
    keep_dh.start()
    with scope("b_s1"):
        small.start("dx", small.finish("dc"))
    start_all(h_first(i, 1) for i in BOTH)
    for half in BOTH:
        a_third(half)
    with scope("b_h2"):
        for i in BOTH:
            h_first(i, 0).wait_recv()
            h_second(i).start()
    with scope("b_s2"):
        small.start("dy", small.finish("dx"))
    for half in BOTH:
        c_second(half)
    with scope("b_s3"):
        small.start("dz", small.finish("dy"))
    for half in BOTH:
        c_third(half)
    with scope("b_s4"):
        total = jnp.sum(small.finish("dz"), axis=0, keepdims=True)
        loss = jnp.sum(total[:, width:], axis=1, keepdims=True) * (1.0 / dims["total"])
        tail_out[...] = jnp.concatenate([total[:, 0:width], jnp.broadcast_to(loss, (1, LANE))], axis=1)

    with scope("b_end_x"):
        keep_dh.wait()
        for i in BOTH:
            for d in range(chunks):
                x_far(d, i).wait_send()
                x_near(d, i).wait_send()
            h_first(i, 0).wait_send()
            h_first(i, 1).wait()
            h_second(i).wait()
    with scope("b_end_a"):
        for half in BOTH:
            for i in BOTH:
                a_near(half, i).wait_send()
                c_far(half, i).wait_send()
                c_near(half, i).wait_send()
            for copy in out_copies(half):
                copy.wait()
    assert (place.n_link, place.n_local) <= dims["back_sems"], (place.n_link, place.n_local)


def back(dims, limit, gain, loss, dz, dzp, et, xnt, xpar, look, h):
    n, tok, vocab, width, tile, per_chunk = (dims[k] for k in ("n", "tok", "vocab", "width", "tile", "per_chunk"))
    rows = width // (n * n)
    half_v = vocab // CORES
    lanes = half_v // 2
    quarter = tok // n
    hq = quarter // 2
    chunk_w = tile * per_chunk
    chunks = width // chunk_w
    tail_w = width + loss.shape[1]
    n_tile, n_half, vt = dz.shape[0], dzp.shape[0], dims["vt"]
    xnt, xpar = (a.reshape(n, n, rows, tok) for a in (xnt, xpar))
    return pl.pallas_call(
        functools.partial(back_kernel, dims),
        name="back",
        out_shape=shapes([
            ((1, width + LANE), F32), ((tok, width), BF16), ((rows // CORES, vocab), F32), ((2, 2, n, rows, lanes), F32),
            ((chunks, 2, quarter, chunk_w), F32),
        ]),
        in_specs=specs(2, 7),
        out_specs=tuple(specs(1, 4)),
        scratch_shapes=scratch([
            ((n_tile, tok, vt), BF16), ((n_half, tok, vt), BF16), ((2, n_tile, tile, vt), BF16), ((chunks, tok, chunk_w), F32),
            ((chunks, 2, hq, chunk_w), F32), ((2, 3, n, rows, lanes), F32), ((2, 2, 2, rows, lanes), F32),
            ((2, 2, rows // 2, lanes), F32), ((2, 2, rows, lanes), F32), ((2, CORES, n, rows, tok), BF16), ((quarter, width), BF16),
            ((quarter, width), BF16), ((SUB, width), F32), ((3 * n + CORES, SUB, tail_w), F32),
        ], dims["back_sems"][0], dims["back_sems"][1]),
        compiler_params=params(1, limit),
    )(gain, loss, dz, dzp, et.reshape(n_tile, width, vt), xnt, xpar, look.reshape(n, n, rows, half_v), h)[:3]


def finish_kernel(n, scale, table_ref, x0_ref, dh_ref, x0_out, dh_out, rows_ref):
    place = Place(n, None, None, None)
    cols = x0_ref.shape[2]
    for zi in range(n):
        for yi in range(n):
            for h in BOTH:
                dz, dy = (zi - place.z) % n, (yi - place.y) % n
                k1, k2 = (dy, dz) if h == 0 else (dz, dy)
                piece = table_ref[(h * n + k1) * n + k2]
                rows_ref[pl.ds(((zi * n + yi) * CORES + h) * cols, cols)] = x0_ref[0, piece]
    x0_out[...] = (rows_ref[...].T.astype(F32) * scale).astype(BF16)
    dh_out[...] = dh_ref[...]


def finish(n, scale, x0, dh):
    _, pieces, cols, quarter = x0.shape
    width = pieces * cols
    table = np.zeros((CORES, n, n), np.int32)
    for u, unit in enumerate(UNITS):
        for h in BOTH:
            for i, (k1, k2) in enumerate(unit):
                table[h, k1, k2] = BASE[u] + h * len(unit) + i
    row = pl.BlockSpec((quarter, width), lambda q, t: (q, 0))
    return pl.pallas_call(
        functools.partial(finish_kernel, n, scale),
        name="finish",
        grid_spec=pltpu.PrefetchScalarGridSpec(
            num_scalar_prefetch=1,
            grid=(n,),
            in_specs=[pl.BlockSpec((1, pieces, cols, quarter), lambda q, t: (q, 0, 0, 0)), row],
            out_specs=(row, row),
            scratch_shapes=[pltpu.VMEM((width, quarter), BF16)],
        ),
        out_shape=shapes([(dh.shape, BF16)] * 2),
        compiler_params=pltpu.CompilerParams(vmem_limit_bytes=40_000_000),
    )(jnp.asarray(table.reshape(-1)), x0, dh)


def solution(mesh):
    return build(mesh, mesh.shape["tp"], 256, 3, 256, 6, 67_000_000)


def build(mesh, n, tile, per_chunk, vt, n_block, limit):
    fsdp_size = mesh.shape["fsdp"]

    def device_step(emb_shard, tok_ids, lab_ids, h_last, g_embed, norm_w):
        vocab_rows, cols = emb_shard.shape
        batch_loc, seq_len, width = h_last.shape
        tok_count = batch_loc * seq_len
        fsdp_id = lax.axis_index("fsdp")
        scale = float(np.asarray(math.sqrt(width)).astype(jnp.bfloat16))
        dims = {
            "n": n, "tok": tok_count, "vocab": vocab_rows, "width": width, "total": tok_count * fsdp_size, "vt": vt,
            "tile": tile, "per_chunk": per_chunk, "scale": scale, "n_block": n_block,
            "units": digits("02 12 01 03") + digits("11 13 00 10"),
            "front_sems": (100, 45), "back_sems": (46, 28),
        }
        h_flat = h_last.reshape(tok_count, width)
        placed = lax.dynamic_update_slice(jnp.zeros((SUB, width), F32), jnp.broadcast_to(norm_w, (SUB, cols)), (0, fsdp_id * cols))
        row_start = lax.axis_index("tp") * vocab_rows
        lab_cols = jnp.broadcast_to(lab_ids.reshape(tok_count)[:, None] - row_start, (tok_count, LANE))
        table, xn_t, xpar_t, dz, dzp, look, x0, _, gain, loss_part = front(
            dims, limit, emb_shard.T, tok_ids.reshape(1, tok_count), lab_cols, placed, h_flat, g_embed.reshape(tok_count, width))
        tail, d_hidden, d_cols = back(dims, limit, gain, loss_part, dz, dzp, table, xn_t, xpar_t, look, h_flat)
        x_emb, d_hidden = finish(n, scale, x0, d_hidden)
        d_norm_w = lax.dynamic_slice(tail[0], (fsdp_id * cols,), (cols,))
        return (x_emb.reshape(h_last.shape), tail[0, width], d_hidden.reshape(h_last.shape), d_norm_w, d_cols.T)

    spec_tok = P("fsdp", None)
    spec_act = P("fsdp", None, None)
    return jax.shard_map(device_step, mesh=mesh, in_specs=(P("tp", "fsdp"), spec_tok, spec_tok, spec_act, spec_act, P("fsdp")), out_specs=(spec_act, P(), spec_act, P("fsdp"), P("tp", "fsdp")), check_vma=False)
```

```python
import functools
import math
import jax
import numpy as np
import jax.numpy as jnp
from jax import lax
from jax.experimental import pallas as pl
from jax.experimental.pallas import tpu as pltpu
from jax.sharding import PartitionSpec as P

SOFT_CAP = 30.0
NORM_EPS = 1e-6
F32, BF16, I32 = jnp.float32, jnp.bfloat16, jnp.int32
LANE, SUB = 128, 8
BOTH = (0, 1)
FOUR = range(4)
WAYS = (1, 3)
FROM = (3, 1)
FAR = 2
CORES = 2


def span(start, size, unit=LANE):
    return pl.ds(pl.multiple_of(start, unit), size)


class Place:
    def __init__(self, n, sends, recvs, local_sems):
        self.n, self.sends, self.recvs, self.local_sems = n, sends, recvs, local_sems
        self.x = lax.axis_index("tp")
        f = lax.axis_index("fsdp")
        self.f = f
        self.c = f % CORES
        self.y = f // CORES % n
        self.z = f // CORES // n
        self.link_of, self.local_of, self.n_link, self.n_local = {}, {}, 0, 0
        self.size = {"dx": n, "dz": n, "dy": n, "dc": CORES}
        self.me = {"dx": self.x, "dz": self.z, "dy": self.y, "dc": self.c}

    def at(self, dx=0, dz=0, dy=0, dc=0):
        n = self.n
        z, y, c = (self.z + dz) % n, (self.y + dy) % n, (self.c + dc) % CORES
        return ((self.x + dx) % n, (z * n + y) * CORES + c)

    def enter(self):
        barrier = pltpu.get_barrier_semaphore()
        peers = [self.at(**{d: k}) for d in self.size for k in range(1, self.size[d])]
        for peer in peers:
            pl.semaphore_signal(barrier, inc=1, device_id=peer, device_id_type=pl.DeviceIdType.MESH)
        pl.semaphore_wait(barrier, len(peers))

    def link(self, key, count=1):
        if key not in self.link_of:
            self.link_of[key] = self.n_link
            self.n_link += count
        return self.link_of[key]

    def send(self, key, src, dst, **step):
        i = self.link(key)
        return pltpu.make_async_remote_copy(
            src, dst, self.sends.at[i], self.recvs.at[i], device_id=self.at(**step), device_id_type=pl.DeviceIdType.MESH)

    def local(self, key, src, dst, slot=0, count=2):
        if key not in self.local_of:
            self.local_of[key] = self.n_local
            self.n_local += count
        return pltpu.make_async_copy(src, dst, self.local_sems.at[self.local_of[key] + slot])


class SmallSum:
    def __init__(self, place, dims, slots):
        self.place, self.slots, self.dims, self.base = place, slots, dims, {}
        count = 0
        for d in dims:
            self.base[d] = count
            count += place.size[d]

    def copies(self, d):
        slot = self.slots.at[self.base[d] + self.place.me[d]]
        for k in range(1, self.place.size[d]):
            yield self.place.send((self.dims, d, k), slot, slot, **{d: k})

    def start(self, d, value):
        self.slots[self.base[d] + self.place.me[d]] = value
        for copy in self.copies(d):
            copy.start()

    def finish(self, d):
        for copy in self.copies(d):
            copy.wait()
        total = self.slots[self.base[d]]
        for k in range(1, self.place.size[d]):
            total = total + self.slots[self.base[d] + k]
        return total


def scope(name):
    return jax.named_scope(name)


def start_all(copies):
    for copy in copies:
        copy.start()


def digits(text):
    return tuple(tuple(int(d) for d in word) for word in text.split())


UNITS = [digits(u) for u in ("00 10 30", "01 03 20", "02 11 31", "13 33 21 23", "12 32 22")]
PAIR, ALL = 1, "all"
PIECES = [2 * len(u) for u in UNITS]
BASE = [sum(PIECES[:i]) for i in range(len(UNITS))]


def front_kernel(
    dims,
    shard_ref, tok_ref, lab_ref, w_ref, h_hbm, g_hbm,
    et_out, xnt_out, xpar_out, gt_out, gpar_out, dz_out, dzpar_out, x0_out, u_hbm, gain_out, loss_out, tokc_out,
    shard_t, chunk, tokr, hit_t, lhs, xp, xo, xr, xf, xg, xq, etb, xn, gl, z_even, z_odd, dzb,
    acc_e, acc_l, inv_s, labc, w_slots, s_slots, sends, recvs, local_sems,
):
    n, tok, vocab, width, vt = dims["n"], dims["tok"], dims["vocab"], dims["width"], dims["vt"]
    place = Place(n, sends, recvs, local_sems)
    x, z, y, c = place.x, place.z, place.y, place.c
    half_v = vocab // CORES
    n_tile = vocab // vt
    n_half = n_tile // CORES
    hh = n_half // 2
    cols = width // (n * n * CORES)
    quarter = tok // n
    row_start = x * vocab

    def ring1(h, k):
        return {"dy": k} if h == 0 else {"dz": k}

    def ring2(h, k):
        return {"dz": k} if h == 0 else {"dy": k}

    def coord(base, k, paired):
        every = slice(None)
        if k == ALL:
            return every, every
        return every if paired else (base + k) % n // 2, (base + k) % 2

    def loc(h, k1, k2, lo=0, size=n_half, pair1=False, pair2=False):
        first, second = coord((y, z)[h], k1, pair1), coord((z, y)[h], k2, pair2)
        return et_out.at[(pl.ds(c * n_half + lo, size), *((second, first)[h]), *((first, second)[h]), h)]

    with scope("f_enter"):
        place.enter()

    load_g = place.local("g", g_hbm, xn)
    load_g.start()
    with scope("f_cast"):
        for t in range(n_tile):
            shard_t[t] = shard_ref[:, pl.ds(t * vt, vt)].astype(BF16)
        tokr[c] = jnp.broadcast_to(tok_ref[...], (SUB, tok))
        give_tok = place.send("tok", tokr.at[c], tokr.at[c], dc=1)
        give_chunk = place.send("chunk", shard_t.at[pl.ds((1 - c) * n_half, n_half)], chunk.at[c], dc=1)
        give_chunk.start()
        give_tok.start()
        chunk[c] = shard_t[pl.ds(c * n_half, n_half)]
        gain_sum = SmallSum(place, ("dc", "dy", "dz"), w_slots)
        gain_sum.start("dc", w_ref[...])

    def p1_send(h, i):
        return place.send(("p1", h, i), chunk.at[h], loc(h, 0, 0), **ring1(h, WAYS[i]))

    def p1_fwd(h, i):
        ref = loc(h, FROM[i], 0, i * hh, hh)
        return place.send(("p1f", h, i), ref, ref, **ring1(h, WAYS[i]))

    def p2_send(h, k1, i):
        ref = loc(h, k1, 0, pair1=k1 == PAIR)
        return place.send(("p2", h, k1, i), chunk.at[h] if k1 == 0 else ref, ref, **ring2(h, WAYS[i]))

    def p2_fwd(h, k1, i):
        ref = loc(h, k1, FROM[i], i * hh, hh, pair1=k1 == PAIR)
        return place.send(("p2f", h, k1, i), ref, ref, **ring2(h, WAYS[i]))

    def keep(h):
        return place.local("keep", chunk.at[h], loc(h, 0, 0), h)

    def share(h, k2):
        ref = loc(h, ALL, k2, pair2=k2 == PAIR)
        return place.send(("share", h, k2), ref, ref, dc=1)

    def pass_first():
        with scope("f_p1"):
            for h in BOTH:
                for i in BOTH:
                    p1_send(h, i).wait_recv()
                    p1_fwd(h, i).start()
                start_all(p2_send(h, PAIR, i) for i in BOTH)

    def pass_first_far():
        with scope("f_p1f"):
            for h in BOTH:
                for i in BOTH:
                    p1_fwd(h, i).wait_recv()
                start_all(p2_send(h, FAR, j) for j in BOTH)

    def pass_second(k1):
        with scope("f_p2"):
            for h in BOTH:
                for i in BOTH:
                    p2_send(h, k1, i).wait_recv()
                    p2_fwd(h, k1, i).start()

    def end_second(k1):
        with scope("f_p2f"):
            for h in BOTH:
                for i in BOTH:
                    p2_fwd(h, k1, i).wait_recv()

    def share_group(k2):
        start_all(share(h, k2) for h in BOTH)

    with scope("f_chunk"):
        give_chunk.wait_recv()
        for h in BOTH:
            start_all(p1_send(h, i) for i in BOTH)
        for h in BOTH:
            start_all(p2_send(h, 0, i) for i in BOTH)
            keep(h).start()

    v_step = min(LANE, half_v)

    def hit_body(j, carry):
        off = j * v_step
        ids = lax.broadcasted_iota(I32, (v_step, tok), 0) + (row_start + c * half_v + off)
        for i, core in enumerate((c, 1 - c)):
            hit_t[span(off, v_step, v_step), pl.ds(i * tok, tok)] = jnp.where(ids == tokr[core, 0:1, :], 1.0, 0.0).astype(BF16)
        return carry

    with scope("f_hit"):
        give_tok.wait_recv()
        lax.fori_loop(0, half_v // v_step, hit_body, 0)

    n_step = min(256, tok)
    most = max(PIECES)

    def whole(u):
        return pl.ds(BASE[u], PIECES[u])

    def unit_copies(u):
        slot = u % 2
        for p, (h, (k1, k2)) in enumerate((h, k) for h in BOTH for k in UNITS[u]):
            yield place.local("lhs", loc(h, k1, k2), lhs.at[slot, p], slot * most + p, 2 * most)

    def load_unit(u):
        start_all(unit_copies(u))

    def look(u):
        pieces = PIECES[u]
        with scope("f_look"):
            if u > 1:
                x_swap(u - 2).wait_send()
            left = lhs.at[u % 2]
            for copy in unit_copies(u):
                copy.wait()
            for i, dst in enumerate((xp.at[whole(u)], xo.at[u % 2])):
                def body(j, carry):
                    off = j * n_step
                    value = jnp.concatenate([left[pl.ds(0, pieces), t].reshape(pieces * cols, vt) for t in range(n_half)], axis=1)
                    rows = jnp.dot(value, hit_t[:, span(i * tok + off, n_step)], preferred_element_type=F32)
                    dst[pl.ds(0, pieces), :, span(off, n_step)] = rows.reshape(pieces, cols, n_step).astype(BF16)
                    return carry

                lax.fori_loop(0, tok // n_step, body, 0)
            x_swap(u).start()

    def x_swap(u):
        return place.send(("swap", u), xo.at[u % 2, pl.ds(0, PIECES[u])], xr.at[whole(u)], dc=1)

    def lanes_of(k):
        return span((x + k) % n * quarter, quarter, quarter)

    def side(u, i):
        return pl.ds(BASE[u] + i * len(UNITS[u]), len(UNITS[u]))

    def x_far(u, i):
        return place.send(("xf", u, i), xp.at[side(u, i), :, lanes_of(FAR)], xf.at[side(u, i)], dx=WAYS[i])

    def x_near(u, i):
        return place.send(("xn", u, i), xp.at[whole(u), :, lanes_of(WAYS[i])], xg.at[i, whole(u)], dx=WAYS[i])

    def x_goal(k, sel):
        return x0_out.at[(x + k) % n, sel]

    def x_put(u, i):
        return place.send(("xp", u, i), xq.at[whole(u)], x_goal(0, whole(u)), dx=WAYS[i])

    def x_keep(u):
        return place.local("x0", xq.at[whole(u)], x_goal(0, whole(u)), u, len(UNITS))

    def x_pass(u, i):
        ref = x_goal(FROM[i], side(u, i))
        return place.send(("xs", u, i), ref, ref, dx=WAYS[i])

    def x_first(u):
        with scope("f_x1"):
            x_swap(u).wait_recv()
            for p in range(BASE[u], BASE[u] + PIECES[u]):
                xp[p] = xp[p] + xr[p]
            start_all(x_far(u, i) for i in BOTH)

    def x_second(u):
        with scope("f_x2"):
            for i in BOTH:
                x_far(u, i).wait_recv()
                sel, lanes = side(u, i), lanes_of(WAYS[i])
                xp[sel, :, lanes] = xp[sel, :, lanes] + xf[sel]
                x_near(u, i).start()

    def x_third(u):
        with scope("f_x3"):
            for i in BOTH:
                x_near(u, i).wait_recv()
            sel = whole(u)
            xq[sel] = xp[sel, :, lanes_of(0)] + xg[0, sel] + xg[1, sel]
            start_all(x_put(u, i) for i in BOTH)
            x_keep(u).start()

    def x_fourth(u):
        with scope("f_x4"):
            for i in BOTH:
                x_put(u, i).wait_recv()
                x_pass(u, i).start()

    block = width // dims["n_block"]

    def transpose_block(j):
        return xn[:, pl.ds(j * block, block)].T

    n_block = dims["n_block"]
    early = n_block // 2

    def moves(key, part, whole, other):
        sel = pl.ds(part * early, early)
        yield place.local(key, gl.at[sel], whole.at[sel], part)
        yield place.send((key, part), gl.at[sel], other.at[sel], dc=1)

    def move_g(part):
        return moves("g", part, gt_out, gpar_out)

    def move_xn(part):
        return moves("xt", part, xnt_out, xpar_out)

    def transpose_part(part, copies):
        for j in range(part * early, (part + 1) * early):
            gl[j] = transpose_block(j)
        start_all(copies)

    def columns(row):
        return jnp.broadcast_to(row.astype(F32), (LANE, tok)).T.astype(I32)

    r_step = min(LANE, tok)

    def xn_body(j, carry):
        sel = span(j * r_step, r_step, r_step)
        h_wide = xn[sel].astype(F32)
        inv_rms = lax.rsqrt(jnp.sum(h_wide * h_wide, axis=1, keepdims=True) * (1.0 / width) + NORM_EPS)
        xn[sel] = (h_wide * inv_rms * gain_out[0:1]).astype(BF16)
        return carry

    x_steps = (x_first, x_second, x_third, x_fourth)

    def x_run(work):
        for step, u in digits(work):
            x_steps[step](u)

    with scope("f_gt"):
        load_g.wait()
        for part in BOTH:
            transpose_part(part, move_g(part))
    load_h = place.local("h", h_hbm, xn)
    load_h.start()
    with scope("f_cols"):
        labc[...] = columns(lab_ref[...] - row_start)
        for i, core in enumerate((c, 1 - c)):
            tokc_out[i] = columns(tokr[core, 0:1, :])
    with scope("f_keep"):
        for h in BOTH:
            keep(h).wait()
    pass_first()
    load_unit(0)
    with scope("f_gain1"):
        gain_sum.start("dy", gain_sum.finish("dc"))
    look(0)
    pass_second(0)
    pass_first_far()
    load_unit(1)
    share_group(0)
    x_run("00")
    look(1)
    x_run("10 01")
    with scope("f_gain2"):
        gain_sum.start("dz", gain_sum.finish("dy"))
    pass_second(PAIR)
    x_run("20 11")
    end_second(0)
    load_unit(FAR)
    x_run("30")
    look(FAR)
    x_run("21 02")
    pass_second(FAR)
    load_unit(3)
    share_group(PAIR)
    x_run("31 12")
    with scope("f_xn"):
        gain_out[...] = 1.0 + gain_sum.finish("dz")
        load_h.wait()
        lax.fori_loop(0, tok // r_step, xn_body, 0)
    look(3)
    x_run("22 03")
    end_second(PAIR)
    end_second(FAR)
    load_unit(4)
    share_group(FAR)
    with scope("f_xt"):
        for part in BOTH:
            for copy in move_g(part):
                copy.wait()
            transpose_part(part, move_xn(part))
    x_run("32 13")
    look(4)
    x_run("23 04")

    e_step = min(LANE, tok)

    def tile_of(j):
        return (c * n_half + j) % n_tile

    def load_tile(j):
        return place.local("et", et_out.at[tile_of(j)], etb.at[j % 4], j % 4, 4)

    def save_u(i, odd):
        return place.local(("u", odd), (z_even, z_odd)[odd].at[i % 2], u_hbm.at[tile_of(2 * i + odd)], i % 2)

    def lane_blocks():
        return [(b, pl.ds(b, LANE)) for b in range(0, vt, LANE)]

    def post_tile(i, odd):
        base = tile_of(2 * i + odd) * vt
        buf, slot = (z_even, z_odd)[odd], i % 2
        for e in range(0, tok, e_step):
            sel = pl.ds(e, e_step)
            ids = lax.broadcasted_iota(I32, (e_step, LANE), 1) + base
            for b, lanes in lane_blocks():
                tanh_z = jnp.tanh(buf[slot, sel, lanes] * (1.0 / SOFT_CAP))
                buf[slot, sel, lanes] = tanh_z
                acc_e[sel] = acc_e[sel] + jnp.exp(SOFT_CAP * tanh_z - SOFT_CAP)
                acc_l[sel] = acc_l[sel] + jnp.where(ids + b == labc[sel], tanh_z, 0.0)

    def dot_pair(i):
        for odd in BOTH:
            value = etb[(2 * i + odd) % 4].reshape(width, vt)
            (z_even, z_odd)[odd][i % 2] = jnp.dot(xn[...], value, preferred_element_type=F32)

    def load_pair(i):
        start_all(load_tile(2 * i + odd) for odd in BOTH)

    def pair(i, carry):
        for odd in BOTH:
            load_tile(2 * i + odd).wait()

        @pl.when(i > 1)
        def _():
            for odd in BOTH:
                save_u(i - 2, odd).wait()

        for odd in BOTH:
            post_tile(i - 1, odd)
        dot_pair(i)
        start_all(save_u(i - 1, odd) for odd in BOTH)

        @pl.when(i + 2 < n_tile // 2)
        def _():
            load_pair(i + 2)

        for k, work in enumerate(during):
            @pl.when(i == k + 1)
            def _():
                x_run(work)
                if k == 0:
                    wait_shares()
        return carry

    def wait_shares():
        with scope("f_share"):
            for h in BOTH:
                for k2 in (0, PAIR, FAR):
                    share(h, k2).wait_recv()

    during = ("14", "33", "24", "", "34")
    if n_half < 4:
        wait_shares()
        for work in during:
            x_run(work)
        during = ()
    acc_e[...] = jnp.zeros_like(acc_e)
    acc_l[...] = jnp.zeros_like(acc_l)
    with scope("f_logits0"):
        for i in BOTH:
            load_pair(i)
        for odd in BOTH:
            load_tile(odd).wait()
        dot_pair(0)
        if n_tile // 2 > 2:
            load_pair(2)
    last = n_tile // 2 - 1
    with scope("f_logits"):
        lax.fori_loop(1, last + 1, pair, 0)
        for odd in BOTH:
            post_tile(last, odd)
            save_u(last, odd).start()

    with scope("f_stats"):
        row = lax.broadcasted_iota(I32, (SUB, tok), 0)
        sum_e = jnp.sum(acc_e[...].T, axis=0, keepdims=True)
        sum_l = SOFT_CAP * jnp.sum(acc_l[...].T, axis=0, keepdims=True)
        stats = SmallSum(place, ("dx",), s_slots)
        stats.start("dx", jnp.where(row == 0, sum_e, sum_l))
    with scope("f_stats2"):
        stat = stats.finish("dx")
        all_e, all_l = stat[0:1], stat[1:2]
        inv_s[...] = jnp.broadcast_to((1.0 / dims["total"]) / all_e, (LANE, tok)).T
        s_slots[0, 0:1, :] = jnp.log(all_e) + SOFT_CAP - all_l
        own = s_slots[0, 0:1, lanes_of(0)]
        part_w = min(LANE, quarter)
        folded = own[:, 0:part_w]
        for j in range(part_w, quarter, part_w):
            folded = folded + own[:, j:j + part_w]
        loss_out[...] = jnp.where(lax.broadcasted_iota(I32, (SUB, part_w), 0) == 0, folded, 0.0)

    def dz_tile(j):
        return ((1 - c) * n_half + j) % n_tile

    def load_u(i, odd):
        return place.local(("u", odd), u_hbm.at[dz_tile(2 * i + odd)], (z_even, z_odd)[odd].at[i % 2], i % 2)

    def put_dz(i, odd):
        return place.local(("dz", odd), dzb.at[odd, i % 2], dz_out.at[dz_tile(2 * i + odd)], i % 2)

    def give_dz(part):
        src = dz_out.at[pl.ds((1 - c) * n_half + part * hh, hh)]
        return place.send(("dz", part), src, dzpar_out.at[pl.ds(part * hh, hh)], dc=1)

    d_step = min(256, tok)

    def dz_rows(i, odd):
        base = dz_tile(2 * i + odd) * vt
        buf, slot = (z_even, z_odd)[odd], i % 2

        def body(e, carry):
            sel = span(e * d_step, d_step, d_step)
            ids = lax.broadcasted_iota(I32, (d_step, LANE), 1) + base
            for b, lanes in lane_blocks():
                tanh_z = buf[slot, sel, lanes]
                prob = jnp.exp(SOFT_CAP * tanh_z - SOFT_CAP) * inv_s[sel]
                prob = jnp.where(ids + b == labc[sel], prob - 1.0 / dims["total"], prob)
                dzb[odd, slot, sel, lanes] = (prob * (1.0 - tanh_z * tanh_z)).astype(BF16)
            return carry

        lax.fori_loop(0, tok // d_step, body, 0)

    def dz_pair(i, carry):
        for odd in BOTH:
            load_u(i, odd).wait()

            @pl.when(i > hh + 1)
            def _():
                put_dz(i - 2, odd).wait()

            dz_rows(i, odd)
            put_dz(i, odd).start()

            @pl.when(i + 2 < n_tile // 2)
            def _():
                load_u(i + 2, odd).start()

        return carry

    with scope("f_dz"):
        for i in range(n_tile // 2 - 2, n_tile // 2):
            for odd in BOTH:
                save_u(i, odd).wait()
        for i in BOTH:
            start_all(load_u(i, odd) for odd in BOTH)
        for part in BOTH:
            lo, hi = part * hh // 2, (part + 1) * hh // 2
            lax.fori_loop(lo, hi, dz_pair, 0)
            for i in range(max(lo, hi - 2), hi):
                for odd in BOTH:
                    put_dz(i, odd).wait()
            give_dz(part).start()
        lax.fori_loop(hh, n_tile // 2, dz_pair, 0)

    with scope("f_end"):
        for part in BOTH:
            give_dz(part).wait()
        for i in range(n_tile // 2 - 2, n_tile // 2):
            for odd in BOTH:
                put_dz(i, odd).wait()
        give_tok.wait_send()
        give_chunk.wait_send()
        for h in BOTH:
            for i in BOTH:
                p1_send(h, i).wait_send()
                p1_fwd(h, i).wait_send()
                for k in (0, PAIR, FAR):
                    p2_send(h, k, i).wait_send()
                    p2_fwd(h, k, i).wait_send()
            for k in (0, PAIR, FAR):
                share(h, k).wait_send()
        for part in BOTH:
            for copy in move_xn(part):
                copy.wait()
        for u in range(len(UNITS)):
            if u > len(UNITS) - 3:
                x_swap(u).wait_send()
            x_keep(u).wait()
            for i in BOTH:
                x_far(u, i).wait_send()
                x_near(u, i).wait_send()
                x_put(u, i).wait_send()
                x_pass(u, i).wait()
    assert (place.n_link, place.n_local) <= dims["front_sems"], (place.n_link, place.n_local)


def specs(n_vmem, n_any):
    return [pl.BlockSpec(memory_space=pltpu.VMEM)] * n_vmem + [pl.BlockSpec(memory_space=pl.ANY)] * n_any


def shapes(items):
    return tuple(jax.ShapeDtypeStruct(*item) for item in items)


def scratch(items, n_link, n_local):
    dma = pltpu.SemaphoreType.DMA
    return [pltpu.VMEM(*item) for item in items] + [dma((n_link,)), dma((n_link,)), dma((n_local,))]


def params(collective_id, limit):
    return pltpu.CompilerParams(collective_id=collective_id, has_side_effects=True, vmem_limit_bytes=limit)


def front(dims, limit, shard, tok_row, lab_row, w, h, g):
    n, tok, vocab, width, vt = dims["n"], dims["tok"], dims["vocab"], dims["width"], dims["vt"]
    cols = shard.shape[0]
    half_v = vocab // CORES
    quarter = tok // n
    n_tile, n_half, n_block, most = vocab // vt, half_v // vt, dims["n_block"], max(PIECES)
    block = width // n_block
    pieces = n * n * CORES
    grid = (n // 2, 2, n // 2, 2)
    return pl.pallas_call(
        functools.partial(front_kernel, dims),
        name="front",
        out_shape=shapes([
            ((n_tile, *grid, CORES, cols, vt), BF16), *[((n_block, block, tok), BF16)] * 4, ((n_tile, tok, vt), BF16),
            ((n_half, tok, vt), BF16), ((n, pieces, cols, quarter), BF16), ((n_tile, tok, vt), F32),
            ((SUB, width), F32), ((SUB, min(LANE, quarter)), F32), ((CORES, tok, LANE), I32),
        ]),
        in_specs=specs(4, 2),
        out_specs=tuple(specs(0, 9) + specs(3, 0)),
        scratch_shapes=scratch([
            ((n_tile, cols, vt), BF16), ((CORES, n_half, cols, vt), BF16), ((CORES, SUB, tok), I32), ((half_v, CORES * tok), BF16),
            ((2, most, n_half, cols, vt), BF16), ((pieces, cols, tok), BF16), ((2, most, cols, tok), BF16), ((pieces, cols, tok), BF16),
            ((pieces, cols, quarter), BF16), ((2, pieces, cols, quarter), BF16), ((pieces, cols, quarter), BF16),
            ((4, *grid, CORES, cols, vt), BF16), ((tok, width), BF16), ((n_block, block, tok), BF16),
            ((2, tok, vt), F32), ((2, tok, vt), F32), ((2, 2, tok, vt), BF16), ((tok, LANE), F32), ((tok, LANE), F32), ((tok, LANE), F32),
            ((tok, LANE), I32), ((2 * n + CORES, SUB, width), F32), ((n, SUB, tok), F32),
        ], dims["front_sems"][0], dims["front_sems"][1]),
        compiler_params=params(0, limit),
    )(shard, tok_row, lab_row, w, h, g)


def back_kernel(
    dims,
    gain_ref, loss_ref, tokc, dz_hbm, dzp_hbm, et_hbm, xnt_hbm, xpar_hbm, gt_hbm, gpar_hbm, h_hbm,
    tail_out, dh_out, de_out, ra_hbm, rx_hbm,
    dz_own, dz_par, et_buf, part, fx, acc, fa, f2, r2, xb, h_buf, dh_buf, dg_acc, slots,
    sends, recvs, local_sems,
):
    n, tok, vocab, width, tile, per_chunk, vt = (dims[k] for k in ("n", "tok", "vocab", "width", "tile", "per_chunk", "vt"))
    place = Place(n, sends, recvs, local_sems)
    x, z, y, c = place.x, place.z, place.y, place.c
    half_v = vocab // CORES
    n_tile, n_half = vocab // vt, half_v // vt
    lanes = half_v // 2
    rows = width // (n * n)
    half_rows = rows // 2
    quarter = tok // n
    hq = quarter // 2
    chunks = width // (tile * per_chunk)
    per_half = n_half // 2

    with scope("b_enter"):
        place.enter()

    load_h = place.local("h", h_hbm.at[span(x * quarter, quarter, quarter)], h_buf)

    def load_et(t, slot):
        return place.local("et", et_hbm.at[:, span(t * tile, tile, tile)], et_buf.at[slot], slot)

    slot_of = {FAR: 0, 1: 1, 3: 2, 0: 0}
    stages = dims["stages"]

    def load_stage(m, i):
        half, k, kind = stages[m]
        src = ((gt_hbm, gpar_hbm), (xnt_hbm, xpar_hbm))[kind][i]
        src = src.at[(z + k) % n] if half == 0 else src.at[:, (y + k) % n]
        return place.local(("xb", i), src, xb.at[m % 2, i], m % 2)

    def start_stage(m):
        if m < len(stages):
            start_all(load_stage(m, i) for i in BOTH)

    for m in BOTH:
        start_stage(m)
    loads = [place.local("dz", dz_hbm, dz_own), place.local("dzp", dzp_hbm, dz_par)]
    load_et(0, 0).start()
    start_all(loads)
    load_h.start()

    def dxn_chunk(d):
        def body(i, carry):
            t = d * per_chunk + i
            slot = t % 2

            @pl.when(t + 1 < chunks * per_chunk)
            def _():
                load_et(t + 1, 1 - slot).start()

            load_et(t, slot).wait()
            left = jnp.concatenate([dz_own[j] for j in range(n_tile)], axis=1)
            right = jnp.concatenate([et_buf[slot, j] for j in range(n_tile)], axis=1)
            part[d, :, span(i * tile, tile, tile)] = lax.dot_general(
                left, right, (((1,), (1,)), ((), ())), preferred_element_type=F32)
            return carry

        with scope("b_dxn"):
            lax.fori_loop(0, per_chunk, body, 0)

    def qrow(k, lo=0, size=hq):
        return span((x + k) % n * quarter + lo, size, SUB)

    def x_far(d, i):
        return place.send(("xf", d, i), part.at[d, qrow(FAR, i * hq)], fx.at[d, i], dx=WAYS[i])

    def x_near(d, i):
        return place.send(("xn", d, i), part.at[d, qrow(WAYS[i], 0, quarter)], rx_hbm.at[d, i], dx=WAYS[i])

    def x_first(d):
        start_all(x_far(d, i) for i in BOTH)

    def x_second(d):
        with scope("b_x2"):
            for i in BOTH:
                x_far(d, i).wait_recv()
                sel = qrow(WAYS[i], i * hq)
                part[d, sel] = part[d, sel] + fx[d, i]
                x_near(d, i).start()

    def stage_x(d, j, i):
        return place.local("sx", rx_hbm.at[d, i, pl.ds(j * hq, hq)], fx.at[d, i], i)

    def x_third(d):
        with scope("b_x3"):
            for i in BOTH:
                x_near(d, i).wait_recv()
            for j in BOTH:
                start_all(stage_x(d, j, i) for i in BOTH)
                for i in BOTH:
                    stage_x(d, j, i).wait()
                sel = qrow(0, j * hq)
                part[d, sel] = part[d, sel] + fx[d, 0] + fx[d, 1]

    def de_stage(half, k, kind):
        m = stages.index((half, k, kind))
        slot = slot_of[k]

        def right(i, t):
            if kind:
                return dz_par[t] if i else dz_own[c * n_half + t]
            ids = lax.broadcasted_iota(I32, (tok, LANE), 1) + (x * vocab + c * half_v + t * vt)
            hits = [jnp.where(tokc[i] == ids + b, dims["scale"], 0.0).astype(BF16) for b in range(0, vt, LANE)]
            return jnp.concatenate(hits, axis=1)

        def body(j, carry):
            t = half * per_half + j
            sel = span(j * vt, vt)
            total = sum(jnp.dot(xb[m % 2, i].reshape(n * rows, tok), right(i, t), preferred_element_type=F32) for i in BOTH)
            total = total.reshape(n, rows, vt)
            acc[half, slot, :, :, sel] = acc[half, slot, :, :, sel] + total if kind else total
            return carry

        with scope("b_de" if kind else "b_look"):
            for i in BOTH:
                load_stage(m, i).wait()
            lax.fori_loop(0, per_half, body, 0)
            start_stage(m + 2)

    def de_unit(half, k):
        for kind in BOTH:
            de_stage(half, k, kind)

    def ring(half, k):
        return {"dz": k} if half == 0 else {"dy": k}

    def cross(half, k):
        return {"dy": k} if half == 0 else {"dz": k}

    def a_far(half, i):
        return place.send(("af", half, i), acc.at[half, 0, pl.ds(2 * i, 2)], fa.at[half, i], **ring(half, WAYS[i]))

    def a_near(half, i):
        return place.send(("an", half, i), acc.at[half, 1 + i], ra_hbm.at[half, i], **ring(half, WAYS[i]))

    def a_first(half):
        start_all(a_far(half, i) for i in BOTH)

    def a_second(half, i):
        with scope("b_a2"):
            a_far(half, i).wait_recv()
            sel = pl.ds(2 * i, 2)
            acc[half, 1 + i, sel] = acc[half, 1 + i, sel] + fa[half, i]
            a_near(half, i).start()

    def stage_a(half, j, i):
        return place.local(("sa", half), ra_hbm.at[half, i, pl.ds(2 * j, 2)], fa.at[half, i], i)

    def piece(half, k):
        return ((y if half == 0 else z) + k) % n

    def c_far(half, i):
        src = acc.at[half, 0, piece(half, FAR), pl.ds(i * half_rows, half_rows)]
        return place.send(("cf", half, i), src, f2.at[half, i], **cross(half, WAYS[i]))

    def c_near(half, i):
        return place.send(("cn", half, i), acc.at[half, 0, piece(half, WAYS[i])], r2.at[half, i], **cross(half, WAYS[i]))

    def a_third(half):
        with scope("b_a3"):
            for i in BOTH:
                a_near(half, i).wait_recv()
            for j in BOTH:
                start_all(stage_a(half, j, i) for i in BOTH)
                for i in BOTH:
                    stage_a(half, j, i).wait()
                sel = pl.ds(2 * j, 2)
                acc[half, 0, sel] = acc[half, 0, sel] + fa[half, 0] + fa[half, 1]
            start_all(c_far(half, i) for i in BOTH)

    def c_second(half):
        with scope("b_c2"):
            for i in BOTH:
                c_far(half, i).wait_recv()
                at = piece(half, WAYS[i])
                sel = pl.ds(i * half_rows, half_rows)
                acc[half, 0, at, sel] = acc[half, 0, at, sel] + f2[half, i]
                c_near(half, i).start()

    def out_copies(half):
        sel = span(c * half_v + half * lanes, lanes)
        mine = acc.at[half, 0, piece(half, 0)]
        yield place.local("de", mine.at[span(c * half_rows, half_rows, SUB)], de_out.at[:, sel], half)
        yield place.send(("de", half), mine.at[span((1 - c) * half_rows, half_rows, SUB)], de_out.at[:, sel], dc=1)

    def c_third(half):
        with scope("b_c3"):
            for i in BOTH:
                c_near(half, i).wait_recv()
            at = piece(half, 0)
            acc[half, 0, at] = acc[half, 0, at] + r2[half, 0] + r2[half, 1]
            start_all(out_copies(half))

    for half in BOTH:
        de_stage(half, FAR, 0)
    with scope("b_load"):
        for copy in loads:
            copy.wait()
    dxn_chunk(0)
    x_first(0)
    de_stage(0, FAR, 1)
    a_first(0)
    if chunks > 1:
        dxn_chunk(1)
        x_first(1)
    de_stage(1, FAR, 1)
    a_first(1)
    x_second(0)
    for d in range(2, chunks):
        dxn_chunk(d)
        x_first(d)
    de_unit(0, 1)
    if chunks > 1:
        x_second(1)
    de_unit(0, 3)
    for i in BOTH:
        a_second(0, i)
    for k in WAYS:
        de_unit(1, k)
    for i in BOTH:
        a_second(1, i)
    for d in range(2, chunks):
        x_second(d)
    with scope("b_wait_far"):
        for half in BOTH:
            for i in BOTH:
                a_far(half, i).wait_send()
    for half in BOTH:
        de_unit(half, 0)
    for d in range(chunks):
        x_third(d)

    step = min(32, quarter)

    def dh_body(i, carry):
        sel = span(i * step, step, step)
        row = span(x * quarter + i * step, step, step)
        d_x = jnp.concatenate([part[d, row] for d in range(chunks)], axis=1)
        h_wide = h_buf[sel].astype(F32)
        inv_rms = lax.rsqrt(jnp.sum(h_wide * h_wide, axis=1, keepdims=True) * (1.0 / width) + NORM_EPS)
        h_norm = h_wide * inv_rms
        g_dir = d_x * gain_ref[0:1]
        mean = jnp.sum(g_dir * h_norm, axis=1, keepdims=True) * (1.0 / width)
        dh_buf[sel] = (inv_rms * (g_dir - h_norm * mean)).astype(BF16)
        prod = d_x * h_norm
        total = prod[0:SUB]
        for j in range(SUB, step, SUB):
            total = total + prod[j:j + SUB]
        dg_acc[...] = dg_acc[...] + total
        return carry

    with scope("b_dh"):
        load_h.wait()
        dg_acc[...] = jnp.zeros_like(dg_acc)
        lax.fori_loop(0, quarter // step, dh_body, 0)

    def h_first(i, part_of):
        lo = ((i + part_of) % 2) * hq
        return place.send(("hf", i, part_of), dh_buf.at[pl.ds(lo, hq)], dh_out.at[qrow(0, lo)], dx=WAYS[i])

    def h_second(i):
        ref = dh_out.at[qrow(FROM[i], i * hq)]
        return place.send(("hs", i), ref, ref, dx=WAYS[i])

    keep_dh = place.local("dh", dh_buf, dh_out.at[qrow(0, 0, quarter)])
    small = SmallSum(place, ("dc", "dx", "dy", "dz"), slots)
    small.start("dc", jnp.concatenate([dg_acc[...], loss_ref[...]], axis=1))
    start_all(h_first(i, 0) for i in BOTH)
    keep_dh.start()
    with scope("b_s1"):
        small.start("dx", small.finish("dc"))
    start_all(h_first(i, 1) for i in BOTH)
    for half in BOTH:
        a_third(half)
    with scope("b_h2"):
        for i in BOTH:
            h_first(i, 0).wait_recv()
            h_second(i).start()
    with scope("b_s2"):
        small.start("dy", small.finish("dx"))
    for half in BOTH:
        c_second(half)
    with scope("b_s3"):
        small.start("dz", small.finish("dy"))
    for half in BOTH:
        c_third(half)
    with scope("b_s4"):
        total = jnp.sum(small.finish("dz"), axis=0, keepdims=True)
        loss = jnp.sum(total[:, width:], axis=1, keepdims=True) * (1.0 / dims["total"])
        tail_out[...] = jnp.concatenate([total[:, 0:width], jnp.broadcast_to(loss, (1, LANE))], axis=1)

    with scope("b_end_x"):
        keep_dh.wait()
        for i in BOTH:
            for d in range(chunks):
                x_far(d, i).wait_send()
                x_near(d, i).wait_send()
            h_first(i, 0).wait_send()
            h_first(i, 1).wait()
            h_second(i).wait()
    with scope("b_end_a"):
        for half in BOTH:
            for i in BOTH:
                a_near(half, i).wait_send()
                c_far(half, i).wait_send()
                c_near(half, i).wait_send()
            for copy in out_copies(half):
                copy.wait()
    assert (place.n_link, place.n_local) <= dims["back_sems"], (place.n_link, place.n_local)


def back(dims, limit, gain, loss, tokc, dz, dzp, et, xnt, xpar, gt, gpar, h):
    n, tok, vocab, width, tile, per_chunk = (dims[k] for k in ("n", "tok", "vocab", "width", "tile", "per_chunk"))
    rows = width // (n * n)
    half_v = vocab // CORES
    lanes = half_v // 2
    quarter = tok // n
    hq = quarter // 2
    chunk_w = tile * per_chunk
    chunks = width // chunk_w
    tail_w = width + loss.shape[1]
    n_tile, n_half, vt = dz.shape[0], dzp.shape[0], dims["vt"]
    turned = [a.reshape(n, n, rows, tok) for a in (xnt, xpar, gt, gpar)]
    return pl.pallas_call(
        functools.partial(back_kernel, dims),
        name="back",
        out_shape=shapes([
            ((1, width + LANE), F32), ((tok, width), BF16), ((rows // CORES, vocab), F32), ((2, 2, n, rows, lanes), F32),
            ((chunks, 2, quarter, chunk_w), F32),
        ]),
        in_specs=specs(3, 8),
        out_specs=tuple(specs(1, 4)),
        scratch_shapes=scratch([
            ((n_tile, tok, vt), BF16), ((n_half, tok, vt), BF16), ((2, n_tile, tile, vt), BF16), ((chunks, tok, chunk_w), F32),
            ((chunks, 2, hq, chunk_w), F32), ((2, 3, n, rows, lanes), F32), ((2, 2, 2, rows, lanes), F32),
            ((2, 2, rows // 2, lanes), F32), ((2, 2, rows, lanes), F32), ((2, CORES, n, rows, tok), BF16), ((quarter, width), BF16),
            ((quarter, width), BF16), ((SUB, width), F32), ((3 * n + CORES, SUB, tail_w), F32),
        ], dims["back_sems"][0], dims["back_sems"][1]),
        compiler_params=params(1, limit),
    )(gain, loss, tokc, dz, dzp, et.reshape(n_tile, width, vt), *turned, h)[:3]


def finish_kernel(n, scale, table_ref, x0_ref, dh_ref, x0_out, dh_out, rows_ref):
    place = Place(n, None, None, None)
    cols = x0_ref.shape[2]
    for zi in range(n):
        for yi in range(n):
            for h in BOTH:
                dz, dy = (zi - place.z) % n, (yi - place.y) % n
                k1, k2 = (dy, dz) if h == 0 else (dz, dy)
                piece = table_ref[(h * n + k1) * n + k2]
                rows_ref[pl.ds(((zi * n + yi) * CORES + h) * cols, cols)] = x0_ref[0, piece]
    x0_out[...] = (rows_ref[...].T.astype(F32) * scale).astype(BF16)
    dh_out[...] = dh_ref[...]


def finish(n, scale, dims_limit, x0, dh):
    _, pieces, cols, quarter = x0.shape
    width = pieces * cols
    table = np.zeros((CORES, n, n), np.int32)
    for u, unit in enumerate(UNITS):
        for h in BOTH:
            for i, (k1, k2) in enumerate(unit):
                table[h, k1, k2] = BASE[u] + h * len(unit) + i
    row = pl.BlockSpec((quarter, width), lambda q, t: (q, 0))
    return pl.pallas_call(
        functools.partial(finish_kernel, n, scale),
        name="finish",
        grid_spec=pltpu.PrefetchScalarGridSpec(
            num_scalar_prefetch=1,
            grid=(n,),
            in_specs=[pl.BlockSpec((1, pieces, cols, quarter), lambda q, t: (q, 0, 0, 0)), row],
            out_specs=(row, row),
            scratch_shapes=[pltpu.VMEM((width, quarter), BF16)],
        ),
        out_shape=shapes([(dh.shape, BF16)] * 2),
        compiler_params=pltpu.CompilerParams(vmem_limit_bytes=dims_limit),
    )(jnp.asarray(table.reshape(-1)), x0, dh)


def solution(mesh):
    return build(mesh, mesh.shape["tp"], 256, 3, 256, 6, 67_000_000)


def build(mesh, n, tile, per_chunk, vt, n_block, limit):
    fsdp_size = mesh.shape["fsdp"]

    def device_step(emb_shard, tok_ids, lab_ids, h_last, g_embed, norm_w):
        vocab_rows, cols = emb_shard.shape
        batch_loc, seq_len, width = h_last.shape
        tok_count = batch_loc * seq_len
        fsdp_id = lax.axis_index("fsdp")
        scale = float(np.asarray(math.sqrt(width)).astype(jnp.bfloat16))
        dims = {
            "n": n, "tok": tok_count, "vocab": vocab_rows, "width": width, "total": tok_count * fsdp_size, "vt": vt,
            "tile": tile, "per_chunk": per_chunk, "scale": scale, "n_block": n_block,
            "stages": digits("020 120 021 121") + digits("010 011 030 031") + digits("110 111 130 131") + digits("000 001 100 101"),
            "front_sems": (101, 41), "back_sems": (46, 22),
        }
        h_flat = h_last.reshape(tok_count, width)
        placed = lax.dynamic_update_slice(jnp.zeros((SUB, width), F32), jnp.broadcast_to(norm_w, (SUB, cols)), (0, fsdp_id * cols))
        ids = [a.reshape(1, tok_count) for a in (tok_ids, lab_ids)]
        placed = lax.dynamic_update_slice(jnp.zeros((SUB, width), F32), jnp.broadcast_to(norm_w, (SUB, cols)), (0, fsdp_id * cols))
        table, xn_t, xpar_t, g_t, gpar_t, dz, dzp, x0, _, gain, loss_part, tokc = front(
            dims, limit, emb_shard.T, *ids, placed, h_flat, g_embed.reshape(tok_count, width))
        tail, d_hidden, d_cols = back(dims, limit, gain, loss_part, tokc, dz, dzp, table, xn_t, xpar_t, g_t, gpar_t, h_flat)
        x_emb, d_hidden = finish(n, scale, limit, x0, d_hidden)
        d_norm_w = lax.dynamic_slice(tail[0], (fsdp_id * cols,), (cols,))
        return (x_emb.reshape(h_last.shape), tail[0, width], d_hidden.reshape(h_last.shape), d_norm_w, d_cols.T)

    spec_tok = P("fsdp", None)
    spec_act = P("fsdp", None, None)
    return jax.shard_map(device_step, mesh=mesh, in_specs=(P("tp", "fsdp"), spec_tok, spec_tok, spec_act, spec_act, P("fsdp")), out_specs=(spec_act, P(), spec_act, P("fsdp"), P("tp", "fsdp")), check_vma=False)
```

```python
import functools
import math
import jax
import numpy as np
import jax.numpy as jnp
from jax import lax
from jax.experimental import pallas as pl
from jax.experimental.pallas import tpu as pltpu
from jax.sharding import PartitionSpec as P

SOFT_CAP = 30.0
NORM_EPS = 1e-6
F32, BF16, I32 = jnp.float32, jnp.bfloat16, jnp.int32
LANE, SUB = 128, 8
BOTH = (0, 1)
FOUR = range(4)
WAYS = (1, 3)
FROM = (3, 1)
FAR = 2
CORES = 2


def span(start, size, unit=LANE):
    return pl.ds(pl.multiple_of(start, unit), size)


class Place:
    def __init__(self, n, sends, recvs, local_sems):
        self.n, self.sends, self.recvs, self.local_sems = n, sends, recvs, local_sems
        self.x = lax.axis_index("tp")
        f = lax.axis_index("fsdp")
        self.f = f
        self.c = f % CORES
        self.y = f // CORES % n
        self.z = f // CORES // n
        self.link_of, self.local_of, self.n_link, self.n_local = {}, {}, 0, 0
        self.size = {"dx": n, "dz": n, "dy": n, "dc": CORES}
        self.me = {"dx": self.x, "dz": self.z, "dy": self.y, "dc": self.c}

    def at(self, dx=0, dz=0, dy=0, dc=0):
        n = self.n
        z, y, c = (self.z + dz) % n, (self.y + dy) % n, (self.c + dc) % CORES
        return ((self.x + dx) % n, (z * n + y) * CORES + c)

    def enter(self):
        barrier = pltpu.get_barrier_semaphore()
        peers = [self.at(**{d: k}) for d in self.size for k in range(1, self.size[d])]
        for peer in peers:
            pl.semaphore_signal(barrier, inc=1, device_id=peer, device_id_type=pl.DeviceIdType.MESH)
        pl.semaphore_wait(barrier, len(peers))

    def link(self, key, count=1):
        if key not in self.link_of:
            self.link_of[key] = self.n_link
            self.n_link += count
        return self.link_of[key]

    def send(self, key, src, dst, **step):
        i = self.link(key)
        return pltpu.make_async_remote_copy(
            src, dst, self.sends.at[i], self.recvs.at[i], device_id=self.at(**step), device_id_type=pl.DeviceIdType.MESH)

    def local(self, key, src, dst, slot=0, count=2):
        if key not in self.local_of:
            self.local_of[key] = self.n_local
            self.n_local += count
        return pltpu.make_async_copy(src, dst, self.local_sems.at[self.local_of[key] + slot])


class SmallSum:
    def __init__(self, place, dims, slots):
        self.place, self.slots, self.dims, self.base = place, slots, dims, {}
        count = 0
        for d in dims:
            self.base[d] = count
            count += place.size[d]

    def copies(self, d):
        slot = self.slots.at[self.base[d] + self.place.me[d]]
        for k in range(1, self.place.size[d]):
            yield self.place.send((self.dims, d, k), slot, slot, **{d: k})

    def start(self, d, value):
        self.slots[self.base[d] + self.place.me[d]] = value
        for copy in self.copies(d):
            copy.start()

    def finish(self, d):
        for copy in self.copies(d):
            copy.wait()
        total = self.slots[self.base[d]]
        for k in range(1, self.place.size[d]):
            total = total + self.slots[self.base[d] + k]
        return total


def scope(name):
    return jax.named_scope(name)


def start_all(copies):
    for copy in copies:
        copy.start()


def digits(text):
    return tuple(tuple(int(d) for d in word) for word in text.split())


UNITS = [digits(u) for u in ("00", "10 30", "01 03 20", "02 11 31", "13 33 21 23", "12 32 22")]
PAIR, ALL = 1, "all"
PIECES = [2 * len(u) for u in UNITS]
BASE = [sum(PIECES[:i]) for i in range(len(UNITS))]


def front_kernel(
    dims,
    shard_ref, tok_ref, lab_ref, w_ref, h_hbm, g_hbm,
    et_out, xnt_out, xpar_out, gt_out, gpar_out, dz_out, dzpar_out, x0_out, u_hbm, gain_out, loss_out, tokc_out,
    shard_t, chunk, tokr, hit_t, lhs, xp, xo, xr, xf, xg, xq, etb, xn, gl, z_even, z_odd, dzb,
    acc_e, acc_l, inv_s, labc, w_slots, s_slots, sends, recvs, local_sems,
):
    n, tok, vocab, width, vt = dims["n"], dims["tok"], dims["vocab"], dims["width"], dims["vt"]
    place = Place(n, sends, recvs, local_sems)
    x, z, y, c = place.x, place.z, place.y, place.c
    half_v = vocab // CORES
    n_tile = vocab // vt
    n_half = n_tile // CORES
    hh = n_half // 2
    cols = width // (n * n * CORES)
    quarter = tok // n
    row_start = x * vocab

    def ring1(h, k):
        return {"dy": k} if h == 0 else {"dz": k}

    def ring2(h, k):
        return {"dz": k} if h == 0 else {"dy": k}

    def coord(base, k, paired):
        every = slice(None)
        if k == ALL:
            return every, every
        return every if paired else (base + k) % n // 2, (base + k) % 2

    def loc(h, k1, k2, lo=0, size=n_half, pair1=False, pair2=False):
        first, second = coord((y, z)[h], k1, pair1), coord((z, y)[h], k2, pair2)
        return et_out.at[(pl.ds(c * n_half + lo, size), *((second, first)[h]), *((first, second)[h]), h)]

    with scope("f_enter"):
        place.enter()

    load_g = place.local("g", g_hbm, xn)
    load_g.start()
    with scope("f_cast"):
        for t in range(n_tile):
            shard_t[t] = shard_ref[:, pl.ds(t * vt, vt)].astype(BF16)
        tokr[c] = jnp.broadcast_to(tok_ref[...], (SUB, tok))
        give_tok = place.send("tok", tokr.at[c], tokr.at[c], dc=1)
        give_chunk = place.send("chunk", shard_t.at[pl.ds((1 - c) * n_half, n_half)], chunk.at[c], dc=1)
        give_chunk.start()
        give_tok.start()
        chunk[c] = shard_t[pl.ds(c * n_half, n_half)]
        gain_sum = SmallSum(place, ("dc", "dy", "dz"), w_slots)
        own_w = jnp.concatenate([w_ref[...], jnp.zeros((1, width - cols), F32)], axis=1)
        gain_sum.start("dc", pltpu.roll(jnp.broadcast_to(own_w, (SUB, width)), place.f * cols, axis=1))

    def p1_send(h, i):
        return place.send(("p1", h, i), chunk.at[h], loc(h, 0, 0), **ring1(h, WAYS[i]))

    def p1_fwd(h, i):
        ref = loc(h, FROM[i], 0, i * hh, hh)
        return place.send(("p1f", h, i), ref, ref, **ring1(h, WAYS[i]))

    def p2_send(h, k1, i):
        ref = loc(h, k1, 0, pair1=k1 == PAIR)
        return place.send(("p2", h, k1, i), chunk.at[h] if k1 == 0 else ref, ref, **ring2(h, WAYS[i]))

    def p2_fwd(h, k1, i):
        ref = loc(h, k1, FROM[i], i * hh, hh, pair1=k1 == PAIR)
        return place.send(("p2f", h, k1, i), ref, ref, **ring2(h, WAYS[i]))

    def keep(h):
        return place.local("keep", chunk.at[h], loc(h, 0, 0), h)

    def share(h, k2):
        ref = loc(h, ALL, k2, pair2=k2 == PAIR)
        return place.send(("share", h, k2), ref, ref, dc=1)

    def pass_first():
        with scope("f_p1"):
            for h in BOTH:
                for i in BOTH:
                    p1_send(h, i).wait_recv()
                    p1_fwd(h, i).start()
            for h in BOTH:
                start_all(p2_send(h, PAIR, i) for i in BOTH)

    def pass_first_far():
        with scope("f_p1f"):
            for h in BOTH:
                for i in BOTH:
                    p1_fwd(h, i).wait_recv()
                start_all(p2_send(h, FAR, j) for j in BOTH)

    def pass_second(k1):
        with scope("f_p2"):
            for h in BOTH:
                for i in BOTH:
                    p2_send(h, k1, i).wait_recv()
                    p2_fwd(h, k1, i).start()

    def end_second(k1):
        with scope("f_p2f"):
            for h in BOTH:
                for i in BOTH:
                    p2_fwd(h, k1, i).wait_recv()

    def share_group(k2):
        start_all(share(h, k2) for h in BOTH)

    with scope("f_chunk"):
        give_chunk.wait_recv()
        start_all(keep(h) for h in BOTH)
        gain_sum.start("dy", gain_sum.finish("dc"))
        for h in BOTH:
            start_all(p1_send(h, i) for i in BOTH)
        for h in BOTH:
            start_all(p2_send(h, 0, i) for i in BOTH)

    v_step = min(LANE, half_v)

    def hit_body(j, carry):
        off = j * v_step
        ids = lax.broadcasted_iota(I32, (v_step, tok), 0) + (row_start + c * half_v + off)
        for i, core in enumerate((c, 1 - c)):
            hit_t[span(off, v_step, v_step), pl.ds(i * tok, tok)] = jnp.where(ids == tokr[core, 0:1, :], 1.0, 0.0).astype(BF16)
        return carry

    with scope("f_hit"):
        give_tok.wait_recv()
        lax.fori_loop(0, half_v // v_step, hit_body, 0)

    n_step = min(256, tok)
    most = max(PIECES)

    def whole(u):
        return pl.ds(BASE[u], PIECES[u])

    def unit_copies(u):
        slot = u % 2
        for p, (h, (k1, k2)) in enumerate((h, k) for h in BOTH for k in UNITS[u]):
            yield place.local("lhs", loc(h, k1, k2), lhs.at[slot, p], slot * most + p, 2 * most)

    def load_unit(u):
        start_all(unit_copies(u))

    def look(u):
        pieces = PIECES[u]
        with scope("f_look"):
            if u > 1:
                x_swap(u - 2).wait_send()
            left = lhs.at[u % 2]
            for copy in unit_copies(u):
                copy.wait()
            for i, dst in enumerate((xp.at[whole(u)], xo.at[u % 2])):
                def body(j, carry):
                    off = j * n_step
                    value = jnp.concatenate([left[pl.ds(0, pieces), t].reshape(pieces * cols, vt) for t in range(n_half)], axis=1)
                    rows = jnp.dot(value, hit_t[:, span(i * tok + off, n_step)], preferred_element_type=F32)
                    dst[pl.ds(0, pieces), :, span(off, n_step)] = rows.reshape(pieces, cols, n_step).astype(BF16)
                    return carry

                lax.fori_loop(0, tok // n_step, body, 0)
            x_swap(u).start()

    def x_swap(u):
        return place.send(("swap", u), xo.at[u % 2, pl.ds(0, PIECES[u])], xr.at[whole(u)], dc=1)

    def lanes_of(k):
        return span((x + k) % n * quarter, quarter, quarter)

    def side(u, i):
        return pl.ds(BASE[u] + i * len(UNITS[u]), len(UNITS[u]))

    def x_far(u, i):
        return place.send(("xf", u, i), xp.at[side(u, i), :, lanes_of(FAR)], xf.at[side(u, i)], dx=WAYS[i])

    def x_near(u, i):
        return place.send(("xn", u, i), xp.at[whole(u), :, lanes_of(WAYS[i])], xg.at[i, whole(u)], dx=WAYS[i])

    def x_goal(k, sel):
        return x0_out.at[(x + k) % n, sel]

    def x_put(u, i):
        return place.send(("xp", u, i), xq.at[whole(u)], x_goal(0, whole(u)), dx=WAYS[i])

    def x_keep(u):
        return place.local("x0", xq.at[whole(u)], x_goal(0, whole(u)), u, len(UNITS))

    def x_pass(u, i):
        ref = x_goal(FROM[i], side(u, i))
        return place.send(("xs", u, i), ref, ref, dx=WAYS[i])

    def x_first(u):
        with scope("f_x1"):
            x_swap(u).wait_recv()
            for p in range(BASE[u], BASE[u] + PIECES[u]):
                xp[p] = xp[p] + xr[p]
            start_all(x_far(u, i) for i in BOTH)

    def x_second(u):
        with scope("f_x2"):
            for i in BOTH:
                x_far(u, i).wait_recv()
                sel, lanes = side(u, i), lanes_of(WAYS[i])
                xp[sel, :, lanes] = xp[sel, :, lanes] + xf[sel]
                x_near(u, i).start()

    def x_third(u):
        with scope("f_x3"):
            for i in BOTH:
                x_near(u, i).wait_recv()
            sel = whole(u)
            xq[sel] = xp[sel, :, lanes_of(0)] + xg[0, sel] + xg[1, sel]
            start_all(x_put(u, i) for i in BOTH)
            x_keep(u).start()

    def x_fourth(u):
        with scope("f_x4"):
            for i in BOTH:
                x_put(u, i).wait_recv()
                x_pass(u, i).start()

    block = width // dims["n_block"]

    def transpose_block(j):
        return xn[:, pl.ds(j * block, block)].T

    n_block = dims["n_block"]
    early = n_block // 2

    def moves(key, part, whole, other):
        sel = pl.ds(part * early, early)
        yield place.local(key, gl.at[sel], whole.at[sel], part)
        yield place.send((key, part), gl.at[sel], other.at[sel], dc=1)

    def move_g(part):
        return moves("g", part, gt_out, gpar_out)

    def move_xn(part):
        return moves("xt", part, xnt_out, xpar_out)

    def transpose_part(part, copies):
        for j in range(part * early, (part + 1) * early):
            gl[j] = transpose_block(j)
        start_all(copies)

    def columns(row):
        return jnp.broadcast_to(row.astype(F32), (LANE, tok)).T.astype(I32)

    r_step = min(LANE, tok)

    def xn_body(j, carry):
        sel = span(j * r_step, r_step, r_step)
        h_wide = xn[sel].astype(F32)
        inv_rms = lax.rsqrt(jnp.sum(h_wide * h_wide, axis=1, keepdims=True) * (1.0 / width) + NORM_EPS)
        xn[sel] = (h_wide * inv_rms * gain_out[0:1]).astype(BF16)
        return carry

    x_steps = (x_first, x_second, x_third, x_fourth)

    def x_run(work):
        for step, u in digits(work):
            x_steps[step](u)

    with scope("f_keep"):
        for h in BOTH:
            keep(h).wait()
        load_unit(0)
        gain_sum.start("dz", gain_sum.finish("dy"))
    with scope("f_gt"):
        load_g.wait()
        for part in BOTH:
            transpose_part(part, move_g(part))
    load_h = place.local("h", h_hbm, xn)
    load_h.start()
    look(0)
    with scope("f_cols"):
        labc[...] = columns(lab_ref[...] - row_start)
        for i, core in enumerate((c, 1 - c)):
            tokc_out[i] = columns(tokr[core, 0:1, :])
    x_run("00")
    pass_first()
    load_unit(1)
    look(1)
    x_run("10")
    pass_second(0)
    x_run("01")
    pass_first_far()
    load_unit(FAR)
    share_group(0)
    x_run("20")
    look(FAR)
    x_run("11 30 02")
    with scope("f_xn"):
        gain_out[...] = 1.0 + gain_sum.finish("dz")
        load_h.wait()
        lax.fori_loop(0, tok // r_step, xn_body, 0)
    x_run("21")
    pass_second(PAIR)
    with scope("f_xt"):
        for part in BOTH:
            for copy in move_g(part):
                copy.wait()
            transpose_part(part, move_xn(part))
    x_run("31 12")
    end_second(0)
    load_unit(3)
    look(3)
    x_run("22 03")
    pass_second(FAR)
    load_unit(4)
    share_group(PAIR)
    x_run("32 13")
    look(4)
    x_run("04")
    end_second(PAIR)
    end_second(FAR)
    load_unit(5)
    share_group(FAR)
    x_run("23 14")
    look(5)
    x_run("33 05")

    e_step = min(LANE, tok)

    def tile_of(j):
        return (c * n_half + j) % n_tile

    def load_tile(j):
        return place.local("et", et_out.at[tile_of(j)], etb.at[j % 4], j % 4, 4)

    def save_u(i, odd):
        return place.local(("u", odd), (z_even, z_odd)[odd].at[i % 2], u_hbm.at[tile_of(2 * i + odd)], i % 2)

    def lane_blocks():
        return [(b, pl.ds(b, LANE)) for b in range(0, vt, LANE)]

    def post_tile(i, odd):
        base = tile_of(2 * i + odd) * vt
        buf, slot = (z_even, z_odd)[odd], i % 2

        def body(e, carry):
            sel = span(e * e_step, e_step, e_step)
            ids = lax.broadcasted_iota(I32, (e_step, LANE), 1) + base
            sum_e, sum_l = acc_e[sel], acc_l[sel]
            for b, lanes in lane_blocks():
                tanh_z = jnp.tanh(buf[slot, sel, lanes] * (1.0 / SOFT_CAP))
                buf[slot, sel, lanes] = tanh_z
                sum_e = sum_e + jnp.exp(SOFT_CAP * tanh_z - SOFT_CAP)
                sum_l = sum_l + jnp.where(ids + b == labc[sel], tanh_z, 0.0)
            acc_e[sel] = sum_e
            acc_l[sel] = sum_l
            return carry

        lax.fori_loop(0, tok // e_step, body, 0)

    def dot_pair(i):
        for odd in BOTH:
            value = etb[(2 * i + odd) % 4].reshape(width, vt)
            (z_even, z_odd)[odd][i % 2] = jnp.dot(xn[...], value, preferred_element_type=F32)

    def load_pair(i):
        start_all(load_tile(2 * i + odd) for odd in BOTH)

    def pair(i, carry):
        for odd in BOTH:
            load_tile(2 * i + odd).wait()

        @pl.when(i > 1)
        def _():
            for odd in BOTH:
                save_u(i - 2, odd).wait()

        for odd in BOTH:
            post_tile(i - 1, odd)
            save_u(i - 1, odd).start()
        dot_pair(i)

        @pl.when(i + 2 < n_tile // 2)
        def _():
            load_pair(i + 2)

        for k, work in enumerate(during):
            @pl.when(i == k + 1)
            def _():
                x_run(work)
                if k == 0:
                    wait_shares()
        return carry

    def wait_shares():
        with scope("f_share"):
            for h in BOTH:
                for k2 in (0, PAIR, FAR):
                    share(h, k2).wait_recv()

    during = ("24", "15", "34", "25", "", "35")
    if n_half < 4:
        wait_shares()
        for work in during:
            x_run(work)
        during = ()
    acc_e[...] = jnp.zeros_like(acc_e)
    acc_l[...] = jnp.zeros_like(acc_l)
    with scope("f_logits0"):
        for i in BOTH:
            load_pair(i)
        for odd in BOTH:
            load_tile(odd).wait()
        dot_pair(0)
        if n_tile // 2 > 2:
            load_pair(2)
    last = n_tile // 2 - 1
    with scope("f_logits"):
        lax.fori_loop(1, last + 1, pair, 0)
        for odd in BOTH:
            post_tile(last, odd)
            save_u(last, odd).start()

    with scope("f_stats"):
        row = lax.broadcasted_iota(I32, (SUB, tok), 0)
        sum_e = jnp.sum(acc_e[...].T, axis=0, keepdims=True)
        sum_l = SOFT_CAP * jnp.sum(acc_l[...].T, axis=0, keepdims=True)
        stats = SmallSum(place, ("dx",), s_slots)
        stats.start("dx", jnp.where(row == 0, sum_e, sum_l))
    with scope("f_stats2"):
        stat = stats.finish("dx")
        all_e, all_l = stat[0:1], stat[1:2]
        inv_s[...] = jnp.broadcast_to((1.0 / dims["total"]) / all_e, (LANE, tok)).T
        s_slots[0, 0:1, :] = jnp.log(all_e) + SOFT_CAP - all_l
        own = s_slots[0, 0:1, lanes_of(0)]
        part_w = min(LANE, quarter)
        folded = own[:, 0:part_w]
        for j in range(part_w, quarter, part_w):
            folded = folded + own[:, j:j + part_w]
        loss_out[...] = jnp.where(lax.broadcasted_iota(I32, (SUB, part_w), 0) == 0, folded, 0.0)

    def dz_tile(j):
        return ((1 - c) * n_half + j) % n_tile

    def load_u(i, odd):
        return place.local(("u", odd), u_hbm.at[dz_tile(2 * i + odd)], (z_even, z_odd)[odd].at[i % 2], i % 2)

    def put_dz(i, odd):
        return place.local(("dz", odd), dzb.at[odd, i % 2], dz_out.at[dz_tile(2 * i + odd)], i % 2)

    def give_dz(part):
        src = dz_out.at[pl.ds((1 - c) * n_half + part * hh, hh)]
        return place.send(("dz", part), src, dzpar_out.at[pl.ds(part * hh, hh)], dc=1)

    d_step = min(256, tok)

    def dz_rows(i, odd):
        base = dz_tile(2 * i + odd) * vt
        buf, slot = (z_even, z_odd)[odd], i % 2

        def body(e, carry):
            sel = span(e * d_step, d_step, d_step)
            ids = lax.broadcasted_iota(I32, (d_step, LANE), 1) + base
            for b, lanes in lane_blocks():
                tanh_z = buf[slot, sel, lanes]
                prob = jnp.exp(SOFT_CAP * tanh_z - SOFT_CAP) * inv_s[sel]
                prob = jnp.where(ids + b == labc[sel], prob - 1.0 / dims["total"], prob)
                dzb[odd, slot, sel, lanes] = (prob * (1.0 - tanh_z * tanh_z)).astype(BF16)
            return carry

        lax.fori_loop(0, tok // d_step, body, 0)

    def dz_pair(i, carry):
        for odd in BOTH:
            load_u(i, odd).wait()

            @pl.when(i > hh + 1)
            def _():
                put_dz(i - 2, odd).wait()

            dz_rows(i, odd)
            put_dz(i, odd).start()

            @pl.when(i + 2 < n_tile // 2)
            def _():
                load_u(i + 2, odd).start()

        return carry

    with scope("f_dz"):
        for i in range(n_tile // 2 - 2, n_tile // 2):
            for odd in BOTH:
                save_u(i, odd).wait()
        for i in BOTH:
            start_all(load_u(i, odd) for odd in BOTH)
        for part in BOTH:
            lo, hi = part * hh // 2, (part + 1) * hh // 2
            lax.fori_loop(lo, hi, dz_pair, 0)
            for i in range(max(lo, hi - 2), hi):
                for odd in BOTH:
                    put_dz(i, odd).wait()
            give_dz(part).start()
        lax.fori_loop(hh, n_tile // 2, dz_pair, 0)

    with scope("f_end"):
        for part in BOTH:
            give_dz(part).wait()
        for i in range(n_tile // 2 - 2, n_tile // 2):
            for odd in BOTH:
                put_dz(i, odd).wait()
        give_tok.wait_send()
        give_chunk.wait_send()
        for h in BOTH:
            for i in BOTH:
                p1_send(h, i).wait_send()
                p1_fwd(h, i).wait_send()
                for k in (0, PAIR, FAR):
                    p2_send(h, k, i).wait_send()
                    p2_fwd(h, k, i).wait_send()
            for k in (0, PAIR, FAR):
                share(h, k).wait_send()
        for part in BOTH:
            for copy in move_xn(part):
                copy.wait()
        for u in range(len(UNITS)):
            if u > len(UNITS) - 3:
                x_swap(u).wait_send()
            x_keep(u).wait()
            for i in BOTH:
                x_far(u, i).wait_send()
                x_near(u, i).wait_send()
                x_put(u, i).wait_send()
                x_pass(u, i).wait()
    assert (place.n_link, place.n_local) <= dims["front_sems"], (place.n_link, place.n_local)


def specs(n_vmem, n_any):
    return [pl.BlockSpec(memory_space=pltpu.VMEM)] * n_vmem + [pl.BlockSpec(memory_space=pl.ANY)] * n_any


def shapes(items):
    return tuple(jax.ShapeDtypeStruct(*item) for item in items)


def scratch(items, n_link, n_local):
    dma = pltpu.SemaphoreType.DMA
    return [pltpu.VMEM(*item) for item in items] + [dma((n_link,)), dma((n_link,)), dma((n_local,))]


def params(collective_id, limit):
    return pltpu.CompilerParams(collective_id=collective_id, has_side_effects=True, vmem_limit_bytes=limit)


def front(dims, limit, shard, tok_row, lab_row, w, h, g):
    n, tok, vocab, width, vt = dims["n"], dims["tok"], dims["vocab"], dims["width"], dims["vt"]
    cols = shard.shape[0]
    half_v = vocab // CORES
    quarter = tok // n
    n_tile, n_half, n_block, most = vocab // vt, half_v // vt, dims["n_block"], max(PIECES)
    block = width // n_block
    pieces = n * n * CORES
    grid = (n // 2, 2, n // 2, 2)
    return pl.pallas_call(
        functools.partial(front_kernel, dims),
        name="front",
        out_shape=shapes([
            ((n_tile, *grid, CORES, cols, vt), BF16), *[((n_block, block, tok), BF16)] * 4, ((n_tile, tok, vt), BF16),
            ((n_half, tok, vt), BF16), ((n, pieces, cols, quarter), BF16), ((n_tile, tok, vt), F32),
            ((SUB, width), F32), ((SUB, min(LANE, quarter)), F32), ((CORES, tok, LANE), I32),
        ]),
        in_specs=specs(4, 2),
        out_specs=tuple(specs(0, 9) + specs(3, 0)),
        scratch_shapes=scratch([
            ((n_tile, cols, vt), BF16), ((CORES, n_half, cols, vt), BF16), ((CORES, SUB, tok), I32), ((half_v, CORES * tok), BF16),
            ((2, most, n_half, cols, vt), BF16), ((pieces, cols, tok), BF16), ((2, most, cols, tok), BF16), ((pieces, cols, tok), BF16),
            ((pieces, cols, quarter), BF16), ((2, pieces, cols, quarter), BF16), ((pieces, cols, quarter), BF16),
            ((4, *grid, CORES, cols, vt), BF16), ((tok, width), BF16), ((n_block, block, tok), BF16),
            ((2, tok, vt), F32), ((2, tok, vt), F32), ((2, 2, tok, vt), BF16), ((tok, LANE), F32), ((tok, LANE), F32), ((tok, LANE), F32),
            ((tok, LANE), I32), ((2 * n + CORES, SUB, width), F32), ((n, SUB, tok), F32),
        ], dims["front_sems"][0], dims["front_sems"][1]),
        compiler_params=params(0, limit),
    )(shard, tok_row, lab_row, w, h, g)


def back_kernel(
    dims,
    gain_ref, loss_ref, tokc, dz_hbm, dzp_hbm, et_hbm, xnt_hbm, xpar_hbm, gt_hbm, gpar_hbm, h_hbm,
    tail_out, dh_out, de_out, ra_hbm, rx_hbm,
    dz_own, dz_par, et_buf, part, fx, acc, fa, f2, r2, xb, h_buf, dh_buf, dg_acc, slots,
    sends, recvs, local_sems,
):
    n, tok, vocab, width, tile, per_chunk, vt = (dims[k] for k in ("n", "tok", "vocab", "width", "tile", "per_chunk", "vt"))
    place = Place(n, sends, recvs, local_sems)
    x, z, y, c = place.x, place.z, place.y, place.c
    half_v = vocab // CORES
    n_tile, n_half = vocab // vt, half_v // vt
    lanes = half_v // 2
    rows = width // (n * n)
    half_rows = rows // 2
    quarter = tok // n
    hq = quarter // 2
    chunks = width // (tile * per_chunk)
    per_half = n_half // 2

    with scope("b_enter"):
        place.enter()

    load_h = place.local("h", h_hbm.at[span(x * quarter, quarter, quarter)], h_buf)

    def load_et(t, slot):
        return place.local("et", et_hbm.at[:, span(t * tile, tile, tile)], et_buf.at[slot], slot)

    slot_of = {FAR: 0, 1: 1, 3: 2, 0: 0}
    stages = dims["stages"]

    def load_stage(m, i):
        half, k, kind = stages[m]
        src = ((gt_hbm, gpar_hbm), (xnt_hbm, xpar_hbm))[kind][i]
        src = src.at[(z + k) % n] if half == 0 else src.at[:, (y + k) % n]
        return place.local(("xb", i), src, xb.at[m % 2, i], m % 2)

    def start_stage(m):
        if m < len(stages):
            start_all(load_stage(m, i) for i in BOTH)

    for m in BOTH:
        start_stage(m)
    loads = [place.local("dz", dz_hbm, dz_own), place.local("dzp", dzp_hbm, dz_par)]
    load_et(0, 0).start()
    start_all(loads)
    load_h.start()

    def dxn_chunk(d):
        def body(i, carry):
            t = d * per_chunk + i
            slot = t % 2

            @pl.when(t + 1 < chunks * per_chunk)
            def _():
                load_et(t + 1, 1 - slot).start()

            load_et(t, slot).wait()
            left = jnp.concatenate([dz_own[j] for j in range(n_tile)], axis=1)
            right = jnp.concatenate([et_buf[slot, j] for j in range(n_tile)], axis=1)
            part[d, :, span(i * tile, tile, tile)] = lax.dot_general(
                left, right, (((1,), (1,)), ((), ())), preferred_element_type=F32)
            return carry

        with scope("b_dxn"):
            lax.fori_loop(0, per_chunk, body, 0)

    def qrow(k, lo=0, size=hq):
        return span((x + k) % n * quarter + lo, size, SUB)

    def x_far(d, i):
        return place.send(("xf", d, i), part.at[d, qrow(FAR, i * hq)], fx.at[d, i], dx=WAYS[i])

    def x_near(d, i, j):
        src = part.at[d, qrow(WAYS[i], j * hq)]
        return place.send(("xn", d, i, j), src, rx_hbm.at[d, i, pl.ds(j * hq, hq)], dx=WAYS[i])

    def x_first(d):
        start_all(x_far(d, i) for i in BOTH)

    def x_second(d):
        with scope("b_x2"):
            for i in BOTH:
                x_far(d, i).wait_recv()
                sel = qrow(WAYS[i], i * hq)
                part[d, sel] = part[d, sel] + fx[d, i]
                start_all(x_near(d, i, j) for j in BOTH)

    def stage_x(d, j, i):
        return place.local("sx", rx_hbm.at[d, i, pl.ds(j * hq, hq)], fx.at[d, i], i)

    def x_third(d, j):
        with scope("b_x3"):
            for i in BOTH:
                x_near(d, i, j).wait_recv()
                stage_x(d, j, i).start()
            for i in BOTH:
                stage_x(d, j, i).wait()
            sel = qrow(0, j * hq)
            part[d, sel] = part[d, sel] + fx[d, 0] + fx[d, 1]

    def de_stage(half, k, kind):
        m = stages.index((half, k, kind))
        slot = slot_of[k]

        def right(i, t):
            if kind:
                return dz_par[t] if i else dz_own[c * n_half + t]
            ids = lax.broadcasted_iota(I32, (tok, LANE), 1) + (x * vocab + c * half_v + t * vt)
            hits = [jnp.where(tokc[i] == ids + b, dims["scale"], 0.0).astype(BF16) for b in range(0, vt, LANE)]
            return jnp.concatenate(hits, axis=1)

        def body(j, carry):
            t = half * per_half + j
            sel = span(j * vt, vt)
            total = sum(jnp.dot(xb[m % 2, i].reshape(n * rows, tok), right(i, t), preferred_element_type=F32) for i in BOTH)
            total = total.reshape(n, rows, vt)
            acc[half, slot, :, :, sel] = acc[half, slot, :, :, sel] + total if kind else total
            return carry

        with scope("b_de" if kind else "b_look"):
            for i in BOTH:
                load_stage(m, i).wait()
            lax.fori_loop(0, per_half, body, 0)
            start_stage(m + 2)

    def de_unit(half, k):
        for kind in BOTH:
            de_stage(half, k, kind)

    def ring(half, k):
        return {"dz": k} if half == 0 else {"dy": k}

    def cross(half, k):
        return {"dy": k} if half == 0 else {"dz": k}

    def a_far(half, i):
        return place.send(("af", half, i), acc.at[half, 0, pl.ds(2 * i, 2)], fa.at[half, i], **ring(half, WAYS[i]))

    def a_near(half, i, j):
        sel = pl.ds(2 * j, 2)
        return place.send(("an", half, i, j), acc.at[half, 1 + i, sel], ra_hbm.at[half, i, sel], **ring(half, WAYS[i]))

    def a_first(half):
        start_all(a_far(half, i) for i in BOTH)

    def a_second(half, i):
        with scope("b_a2"):
            a_far(half, i).wait_recv()
            sel = pl.ds(2 * i, 2)
            acc[half, 1 + i, sel] = acc[half, 1 + i, sel] + fa[half, i]
            start_all(a_near(half, i, j) for j in BOTH)

    def stage_a(half, j, i):
        return place.local(("sa", half), ra_hbm.at[half, i, pl.ds(2 * j, 2)], fa.at[half, i], i)

    def piece(half, k):
        return ((y if half == 0 else z) + k) % n

    def c_far(half, i):
        src = acc.at[half, 0, piece(half, FAR), pl.ds(i * half_rows, half_rows)]
        return place.send(("cf", half, i), src, f2.at[half, i], **cross(half, WAYS[i]))

    def c_near(half, i):
        return place.send(("cn", half, i), acc.at[half, 0, piece(half, WAYS[i])], r2.at[half, i], **cross(half, WAYS[i]))

    def a_third(half, j):
        with scope("b_a3"):
            for i in BOTH:
                a_near(half, i, j).wait_recv()
                stage_a(half, j, i).start()
            for i in BOTH:
                stage_a(half, j, i).wait()
            sel = pl.ds(2 * j, 2)
            acc[half, 0, sel] = acc[half, 0, sel] + fa[half, 0] + fa[half, 1]

    def c_first(half):
        start_all(c_far(half, i) for i in BOTH)

    def c_second(half):
        with scope("b_c2"):
            for i in BOTH:
                c_far(half, i).wait_recv()
                at = piece(half, WAYS[i])
                sel = pl.ds(i * half_rows, half_rows)
                acc[half, 0, at, sel] = acc[half, 0, at, sel] + f2[half, i]
                c_near(half, i).start()

    def out_copies(half):
        sel = span(c * half_v + half * lanes, lanes)
        mine = acc.at[half, 0, piece(half, 0)]
        yield place.local("de", mine.at[span(c * half_rows, half_rows, SUB)], de_out.at[:, sel], half)
        yield place.send(("de", half), mine.at[span((1 - c) * half_rows, half_rows, SUB)], de_out.at[:, sel], dc=1)

    def c_third(half):
        with scope("b_c3"):
            for i in BOTH:
                c_near(half, i).wait_recv()
            at = piece(half, 0)
            acc[half, 0, at] = acc[half, 0, at] + r2[half, 0] + r2[half, 1]
            start_all(out_copies(half))

    with scope("b_load"):
        for copy in loads:
            copy.wait()
    dxn_chunk(0)
    x_first(0)
    for half in BOTH:
        de_unit(half, FAR)
        a_first(half)
    x_second(0)
    if chunks > 1:
        dxn_chunk(1)
        x_first(1)
    de_unit(0, 1)
    for d in range(2, chunks):
        dxn_chunk(d)
        x_first(d)
    a_second(0, 0)
    de_unit(0, 3)
    a_second(0, 1)
    if chunks > 1:
        x_second(1)
    de_unit(1, 1)
    a_second(1, 0)
    de_unit(1, 3)
    a_second(1, 1)
    for d in range(2, chunks):
        x_second(d)
    with scope("b_wait_far"):
        for half in BOTH:
            for i in BOTH:
                a_far(half, i).wait_send()
    for half in BOTH:
        de_unit(half, 0)

    step = min(32, hq)

    def dh_body(i, carry):
        sel = span(i * step, step, step)
        row = span(x * quarter + i * step, step, step)
        d_x = jnp.concatenate([part[d, row] for d in range(chunks)], axis=1)
        h_wide = h_buf[sel].astype(F32)
        inv_rms = lax.rsqrt(jnp.sum(h_wide * h_wide, axis=1, keepdims=True) * (1.0 / width) + NORM_EPS)
        h_norm = h_wide * inv_rms
        g_dir = d_x * gain_ref[0:1]
        mean = jnp.sum(g_dir * h_norm, axis=1, keepdims=True) * (1.0 / width)
        dh_buf[sel] = (inv_rms * (g_dir - h_norm * mean)).astype(BF16)
        prod = d_x * h_norm
        total = prod[0:SUB]
        for j in range(SUB, step, SUB):
            total = total + prod[j:j + SUB]
        dg_acc[...] = dg_acc[...] + total
        return carry

    def h_first(i, j):
        return place.send(("hf", i, j), dh_buf.at[pl.ds(j * hq, hq)], dh_out.at[qrow(0, j * hq)], dx=WAYS[i])

    def h_second(i):
        ref = dh_out.at[qrow(FROM[i], i * hq)]
        return place.send(("hs", i), ref, ref, dx=WAYS[i])

    dg_acc[...] = jnp.zeros_like(dg_acc)
    load_h.wait()
    per_j = hq // step
    for j in BOTH:
        for d in range(chunks):
            x_third(d, j)
        with scope("b_dh"):
            lax.fori_loop(j * per_j, (j + 1) * per_j, dh_body, 0)
            start_all(h_first(i, j) for i in BOTH)
    keep_dh = place.local("dh", dh_buf, dh_out.at[qrow(0, 0, quarter)])
    small = SmallSum(place, ("dc", "dx", "dy", "dz"), slots)
    small.start("dc", jnp.concatenate([dg_acc[...], loss_ref[...]], axis=1))
    keep_dh.start()
    with scope("b_s1"):
        small.start("dx", small.finish("dc"))
    for half in BOTH:
        for j in BOTH:
            a_third(half, j)
        c_first(half)
    with scope("b_h2"):
        for i in BOTH:
            h_first(i, i).wait_recv()
            h_second(i).start()
    with scope("b_s2"):
        small.start("dy", small.finish("dx"))
    for half in BOTH:
        c_second(half)
    with scope("b_s3"):
        small.start("dz", small.finish("dy"))
    for half in BOTH:
        c_third(half)
    with scope("b_s4"):
        total = jnp.sum(small.finish("dz"), axis=0, keepdims=True)
        loss = jnp.sum(total[:, width:], axis=1, keepdims=True) * (1.0 / dims["total"])
        tail_out[...] = jnp.concatenate([total[:, 0:width], jnp.broadcast_to(loss, (1, LANE))], axis=1)

    with scope("b_end_x"):
        keep_dh.wait()
        for i in BOTH:
            for d in range(chunks):
                x_far(d, i).wait_send()
                for j in BOTH:
                    x_near(d, i, j).wait_send()
            h_first(i, i).wait_send()
            h_first(i, 1 - i).wait()
            h_second(i).wait()
    with scope("b_end_a"):
        for half in BOTH:
            for i in BOTH:
                for j in BOTH:
                    a_near(half, i, j).wait_send()
                c_far(half, i).wait_send()
                c_near(half, i).wait_send()
            for copy in out_copies(half):
                copy.wait()
    assert (place.n_link, place.n_local) <= dims["back_sems"], (place.n_link, place.n_local)


def back(dims, limit, gain, loss, tokc, dz, dzp, et, xnt, xpar, gt, gpar, h):
    n, tok, vocab, width, tile, per_chunk = (dims[k] for k in ("n", "tok", "vocab", "width", "tile", "per_chunk"))
    rows = width // (n * n)
    half_v = vocab // CORES
    lanes = half_v // 2
    quarter = tok // n
    hq = quarter // 2
    chunk_w = tile * per_chunk
    chunks = width // chunk_w
    tail_w = width + loss.shape[1]
    n_tile, n_half, vt = dz.shape[0], dzp.shape[0], dims["vt"]
    turned = [a.reshape(n, n, rows, tok) for a in (xnt, xpar, gt, gpar)]
    return pl.pallas_call(
        functools.partial(back_kernel, dims),
        name="back",
        out_shape=shapes([
            ((1, width + LANE), F32), ((tok, width), BF16), ((rows // CORES, vocab), F32), ((2, 2, n, rows, lanes), F32),
            ((chunks, 2, quarter, chunk_w), F32),
        ]),
        in_specs=specs(3, 8),
        out_specs=tuple(specs(1, 4)),
        scratch_shapes=scratch([
            ((n_tile, tok, vt), BF16), ((n_half, tok, vt), BF16), ((2, n_tile, tile, vt), BF16), ((chunks, tok, chunk_w), F32),
            ((chunks, 2, hq, chunk_w), F32), ((2, 3, n, rows, lanes), F32), ((2, 2, 2, rows, lanes), F32),
            ((2, 2, rows // 2, lanes), F32), ((2, 2, rows, lanes), F32), ((2, CORES, n, rows, tok), BF16), ((quarter, width), BF16),
            ((quarter, width), BF16), ((SUB, width), F32), ((3 * n + CORES, SUB, tail_w), F32),
        ], dims["back_sems"][0], dims["back_sems"][1]),
        compiler_params=params(1, limit),
    )(gain, loss, tokc, dz, dzp, et.reshape(n_tile, width, vt), *turned, h)[:3]


def finish_kernel(n, scale, table_ref, tail_ref, x0_ref, dh_ref, de_ref, dg_out, loss_out, x0_out, dh_out, de_out, rows_ref):
    place = Place(n, None, None, None)
    cols = x0_ref.shape[2]
    for zi in range(n):
        for yi in range(n):
            for h in BOTH:
                dz, dy = (zi - place.z) % n, (yi - place.y) % n
                k1, k2 = (dy, dz) if h == 0 else (dz, dy)
                piece = table_ref[(h * n + k1) * n + k2]
                rows_ref[pl.ds(((zi * n + yi) * CORES + h) * cols, cols)] = x0_ref[0, piece]
    x0_out[...] = (rows_ref[...].T.astype(F32) * scale).astype(BF16)
    dh_out[...] = dh_ref[...]
    de_out[...] = de_ref[...]
    width = tail_ref.shape[1] - LANE
    gain = jnp.broadcast_to(tail_ref[:, 0:width], (SUB, width))
    dg_out[...] = pltpu.roll(gain, width - place.f * cols, axis=1)[0:1, 0:cols]
    loss_out[...] = tail_ref[:, width:width + 1]


def finish(n, scale, limit, tail, x0, dh, de):
    _, pieces, cols, quarter = x0.shape
    width = pieces * cols
    table = np.zeros((CORES, n, n), np.int32)
    for u, unit in enumerate(UNITS):
        for h in BOTH:
            for i, (k1, k2) in enumerate(unit):
                table[h, k1, k2] = BASE[u] + h * len(unit) + i
    row = pl.BlockSpec((quarter, width), lambda q, t: (q, 0))
    column = pl.BlockSpec((cols, de.shape[1] // n), lambda q, t: (0, q))
    dg, loss = (pl.BlockSpec((1, size), lambda q, t: (0, 0)) for size in (cols, 1))
    return pl.pallas_call(
        functools.partial(finish_kernel, n, scale),
        name="finish",
        grid_spec=pltpu.PrefetchScalarGridSpec(
            num_scalar_prefetch=1,
            grid=(n,),
            in_specs=[
                pl.BlockSpec(tail.shape, lambda q, t: (0, 0)),
                pl.BlockSpec((1, pieces, cols, quarter), lambda q, t: (q, 0, 0, 0)), row, column,
            ],
            out_specs=(dg, loss, row, row, column),
            scratch_shapes=[pltpu.VMEM((width, quarter), BF16)],
        ),
        out_shape=shapes([((1, cols), F32), ((1, 1), F32), (dh.shape, BF16), (dh.shape, BF16), (de.shape, F32)]),
        compiler_params=pltpu.CompilerParams(vmem_limit_bytes=limit),
    )(jnp.asarray(table.reshape(-1)), tail, x0, dh, de)


def solution(mesh):
    return build(mesh, mesh.shape["tp"], 256, 3, 256, 6, 67_000_000)


def build(mesh, n, tile, per_chunk, vt, n_block, limit):
    fsdp_size = mesh.shape["fsdp"]

    def device_step(emb_shard, tok_ids, lab_ids, h_last, g_embed, norm_w):
        vocab_rows, cols = emb_shard.shape
        batch_loc, seq_len, width = h_last.shape
        tok_count = batch_loc * seq_len
        fsdp_id = lax.axis_index("fsdp")
        scale = float(np.asarray(math.sqrt(width)).astype(jnp.bfloat16))
        dims = {
            "n": n, "tok": tok_count, "vocab": vocab_rows, "width": width, "total": tok_count * fsdp_size, "vt": vt,
            "tile": tile, "per_chunk": per_chunk, "scale": scale, "n_block": n_block,
            "stages": digits("020 021 120 121") + digits("010 011 030 031") + digits("110 111 130 131") + digits("000 001 100 101"),
            "front_sems": (110, 42), "back_sems": (56, 22),
        }
        h_flat = h_last.reshape(tok_count, width)
        placed = lax.dynamic_update_slice(jnp.zeros((SUB, width), F32), jnp.broadcast_to(norm_w, (SUB, cols)), (0, fsdp_id * cols))
        ids = [a.reshape(1, tok_count) for a in (tok_ids, lab_ids)]
        table, xn_t, xpar_t, g_t, gpar_t, dz, dzp, x0, _, gain, loss_part, tokc = front(
            dims, limit, emb_shard.T, *ids, norm_w.reshape(1, cols), h_flat, g_embed.reshape(tok_count, width))
        tail, d_hidden, d_cols = back(dims, limit, gain, loss_part, tokc, dz, dzp, table, xn_t, xpar_t, g_t, gpar_t, h_flat)
        d_norm_w, loss, x_emb, d_hidden, d_cols = finish(n, scale, limit, tail, x0, d_hidden, d_cols)
        return (x_emb.reshape(h_last.shape), loss.reshape(()), d_hidden.reshape(h_last.shape), d_norm_w.reshape(cols), d_cols.T)

    spec_tok = P("fsdp", None)
    spec_act = P("fsdp", None, None)
    return jax.shard_map(device_step, mesh=mesh, in_specs=(P("tp", "fsdp"), spec_tok, spec_tok, spec_act, spec_act, P("fsdp")), out_specs=(spec_act, P(), spec_act, P("fsdp"), P("tp", "fsdp")), check_vma=False)
```

```python
import functools
import math
import jax
import numpy as np
import jax.numpy as jnp
from jax import lax
from jax.experimental import pallas as pl
from jax.experimental.pallas import tpu as pltpu
from jax.sharding import PartitionSpec as P

SOFT_CAP = 30.0
NORM_EPS = 1e-6
F32, BF16, I32 = jnp.float32, jnp.bfloat16, jnp.int32
LANE, SUB = 128, 8
BOTH = (0, 1)
FOUR = range(4)
WAYS = (1, 3)
FROM = (3, 1)
FAR = 2
CORES = 2


def span(start, size, unit=LANE):
    return pl.ds(pl.multiple_of(start, unit), size)


class Place:
    def __init__(self, n, sends, recvs, local_sems):
        self.n, self.sends, self.recvs, self.local_sems = n, sends, recvs, local_sems
        self.x = lax.axis_index("tp")
        f = lax.axis_index("fsdp")
        self.f = f
        self.c = f % CORES
        self.y = f // CORES % n
        self.z = f // CORES // n
        self.link_of, self.local_of, self.n_link, self.n_local = {}, {}, 0, 0
        self.size = {"dx": n, "dz": n, "dy": n, "dc": CORES}
        self.me = {"dx": self.x, "dz": self.z, "dy": self.y, "dc": self.c}

    def at(self, dx=0, dz=0, dy=0, dc=0):
        n = self.n
        z, y, c = (self.z + dz) % n, (self.y + dy) % n, (self.c + dc) % CORES
        return ((self.x + dx) % n, (z * n + y) * CORES + c)

    def enter(self):
        barrier = pltpu.get_barrier_semaphore()
        peers = [self.at(**{d: k}) for d in self.size for k in range(1, self.size[d])]
        for peer in peers:
            pl.semaphore_signal(barrier, inc=1, device_id=peer, device_id_type=pl.DeviceIdType.MESH)
        pl.semaphore_wait(barrier, len(peers))

    def link(self, key, count=1):
        if key not in self.link_of:
            self.link_of[key] = self.n_link
            self.n_link += count
        return self.link_of[key]

    def send(self, key, src, dst, **step):
        i = self.link(key)
        return pltpu.make_async_remote_copy(
            src, dst, self.sends.at[i], self.recvs.at[i], device_id=self.at(**step), device_id_type=pl.DeviceIdType.MESH)

    def local(self, key, src, dst, slot=0, count=2):
        if key not in self.local_of:
            self.local_of[key] = self.n_local
            self.n_local += count
        return pltpu.make_async_copy(src, dst, self.local_sems.at[self.local_of[key] + slot])


class SmallSum:
    def __init__(self, place, dims, slots):
        self.place, self.slots, self.dims, self.base = place, slots, dims, {}
        count = 0
        for d in dims:
            self.base[d] = count
            count += place.size[d]

    def copies(self, d):
        slot = self.slots.at[self.base[d] + self.place.me[d]]
        for k in range(1, self.place.size[d]):
            yield self.place.send((self.dims, d, k), slot, slot, **{d: k})

    def start(self, d, value):
        self.slots[self.base[d] + self.place.me[d]] = value
        for copy in self.copies(d):
            copy.start()

    def finish(self, d):
        for copy in self.copies(d):
            copy.wait()
        total = self.slots[self.base[d]]
        for k in range(1, self.place.size[d]):
            total = total + self.slots[self.base[d] + k]
        return total


def scope(name):
    return jax.named_scope(name)


def start_all(copies):
    for copy in copies:
        copy.start()


def digits(text):
    return tuple(tuple(int(d) for d in word) for word in text.split())


UNITS = [digits(u) for u in ("00", "10 30", "01 03 20", "02 11 31", "13 33 21 23", "12 32 22")]
PAIR, ALL = 1, "all"
PIECES = [2 * len(u) for u in UNITS]
EXP_RATE = SOFT_CAP * math.log2(math.e)
BASE = [sum(PIECES[:i]) for i in range(len(UNITS))]


def front_kernel(
    dims,
    shard_ref, tok_ref, lab_ref, w_ref, h_hbm, g_hbm,
    et_out, xnt_out, xpar_out, gt_out, gpar_out, dz_out, dzpar_out, x0_out, u_hbm, gain_out, loss_out, tokc_out,
    shard_t, chunk, tokr, hit_t, lhs, xp, xo, xr, xf, xg, xq, etb, xn, gl, z_even, z_odd, dzb,
    acc_e, acc_l, inv_s, labc, w_slots, s_slots, sends, recvs, local_sems,
):
    n, tok, vocab, width, vt = dims["n"], dims["tok"], dims["vocab"], dims["width"], dims["vt"]
    place = Place(n, sends, recvs, local_sems)
    x, z, y, c = place.x, place.z, place.y, place.c
    half_v = vocab // CORES
    n_tile = vocab // vt
    n_half = n_tile // CORES
    hh = n_half // 2
    cols = width // (n * n * CORES)
    quarter = tok // n
    row_start = x * vocab

    def ring1(h, k):
        return {"dy": k} if h == 0 else {"dz": k}

    def ring2(h, k):
        return {"dz": k} if h == 0 else {"dy": k}

    def coord(base, k, paired):
        every = slice(None)
        if k == ALL:
            return every, every
        return every if paired else (base + k) % n // 2, (base + k) % 2

    def loc(h, k1, k2, lo=0, size=n_half, pair1=False, pair2=False):
        first, second = coord((y, z)[h], k1, pair1), coord((z, y)[h], k2, pair2)
        return et_out.at[(pl.ds(c * n_half + lo, size), *((second, first)[h]), *((first, second)[h]), h)]

    with scope("f_enter"):
        place.enter()

    load_g = place.local("g", g_hbm, xn)
    load_g.start()
    with scope("f_cast"):
        for t in range(n_tile):
            shard_t[t] = shard_ref[:, pl.ds(t * vt, vt)].astype(BF16)
        tokr[c] = jnp.broadcast_to(tok_ref[...], (SUB, tok))
        give_tok = place.send("tok", tokr.at[c], tokr.at[c], dc=1)
        give_chunk = place.send("chunk", shard_t.at[pl.ds((1 - c) * n_half, n_half)], chunk.at[c], dc=1)
        give_chunk.start()
        give_tok.start()
        chunk[c] = shard_t[pl.ds(c * n_half, n_half)]
        gain_sum = SmallSum(place, ("dc", "dy", "dz"), w_slots)
        own_w = jnp.concatenate([w_ref[...], jnp.zeros((1, width - cols), F32)], axis=1)
        gain_sum.start("dc", pltpu.roll(jnp.broadcast_to(own_w, (SUB, width)), place.f * cols, axis=1))

    def p1_send(h, i):
        return place.send(("p1", h, i), chunk.at[h], loc(h, 0, 0), **ring1(h, WAYS[i]))

    def p1_fwd(h, i):
        ref = loc(h, FROM[i], 0, i * hh, hh)
        return place.send(("p1f", h, i), ref, ref, **ring1(h, WAYS[i]))

    def p2_send(h, k1, i):
        ref = loc(h, k1, 0, pair1=k1 == PAIR)
        return place.send(("p2", h, k1, i), chunk.at[h] if k1 == 0 else ref, ref, **ring2(h, WAYS[i]))

    def p2_fwd(h, k1, i):
        ref = loc(h, k1, FROM[i], i * hh, hh, pair1=k1 == PAIR)
        return place.send(("p2f", h, k1, i), ref, ref, **ring2(h, WAYS[i]))

    def keep(h):
        return place.local("keep", chunk.at[h], loc(h, 0, 0), h)

    def share(h, k2):
        ref = loc(h, ALL, k2, pair2=k2 == PAIR)
        return place.send(("share", h, k2), ref, ref, dc=1)

    def pass_first():
        with scope("f_p1"):
            for h in BOTH:
                for i in BOTH:
                    p1_send(h, i).wait_recv()
                    p1_fwd(h, i).start()
            for h in BOTH:
                start_all(p2_send(h, PAIR, i) for i in BOTH)

    def pass_first_far():
        with scope("f_p1f"):
            for h in BOTH:
                for i in BOTH:
                    p1_fwd(h, i).wait_recv()
                start_all(p2_send(h, FAR, j) for j in BOTH)

    def pass_second(k1):
        with scope("f_p2"):
            for h in BOTH:
                for i in BOTH:
                    p2_send(h, k1, i).wait_recv()
                    p2_fwd(h, k1, i).start()

    def end_second(k1):
        with scope("f_p2f"):
            for h in BOTH:
                for i in BOTH:
                    p2_fwd(h, k1, i).wait_recv()

    def share_group(k2):
        start_all(share(h, k2) for h in BOTH)

    with scope("f_chunk"):
        give_chunk.wait_recv()
        start_all(keep(h) for h in BOTH)
        gain_sum.start("dy", gain_sum.finish("dc"))
        for h in BOTH:
            start_all(p1_send(h, i) for i in BOTH)
        for h in BOTH:
            start_all(p2_send(h, 0, i) for i in BOTH)

    v_step = min(LANE, half_v)

    def hit_body(j, carry):
        off = j * v_step
        ids = lax.broadcasted_iota(I32, (v_step, tok), 0) + (row_start + c * half_v + off)
        for i, core in enumerate((c, 1 - c)):
            hit_t[span(off, v_step, v_step), pl.ds(i * tok, tok)] = jnp.where(ids == tokr[core, 0:1, :], 1.0, 0.0).astype(BF16)
        return carry

    with scope("f_hit"):
        give_tok.wait_recv()
        lax.fori_loop(0, half_v // v_step, hit_body, 0)

    n_step = min(512, tok)
    most = max(PIECES)

    def whole(u):
        return pl.ds(BASE[u], PIECES[u])

    def unit_copies(u):
        slot = u % 2
        for p, (h, (k1, k2)) in enumerate((h, k) for h in BOTH for k in UNITS[u]):
            yield place.local("lhs", loc(h, k1, k2), lhs.at[slot, p], slot * most + p, 2 * most)

    def load_unit(u):
        start_all(unit_copies(u))

    def look(u):
        pieces = PIECES[u]
        with scope("f_look"):
            if u > 1:
                x_swap(u - 2).wait_send()
            left = lhs.at[u % 2]
            for copy in unit_copies(u):
                copy.wait()
            for i, dst in enumerate((xp.at[whole(u)], xo.at[u % 2])):
                def body(j, carry):
                    off = j * n_step
                    value = jnp.concatenate([left[pl.ds(0, pieces), t].reshape(pieces * cols, vt) for t in range(n_half)], axis=1)
                    rows = jnp.dot(value, hit_t[:, span(i * tok + off, n_step)], preferred_element_type=F32)
                    dst[pl.ds(0, pieces), :, span(off, n_step)] = rows.reshape(pieces, cols, n_step).astype(BF16)
                    return carry

                lax.fori_loop(0, tok // n_step, body, 0)
            x_swap(u).start()

    def x_swap(u):
        return place.send(("swap", u), xo.at[u % 2, pl.ds(0, PIECES[u])], xr.at[whole(u)], dc=1)

    def lanes_of(k):
        return span((x + k) % n * quarter, quarter, quarter)

    def side(u, i):
        return pl.ds(BASE[u] + i * len(UNITS[u]), len(UNITS[u]))

    def x_far(u, i):
        return place.send(("xf", u, i), xp.at[side(u, i), :, lanes_of(FAR)], xf.at[side(u, i)], dx=WAYS[i])

    def x_near(u, i):
        return place.send(("xn", u, i), xp.at[whole(u), :, lanes_of(WAYS[i])], xg.at[i, whole(u)], dx=WAYS[i])

    def x_goal(k, sel):
        return x0_out.at[(x + k) % n, sel]

    def x_put(u, i):
        return place.send(("xp", u, i), xq.at[whole(u)], x_goal(0, whole(u)), dx=WAYS[i])

    def x_keep(u):
        return place.local("x0", xq.at[whole(u)], x_goal(0, whole(u)), u, len(UNITS))

    def x_pass(u, i):
        ref = x_goal(FROM[i], side(u, i))
        return place.send(("xs", u, i), ref, ref, dx=WAYS[i])

    def x_first(u):
        with scope("f_x1"):
            x_swap(u).wait_recv()
            for p in range(BASE[u], BASE[u] + PIECES[u]):
                xp[p] = xp[p] + xr[p]
            start_all(x_far(u, i) for i in BOTH)

    def x_second(u):
        with scope("f_x2"):
            for i in BOTH:
                x_far(u, i).wait_recv()
                sel, lanes = side(u, i), lanes_of(WAYS[i])
                xp[sel, :, lanes] = xp[sel, :, lanes] + xf[sel]
                x_near(u, i).start()

    def x_third(u):
        with scope("f_x3"):
            for i in BOTH:
                x_near(u, i).wait_recv()
            sel = whole(u)
            xq[sel] = xp[sel, :, lanes_of(0)] + xg[0, sel] + xg[1, sel]
            start_all(x_put(u, i) for i in BOTH)
            x_keep(u).start()

    def x_fourth(u):
        with scope("f_x4"):
            for i in BOTH:
                x_put(u, i).wait_recv()
                x_pass(u, i).start()

    block = width // dims["n_block"]

    def transpose_block(j):
        return xn[:, pl.ds(j * block, block)].T

    n_block = dims["n_block"]
    early = n_block // 2

    def moves(key, part, whole, other):
        sel = pl.ds(part * early, early)
        yield place.local(key, gl.at[sel], whole.at[sel], part)
        yield place.send((key, part), gl.at[sel], other.at[sel], dc=1)

    def move_g(part):
        return moves("g", part, gt_out, gpar_out)

    def move_xn(part):
        return moves("xt", part, xnt_out, xpar_out)

    def transpose_part(part, copies):
        for j in range(part * early, (part + 1) * early):
            gl[j] = transpose_block(j)
        start_all(copies)

    def columns(row):
        return jnp.broadcast_to(row.astype(F32), (LANE, tok)).T.astype(I32)

    r_step = min(LANE, tok)

    def xn_body(j, carry):
        sel = span(j * r_step, r_step, r_step)
        h_wide = xn[sel].astype(F32)
        inv_rms = lax.rsqrt(jnp.sum(h_wide * h_wide, axis=1, keepdims=True) * (1.0 / width) + NORM_EPS)
        xn[sel] = (h_wide * inv_rms * gain_out[0:1]).astype(BF16)
        return carry

    x_steps = (x_first, x_second, x_third, x_fourth)

    def x_run(work):
        for step, u in digits(work):
            x_steps[step](u)

    with scope("f_keep"):
        for h in BOTH:
            keep(h).wait()
        load_unit(0)
    with scope("f_gt"):
        load_g.wait()
        for part in BOTH:
            transpose_part(part, move_g(part))
    load_h = place.local("h", h_hbm, xn)
    load_h.start()
    look(0)
    pass_first()
    load_unit(1)
    with scope("f_cols"):
        labc[...] = columns(lab_ref[...] - row_start)
        for i, core in enumerate((c, 1 - c)):
            tokc_out[i] = columns(tokr[core, 0:1, :])
    with scope("f_gain2"):
        gain_sum.start("dz", gain_sum.finish("dy"))
    x_run("00")
    look(1)
    pass_second(0)
    pass_first_far()
    load_unit(FAR)
    share_group(0)
    x_run("10 01")
    look(FAR)
    x_run("20 11")
    with scope("f_xn"):
        gain_out[...] = 1.0 + gain_sum.finish("dz")
        load_h.wait()
        lax.fori_loop(0, tok // r_step, xn_body, 0)
    pass_second(PAIR)
    end_second(0)
    load_unit(3)
    with scope("f_xt"):
        for part in BOTH:
            for copy in move_g(part):
                copy.wait()
            transpose_part(part, move_xn(part))
    x_run("30 02 21")
    look(3)
    pass_second(FAR)
    load_unit(4)
    share_group(PAIR)
    x_run("12 31 03")
    look(4)
    end_second(PAIR)
    end_second(FAR)
    load_unit(5)
    share_group(FAR)
    x_run("22 13 04")
    look(5)
    x_run("14 23 05")

    e_step = min(LANE, tok)

    def tile_of(j):
        return (c * n_half + j) % n_tile

    def load_tile(j):
        return place.local("et", et_out.at[tile_of(j)], etb.at[j % 4], j % 4, 4)

    def save_u(i, odd):
        return place.local(("u", odd), (z_even, z_odd)[odd].at[i % 2], u_hbm.at[tile_of(2 * i + odd)], i % 2)

    def lane_blocks():
        return [(b, pl.ds(b, LANE)) for b in range(0, vt, LANE)]

    def post_tile(i, odd):
        base = tile_of(2 * i + odd) * vt
        buf, slot = (z_even, z_odd)[odd], i % 2

        def body(e, carry):
            sel = span(e * e_step, e_step, e_step)
            ids = lax.broadcasted_iota(I32, (e_step, LANE), 1) + base
            sum_e, sum_l = acc_e[sel], acc_l[sel]
            for b, lanes in lane_blocks():
                tanh_z = jnp.tanh(buf[slot, sel, lanes] * (1.0 / SOFT_CAP))
                buf[slot, sel, lanes] = tanh_z
                sum_e = sum_e + jnp.exp2(EXP_RATE * tanh_z - EXP_RATE)
                sum_l = sum_l + jnp.where(ids + b == labc[sel], tanh_z, 0.0)
            acc_e[sel] = sum_e
            acc_l[sel] = sum_l
            return carry

        lax.fori_loop(0, tok // e_step, body, 0)

    def dot_pair(i):
        for odd in BOTH:
            value = etb[(2 * i + odd) % 4].reshape(width, vt)
            (z_even, z_odd)[odd][i % 2] = jnp.dot(xn[...], value, preferred_element_type=F32)

    def load_pair(i):
        start_all(load_tile(2 * i + odd) for odd in BOTH)

    def pair(i, carry):
        for odd in BOTH:
            load_tile(2 * i + odd).wait()

        @pl.when(i > 1)
        def _():
            for odd in BOTH:
                save_u(i - 2, odd).wait()

        for odd in BOTH:
            post_tile(i - 1, odd)
            save_u(i - 1, odd).start()
        dot_pair(i)

        @pl.when(i + 2 < n_tile // 2)
        def _():
            load_pair(i + 2)

        for k, work in enumerate(during):
            @pl.when(i == k + 1)
            def _():
                x_run(work)
                if k == 0:
                    wait_shares()
        return carry

    def wait_shares():
        with scope("f_share"):
            for h in BOTH:
                for k2 in (0, PAIR, FAR):
                    share(h, k2).wait_recv()

    during = ("32 15", "24", "33", "25", "34", "35")
    if n_half < 4:
        wait_shares()
        for work in during:
            x_run(work)
        during = ()
    acc_e[...] = jnp.zeros_like(acc_e)
    acc_l[...] = jnp.zeros_like(acc_l)
    with scope("f_logits0"):
        for i in BOTH:
            load_pair(i)
        for odd in BOTH:
            load_tile(odd).wait()
        dot_pair(0)
        if n_tile // 2 > 2:
            load_pair(2)
    last = n_tile // 2 - 1
    with scope("f_logits"):
        lax.fori_loop(1, last + 1, pair, 0)
        for odd in BOTH:
            post_tile(last, odd)
            save_u(last, odd).start()

    with scope("f_stats"):
        row = lax.broadcasted_iota(I32, (SUB, tok), 0)
        sum_e = jnp.sum(acc_e[...].T, axis=0, keepdims=True)
        sum_l = SOFT_CAP * jnp.sum(acc_l[...].T, axis=0, keepdims=True)
        stats = SmallSum(place, ("dx",), s_slots)
        stats.start("dx", jnp.where(row == 0, sum_e, sum_l))
    with scope("f_stats2"):
        stat = stats.finish("dx")
        all_e, all_l = stat[0:1], stat[1:2]
        inv_s[...] = jnp.broadcast_to((1.0 / dims["total"]) / all_e, (LANE, tok)).T
        s_slots[0, 0:1, :] = jnp.log(all_e) + SOFT_CAP - all_l
        own = s_slots[0, 0:1, lanes_of(0)]
        part_w = min(LANE, quarter)
        folded = own[:, 0:part_w]
        for j in range(part_w, quarter, part_w):
            folded = folded + own[:, j:j + part_w]
        loss_out[...] = jnp.where(lax.broadcasted_iota(I32, (SUB, part_w), 0) == 0, folded, 0.0)

    def dz_tile(j):
        return ((1 - c) * n_half + j) % n_tile

    def load_u(i, odd):
        return place.local(("u", odd), u_hbm.at[dz_tile(2 * i + odd)], (z_even, z_odd)[odd].at[i % 2], i % 2)

    def put_dz(i, odd):
        return place.local(("dz", odd), dzb.at[odd, i % 2], dz_out.at[dz_tile(2 * i + odd)], i % 2)

    def give_dz(part):
        src = dz_out.at[pl.ds((1 - c) * n_half + part * hh, hh)]
        return place.send(("dz", part), src, dzpar_out.at[pl.ds(part * hh, hh)], dc=1)

    d_step = min(256, tok)

    def dz_rows(i, odd):
        base = dz_tile(2 * i + odd) * vt
        buf, slot = (z_even, z_odd)[odd], i % 2

        def body(e, carry):
            sel = span(e * d_step, d_step, d_step)
            ids = lax.broadcasted_iota(I32, (d_step, LANE), 1) + base
            for b, lanes in lane_blocks():
                tanh_z = buf[slot, sel, lanes]
                prob = jnp.exp2(EXP_RATE * tanh_z - EXP_RATE) * inv_s[sel]
                prob = jnp.where(ids + b == labc[sel], prob - 1.0 / dims["total"], prob)
                dzb[odd, slot, sel, lanes] = (prob * (1.0 - tanh_z * tanh_z)).astype(BF16)
            return carry

        lax.fori_loop(0, tok // d_step, body, 0)

    def dz_pair(i, carry):
        for odd in BOTH:
            load_u(i, odd).wait()

            @pl.when(i > hh + 1)
            def _():
                put_dz(i - 2, odd).wait()

            dz_rows(i, odd)
            put_dz(i, odd).start()

            @pl.when(i + 2 < n_tile // 2)
            def _():
                load_u(i + 2, odd).start()

        return carry

    with scope("f_dz"):
        for i in range(n_tile // 2 - 2, n_tile // 2):
            for odd in BOTH:
                save_u(i, odd).wait()
        for i in BOTH:
            start_all(load_u(i, odd) for odd in BOTH)
        for part in BOTH:
            lo, hi = part * hh // 2, (part + 1) * hh // 2
            lax.fori_loop(lo, hi, dz_pair, 0)
            for i in range(max(lo, hi - 2), hi):
                for odd in BOTH:
                    put_dz(i, odd).wait()
            give_dz(part).start()
        lax.fori_loop(hh, n_tile // 2, dz_pair, 0)

    with scope("f_end"):
        for part in BOTH:
            give_dz(part).wait()
        for i in range(n_tile // 2 - 2, n_tile // 2):
            for odd in BOTH:
                put_dz(i, odd).wait()
        give_tok.wait_send()
        give_chunk.wait_send()
        for h in BOTH:
            for i in BOTH:
                p1_send(h, i).wait_send()
                p1_fwd(h, i).wait_send()
                for k in (0, PAIR, FAR):
                    p2_send(h, k, i).wait_send()
                    p2_fwd(h, k, i).wait_send()
            for k in (0, PAIR, FAR):
                share(h, k).wait_send()
        for part in BOTH:
            for copy in move_xn(part):
                copy.wait()
        for u in range(len(UNITS)):
            if u > len(UNITS) - 3:
                x_swap(u).wait_send()
            x_keep(u).wait()
            for i in BOTH:
                x_far(u, i).wait_send()
                x_near(u, i).wait_send()
                x_put(u, i).wait_send()
                x_pass(u, i).wait()
    assert (place.n_link, place.n_local) <= dims["front_sems"], (place.n_link, place.n_local)


def specs(n_vmem, n_any):
    return [pl.BlockSpec(memory_space=pltpu.VMEM)] * n_vmem + [pl.BlockSpec(memory_space=pl.ANY)] * n_any


def shapes(items):
    return tuple(jax.ShapeDtypeStruct(*item) for item in items)


def scratch(items, n_link, n_local):
    dma = pltpu.SemaphoreType.DMA
    return [pltpu.VMEM(*item) for item in items] + [dma((n_link,)), dma((n_link,)), dma((n_local,))]


def params(collective_id, limit):
    return pltpu.CompilerParams(collective_id=collective_id, has_side_effects=True, vmem_limit_bytes=limit)


def front(dims, limit, shard, tok_row, lab_row, w, h, g):
    n, tok, vocab, width, vt = dims["n"], dims["tok"], dims["vocab"], dims["width"], dims["vt"]
    cols = shard.shape[0]
    half_v = vocab // CORES
    quarter = tok // n
    n_tile, n_half, n_block, most = vocab // vt, half_v // vt, dims["n_block"], max(PIECES)
    block = width // n_block
    pieces = n * n * CORES
    grid = (n // 2, 2, n // 2, 2)
    return pl.pallas_call(
        functools.partial(front_kernel, dims),
        name="front",
        out_shape=shapes([
            ((n_tile, *grid, CORES, cols, vt), BF16), *[((n_block, block, tok), BF16)] * 4, ((n_tile, tok, vt), BF16),
            ((n_half, tok, vt), BF16), ((n, pieces, cols, quarter), BF16), ((n_tile, tok, vt), F32),
            ((SUB, width), F32), ((SUB, min(LANE, quarter)), F32), ((CORES, tok, LANE), I32),
        ]),
        in_specs=specs(4, 2),
        out_specs=tuple(specs(0, 9) + specs(3, 0)),
        scratch_shapes=scratch([
            ((n_tile, cols, vt), BF16), ((CORES, n_half, cols, vt), BF16), ((CORES, SUB, tok), I32), ((half_v, CORES * tok), BF16),
            ((2, most, n_half, cols, vt), BF16), ((pieces, cols, tok), BF16), ((2, most, cols, tok), BF16), ((pieces, cols, tok), BF16),
            ((pieces, cols, quarter), BF16), ((2, pieces, cols, quarter), BF16), ((pieces, cols, quarter), BF16),
            ((4, *grid, CORES, cols, vt), BF16), ((tok, width), BF16), ((n_block, block, tok), BF16),
            ((2, tok, vt), F32), ((2, tok, vt), F32), ((2, 2, tok, vt), BF16), ((tok, LANE), F32), ((tok, LANE), F32), ((tok, LANE), F32),
            ((tok, LANE), I32), ((2 * n + CORES, SUB, width), F32), ((n, SUB, tok), F32),
        ], dims["front_sems"][0], dims["front_sems"][1]),
        compiler_params=params(0, limit),
    )(shard, tok_row, lab_row, w, h, g)


def back_kernel(
    dims,
    gain_ref, loss_ref, tokc, dz_hbm, dzp_hbm, et_hbm, xnt_hbm, xpar_hbm, gt_hbm, gpar_hbm, h_hbm,
    tail_out, dh_out, de_out, ra_hbm, rx_hbm,
    dz_own, dz_par, et_buf, part, fx, acc, fa, f2, r2, xb, h_buf, dh_buf, dg_acc, slots,
    sends, recvs, local_sems,
):
    n, tok, vocab, width, tile, per_chunk, vt = (dims[k] for k in ("n", "tok", "vocab", "width", "tile", "per_chunk", "vt"))
    place = Place(n, sends, recvs, local_sems)
    x, z, y, c = place.x, place.z, place.y, place.c
    half_v = vocab // CORES
    n_tile, n_half = vocab // vt, half_v // vt
    lanes = half_v // 2
    rows = width // (n * n)
    half_rows = rows // 2
    quarter = tok // n
    hq = quarter // 2
    chunks = width // (tile * per_chunk)
    per_half = n_half // 2

    with scope("b_enter"):
        place.enter()

    load_h = place.local("h", h_hbm.at[span(x * quarter, quarter, quarter)], h_buf)

    def load_et(t, slot):
        return place.local("et", et_hbm.at[:, span(t * tile, tile, tile)], et_buf.at[slot], slot)

    slot_of = {FAR: 0, 1: 1, 3: 2, 0: 0}
    stages = dims["stages"]

    def load_stage(m, i):
        half, k, kind = stages[m]
        src = ((gt_hbm, gpar_hbm), (xnt_hbm, xpar_hbm))[kind][i]
        src = src.at[(z + k) % n] if half == 0 else src.at[:, (y + k) % n]
        return place.local(("xb", i), src, xb.at[m % 2, i], m % 2)

    def start_stage(m):
        if m < len(stages):
            start_all(load_stage(m, i) for i in BOTH)

    loads = [place.local("dz", dz_hbm, dz_own), place.local("dzp", dzp_hbm, dz_par)]
    load_et(0, 0).start()
    start_all(loads)
    for m in BOTH:
        start_stage(m)
    load_h.start()

    def dxn_chunk(d):
        def body(i, carry):
            t = d * per_chunk + i
            slot = t % 2

            @pl.when(t + 1 < chunks * per_chunk)
            def _():
                load_et(t + 1, 1 - slot).start()

            load_et(t, slot).wait()
            left = jnp.concatenate([dz_own[j] for j in range(n_tile)], axis=1)
            right = jnp.concatenate([et_buf[slot, j] for j in range(n_tile)], axis=1)
            part[d, :, span(i * tile, tile, tile)] = lax.dot_general(
                left, right, (((1,), (1,)), ((), ())), preferred_element_type=F32)
            return carry

        with scope("b_dxn"):
            lax.fori_loop(0, per_chunk, body, 0)

    def qrow(k, lo=0, size=hq):
        return span((x + k) % n * quarter + lo, size, SUB)

    def x_far(d, i):
        return place.send(("xf", d, i), part.at[d, qrow(FAR, i * hq)], fx.at[d, i], dx=WAYS[i])

    def x_near(d, i, j):
        src = part.at[d, qrow(WAYS[i], j * hq)]
        return place.send(("xn", d, i, j), src, rx_hbm.at[d, i, pl.ds(j * hq, hq)], dx=WAYS[i])

    def x_first(d):
        start_all(x_far(d, i) for i in BOTH)

    def x_second(d):
        with scope("b_x2"):
            for i in BOTH:
                x_far(d, i).wait_recv()
                sel = qrow(WAYS[i], i * hq)
                part[d, sel] = part[d, sel] + fx[d, i]
                start_all(x_near(d, i, j) for j in BOTH)

    def stage_x(d, j, i):
        return place.local("sx", rx_hbm.at[d, i, pl.ds(j * hq, hq)], fx.at[d, i], i)

    def x_third(d, j):
        with scope("b_x3"):
            for i in BOTH:
                x_near(d, i, j).wait_recv()
                stage_x(d, j, i).start()
            for i in BOTH:
                stage_x(d, j, i).wait()
            sel = qrow(0, j * hq)
            part[d, sel] = part[d, sel] + fx[d, 0] + fx[d, 1]

    def de_stage(half, k, kind):
        m = stages.index((half, k, kind))
        slot = slot_of[k]

        wide = min(2, per_half)

        def right(i, t):
            if kind:
                return dz_par[t] if i else dz_own[c * n_half + t]
            ids = lax.broadcasted_iota(I32, (tok, LANE), 1) + (x * vocab + c * half_v + t * vt)
            hits = [jnp.where(tokc[i] == ids + b, dims["scale"], 0.0).astype(BF16) for b in range(0, vt, LANE)]
            return jnp.concatenate(hits, axis=1)

        def body(j, carry):
            t = half * per_half + j * wide
            sel = span(j * wide * vt, wide * vt)
            left = jnp.concatenate([xb[m % 2, i].reshape(n * rows, tok) for i in BOTH], axis=1)
            both_right = [jnp.concatenate([right(i, t + q) for i in BOTH], axis=0) for q in range(wide)]
            total = jnp.dot(left, jnp.concatenate(both_right, axis=1), preferred_element_type=F32)
            total = total.reshape(n, rows, wide * vt)
            acc[half, slot, :, :, sel] = acc[half, slot, :, :, sel] + total if kind else total
            return carry

        with scope("b_de" if kind else "b_look"):
            for i in BOTH:
                load_stage(m, i).wait()
            lax.fori_loop(0, per_half // wide, body, 0)
            start_stage(m + 2)

    def de_unit(half, k):
        for kind in BOTH:
            de_stage(half, k, kind)

    def ring(half, k):
        return {"dz": k} if half == 0 else {"dy": k}

    def cross(half, k):
        return {"dy": k} if half == 0 else {"dz": k}

    def a_far(half, i):
        return place.send(("af", half, i), acc.at[half, 0, pl.ds(2 * i, 2)], fa.at[half, i], **ring(half, WAYS[i]))

    def a_near(half, i, j):
        sel = pl.ds(2 * j, 2)
        return place.send(("an", half, i, j), acc.at[half, 1 + i, sel], ra_hbm.at[half, i, sel], **ring(half, WAYS[i]))

    def a_first(half):
        start_all(a_far(half, i) for i in BOTH)

    def a_second(half, i):
        with scope("b_a2"):
            a_far(half, i).wait_recv()
            sel = pl.ds(2 * i, 2)
            acc[half, 1 + i, sel] = acc[half, 1 + i, sel] + fa[half, i]
            start_all(a_near(half, i, j) for j in BOTH)

    def stage_a(half, j, i):
        return place.local(("sa", half), ra_hbm.at[half, i, pl.ds(2 * j, 2)], fa.at[half, i], i)

    def piece(half, k):
        return ((y if half == 0 else z) + k) % n

    def c_far(half, i):
        src = acc.at[half, 0, piece(half, FAR), pl.ds(i * half_rows, half_rows)]
        return place.send(("cf", half, i), src, f2.at[half, i], **cross(half, WAYS[i]))

    def c_near(half, i):
        return place.send(("cn", half, i), acc.at[half, 0, piece(half, WAYS[i])], r2.at[half, i], **cross(half, WAYS[i]))

    def a_third(half, j):
        with scope("b_a3"):
            for i in BOTH:
                a_near(half, i, j).wait_recv()
                stage_a(half, j, i).start()
            for i in BOTH:
                stage_a(half, j, i).wait()
            sel = pl.ds(2 * j, 2)
            acc[half, 0, sel] = acc[half, 0, sel] + fa[half, 0] + fa[half, 1]

    def c_first(half):
        start_all(c_far(half, i) for i in BOTH)

    def c_second(half):
        with scope("b_c2"):
            for i in BOTH:
                c_far(half, i).wait_recv()
                at = piece(half, WAYS[i])
                sel = pl.ds(i * half_rows, half_rows)
                acc[half, 0, at, sel] = acc[half, 0, at, sel] + f2[half, i]
                c_near(half, i).start()

    def out_copies(half):
        sel = span(c * half_v + half * lanes, lanes)
        mine = acc.at[half, 0, piece(half, 0)]
        yield place.local("de", mine.at[span(c * half_rows, half_rows, SUB)], de_out.at[:, sel], half)
        yield place.send(("de", half), mine.at[span((1 - c) * half_rows, half_rows, SUB)], de_out.at[:, sel], dc=1)

    def c_third(half):
        with scope("b_c3"):
            for i in BOTH:
                c_near(half, i).wait_recv()
            at = piece(half, 0)
            acc[half, 0, at] = acc[half, 0, at] + r2[half, 0] + r2[half, 1]
            start_all(out_copies(half))

    with scope("b_load"):
        loads[0].wait()
    dxn_chunk(0)
    x_first(0)
    loads[1].wait()
    for half in BOTH:
        de_unit(half, FAR)
        a_first(half)
    x_second(0)
    if chunks > 1:
        dxn_chunk(1)
        x_first(1)
    de_unit(0, 1)
    for d in range(2, chunks):
        dxn_chunk(d)
        x_first(d)
    a_second(0, 0)
    de_unit(0, 3)
    a_second(0, 1)
    if chunks > 1:
        x_second(1)
    de_unit(1, 1)
    a_second(1, 0)
    de_unit(1, 3)
    a_second(1, 1)
    for d in range(2, chunks):
        x_second(d)
    with scope("b_wait_far"):
        for half in BOTH:
            for i in BOTH:
                a_far(half, i).wait_send()
    for half in BOTH:
        de_unit(half, 0)

    step = min(32, hq)

    def dh_body(i, carry):
        sel = span(i * step, step, step)
        row = span(x * quarter + i * step, step, step)
        d_x = jnp.concatenate([part[d, row] for d in range(chunks)], axis=1)
        h_wide = h_buf[sel].astype(F32)
        inv_rms = lax.rsqrt(jnp.sum(h_wide * h_wide, axis=1, keepdims=True) * (1.0 / width) + NORM_EPS)
        h_norm = h_wide * inv_rms
        g_dir = d_x * gain_ref[0:1]
        mean = jnp.sum(g_dir * h_norm, axis=1, keepdims=True) * (1.0 / width)
        dh_buf[sel] = (inv_rms * (g_dir - h_norm * mean)).astype(BF16)
        prod = d_x * h_norm
        total = prod[0:SUB]
        for j in range(SUB, step, SUB):
            total = total + prod[j:j + SUB]
        dg_acc[...] = dg_acc[...] + total
        return carry

    def h_first(i, j):
        return place.send(("hf", i, j), dh_buf.at[pl.ds(j * hq, hq)], dh_out.at[qrow(0, j * hq)], dx=WAYS[i])

    def h_second(i):
        ref = dh_out.at[qrow(FROM[i], i * hq)]
        return place.send(("hs", i), ref, ref, dx=WAYS[i])

    dg_acc[...] = jnp.zeros_like(dg_acc)
    load_h.wait()
    per_j = hq // step
    for j in BOTH:
        for d in range(chunks):
            x_third(d, j)
        with scope("b_dh"):
            lax.fori_loop(j * per_j, (j + 1) * per_j, dh_body, 0)
            start_all(h_first(i, j) for i in BOTH)
    keep_dh = place.local("dh", dh_buf, dh_out.at[qrow(0, 0, quarter)])
    small = SmallSum(place, ("dc", "dx", "dy", "dz"), slots)
    small.start("dc", jnp.concatenate([dg_acc[...], loss_ref[...]], axis=1))
    keep_dh.start()
    with scope("b_s1"):
        small.start("dx", small.finish("dc"))
    for half in BOTH:
        for j in BOTH:
            a_third(half, j)
        c_first(half)
    with scope("b_h2"):
        for i in BOTH:
            h_first(i, i).wait_recv()
            h_second(i).start()
    with scope("b_s2"):
        small.start("dy", small.finish("dx"))
    for half in BOTH:
        c_second(half)
    with scope("b_s3"):
        small.start("dz", small.finish("dy"))
    for half in BOTH:
        c_third(half)
    with scope("b_s4"):
        total = jnp.sum(small.finish("dz"), axis=0, keepdims=True)
        loss = jnp.sum(total[:, width:], axis=1, keepdims=True) * (1.0 / dims["total"])
        tail_out[...] = jnp.concatenate([total[:, 0:width], jnp.broadcast_to(loss, (1, LANE))], axis=1)

    with scope("b_end_x"):
        keep_dh.wait()
        for i in BOTH:
            for d in range(chunks):
                x_far(d, i).wait_send()
                for j in BOTH:
                    x_near(d, i, j).wait_send()
            h_first(i, i).wait_send()
            h_first(i, 1 - i).wait()
            h_second(i).wait()
    with scope("b_end_a"):
        for half in BOTH:
            for i in BOTH:
                for j in BOTH:
                    a_near(half, i, j).wait_send()
                c_far(half, i).wait_send()
                c_near(half, i).wait_send()
            for copy in out_copies(half):
                copy.wait()
    assert (place.n_link, place.n_local) <= dims["back_sems"], (place.n_link, place.n_local)


def back(dims, limit, gain, loss, tokc, dz, dzp, et, xnt, xpar, gt, gpar, h):
    n, tok, vocab, width, tile, per_chunk = (dims[k] for k in ("n", "tok", "vocab", "width", "tile", "per_chunk"))
    rows = width // (n * n)
    half_v = vocab // CORES
    lanes = half_v // 2
    quarter = tok // n
    hq = quarter // 2
    chunk_w = tile * per_chunk
    chunks = width // chunk_w
    tail_w = width + loss.shape[1]
    n_tile, n_half, vt = dz.shape[0], dzp.shape[0], dims["vt"]
    turned = [a.reshape(n, n, rows, tok) for a in (xnt, xpar, gt, gpar)]
    return pl.pallas_call(
        functools.partial(back_kernel, dims),
        name="back",
        out_shape=shapes([
            ((1, width + LANE), F32), ((tok, width), BF16), ((rows // CORES, vocab), F32), ((2, 2, n, rows, lanes), F32),
            ((chunks, 2, quarter, chunk_w), F32),
        ]),
        in_specs=specs(3, 8),
        out_specs=tuple(specs(1, 4)),
        scratch_shapes=scratch([
            ((n_tile, tok, vt), BF16), ((n_half, tok, vt), BF16), ((2, n_tile, tile, vt), BF16), ((chunks, tok, chunk_w), F32),
            ((chunks, 2, hq, chunk_w), F32), ((2, 3, n, rows, lanes), F32), ((2, 2, 2, rows, lanes), F32),
            ((2, 2, rows // 2, lanes), F32), ((2, 2, rows, lanes), F32), ((2, CORES, n, rows, tok), BF16), ((quarter, width), BF16),
            ((quarter, width), BF16), ((SUB, width), F32), ((3 * n + CORES, SUB, tail_w), F32),
        ], dims["back_sems"][0], dims["back_sems"][1]),
        compiler_params=params(1, limit),
    )(gain, loss, tokc, dz, dzp, et.reshape(n_tile, width, vt), *turned, h)[:3]


def finish_kernel(n, scale, table_ref, tail_ref, x0_ref, dh_ref, de_ref, dg_out, loss_out, x0_out, dh_out, de_out, rows_ref):
    place = Place(n, None, None, None)
    cols, width, part_w = x0_ref.shape[2], tail_ref.shape[1] - LANE, x0_out.shape[1]
    part = pl.program_id(1)
    for zi in range(n // 2):
        for yi in range(n):
            for h in BOTH:
                dz, dy = (part * (n // 2) + zi - place.z) % n, (yi - place.y) % n
                k1, k2 = (dy, dz) if h == 0 else (dz, dy)
                piece = table_ref[(h * n + k1) * n + k2]
                rows_ref[pl.ds(((zi * n + yi) * CORES + h) * cols, cols)] = x0_ref[0, piece]
    x0_out[...] = (rows_ref[...].T.astype(F32) * scale).astype(BF16)
    dh_out[...] = dh_ref[...]
    de_out[...] = de_ref[...]
    gain = jnp.broadcast_to(tail_ref[:, 0:width], (SUB, width))
    dg_out[...] = pltpu.roll(gain, width - place.f * cols, axis=1)[0:1, 0:cols]
    loss_out[...] = tail_ref[:, width:width + 1]


def finish(n, scale, limit, tail, x0, dh, de):
    _, pieces, cols, quarter = x0.shape
    width = pieces * cols
    table = np.zeros((CORES, n, n), np.int32)
    for u, unit in enumerate(UNITS):
        for h in BOTH:
            for i, (k1, k2) in enumerate(unit):
                table[h, k1, k2] = BASE[u] + h * len(unit) + i
    row = pl.BlockSpec((quarter // 2, width), lambda q, p, t: (2 * q + p, 0))
    block = pl.BlockSpec((quarter, width // 2), lambda q, p, t: (q, p))
    column = pl.BlockSpec((cols, de.shape[1] // (2 * n)), lambda q, p, t: (0, 2 * q + p))
    dg, loss = (pl.BlockSpec((1, size), lambda q, p, t: (0, 0)) for size in (cols, 1))
    return pl.pallas_call(
        functools.partial(finish_kernel, n, scale),
        name="finish",
        grid_spec=pltpu.PrefetchScalarGridSpec(
            num_scalar_prefetch=1,
            grid=(n, 2),
            in_specs=[
                pl.BlockSpec(tail.shape, lambda q, p, t: (0, 0)),
                pl.BlockSpec((1, pieces, cols, quarter), lambda q, p, t: (q, 0, 0, 0)), row, column,
            ],
            out_specs=(dg, loss, block, row, column),
            scratch_shapes=[pltpu.VMEM((width // 2, quarter), BF16)],
        ),
        out_shape=shapes([((1, cols), F32), ((1, 1), F32), (dh.shape, BF16), (dh.shape, BF16), (de.shape, F32)]),
        compiler_params=pltpu.CompilerParams(vmem_limit_bytes=limit),
    )(jnp.asarray(table.reshape(-1)), tail, x0, dh, de)


def solution(mesh):
    return build(mesh, mesh.shape["tp"], 256, 3, 256, 6, 67_000_000)


def build(mesh, n, tile, per_chunk, vt, n_block, limit):
    fsdp_size = mesh.shape["fsdp"]

    def device_step(emb_shard, tok_ids, lab_ids, h_last, g_embed, norm_w):
        vocab_rows, cols = emb_shard.shape
        batch_loc, seq_len, width = h_last.shape
        tok_count = batch_loc * seq_len
        fsdp_id = lax.axis_index("fsdp")
        scale = float(np.asarray(math.sqrt(width)).astype(jnp.bfloat16))
        dims = {
            "n": n, "tok": tok_count, "vocab": vocab_rows, "width": width, "total": tok_count * fsdp_size, "vt": vt,
            "tile": tile, "per_chunk": per_chunk, "scale": scale, "n_block": n_block,
            "stages": digits("020 021 120 121") + digits("010 011 030 031") + digits("110 111 130 131") + digits("000 001 100 101"),
            "front_sems": (110, 42), "back_sems": (56, 22),
        }
        h_flat = h_last.reshape(tok_count, width)
        placed = lax.dynamic_update_slice(jnp.zeros((SUB, width), F32), jnp.broadcast_to(norm_w, (SUB, cols)), (0, fsdp_id * cols))
        ids = [a.reshape(1, tok_count) for a in (tok_ids, lab_ids)]
        table, xn_t, xpar_t, g_t, gpar_t, dz, dzp, x0, _, gain, loss_part, tokc = front(
            dims, limit, emb_shard.T, *ids, norm_w.reshape(1, cols), h_flat, g_embed.reshape(tok_count, width))
        tail, d_hidden, d_cols = back(dims, limit, gain, loss_part, tokc, dz, dzp, table, xn_t, xpar_t, g_t, gpar_t, h_flat)
        d_norm_w, loss, x_emb, d_hidden, d_cols = finish(n, scale, limit, tail, x0, d_hidden, d_cols)
        return (x_emb.reshape(h_last.shape), loss.reshape(()), d_hidden.reshape(h_last.shape), d_norm_w.reshape(cols), d_cols.T)

    spec_tok = P("fsdp", None)
    spec_act = P("fsdp", None, None)
    return jax.shard_map(device_step, mesh=mesh, in_specs=(P("tp", "fsdp"), spec_tok, spec_tok, spec_act, spec_act, P("fsdp")), out_specs=(spec_act, P(), spec_act, P("fsdp"), P("tp", "fsdp")), check_vma=False)
```

```python
import functools
import math
import jax
import numpy as np
import jax.numpy as jnp
from jax import lax
from jax.experimental import pallas as pl
from jax.experimental.pallas import tpu as pltpu
from jax.sharding import PartitionSpec as P

SOFT_CAP = 30.0
NORM_EPS = 1e-6
F32, BF16, I32 = jnp.float32, jnp.bfloat16, jnp.int32
LANE, SUB = 128, 8
BOTH = (0, 1)
FOUR = range(4)
WAYS = (1, 3)
FROM = (3, 1)
FAR = 2
CORES = 2


def span(start, size, unit=LANE):
    return pl.ds(pl.multiple_of(start, unit), size)


class Place:
    def __init__(self, n, sends, recvs, local_sems):
        self.n, self.sends, self.recvs, self.local_sems = n, sends, recvs, local_sems
        self.x = lax.axis_index("tp")
        f = lax.axis_index("fsdp")
        self.f = f
        self.c = f % CORES
        self.y = f // CORES % n
        self.z = f // CORES // n
        self.link_of, self.local_of, self.n_link, self.n_local = {}, {}, 0, 0
        self.size = {"dx": n, "dz": n, "dy": n, "dc": CORES}
        self.me = {"dx": self.x, "dz": self.z, "dy": self.y, "dc": self.c}

    def at(self, dx=0, dz=0, dy=0, dc=0):
        n = self.n
        z, y, c = (self.z + dz) % n, (self.y + dy) % n, (self.c + dc) % CORES
        return ((self.x + dx) % n, (z * n + y) * CORES + c)

    def enter(self):
        barrier = pltpu.get_barrier_semaphore()
        peers = [self.at(**{d: k}) for d in self.size for k in range(1, self.size[d])]
        for peer in peers:
            pl.semaphore_signal(barrier, inc=1, device_id=peer, device_id_type=pl.DeviceIdType.MESH)
        pl.semaphore_wait(barrier, len(peers))

    def link(self, key, count=1):
        if key not in self.link_of:
            self.link_of[key] = self.n_link
            self.n_link += count
        return self.link_of[key]

    def send(self, key, src, dst, **step):
        i = self.link(key)
        return pltpu.make_async_remote_copy(
            src, dst, self.sends.at[i], self.recvs.at[i], device_id=self.at(**step), device_id_type=pl.DeviceIdType.MESH)

    def local(self, key, src, dst, slot=0, count=2):
        if key not in self.local_of:
            self.local_of[key] = self.n_local
            self.n_local += count
        return pltpu.make_async_copy(src, dst, self.local_sems.at[self.local_of[key] + slot])


class SmallSum:
    def __init__(self, place, dims, slots):
        self.place, self.slots, self.dims, self.base = place, slots, dims, {}
        count = 0
        for d in dims:
            self.base[d] = count
            count += place.size[d]

    def copies(self, d):
        slot = self.slots.at[self.base[d] + self.place.me[d]]
        for k in range(1, self.place.size[d]):
            yield self.place.send((self.dims, d, k), slot, slot, **{d: k})

    def start(self, d, value):
        self.slots[self.base[d] + self.place.me[d]] = value
        for copy in self.copies(d):
            copy.start()

    def finish(self, d):
        for copy in self.copies(d):
            copy.wait()
        total = self.slots[self.base[d]]
        for k in range(1, self.place.size[d]):
            total = total + self.slots[self.base[d] + k]
        return total


def scope(name):
    return jax.named_scope(name)


def start_all(copies):
    for copy in copies:
        copy.start()


def digits(text):
    return tuple(tuple(int(d) for d in word) for word in text.split())


UNITS = [digits(u) for u in ("00", "10 30", "01 03 20", "02 11 31", "13 33 21 23", "12 32 22")]
PAIR, ALL = 1, "all"
PIECES = [2 * len(u) for u in UNITS]
EXP_RATE = SOFT_CAP * math.log2(math.e)
BASE = [sum(PIECES[:i]) for i in range(len(UNITS))]


def front_kernel(
    dims,
    shard_ref, tok_ref, lab_ref, w_ref, h_hbm, g_hbm,
    et_out, xnt_out, xpar_out, gt_out, gpar_out, dz_out, dzpar_out, x0_out, u_hbm, gain_out, loss_out, tokc_out,
    shard_t, chunk, tokr, hit_t, lhs, xp, xw, xr, xf, xg, xq, etb, xn, gl, z_even, z_odd, dzb,
    acc_e, acc_l, inv_s, labc, w_slots, s_slots, sends, recvs, local_sems,
):
    n, tok, vocab, width, vt = dims["n"], dims["tok"], dims["vocab"], dims["width"], dims["vt"]
    place = Place(n, sends, recvs, local_sems)
    x, z, y, c = place.x, place.z, place.y, place.c
    half_v = vocab // CORES
    n_tile = vocab // vt
    n_half = n_tile // CORES
    hh = n_half // 2
    cols = width // (n * n * CORES)
    quarter = tok // n
    row_start = x * vocab

    def ring1(h, k):
        return {"dy": k} if h == 0 else {"dz": k}

    def ring2(h, k):
        return {"dz": k} if h == 0 else {"dy": k}

    def coord(base, k, paired):
        every = slice(None)
        if k == ALL:
            return every, every
        return every if paired else (base + k) % n // 2, (base + k) % 2

    def loc(h, k1, k2, lo=0, size=n_half, pair1=False, pair2=False):
        first, second = coord((y, z)[h], k1, pair1), coord((z, y)[h], k2, pair2)
        return et_out.at[(pl.ds(c * n_half + lo, size), *((second, first)[h]), *((first, second)[h]), h)]

    with scope("f_enter"):
        place.enter()

    load_g = place.local("g", g_hbm, xn)
    load_g.start()
    with scope("f_cast"):
        for t in range(n_tile):
            shard_t[t] = shard_ref[:, pl.ds(t * vt, vt)].astype(BF16)
        tokr[c] = jnp.broadcast_to(tok_ref[...], (SUB, tok))
        give_tok = place.send("tok", tokr.at[c], tokr.at[c], dc=1)
        give_chunk = place.send("chunk", shard_t.at[pl.ds((1 - c) * n_half, n_half)], chunk.at[c], dc=1)
        give_chunk.start()
        give_tok.start()
        chunk[c] = shard_t[pl.ds(c * n_half, n_half)]
        gain_sum = SmallSum(place, ("dc", "dy", "dz"), w_slots)
        own_w = jnp.concatenate([w_ref[...], jnp.zeros((1, width - cols), F32)], axis=1)
        gain_sum.start("dc", pltpu.roll(jnp.broadcast_to(own_w, (SUB, width)), place.f * cols, axis=1)[0:1])

    def p1_send(h, i):
        return place.send(("p1", h, i), chunk.at[h], loc(h, 0, 0), **ring1(h, WAYS[i]))

    def p1_fwd(h, i):
        ref = loc(h, FROM[i], 0, i * hh, hh)
        return place.send(("p1f", h, i), ref, ref, **ring1(h, WAYS[i]))

    def p2_send(h, k1, i):
        ref = loc(h, k1, 0, pair1=k1 == PAIR)
        return place.send(("p2", h, k1, i), chunk.at[h] if k1 == 0 else ref, ref, **ring2(h, WAYS[i]))

    def p2_fwd(h, k1, i):
        ref = loc(h, k1, FROM[i], i * hh, hh, pair1=k1 == PAIR)
        return place.send(("p2f", h, k1, i), ref, ref, **ring2(h, WAYS[i]))

    def keep(h):
        return place.local("keep", chunk.at[h], loc(h, 0, 0), h)

    def share(h, k2):
        ref = loc(h, ALL, k2, pair2=k2 == PAIR)
        return place.send(("share", h, k2), ref, ref, dc=1)

    def pass_first():
        with scope("f_p1"):
            for h in BOTH:
                for i in BOTH:
                    p1_send(h, i).wait_recv()
                    p1_fwd(h, i).start()
            for h in BOTH:
                start_all(p2_send(h, PAIR, i) for i in BOTH)

    def pass_first_far():
        with scope("f_p1f"):
            for h in BOTH:
                for i in BOTH:
                    p1_fwd(h, i).wait_recv()
                start_all(p2_send(h, FAR, j) for j in BOTH)

    def pass_second(k1):
        with scope("f_p2"):
            for h in BOTH:
                for i in BOTH:
                    p2_send(h, k1, i).wait_recv()
                    p2_fwd(h, k1, i).start()

    def end_second(k1):
        with scope("f_p2f"):
            for h in BOTH:
                for i in BOTH:
                    p2_fwd(h, k1, i).wait_recv()

    def share_group(k2):
        start_all(share(h, k2) for h in BOTH)

    with scope("f_chunk"):
        give_chunk.wait_recv()
        start_all(keep(h) for h in BOTH)
        gain_sum.start("dy", gain_sum.finish("dc"))
        for h in BOTH:
            start_all(p1_send(h, i) for i in BOTH)
        for h in BOTH:
            start_all(p2_send(h, 0, i) for i in BOTH)

    v_step = min(LANE, half_v)

    def hit_body(j, carry):
        off = j * v_step
        ids = lax.broadcasted_iota(I32, (v_step, tok), 0) + (row_start + c * half_v + off)
        for i, core in enumerate((c, 1 - c)):
            hit_t[span(off, v_step, v_step), pl.ds(i * tok, tok)] = jnp.where(ids == tokr[core, 0:1, :], 1.0, 0.0).astype(BF16)
        return carry

    with scope("f_hit"):
        give_tok.wait_recv()
        lax.fori_loop(0, half_v // v_step, hit_body, 0)

    n_step = min(512, tok)
    most = max(PIECES)

    def whole(u):
        return pl.ds(BASE[u], PIECES[u])

    def unit_copies(u):
        slot = u % 2
        for p, (h, (k1, k2)) in enumerate((h, k) for h in BOTH for k in UNITS[u]):
            yield place.local("lhs", loc(h, k1, k2), lhs.at[slot, p], slot * most + p, 2 * most)

    def load_unit(u):
        start_all(unit_copies(u))

    def look(u):
        pieces = PIECES[u]
        with scope("f_look"):
            if u > 1:
                x_swap(u - 2).wait_send()
            left = lhs.at[u % 2]
            for copy in unit_copies(u):
                copy.wait()
            per_core = tok // n_step

            def body(j, carry):
                value = jnp.concatenate([left[pl.ds(0, pieces), t].reshape(pieces * cols, vt) for t in range(n_half)], axis=1)
                rows = jnp.dot(value, hit_t[:, span(j * n_step, n_step)], preferred_element_type=F32)
                rows = rows.reshape(pieces, cols, n_step).astype(BF16)
                xw[u % 2, j // per_core, pl.ds(0, pieces), :, span(j % per_core * n_step, n_step)] = rows
                return carry

            lax.fori_loop(0, CORES * per_core, body, 0)
            x_swap(u).start()

    def x_swap(u):
        return place.send(("swap", u), xw.at[u % 2, 1, pl.ds(0, PIECES[u])], xr.at[whole(u)], dc=1)

    def lanes_of(k):
        return span((x + k) % n * quarter, quarter, quarter)

    def side(u, i):
        return pl.ds(BASE[u] + i * len(UNITS[u]), len(UNITS[u]))

    def x_far(u, i):
        return place.send(("xf", u, i), xp.at[side(u, i), :, lanes_of(FAR)], xf.at[side(u, i)], dx=WAYS[i])

    def x_near(u, i):
        return place.send(("xn", u, i), xp.at[whole(u), :, lanes_of(WAYS[i])], xg.at[i, whole(u)], dx=WAYS[i])

    def x_goal(k, sel):
        return x0_out.at[(x + k) % n, sel]

    def x_put(u, i):
        return place.send(("xp", u, i), xq.at[whole(u)], x_goal(0, whole(u)), dx=WAYS[i])

    def x_keep(u):
        return place.local("x0", xq.at[whole(u)], x_goal(0, whole(u)), u, len(UNITS))

    def x_pass(u, i):
        ref = x_goal(FROM[i], side(u, i))
        return place.send(("xs", u, i), ref, ref, dx=WAYS[i])

    def x_first(u):
        with scope("f_x1"):
            x_swap(u).wait_recv()
            def body(p, carry):
                xp[BASE[u] + p] = xw[u % 2, 0, p] + xr[BASE[u] + p]
                return carry

            lax.fori_loop(0, PIECES[u], body, 0)
            start_all(x_far(u, i) for i in BOTH)

    def x_second(u):
        with scope("f_x2"):
            for i in BOTH:
                x_far(u, i).wait_recv()
                sel, lanes = side(u, i), lanes_of(WAYS[i])
                xp[sel, :, lanes] = xp[sel, :, lanes] + xf[sel]
                x_near(u, i).start()

    def x_third(u):
        with scope("f_x3"):
            for i in BOTH:
                x_near(u, i).wait_recv()
            sel = whole(u)
            xq[sel] = xp[sel, :, lanes_of(0)] + xg[0, sel] + xg[1, sel]
            start_all(x_put(u, i) for i in BOTH)
            x_keep(u).start()

    def x_fourth(u):
        with scope("f_x4"):
            for i in BOTH:
                x_put(u, i).wait_recv()
                x_pass(u, i).start()

    block = width // dims["n_block"]

    def transpose_block(j):
        return xn[:, pl.ds(j * block, block)].T

    n_block = dims["n_block"]
    early = n_block // 2

    def moves(key, part, whole, other):
        sel = pl.ds(part * early, early)
        yield place.local(key, gl.at[sel], whole.at[sel], part)
        yield place.send((key, part), gl.at[sel], other.at[sel], dc=1)

    def move_g(part):
        return moves("g", part, gt_out, gpar_out)

    def move_xn(part):
        return moves("xt", part, xnt_out, xpar_out)

    def transpose_part(part, copies):
        for j in range(part * early, (part + 1) * early):
            gl[j] = transpose_block(j)
        start_all(copies)

    def columns(row):
        return jnp.broadcast_to(row.astype(F32), (LANE, tok)).T.astype(I32)

    r_step = min(LANE, tok)

    def xn_body(j, carry):
        sel = span(j * r_step, r_step, r_step)
        h_wide = xn[sel].astype(F32)
        inv_rms = lax.rsqrt(jnp.sum(h_wide * h_wide, axis=1, keepdims=True) * (1.0 / width) + NORM_EPS)
        xn[sel] = (h_wide * inv_rms * gain_out[0:1]).astype(BF16)
        return carry

    x_steps = (x_first, x_second, x_third, x_fourth)

    def x_run(work):
        for step, u in digits(work):
            x_steps[step](u)

    with scope("f_keep"):
        for h in BOTH:
            keep(h).wait()
        load_unit(0)
    with scope("f_gt"):
        load_g.wait()
        for part in BOTH:
            transpose_part(part, move_g(part))
    load_h = place.local("h", h_hbm, xn)
    load_h.start()
    look(0)
    with scope("f_cols"):
        labc[...] = columns(lab_ref[...] - row_start)
        for i, core in enumerate((c, 1 - c)):
            tokc_out[i] = columns(tokr[core, 0:1, :])
    with scope("f_gain2"):
        gain_sum.start("dz", gain_sum.finish("dy"))
    x_run("00")
    pass_first()
    load_unit(1)
    look(1)
    x_run("10")
    pass_second(0)
    pass_first_far()
    load_unit(FAR)
    share_group(0)
    x_run("01")
    look(FAR)
    x_run("20 11")
    pass_second(PAIR)
    x_run("02")
    end_second(0)
    load_unit(3)
    x_run("30 21")
    look(3)
    x_run("12")
    pass_second(FAR)
    load_unit(4)
    share_group(PAIR)
    with scope("f_xn"):
        gain_out[...] = 1.0 + gain_sum.finish("dz")
        load_h.wait()
        lax.fori_loop(0, tok // r_step, xn_body, 0)
    with scope("f_xt"):
        for part in BOTH:
            for copy in move_g(part):
                copy.wait()
            transpose_part(part, move_xn(part))
    x_run("31 03")
    look(4)
    x_run("22")
    end_second(PAIR)
    end_second(FAR)
    load_unit(5)
    share_group(FAR)
    x_run("04")
    look(5)
    x_run("13 05")

    e_step = min(LANE, tok)

    def tile_of(j):
        return (c * n_half + j) % n_tile

    def load_tile(j):
        return place.local("et", et_out.at[tile_of(j)], etb.at[j % 4], j % 4, 4)

    def save_u(i, odd):
        return place.local(("u", odd), (z_even, z_odd)[odd].at[i % 2], u_hbm.at[tile_of(2 * i + odd)], i % 2)

    def lane_blocks():
        return [(b, pl.ds(b, LANE)) for b in range(0, vt, LANE)]

    def post_tile(i, odd):
        base = tile_of(2 * i + odd) * vt
        buf, slot = (z_even, z_odd)[odd], i % 2

        def body(e, carry):
            sel = span(e * e_step, e_step, e_step)
            ids = lax.broadcasted_iota(I32, (e_step, LANE), 1) + base
            sum_e, sum_l = acc_e[sel], acc_l[sel]
            for b, lanes in lane_blocks():
                tanh_z = jnp.tanh(buf[slot, sel, lanes] * (1.0 / SOFT_CAP))
                buf[slot, sel, lanes] = tanh_z
                sum_e = sum_e + jnp.exp2(EXP_RATE * tanh_z - EXP_RATE)
                sum_l = sum_l + jnp.where(ids + b == labc[sel], tanh_z, 0.0)
            acc_e[sel] = sum_e
            acc_l[sel] = sum_l
            return carry

        lax.fori_loop(0, tok // e_step, body, 0)

    def dot_pair(i):
        for odd in BOTH:
            value = etb[(2 * i + odd) % 4].reshape(width, vt)
            (z_even, z_odd)[odd][i % 2] = jnp.dot(xn[...], value, preferred_element_type=F32)

    def load_pair(i):
        start_all(load_tile(2 * i + odd) for odd in BOTH)

    def pair(i, carry):
        for odd in BOTH:
            load_tile(2 * i + odd).wait()

        @pl.when(i > 1)
        def _():
            for odd in BOTH:
                save_u(i - 2, odd).wait()

        for odd in BOTH:
            post_tile(i - 1, odd)
            save_u(i - 1, odd).start()
        dot_pair(i)

        @pl.when(i + 2 < n_tile // 2)
        def _():
            load_pair(i + 2)

        for k, work in enumerate(during):
            @pl.when(i == k + 1)
            def _():
                x_run(work)
                if k == 0:
                    wait_shares()
        return carry

    def wait_shares():
        with scope("f_share"):
            for h in BOTH:
                for k2 in (0, PAIR, FAR):
                    share(h, k2).wait_recv()

    during = ("14 32", "23 15", "24", "33", "25", "34")
    if n_half < 4:
        wait_shares()
        for work in during:
            x_run(work)
        during = ()
    acc_e[...] = jnp.zeros_like(acc_e)
    acc_l[...] = jnp.zeros_like(acc_l)
    with scope("f_logits0"):
        for i in BOTH:
            load_pair(i)
        for odd in BOTH:
            load_tile(odd).wait()
        dot_pair(0)
        if n_tile // 2 > 2:
            load_pair(2)
    last = n_tile // 2 - 1
    with scope("f_logits"):
        lax.fori_loop(1, last + 1, pair, 0)
        for odd in BOTH:
            post_tile(last, odd)
            save_u(last, odd).start()

    with scope("f_stats"):
        row = lax.broadcasted_iota(I32, (2, tok), 0)
        sum_e = jnp.sum(acc_e[...].T, axis=0, keepdims=True)
        sum_l = SOFT_CAP * jnp.sum(acc_l[...].T, axis=0, keepdims=True)
        stats = SmallSum(place, ("dx",), s_slots)
        stats.start("dx", jnp.where(row == 0, sum_e, sum_l))
    x_run("35")
    with scope("f_stats2"):
        stat = stats.finish("dx")
        all_e, all_l = stat[0:1], stat[1:2]
        inv_s[...] = jnp.broadcast_to((1.0 / dims["total"]) / all_e, (LANE, tok)).T
        s_slots[0, 0:1, :] = jnp.log(all_e) + SOFT_CAP - all_l
        own = s_slots[0, 0:1, lanes_of(0)]
        part_w = min(LANE, quarter)
        folded = own[:, 0:part_w]
        for j in range(part_w, quarter, part_w):
            folded = folded + own[:, j:j + part_w]
        loss_out[...] = jnp.where(lax.broadcasted_iota(I32, (SUB, part_w), 0) == 0, folded, 0.0)

    def dz_tile(j):
        return ((1 - c) * n_half + j) % n_tile

    def load_u(i, odd):
        return place.local(("u", odd), u_hbm.at[dz_tile(2 * i + odd)], (z_even, z_odd)[odd].at[i % 2], i % 2)

    def put_dz(i, odd):
        return place.local(("dz", odd), dzb.at[odd, i % 2], dz_out.at[dz_tile(2 * i + odd)], i % 2)

    def give_dz(part):
        src = dz_out.at[pl.ds((1 - c) * n_half + part * hh, hh)]
        return place.send(("dz", part), src, dzpar_out.at[pl.ds(part * hh, hh)], dc=1)

    d_step = min(256, tok)

    def dz_rows(i, odd):
        base = dz_tile(2 * i + odd) * vt
        buf, slot = (z_even, z_odd)[odd], i % 2

        def body(e, carry):
            sel = span(e * d_step, d_step, d_step)
            ids = lax.broadcasted_iota(I32, (d_step, LANE), 1) + base
            for b, lanes in lane_blocks():
                tanh_z = buf[slot, sel, lanes]
                prob = jnp.exp2(EXP_RATE * tanh_z - EXP_RATE) * inv_s[sel]
                prob = jnp.where(ids + b == labc[sel], prob - 1.0 / dims["total"], prob)
                dzb[odd, slot, sel, lanes] = (prob * (1.0 - tanh_z * tanh_z)).astype(BF16)
            return carry

        lax.fori_loop(0, tok // d_step, body, 0)

    def dz_pair(i, carry):
        for odd in BOTH:
            load_u(i, odd).wait()

            @pl.when(i > hh + 1)
            def _():
                put_dz(i - 2, odd).wait()

            dz_rows(i, odd)
            put_dz(i, odd).start()

            @pl.when(i + 2 < n_tile // 2)
            def _():
                load_u(i + 2, odd).start()

        return carry

    with scope("f_dz"):
        for i in range(n_tile // 2 - 2, n_tile // 2):
            for odd in BOTH:
                save_u(i, odd).wait()
        for i in BOTH:
            start_all(load_u(i, odd) for odd in BOTH)
        for part in BOTH:
            lo, hi = part * hh // 2, (part + 1) * hh // 2
            lax.fori_loop(lo, hi, dz_pair, 0)
            for i in range(max(lo, hi - 2), hi):
                for odd in BOTH:
                    put_dz(i, odd).wait()
            give_dz(part).start()
        lax.fori_loop(hh, n_tile // 2, dz_pair, 0)

    with scope("f_end"):
        for part in BOTH:
            give_dz(part).wait()
        for i in range(n_tile // 2 - 2, n_tile // 2):
            for odd in BOTH:
                put_dz(i, odd).wait()
        give_tok.wait_send()
        give_chunk.wait_send()
        for h in BOTH:
            for i in BOTH:
                p1_send(h, i).wait_send()
                p1_fwd(h, i).wait_send()
                for k in (0, PAIR, FAR):
                    p2_send(h, k, i).wait_send()
                    p2_fwd(h, k, i).wait_send()
            for k in (0, PAIR, FAR):
                share(h, k).wait_send()
        for part in BOTH:
            for copy in move_xn(part):
                copy.wait()
        for u in range(len(UNITS)):
            if u > len(UNITS) - 3:
                x_swap(u).wait_send()
            x_keep(u).wait()
            for i in BOTH:
                x_far(u, i).wait_send()
                x_near(u, i).wait_send()
                x_put(u, i).wait_send()
                x_pass(u, i).wait()
    assert (place.n_link, place.n_local) <= dims["front_sems"], (place.n_link, place.n_local)


def specs(n_vmem, n_any):
    return [pl.BlockSpec(memory_space=pltpu.VMEM)] * n_vmem + [pl.BlockSpec(memory_space=pl.ANY)] * n_any


def shapes(items):
    return tuple(jax.ShapeDtypeStruct(*item) for item in items)


def scratch(items, n_link, n_local):
    dma = pltpu.SemaphoreType.DMA
    return [pltpu.VMEM(*item) for item in items] + [dma((n_link,)), dma((n_link,)), dma((n_local,))]


def params(collective_id, limit):
    return pltpu.CompilerParams(collective_id=collective_id, has_side_effects=True, vmem_limit_bytes=limit)


def front(dims, limit, shard, tok_row, lab_row, w, h, g):
    n, tok, vocab, width, vt = dims["n"], dims["tok"], dims["vocab"], dims["width"], dims["vt"]
    cols = shard.shape[0]
    half_v = vocab // CORES
    quarter = tok // n
    n_tile, n_half, n_block, most = vocab // vt, half_v // vt, dims["n_block"], max(PIECES)
    block = width // n_block
    pieces = n * n * CORES
    grid = (n // 2, 2, n // 2, 2)
    return pl.pallas_call(
        functools.partial(front_kernel, dims),
        name="front",
        out_shape=shapes([
            ((n_tile, *grid, CORES, cols, vt), BF16), *[((n_block, block, tok), BF16)] * 4, ((n_tile, tok, vt), BF16),
            ((n_half, tok, vt), BF16), ((n, pieces, cols, quarter), BF16), ((n_tile, tok, vt), F32),
            ((1, width), F32), ((SUB, min(LANE, quarter)), F32), ((CORES, tok, LANE), I32),
        ]),
        in_specs=specs(4, 2),
        out_specs=tuple(specs(0, 9) + specs(3, 0)),
        scratch_shapes=scratch([
            ((n_tile, cols, vt), BF16), ((CORES, n_half, cols, vt), BF16), ((CORES, SUB, tok), I32), ((half_v, CORES * tok), BF16),
            ((2, most, n_half, cols, vt), BF16), ((pieces, cols, tok), BF16), ((2, CORES, most, cols, tok), BF16), ((pieces, cols, tok), BF16),
            ((pieces, cols, quarter), BF16), ((2, pieces, cols, quarter), BF16), ((pieces, cols, quarter), BF16),
            ((4, *grid, CORES, cols, vt), BF16), ((tok, width), BF16), ((n_block, block, tok), BF16),
            ((2, tok, vt), F32), ((2, tok, vt), F32), ((2, 2, tok, vt), BF16), ((tok, LANE), F32), ((tok, LANE), F32), ((tok, LANE), F32),
            ((tok, LANE), I32), ((2 * n + CORES, 1, width), F32), ((n, 2, tok), F32),
        ], dims["front_sems"][0], dims["front_sems"][1]),
        compiler_params=params(0, limit),
    )(shard, tok_row, lab_row, w, h, g)


def back_kernel(
    dims,
    gain_ref, loss_ref, tokc, dz_hbm, dzp_hbm, et_hbm, xnt_hbm, xpar_hbm, gt_hbm, gpar_hbm, h_hbm,
    tail_out, dh_out, de_out, ra_hbm, rx_hbm,
    dz_own, dz_par, et_buf, part, fx, acc, fa, f2, r2, xb, h_buf, dh_buf, dg_acc, slots,
    sends, recvs, local_sems,
):
    n, tok, vocab, width, tile, vt = (dims[k] for k in ("n", "tok", "vocab", "width", "tile", "vt"))
    place = Place(n, sends, recvs, local_sems)
    x, z, y, c = place.x, place.z, place.y, place.c
    half_v = vocab // CORES
    n_tile, n_half = vocab // vt, half_v // vt
    lanes = half_v // 2
    rows = width // (n * n)
    half_rows = rows // 2
    quarter = tok // n
    hq = quarter // 2
    tiles = dims["tiles"]
    chunks = len(tiles)
    edges = [sum(tiles[:d]) for d in range(chunks + 1)]
    per_half = n_half // 2

    with scope("b_enter"):
        place.enter()

    load_h = place.local("h", h_hbm.at[span(x * quarter, quarter, quarter)], h_buf)

    def load_et(t, slot):
        return place.local("et", et_hbm.at[:, span(t * tile, tile, tile)], et_buf.at[slot], slot)

    slot_of = {FAR: 0, 1: 1, 3: 2, 0: 0}
    stages = dims["stages"]

    def load_stage(m, i):
        half, k, kind = stages[m]
        src = ((gt_hbm, gpar_hbm), (xnt_hbm, xpar_hbm))[kind][i]
        src = src.at[(z + k) % n] if half == 0 else src.at[:, (y + k) % n]
        return place.local(("xb", i), src, xb.at[m % 2, i], m % 2)

    def start_stage(m):
        if m < len(stages):
            start_all(load_stage(m, i) for i in BOTH)

    loads = [place.local("dz", dz_hbm, dz_own), place.local("dzp", dzp_hbm, dz_par)]
    load_et(0, 0).start()
    start_all(loads)
    for m in BOTH:
        start_stage(m)
    load_h.start()

    def columns(d):
        return pl.ds(edges[d] * tile, tiles[d] * tile)

    def dxn_chunk(d):
        def body(t, carry):
            slot = t % 2

            @pl.when(t + 1 < edges[chunks])
            def _():
                load_et(t + 1, 1 - slot).start()

            load_et(t, slot).wait()
            left = jnp.concatenate([dz_own[j] for j in range(n_tile)], axis=1)
            right = jnp.concatenate([et_buf[slot, j] for j in range(n_tile)], axis=1)
            part[:, span(t * tile, tile, tile)] = lax.dot_general(
                left, right, (((1,), (1,)), ((), ())), preferred_element_type=F32)
            return carry

        with scope("b_dxn"):
            lax.fori_loop(edges[d], edges[d + 1], body, 0)

    def qrow(k, lo=0, size=hq):
        return span((x + k) % n * quarter + lo, size, SUB)

    def x_far(d, i):
        return place.send(("xf", d, i), part.at[qrow(FAR, i * hq), columns(d)], fx.at[i, :, columns(d)], dx=WAYS[i])

    def x_near(d, i, j):
        src = part.at[qrow(WAYS[i], j * hq), columns(d)]
        return place.send(("xn", d, i, j), src, rx_hbm.at[i, pl.ds(j * hq, hq), columns(d)], dx=WAYS[i])

    def x_first(d):
        start_all(x_far(d, i) for i in BOTH)

    def x_second(d):
        with scope("b_x2"):
            for i in BOTH:
                x_far(d, i).wait_recv()
                sel = qrow(WAYS[i], i * hq)
                part[sel, columns(d)] = part[sel, columns(d)] + fx[i, :, columns(d)]
                start_all(x_near(d, i, j) for j in BOTH)

    def stage_x(d, j, i):
        return place.local("sx", rx_hbm.at[i, pl.ds(j * hq, hq), columns(d)], fx.at[i, :, columns(d)], i)

    def x_third(d, j):
        with scope("b_x3"):
            for i in BOTH:
                x_near(d, i, j).wait_recv()
                stage_x(d, j, i).start()
            for i in BOTH:
                stage_x(d, j, i).wait()
            sel = qrow(0, j * hq)
            part[sel, columns(d)] = part[sel, columns(d)] + fx[0, :, columns(d)] + fx[1, :, columns(d)]

    def de_stage(half, k, kind):
        m = stages.index((half, k, kind))
        slot = slot_of[k]

        wide = min(2, per_half) if k else 1

        def right(i, t):
            if kind:
                return dz_par[t] if i else dz_own[c * n_half + t]
            ids = lax.broadcasted_iota(I32, (tok, LANE), 1) + (x * vocab + c * half_v + t * vt)
            hits = [jnp.where(tokc[i] == ids + b, dims["scale"], 0.0).astype(BF16) for b in range(0, vt, LANE)]
            return jnp.concatenate(hits, axis=1)

        def body(j, carry):
            t = half * per_half + j * wide
            sel = span(j * wide * vt, wide * vt)
            left = jnp.concatenate([xb[m % 2, i].reshape(n * rows, tok) for i in BOTH], axis=1)
            both_right = [jnp.concatenate([right(i, t + q) for i in BOTH], axis=0) for q in range(wide)]
            total = jnp.dot(left, jnp.concatenate(both_right, axis=1), preferred_element_type=F32)
            total = total.reshape(n, rows, wide * vt)
            acc[half, slot, :, :, sel] = acc[half, slot, :, :, sel] + total if kind else total
            return carry

        with scope("b_de" if kind else "b_look"):
            for i in BOTH:
                load_stage(m, i).wait()
            lax.fori_loop(0, per_half // wide, body, 0)
            start_stage(m + 2)

    def de_unit(half, k):
        for kind in BOTH:
            de_stage(half, k, kind)

    def ring(half, k):
        return {"dz": k} if half == 0 else {"dy": k}

    def cross(half, k):
        return {"dy": k} if half == 0 else {"dz": k}

    def a_far(half, i):
        return place.send(("af", half, i), acc.at[half, 0, pl.ds(2 * i, 2)], fa.at[half, i], **ring(half, WAYS[i]))

    def a_near(half, i, j):
        sel = pl.ds(2 * j, 2)
        return place.send(("an", half, i, j), acc.at[half, 1 + i, sel], ra_hbm.at[half, i, sel], **ring(half, WAYS[i]))

    def a_first(half):
        start_all(a_far(half, i) for i in BOTH)

    def a_second(half, i):
        with scope("b_a2"):
            a_far(half, i).wait_recv()
            sel = pl.ds(2 * i, 2)
            acc[half, 1 + i, sel] = acc[half, 1 + i, sel] + fa[half, i]
            start_all(a_near(half, i, j) for j in BOTH)

    def stage_a(half, j, i):
        return place.local(("sa", half), ra_hbm.at[half, i, pl.ds(2 * j, 2)], fa.at[half, i], i)

    def piece(half, k):
        return ((y if half == 0 else z) + k) % n

    def c_far(half, i):
        src = acc.at[half, 0, piece(half, FAR), pl.ds(i * half_rows, half_rows)]
        return place.send(("cf", half, i), src, f2.at[half, i], **cross(half, WAYS[i]))

    def c_near(half, i):
        return place.send(("cn", half, i), acc.at[half, 0, piece(half, WAYS[i])], r2.at[half, i], **cross(half, WAYS[i]))

    def a_third(half, j):
        with scope("b_a3"):
            for i in BOTH:
                a_near(half, i, j).wait_recv()
                stage_a(half, j, i).start()
            for i in BOTH:
                stage_a(half, j, i).wait()
            sel = pl.ds(2 * j, 2)
            acc[half, 0, sel] = acc[half, 0, sel] + fa[half, 0] + fa[half, 1]

    def c_first(half):
        start_all(c_far(half, i) for i in BOTH)

    def c_second(half):
        with scope("b_c2"):
            for i in BOTH:
                c_far(half, i).wait_recv()
                at = piece(half, WAYS[i])
                sel = pl.ds(i * half_rows, half_rows)
                acc[half, 0, at, sel] = acc[half, 0, at, sel] + f2[half, i]
                c_near(half, i).start()

    def out_copies(half):
        sel = span(c * half_v + half * lanes, lanes)
        mine = acc.at[half, 0, piece(half, 0)]
        yield place.local("de", mine.at[span(c * half_rows, half_rows, SUB)], de_out.at[:, sel], half)
        yield place.send(("de", half), mine.at[span((1 - c) * half_rows, half_rows, SUB)], de_out.at[:, sel], dc=1)

    def c_third(half):
        with scope("b_c3"):
            for i in BOTH:
                c_near(half, i).wait_recv()
            at = piece(half, 0)
            acc[half, 0, at] = acc[half, 0, at] + r2[half, 0] + r2[half, 1]
            start_all(out_copies(half))

    with scope("b_load"):
        loads[0].wait()
    def dxn(d):
        if d < chunks:
            dxn_chunk(d)
            x_first(d)

    def x_next(d):
        if d < chunks:
            x_second(d)

    dxn(0)
    loads[1].wait()
    de_unit(0, FAR)
    a_first(0)
    x_next(0)
    dxn(1)
    de_unit(1, FAR)
    a_first(1)
    x_next(1)
    dxn(2)
    de_unit(0, 1)
    x_next(2)
    dxn(3)
    de_unit(0, 3)
    for i in BOTH:
        a_second(0, i)
    de_unit(1, 1)
    a_second(1, 0)
    x_next(3)
    de_unit(1, 3)
    a_second(1, 1)
    with scope("b_wait_far"):
        for half in BOTH:
            for i in BOTH:
                a_far(half, i).wait_send()
    for half in BOTH:
        de_unit(half, 0)

    step = min(32, hq)

    def dh_body(i, carry):
        sel = span(i * step, step, step)
        row = span(x * quarter + i * step, step, step)
        d_x = part[row]
        h_wide = h_buf[sel].astype(F32)
        inv_rms = lax.rsqrt(jnp.sum(h_wide * h_wide, axis=1, keepdims=True) * (1.0 / width) + NORM_EPS)
        h_norm = h_wide * inv_rms
        g_dir = d_x * gain_ref[0:1]
        mean = jnp.sum(g_dir * h_norm, axis=1, keepdims=True) * (1.0 / width)
        dh_buf[sel] = (inv_rms * (g_dir - h_norm * mean)).astype(BF16)
        prod = d_x * h_norm
        total = prod[0:SUB]
        for j in range(SUB, step, SUB):
            total = total + prod[j:j + SUB]
        dg_acc[...] = dg_acc[...] + total
        return carry

    def h_first(i, j):
        return place.send(("hf", i, j), dh_buf.at[pl.ds(j * hq, hq)], dh_out.at[qrow(0, j * hq)], dx=WAYS[i])

    def h_second(i):
        ref = dh_out.at[qrow(FROM[i], i * hq)]
        return place.send(("hs", i), ref, ref, dx=WAYS[i])

    dg_acc[...] = jnp.zeros_like(dg_acc)
    load_h.wait()
    per_j = hq // step
    for j in BOTH:
        for d in range(chunks):
            x_third(d, j)
        with scope("b_dh"):
            lax.fori_loop(j * per_j, (j + 1) * per_j, dh_body, 0)
            start_all(h_first(i, j) for i in BOTH)
    keep_dh = place.local("dh", dh_buf, dh_out.at[qrow(0, 0, quarter)])
    small = SmallSum(place, ("dc", "dx", "dy", "dz"), slots)
    sums = [jnp.sum(part_sum, axis=0, keepdims=True) for part_sum in (dg_acc[...], loss_ref[...])]
    small.start("dc", jnp.concatenate(sums, axis=1))
    keep_dh.start()
    with scope("b_s1"):
        small.start("dx", small.finish("dc"))
    for half in BOTH:
        for j in BOTH:
            a_third(half, j)
        c_first(half)
    with scope("b_h2"):
        for i in BOTH:
            h_first(i, i).wait_recv()
            h_second(i).start()
    with scope("b_s2"):
        small.start("dy", small.finish("dx"))
    for half in BOTH:
        c_second(half)
    with scope("b_s3"):
        small.start("dz", small.finish("dy"))
    for half in BOTH:
        c_third(half)
    with scope("b_s4"):
        total = small.finish("dz")
        loss = jnp.sum(total[:, width:], axis=1, keepdims=True) * (1.0 / dims["total"])
        tail_out[...] = jnp.concatenate([total[:, 0:width], jnp.broadcast_to(loss, (1, LANE))], axis=1)

    with scope("b_end_x"):
        keep_dh.wait()
        for i in BOTH:
            for d in range(chunks):
                x_far(d, i).wait_send()
                for j in BOTH:
                    x_near(d, i, j).wait_send()
            h_first(i, i).wait_send()
            h_first(i, 1 - i).wait()
            h_second(i).wait()
    with scope("b_end_a"):
        for half in BOTH:
            for i in BOTH:
                for j in BOTH:
                    a_near(half, i, j).wait_send()
                c_far(half, i).wait_send()
                c_near(half, i).wait_send()
            for copy in out_copies(half):
                copy.wait()
    assert (place.n_link, place.n_local) <= dims["back_sems"], (place.n_link, place.n_local)


def back(dims, limit, gain, loss, tokc, dz, dzp, et, xnt, xpar, gt, gpar, h):
    n, tok, vocab, width, tile = (dims[k] for k in ("n", "tok", "vocab", "width", "tile"))
    rows = width // (n * n)
    half_v = vocab // CORES
    lanes = half_v // 2
    quarter = tok // n
    hq = quarter // 2
    tail_w = width + loss.shape[1]
    n_tile, n_half, vt = dz.shape[0], dzp.shape[0], dims["vt"]
    turned = [a.reshape(n, n, rows, tok) for a in (xnt, xpar, gt, gpar)]
    return pl.pallas_call(
        functools.partial(back_kernel, dims),
        name="back",
        out_shape=shapes([
            ((1, width + LANE), F32), ((tok, width), BF16), ((rows // CORES, vocab), F32), ((2, 2, n, rows, lanes), F32),
            ((2, quarter, width), F32),
        ]),
        in_specs=specs(3, 8),
        out_specs=tuple(specs(1, 4)),
        scratch_shapes=scratch([
            ((n_tile, tok, vt), BF16), ((n_half, tok, vt), BF16), ((2, n_tile, tile, vt), BF16), ((tok, width), F32),
            ((2, hq, width), F32), ((2, 3, n, rows, lanes), F32), ((2, 2, 2, rows, lanes), F32),
            ((2, 2, rows // 2, lanes), F32), ((2, 2, rows, lanes), F32), ((2, CORES, n, rows, tok), BF16), ((quarter, width), BF16),
            ((quarter, width), BF16), ((SUB, width), F32), ((3 * n + CORES, 1, tail_w), F32),
        ], dims["back_sems"][0], dims["back_sems"][1]),
        compiler_params=params(1, limit),
    )(gain, loss, tokc, dz, dzp, et.reshape(n_tile, width, vt), *turned, h)[:3]


def finish_kernel(
    n, scale, table_ref, tail_ref, x0_hbm, dh_hbm, de_hbm, dg_out, loss_out, x0_out, dh_out, de_out,
    x0_in, x0_buf, rows_ref, dh_buf, de_buf, sems,
):
    place = Place(n, None, None, sems)
    quarter, cols, width = x0_in.shape[3], x0_in.shape[2], x0_buf.shape[2]

    def step(q):
        rows = span(q * quarter, quarter, quarter)
        return (
            place.local("x0", x0_hbm.at[q], x0_in.at[q], q, n), place.local("x0o", x0_buf.at[q], x0_out.at[rows], q, n),
            place.local("dh", dh_hbm.at[rows], dh_buf.at[q], q, n), place.local("dho", dh_buf.at[q], dh_out.at[rows], q, n),
        )

    moves = [step(q) for q in range(n)]
    de_in, de_put = place.local("de", de_hbm, de_buf, 0), place.local("de", de_buf, de_out, 1)
    for x0_load, _, dh_load, _ in moves:
        x0_load.start()
        dh_load.start()
    de_in.start()
    gain = jnp.broadcast_to(tail_ref[:, 0:width], (SUB, width))
    dg_out[...] = pltpu.roll(gain, width - place.f * cols, axis=1)[0:1, 0:cols]
    loss_out[...] = tail_ref[:, width:width + 1]

    def body(q, carry):
        x0_load, x0_put, dh_load, dh_put = step(q)
        x0_load.wait()
        for zi in range(n):
            for yi in range(n):
                for h in BOTH:
                    dz, dy = (zi - place.z) % n, (yi - place.y) % n
                    k1, k2 = (dy, dz) if h == 0 else (dz, dy)
                    piece = table_ref[(h * n + k1) * n + k2]
                    rows_ref[pl.ds(((zi * n + yi) * CORES + h) * cols, cols)] = x0_in[q, piece]
        x0_buf[q] = (rows_ref[...].T.astype(F32) * scale).astype(BF16)
        x0_put.start()
        dh_load.wait()
        dh_put.start()
        return carry

    lax.fori_loop(0, n, body, 0)
    de_in.wait()
    de_put.start()
    for _, x0_put, _, dh_put in moves:
        x0_put.wait()
        dh_put.wait()
    de_put.wait()


def finish(n, scale, limit, tail, x0, dh, de):
    _, pieces, cols, quarter = x0.shape
    width = pieces * cols
    table = np.zeros((CORES, n, n), np.int32)
    for u, unit in enumerate(UNITS):
        for h in BOTH:
            for i, (k1, k2) in enumerate(unit):
                table[h, k1, k2] = BASE[u] + h * len(unit) + i
    return pl.pallas_call(
        functools.partial(finish_kernel, n, scale),
        name="finish",
        in_specs=[pl.BlockSpec(memory_space=pltpu.SMEM)] + specs(1, 3),
        out_specs=tuple(specs(2, 3)),
        out_shape=shapes([((1, cols), F32), ((1, 1), F32), (dh.shape, BF16), (dh.shape, BF16), (de.shape, F32)]),
        scratch_shapes=[
            pltpu.VMEM(x0.shape, BF16), pltpu.VMEM((n, quarter, width), BF16), pltpu.VMEM((width, quarter), BF16),
            pltpu.VMEM((n, quarter, width), BF16), pltpu.VMEM(de.shape, F32), pltpu.SemaphoreType.DMA((4 * n + 2,)),
        ],
        compiler_params=pltpu.CompilerParams(vmem_limit_bytes=limit),
    )(jnp.asarray(table.reshape(-1)), tail, x0, dh, de)


def solution(mesh):
    return build(mesh, mesh.shape["tp"], 256, digits("1233")[0], 256, 6, 67_000_000)


def build(mesh, n, tile, tiles, vt, n_block, limit):
    fsdp_size = mesh.shape["fsdp"]

    def device_step(emb_shard, tok_ids, lab_ids, h_last, g_embed, norm_w):
        vocab_rows, cols = emb_shard.shape
        batch_loc, seq_len, width = h_last.shape
        tok_count = batch_loc * seq_len
        fsdp_id = lax.axis_index("fsdp")
        scale = float(np.asarray(math.sqrt(width)).astype(jnp.bfloat16))
        dims = {
            "n": n, "tok": tok_count, "vocab": vocab_rows, "width": width, "total": tok_count * fsdp_size, "vt": vt,
            "tile": tile, "tiles": tiles, "scale": scale, "n_block": n_block,
            "stages": digits("020 021 120 121") + digits("010 011 030 031") + digits("110 111 130 131") + digits("000 001 100 101"),
            "front_sems": (110, 42), "back_sems": (62, 22),
        }
        h_flat = h_last.reshape(tok_count, width)
        placed = lax.dynamic_update_slice(jnp.zeros((SUB, width), F32), jnp.broadcast_to(norm_w, (SUB, cols)), (0, fsdp_id * cols))
        ids = [a.reshape(1, tok_count) for a in (tok_ids, lab_ids)]
        table, xn_t, xpar_t, g_t, gpar_t, dz, dzp, x0, _, gain, loss_part, tokc = front(
            dims, limit, emb_shard.T, *ids, norm_w.reshape(1, cols), h_flat, g_embed.reshape(tok_count, width))
        tail, d_hidden, d_cols = back(dims, limit, gain, loss_part, tokc, dz, dzp, table, xn_t, xpar_t, g_t, gpar_t, h_flat)
        d_norm_w, loss, x_emb, d_hidden, d_cols = finish(n, scale, limit, tail, x0, d_hidden, d_cols)
        return (x_emb.reshape(h_last.shape), loss.reshape(()), d_hidden.reshape(h_last.shape), d_norm_w.reshape(cols), d_cols.T)

    spec_tok = P("fsdp", None)
    spec_act = P("fsdp", None, None)
    return jax.shard_map(device_step, mesh=mesh, in_specs=(P("tp", "fsdp"), spec_tok, spec_tok, spec_act, spec_act, P("fsdp")), out_specs=(spec_act, P(), spec_act, P("fsdp"), P("tp", "fsdp")), check_vma=False)
```

```python
import functools
import math
import jax
import numpy as np
import jax.numpy as jnp
from jax import lax
from jax.experimental import pallas as pl
from jax.experimental.pallas import tpu as pltpu
from jax.sharding import PartitionSpec as P

SOFT_CAP = 30.0
NORM_EPS = 1e-6
F32, BF16, I32 = jnp.float32, jnp.bfloat16, jnp.int32
LANE, SUB = 128, 8
BOTH = (0, 1)
FOUR = range(4)
WAYS = (1, 3)
FROM = (3, 1)
FAR = 2
CORES = 2


def span(start, size, unit=LANE):
    return pl.ds(pl.multiple_of(start, unit), size)


class Place:
    def __init__(self, n, sends, recvs, local_sems):
        self.n, self.sends, self.recvs, self.local_sems = n, sends, recvs, local_sems
        self.x = lax.axis_index("tp")
        f = lax.axis_index("fsdp")
        self.f = f
        self.c = f % CORES
        self.y = f // CORES % n
        self.z = f // CORES // n
        self.link_of, self.local_of, self.n_link, self.n_local = {}, {}, 0, 0
        self.size = {"dx": n, "dz": n, "dy": n, "dc": CORES}
        self.me = {"dx": self.x, "dz": self.z, "dy": self.y, "dc": self.c}

    def at(self, dx=0, dz=0, dy=0, dc=0):
        n = self.n
        z, y, c = (self.z + dz) % n, (self.y + dy) % n, (self.c + dc) % CORES
        return ((self.x + dx) % n, (z * n + y) * CORES + c)

    def enter(self):
        barrier = pltpu.get_barrier_semaphore()
        peers = [self.at(**{d: k}) for d in self.size for k in range(1, self.size[d])]
        for peer in peers:
            pl.semaphore_signal(barrier, inc=1, device_id=peer, device_id_type=pl.DeviceIdType.MESH)
        pl.semaphore_wait(barrier, len(peers))

    def link(self, key, count=1):
        if key not in self.link_of:
            self.link_of[key] = self.n_link
            self.n_link += count
        return self.link_of[key]

    def send(self, key, src, dst, **step):
        i = self.link(key)
        return pltpu.make_async_remote_copy(
            src, dst, self.sends.at[i], self.recvs.at[i], device_id=self.at(**step), device_id_type=pl.DeviceIdType.MESH)

    def local(self, key, src, dst, slot=0, count=2):
        if key not in self.local_of:
            self.local_of[key] = self.n_local
            self.n_local += count
        return pltpu.make_async_copy(src, dst, self.local_sems.at[self.local_of[key] + slot])


class SmallSum:
    def __init__(self, place, dims, slots):
        self.place, self.slots, self.dims, self.base = place, slots, dims, {}
        count = 0
        for d in dims:
            self.base[d] = count
            count += place.size[d]

    def copies(self, d):
        slot = self.slots.at[self.base[d] + self.place.me[d]]
        for k in range(1, self.place.size[d]):
            yield self.place.send((self.dims, d, k), slot, slot, **{d: k})

    def start(self, d, value):
        self.slots[self.base[d] + self.place.me[d]] = value
        for copy in self.copies(d):
            copy.start()

    def finish(self, d):
        for copy in self.copies(d):
            copy.wait()
        total = self.slots[self.base[d]]
        for k in range(1, self.place.size[d]):
            total = total + self.slots[self.base[d] + k]
        return total


def scope(name):
    return jax.named_scope(name)


def start_all(copies):
    for copy in copies:
        copy.start()


def digits(text):
    return tuple(tuple(int(d) for d in word) for word in text.split())


UNITS = [digits(u) for u in ("00", "10 30", "01 03 20", "02 11 31", "13 33 21 23", "12 32 22")]
PAIR, ALL = 1, "all"
PIECES = [2 * len(u) for u in UNITS]
EXP_RATE = SOFT_CAP * math.log2(math.e)
BASE = [sum(PIECES[:i]) for i in range(len(UNITS))]


def front_kernel(
    dims,
    shard_ref, tok_ref, lab_ref, w_ref, h_hbm, g_hbm,
    et_out, xnt_out, xpar_out, gt_out, gpar_out, dz_out, dzpar_out, x0_out, u_hbm, gain_out, loss_out, tokc_out,
    shard_t, chunk, tokr, hit_t, lhs, xp, xw, xr, xf, xg, xq, etb, xn, gl, z_even, z_odd, dzb,
    acc_e, acc_l, inv_s, labc, w_slots, s_slots, sends, recvs, local_sems,
):
    n, tok, vocab, width, vt = dims["n"], dims["tok"], dims["vocab"], dims["width"], dims["vt"]
    place = Place(n, sends, recvs, local_sems)
    x, z, y, c = place.x, place.z, place.y, place.c
    half_v = vocab // CORES
    n_tile = vocab // vt
    n_half = n_tile // CORES
    hh = n_half // 2
    cols = width // (n * n * CORES)
    quarter = tok // n
    row_start = x * vocab

    def ring1(h, k):
        return {"dy": k} if h == 0 else {"dz": k}

    def ring2(h, k):
        return {"dz": k} if h == 0 else {"dy": k}

    def coord(base, k, paired):
        every = slice(None)
        if k == ALL:
            return every, every
        return every if paired else (base + k) % n // 2, (base + k) % 2

    def loc(h, k1, k2, lo=0, size=n_half, pair1=False, pair2=False):
        first, second = coord((y, z)[h], k1, pair1), coord((z, y)[h], k2, pair2)
        return et_out.at[(pl.ds(c * n_half + lo, size), *((second, first)[h]), *((first, second)[h]), h)]

    with scope("f_enter"):
        place.enter()

    load_g = place.local("g", g_hbm, xn)
    load_g.start()
    with scope("f_cast"):
        for t in range(n_tile):
            shard_t[t] = shard_ref[:, pl.ds(t * vt, vt)].astype(BF16)
        tokr[c] = jnp.broadcast_to(tok_ref[...], (SUB, tok))
        give_tok = place.send("tok", tokr.at[c], tokr.at[c], dc=1)
        give_chunk = place.send("chunk", shard_t.at[pl.ds((1 - c) * n_half, n_half)], chunk.at[c], dc=1)
        give_chunk.start()
        give_tok.start()
        chunk[c] = shard_t[pl.ds(c * n_half, n_half)]
        gain_sum = SmallSum(place, ("dc", "dy", "dz"), w_slots)
        own_w = jnp.concatenate([w_ref[...], jnp.zeros((1, width - cols), F32)], axis=1)
        gain_sum.start("dc", pltpu.roll(jnp.broadcast_to(own_w, (SUB, width)), place.f * cols, axis=1)[0:1])

    def p1_send(h, i):
        return place.send(("p1", h, i), chunk.at[h], loc(h, 0, 0), **ring1(h, WAYS[i]))

    def p1_fwd(h, i):
        ref = loc(h, FROM[i], 0, i * hh, hh)
        return place.send(("p1f", h, i), ref, ref, **ring1(h, WAYS[i]))

    def p2_send(h, k1, i):
        ref = loc(h, k1, 0, pair1=k1 == PAIR)
        return place.send(("p2", h, k1, i), chunk.at[h] if k1 == 0 else ref, ref, **ring2(h, WAYS[i]))

    def p2_fwd(h, k1, i):
        ref = loc(h, k1, FROM[i], i * hh, hh, pair1=k1 == PAIR)
        return place.send(("p2f", h, k1, i), ref, ref, **ring2(h, WAYS[i]))

    def keep(h):
        return place.local("keep", chunk.at[h], loc(h, 0, 0), h)

    def share(h, k2):
        ref = loc(h, ALL, k2, pair2=k2 == PAIR)
        return place.send(("share", h, k2), ref, ref, dc=1)

    def pass_first():
        with scope("f_p1"):
            for h in BOTH:
                for i in BOTH:
                    p1_send(h, i).wait_recv()
                    p1_fwd(h, i).start()
            for h in BOTH:
                start_all(p2_send(h, PAIR, i) for i in BOTH)

    def pass_first_far():
        with scope("f_p1f"):
            for h in BOTH:
                for i in BOTH:
                    p1_fwd(h, i).wait_recv()
                start_all(p2_send(h, FAR, j) for j in BOTH)

    def pass_second(k1):
        with scope("f_p2"):
            for h in BOTH:
                for i in BOTH:
                    p2_send(h, k1, i).wait_recv()
                    p2_fwd(h, k1, i).start()

    def end_second(k1):
        with scope("f_p2f"):
            for h in BOTH:
                for i in BOTH:
                    p2_fwd(h, k1, i).wait_recv()

    def share_group(k2):
        start_all(share(h, k2) for h in BOTH)

    with scope("f_chunk"):
        give_chunk.wait_recv()
        start_all(keep(h) for h in BOTH)
        gain_sum.start("dy", gain_sum.finish("dc"))
        for h in BOTH:
            start_all(p1_send(h, i) for i in BOTH)
        for h in BOTH:
            start_all(p2_send(h, 0, i) for i in BOTH)

    v_step = min(LANE, half_v)

    def hit_body(j, carry):
        off = j * v_step
        ids = lax.broadcasted_iota(I32, (v_step, tok), 0) + (row_start + c * half_v + off)
        for i, core in enumerate((c, 1 - c)):
            hit_t[span(off, v_step, v_step), pl.ds(i * tok, tok)] = jnp.where(ids == tokr[core, 0:1, :], 1.0, 0.0).astype(BF16)
        return carry

    def make_hits():
        with scope("f_hit"):
            give_tok.wait_recv()
            lax.fori_loop(0, half_v // v_step, hit_body, 0)

    n_step = min(512, tok)
    most = max(PIECES)

    def whole(u):
        return pl.ds(BASE[u], PIECES[u])

    def unit_copies(u):
        slot = u % 2
        for p, (h, (k1, k2)) in enumerate((h, k) for h in BOTH for k in UNITS[u]):
            yield place.local("lhs", loc(h, k1, k2), lhs.at[slot, p], slot * most + p, 2 * most)

    def load_unit(u):
        start_all(unit_copies(u))

    def look(u):
        pieces = PIECES[u]
        with scope("f_look"):
            if u > 1:
                x_swap(u - 2).wait_send()
            left = lhs.at[u % 2]
            for copy in unit_copies(u):
                copy.wait()
            per_core = tok // n_step

            def body(j, carry):
                value = jnp.concatenate([left[pl.ds(0, pieces), t].reshape(pieces * cols, vt) for t in range(n_half)], axis=1)
                rows = jnp.dot(value, hit_t[:, span(j * n_step, n_step)], preferred_element_type=F32)
                rows = rows.reshape(pieces, cols, n_step).astype(BF16)
                xw[u % 2, j // per_core, pl.ds(0, pieces), :, span(j % per_core * n_step, n_step)] = rows
                return carry

            lax.fori_loop(0, CORES * per_core, body, 0)
            x_swap(u).start()

    def x_swap(u):
        return place.send(("swap", u), xw.at[u % 2, 1, pl.ds(0, PIECES[u])], xr.at[whole(u)], dc=1)

    def lanes_of(k):
        return span((x + k) % n * quarter, quarter, quarter)

    def side(u, i):
        return pl.ds(BASE[u] + i * len(UNITS[u]), len(UNITS[u]))

    def x_far(u, i):
        return place.send(("xf", u, i), xp.at[side(u, i), :, lanes_of(FAR)], xf.at[side(u, i)], dx=WAYS[i])

    def x_near(u, i):
        return place.send(("xn", u, i), xp.at[whole(u), :, lanes_of(WAYS[i])], xg.at[i, whole(u)], dx=WAYS[i])

    def x_goal(k, sel):
        return x0_out.at[(x + k) % n, sel]

    def x_put(u, i):
        return place.send(("xp", u, i), xq.at[whole(u)], x_goal(0, whole(u)), dx=WAYS[i])

    def x_keep(u):
        return place.local("x0", xq.at[whole(u)], x_goal(0, whole(u)), u, len(UNITS))

    def x_pass(u, i):
        ref = x_goal(FROM[i], side(u, i))
        return place.send(("xs", u, i), ref, ref, dx=WAYS[i])

    def x_first(u):
        with scope("f_x1"):
            x_swap(u).wait_recv()
            def body(p, carry):
                xp[BASE[u] + p] = xw[u % 2, 0, p] + xr[BASE[u] + p]
                return carry

            lax.fori_loop(0, PIECES[u], body, 0)
            start_all(x_far(u, i) for i in BOTH)

    def x_second(u):
        with scope("f_x2"):
            for i in BOTH:
                x_far(u, i).wait_recv()
                sel, lanes = side(u, i), lanes_of(WAYS[i])
                xp[sel, :, lanes] = xp[sel, :, lanes] + xf[sel]
                x_near(u, i).start()

    def x_third(u):
        with scope("f_x3"):
            for i in BOTH:
                x_near(u, i).wait_recv()
            sel = whole(u)
            xq[sel] = xp[sel, :, lanes_of(0)] + xg[0, sel] + xg[1, sel]
            start_all(x_put(u, i) for i in BOTH)
            x_keep(u).start()

    def x_fourth(u):
        with scope("f_x4"):
            for i in BOTH:
                x_put(u, i).wait_recv()
                x_pass(u, i).start()

    block = width // dims["n_block"]

    def transpose_block(j):
        return xn[:, pl.ds(j * block, block)].T

    n_block = dims["n_block"]
    early = n_block // 2

    def moves(key, part, whole, other):
        sel = pl.ds(part * early, early)
        yield place.local(key, gl.at[sel], whole.at[sel], part)
        yield place.send((key, part), gl.at[sel], other.at[sel], dc=1)

    def move_g(part):
        return moves("g", part, gt_out, gpar_out)

    def move_xn(part):
        return moves("xt", part, xnt_out, xpar_out)

    def transpose_part(part, copies):
        for j in range(part * early, (part + 1) * early):
            gl[j] = transpose_block(j)
        start_all(copies)

    def columns(row):
        return jnp.broadcast_to(row.astype(F32), (LANE, tok)).T.astype(I32)

    r_step = min(LANE, tok)

    def xn_body(j, carry):
        sel = span(j * r_step, r_step, r_step)
        h_wide = xn[sel].astype(F32)
        inv_rms = lax.rsqrt(jnp.sum(h_wide * h_wide, axis=1, keepdims=True) * (1.0 / width) + NORM_EPS)
        xn[sel] = (h_wide * inv_rms * gain_out[0:1]).astype(BF16)
        return carry

    e_step = min(LANE, tok)

    def tile_of(j):
        return (c * n_half + j) % n_tile

    def load_tile(j):
        return place.local("et", et_out.at[tile_of(j)], etb.at[j % 4], j % 4, 4)

    def save_u(i, odd):
        return place.local(("u", odd), (z_even, z_odd)[odd].at[i % 2], u_hbm.at[tile_of(2 * i + odd)], i % 2)

    def lane_blocks():
        return [(b, pl.ds(b, LANE)) for b in range(0, vt, LANE)]

    def post_tile(i, odd):
        base = tile_of(2 * i + odd) * vt
        buf, slot = (z_even, z_odd)[odd], i % 2

        def body(e, carry):
            sel = span(e * e_step, e_step, e_step)
            ids = lax.broadcasted_iota(I32, (e_step, LANE), 1) + base
            sum_e, sum_l = acc_e[sel], acc_l[sel]
            for b, lanes in lane_blocks():
                tanh_z = jnp.tanh(buf[slot, sel, lanes] * (1.0 / SOFT_CAP))
                buf[slot, sel, lanes] = tanh_z
                sum_e = sum_e + jnp.exp2(EXP_RATE * tanh_z - EXP_RATE)
                sum_l = sum_l + jnp.where(ids + b == labc[sel], tanh_z, 0.0)
            acc_e[sel] = sum_e
            acc_l[sel] = sum_l
            return carry

        lax.fori_loop(0, tok // e_step, body, 0)

    def dot_pair(i):
        for odd in BOTH:
            value = etb[(2 * i + odd) % 4].reshape(width, vt)
            (z_even, z_odd)[odd][i % 2] = jnp.dot(xn[...], value, preferred_element_type=F32)

    def load_pair(i):
        start_all(load_tile(2 * i + odd) for odd in BOTH)

    def pair(i, carry):
        for odd in BOTH:
            load_tile(2 * i + odd).wait()

        @pl.when(i > 1)
        def _():
            for odd in BOTH:
                save_u(i - 2, odd).wait()

        for odd in BOTH:
            post_tile(i - 1, odd)
            save_u(i - 1, odd).start()
        dot_pair(i)

        @pl.when(i + 2 < n_tile // 2)
        def _():
            load_pair(i + 2)

        for k, work in enumerate(during):
            @pl.when(i == k + 1)
            def _():
                if k == 0:
                    wait_shares()
                perform(work)
        return carry

    def wait_shares():
        with scope("f_share"):
            for h in BOTH:
                for k2 in (0, PAIR, FAR):
                    share(h, k2).wait_recv()

    def logits_first():
        acc_e[...] = jnp.zeros_like(acc_e)
        acc_l[...] = jnp.zeros_like(acc_l)
        with scope("f_logits0"):
            for i in BOTH:
                load_pair(i)
            for odd in BOTH:
                load_tile(odd).wait()
            dot_pair(0)
            if n_tile // 2 > 2:
                load_pair(2)

    def lay_columns():
        with scope("f_cols"):
            labc[...] = columns(lab_ref[...] - row_start)
            for i, core in enumerate((c, 1 - c)):
                tokc_out[i] = columns(tokr[core, 0:1, :])

    def turn_g():
        with scope("f_gt"):
            load_g.wait()
            for part in BOTH:
                transpose_part(part, move_g(part))
            load_h.start()

    def gain_next():
        with scope("f_gain2"):
            gain_sum.start("dz", gain_sum.finish("dy"))

    def normalize():
        with scope("f_xn"):
            gain_out[...] = 1.0 + gain_sum.finish("dz")
            load_h.wait()
            lax.fori_loop(0, tok // r_step, xn_body, 0)

    def turn_xn():
        with scope("f_xt"):
            for part in BOTH:
                for copy in move_g(part):
                    copy.wait()
                transpose_part(part, move_xn(part))

    def begin_unit(u):
        if u == 0:
            for h in BOTH:
                keep(h).wait()
        load_unit(u)

    load_h = place.local("h", h_hbm, xn)
    works = {
        "HIT": make_hits, "GT": turn_g, "COL": lay_columns, "G2": gain_next, "XN": normalize, "XT": turn_xn, "L0": logits_first,
        "PF": pass_first, "PFF": pass_first_far,
    }
    groups = {"0": 0, "P": PAIR, "F": FAR}
    families = {"LU": begin_unit, "LK": look, "X1": x_first, "X2": x_second, "X3": x_third, "X4": x_fourth}
    families_k = {"SH": share_group, "S": pass_second, "E": end_second}

    def perform(text):
        for word in text.split():
            if word in works:
                works[word]()
            elif word[:-1] in families:
                families[word[:-1]](int(word[-1]))
            else:
                families_k[word[:-1]](groups[word[-1]])

    during = (
        "X15 X24",
        "",
        "X25",
        "X34",
        "",
        "X35",
        "",
    )
    for text in (
        "LU0 HIT G2 LK0", "GT PF LU1 LK1", "X10 S0 XN PFF", "LU2 X20 SH0 X11", "LK2 X30 COL X21",
        "X12 XT E0 SP", "LU3 X22 X31 LK3", "SF LU4 X40 SHP", "X32 LK4 X13 EP", "EF X41 LU5 L0",
        "X23 SHF LK5 X14", "X33",
    ):
        perform(text)
    if n_half < 4:
        wait_shares()
        for text in during:
            perform(text)
        during = ()
    last = n_tile // 2 - 1
    with scope("f_logits"):
        lax.fori_loop(1, last + 1, pair, 0)
        for odd in BOTH:
            post_tile(last, odd)
            save_u(last, odd).start()

    with scope("f_stats"):
        row = lax.broadcasted_iota(I32, (2, tok), 0)
        sum_e = jnp.sum(acc_e[...].T, axis=0, keepdims=True)
        sum_l = SOFT_CAP * jnp.sum(acc_l[...].T, axis=0, keepdims=True)
        stats = SmallSum(place, ("dx",), s_slots)
        stats.start("dx", jnp.where(row == 0, sum_e, sum_l))
    perform("X43 X42 X45 X44")
    with scope("f_stats2"):
        stat = stats.finish("dx")
        all_e, all_l = stat[0:1], stat[1:2]
        inv_s[...] = jnp.broadcast_to((1.0 / dims["total"]) / all_e, (LANE, tok)).T
        s_slots[0, 0:1, :] = jnp.log(all_e) + SOFT_CAP - all_l
        own = s_slots[0, 0:1, lanes_of(0)]
        part_w = min(LANE, quarter)
        folded = own[:, 0:part_w]
        for j in range(part_w, quarter, part_w):
            folded = folded + own[:, j:j + part_w]
        loss_out[...] = jnp.where(lax.broadcasted_iota(I32, (SUB, part_w), 0) == 0, folded, 0.0)

    def dz_tile(j):
        return ((1 - c) * n_half + j) % n_tile

    def load_u(i, odd):
        return place.local(("u", odd), u_hbm.at[dz_tile(2 * i + odd)], (z_even, z_odd)[odd].at[i % 2], i % 2)

    def put_dz(i, odd):
        return place.local(("dz", odd), dzb.at[odd, i % 2], dz_out.at[dz_tile(2 * i + odd)], i % 2)

    def give_dz(part):
        src = dz_out.at[pl.ds((1 - c) * n_half + part * hh, hh)]
        return place.send(("dz", part), src, dzpar_out.at[pl.ds(part * hh, hh)], dc=1)

    d_step = min(256, tok)

    def dz_rows(i, odd):
        base = dz_tile(2 * i + odd) * vt
        buf, slot = (z_even, z_odd)[odd], i % 2

        def body(e, carry):
            sel = span(e * d_step, d_step, d_step)
            ids = lax.broadcasted_iota(I32, (d_step, LANE), 1) + base
            for b, lanes in lane_blocks():
                tanh_z = buf[slot, sel, lanes]
                prob = jnp.exp2(EXP_RATE * tanh_z - EXP_RATE) * inv_s[sel]
                prob = jnp.where(ids + b == labc[sel], prob - 1.0 / dims["total"], prob)
                dzb[odd, slot, sel, lanes] = (prob * (1.0 - tanh_z * tanh_z)).astype(BF16)
            return carry

        lax.fori_loop(0, tok // d_step, body, 0)

    def dz_pair(i, carry):
        for odd in BOTH:
            load_u(i, odd).wait()

            @pl.when(i > hh + 1)
            def _():
                put_dz(i - 2, odd).wait()

            dz_rows(i, odd)
            put_dz(i, odd).start()

            @pl.when(i + 2 < n_tile // 2)
            def _():
                load_u(i + 2, odd).start()

        return carry

    with scope("f_dz"):
        for i in range(n_tile // 2 - 2, n_tile // 2):
            for odd in BOTH:
                save_u(i, odd).wait()
        for i in BOTH:
            start_all(load_u(i, odd) for odd in BOTH)
        for part in BOTH:
            lo, hi = part * hh // 2, (part + 1) * hh // 2
            lax.fori_loop(lo, hi, dz_pair, 0)
            for i in range(max(lo, hi - 2), hi):
                for odd in BOTH:
                    put_dz(i, odd).wait()
            give_dz(part).start()
        lax.fori_loop(hh, n_tile // 2, dz_pair, 0)

    with scope("f_end"):
        for part in BOTH:
            give_dz(part).wait()
        for i in range(n_tile // 2 - 2, n_tile // 2):
            for odd in BOTH:
                put_dz(i, odd).wait()
        give_tok.wait_send()
        give_chunk.wait_send()
        for h in BOTH:
            for i in BOTH:
                p1_send(h, i).wait_send()
                p1_fwd(h, i).wait_send()
                for k in (0, PAIR, FAR):
                    p2_send(h, k, i).wait_send()
                    p2_fwd(h, k, i).wait_send()
            for k in (0, PAIR, FAR):
                share(h, k).wait_send()
        for part in BOTH:
            for copy in move_xn(part):
                copy.wait()
        for u in range(len(UNITS)):
            if u > len(UNITS) - 3:
                x_swap(u).wait_send()
            x_keep(u).wait()
            for i in BOTH:
                x_far(u, i).wait_send()
                x_near(u, i).wait_send()
                x_put(u, i).wait_send()
                x_pass(u, i).wait()
    assert (place.n_link, place.n_local) <= dims["front_sems"], (place.n_link, place.n_local)


def specs(n_vmem, n_any):
    return [pl.BlockSpec(memory_space=pltpu.VMEM)] * n_vmem + [pl.BlockSpec(memory_space=pl.ANY)] * n_any


def shapes(items):
    return tuple(jax.ShapeDtypeStruct(*item) for item in items)


def scratch(items, n_link, n_local):
    dma = pltpu.SemaphoreType.DMA
    return [pltpu.VMEM(*item) for item in items] + [dma((n_link,)), dma((n_link,)), dma((n_local,))]


def params(collective_id, limit):
    return pltpu.CompilerParams(collective_id=collective_id, has_side_effects=True, vmem_limit_bytes=limit)


def front(dims, limit, shard, tok_row, lab_row, w, h, g):
    n, tok, vocab, width, vt = dims["n"], dims["tok"], dims["vocab"], dims["width"], dims["vt"]
    cols = shard.shape[0]
    half_v = vocab // CORES
    quarter = tok // n
    n_tile, n_half, n_block, most = vocab // vt, half_v // vt, dims["n_block"], max(PIECES)
    block = width // n_block
    pieces = n * n * CORES
    grid = (n // 2, 2, n // 2, 2)
    return pl.pallas_call(
        functools.partial(front_kernel, dims),
        name="front",
        out_shape=shapes([
            ((n_tile, *grid, CORES, cols, vt), BF16), *[((n_block, block, tok), BF16)] * 4, ((n_tile, tok, vt), BF16),
            ((n_half, tok, vt), BF16), ((n, pieces, cols, quarter), BF16), ((n_tile, tok, vt), F32),
            ((1, width), F32), ((SUB, min(LANE, quarter)), F32), ((CORES, tok, LANE), I32),
        ]),
        in_specs=specs(4, 2),
        out_specs=tuple(specs(0, 9) + specs(3, 0)),
        scratch_shapes=scratch([
            ((n_tile, cols, vt), BF16), ((CORES, n_half, cols, vt), BF16), ((CORES, SUB, tok), I32), ((half_v, CORES * tok), BF16),
            ((2, most, n_half, cols, vt), BF16), ((pieces, cols, tok), BF16), ((2, CORES, most, cols, tok), BF16), ((pieces, cols, tok), BF16),
            ((pieces, cols, quarter), BF16), ((2, pieces, cols, quarter), BF16), ((pieces, cols, quarter), BF16),
            ((4, *grid, CORES, cols, vt), BF16), ((tok, width), BF16), ((n_block, block, tok), BF16),
            ((2, tok, vt), F32), ((2, tok, vt), F32), ((2, 2, tok, vt), BF16), ((tok, LANE), F32), ((tok, LANE), F32), ((tok, LANE), F32),
            ((tok, LANE), I32), ((2 * n + CORES, 1, width), F32), ((n, 2, tok), F32),
        ], dims["front_sems"][0], dims["front_sems"][1]),
        compiler_params=params(0, limit),
    )(shard, tok_row, lab_row, w, h, g)


def back_kernel(
    dims,
    gain_ref, loss_ref, tokc, dz_hbm, dzp_hbm, et_hbm, xnt_hbm, xpar_hbm, gt_hbm, gpar_hbm, h_hbm,
    tail_out, dh_out, de_out, ra_hbm, rx_hbm,
    dz_own, dz_par, et_buf, part, fx, acc, fa, f2, r2, xb, h_buf, dh_buf, dg_acc, slots,
    sends, recvs, local_sems,
):
    n, tok, vocab, width, tile, vt = (dims[k] for k in ("n", "tok", "vocab", "width", "tile", "vt"))
    place = Place(n, sends, recvs, local_sems)
    x, z, y, c = place.x, place.z, place.y, place.c
    half_v = vocab // CORES
    n_tile, n_half = vocab // vt, half_v // vt
    lanes = half_v // 2
    rows = width // (n * n)
    half_rows = rows // 2
    quarter = tok // n
    hq = quarter // 2
    tiles = dims["tiles"]
    chunks = len(tiles)
    edges = [sum(tiles[:d]) for d in range(chunks + 1)]
    per_half = n_half // 2

    with scope("b_enter"):
        place.enter()

    load_h = place.local("h", h_hbm.at[span(x * quarter, quarter, quarter)], h_buf)

    def load_et(t, slot):
        return place.local("et", et_hbm.at[:, span(t * tile, tile, tile)], et_buf.at[slot], slot)

    slot_of = {FAR: 0, 1: 1, 3: 2, 0: 0}
    stages = dims["stages"]

    def load_stage(m, i):
        half, k, kind = stages[m]
        src = ((gt_hbm, gpar_hbm), (xnt_hbm, xpar_hbm))[kind][i]
        src = src.at[(z + k) % n] if half == 0 else src.at[:, (y + k) % n]
        return place.local(("xb", i), src, xb.at[m % 2, i], m % 2)

    def start_stage(m):
        if m < len(stages):
            start_all(load_stage(m, i) for i in BOTH)

    loads = [place.local("dz", dz_hbm, dz_own), place.local("dzp", dzp_hbm, dz_par)]
    load_et(0, 0).start()
    start_all(loads)
    for m in BOTH:
        start_stage(m)
    load_h.start()

    def columns(d):
        return pl.ds(edges[d] * tile, tiles[d] * tile)

    def dxn_chunk(d):
        def body(t, carry):
            slot = t % 2

            @pl.when(t + 1 < edges[chunks])
            def _():
                load_et(t + 1, 1 - slot).start()

            load_et(t, slot).wait()
            left = jnp.concatenate([dz_own[j] for j in range(n_tile)], axis=1)
            right = jnp.concatenate([et_buf[slot, j] for j in range(n_tile)], axis=1)
            part[:, span(t * tile, tile, tile)] = lax.dot_general(
                left, right, (((1,), (1,)), ((), ())), preferred_element_type=F32)
            return carry

        with scope("b_dxn"):
            lax.fori_loop(edges[d], edges[d + 1], body, 0)

    def qrow(k, lo=0, size=hq):
        return span((x + k) % n * quarter + lo, size, SUB)

    def x_far(d, i):
        return place.send(("xf", d, i), part.at[qrow(FAR, i * hq), columns(d)], fx.at[i, :, columns(d)], dx=WAYS[i])

    def x_near(d, i, j):
        src = part.at[qrow(WAYS[i], j * hq), columns(d)]
        return place.send(("xn", d, i, j), src, rx_hbm.at[i, pl.ds(j * hq, hq), columns(d)], dx=WAYS[i])

    def x_first(d):
        start_all(x_far(d, i) for i in BOTH)

    def x_second(d):
        with scope("b_x2"):
            for i in BOTH:
                x_far(d, i).wait_recv()
                sel = qrow(WAYS[i], i * hq)
                part[sel, columns(d)] = part[sel, columns(d)] + fx[i, :, columns(d)]
                start_all(x_near(d, i, j) for j in BOTH)

    def stage_x(d, j, i):
        return place.local("sx", rx_hbm.at[i, pl.ds(j * hq, hq), columns(d)], fx.at[i, :, columns(d)], i)

    def x_third(d, j):
        with scope("b_x3"):
            for i in BOTH:
                x_near(d, i, j).wait_recv()
                stage_x(d, j, i).start()
            for i in BOTH:
                stage_x(d, j, i).wait()
            sel = qrow(0, j * hq)
            part[sel, columns(d)] = part[sel, columns(d)] + fx[0, :, columns(d)] + fx[1, :, columns(d)]

    def de_stage(half, k, kind):
        m = stages.index((half, k, kind))
        slot = slot_of[k]

        wide = min(2, per_half) if k == FAR or kind and k else 1

        def right(i, t):
            if kind:
                return dz_par[t] if i else dz_own[c * n_half + t]
            ids = lax.broadcasted_iota(I32, (tok, LANE), 1) + (x * vocab + c * half_v + t * vt)
            hits = [jnp.where(tokc[i] == ids + b, dims["scale"], 0.0).astype(BF16) for b in range(0, vt, LANE)]
            return jnp.concatenate(hits, axis=1)

        def body(j, carry):
            t = half * per_half + j * wide
            sel = span(j * wide * vt, wide * vt)
            left = jnp.concatenate([xb[m % 2, i].reshape(n * rows, tok) for i in BOTH], axis=1)
            both_right = [jnp.concatenate([right(i, t + q) for i in BOTH], axis=0) for q in range(wide)]
            total = jnp.dot(left, jnp.concatenate(both_right, axis=1), preferred_element_type=F32)
            total = total.reshape(n, rows, wide * vt)
            acc[half, slot, :, :, sel] = acc[half, slot, :, :, sel] + total if kind else total
            return carry

        with scope("b_de" if kind else "b_look"):
            for i in BOTH:
                load_stage(m, i).wait()
            lax.fori_loop(0, per_half // wide, body, 0)
            start_stage(m + 2)

    def de_unit(half, k):
        for kind in BOTH:
            de_stage(half, k, kind)

    def ring(half, k):
        return {"dz": k} if half == 0 else {"dy": k}

    def cross(half, k):
        return {"dy": k} if half == 0 else {"dz": k}

    def a_far(half, i):
        return place.send(("af", half, i), acc.at[half, 0, pl.ds(2 * i, 2)], fa.at[half, i], **ring(half, WAYS[i]))

    def a_near(half, i, j):
        sel = pl.ds(2 * j, 2)
        return place.send(("an", half, i, j), acc.at[half, 1 + i, sel], ra_hbm.at[half, i, sel], **ring(half, WAYS[i]))

    def a_first(half):
        start_all(a_far(half, i) for i in BOTH)

    def a_second(half, i):
        with scope("b_a2"):
            a_far(half, i).wait_recv()
            sel = pl.ds(2 * i, 2)
            acc[half, 1 + i, sel] = acc[half, 1 + i, sel] + fa[half, i]
            start_all(a_near(half, i, j) for j in BOTH)

    def stage_a(half, j, i):
        return place.local(("sa", half), ra_hbm.at[half, i, pl.ds(2 * j, 2)], fa.at[half, i], i)

    def piece(half, k):
        return ((y if half == 0 else z) + k) % n

    def c_far(half, i):
        src = acc.at[half, 0, piece(half, FAR), pl.ds(i * half_rows, half_rows)]
        return place.send(("cf", half, i), src, f2.at[half, i], **cross(half, WAYS[i]))

    def c_near(half, i):
        return place.send(("cn", half, i), acc.at[half, 0, piece(half, WAYS[i])], r2.at[half, i], **cross(half, WAYS[i]))

    def a_third(half, j):
        with scope("b_a3"):
            for i in BOTH:
                a_near(half, i, j).wait_recv()
                stage_a(half, j, i).start()
            for i in BOTH:
                stage_a(half, j, i).wait()
            sel = pl.ds(2 * j, 2)
            acc[half, 0, sel] = acc[half, 0, sel] + fa[half, 0] + fa[half, 1]

    def c_first(half):
        start_all(c_far(half, i) for i in BOTH)

    def c_second(half):
        with scope("b_c2"):
            for i in BOTH:
                c_far(half, i).wait_recv()
                at = piece(half, WAYS[i])
                sel = pl.ds(i * half_rows, half_rows)
                acc[half, 0, at, sel] = acc[half, 0, at, sel] + f2[half, i]
                c_near(half, i).start()

    def out_copies(half):
        sel = span(c * half_v + half * lanes, lanes)
        mine = acc.at[half, 0, piece(half, 0)]
        yield place.local("de", mine.at[span(c * half_rows, half_rows, SUB)], de_out.at[:, sel], half)
        yield place.send(("de", half), mine.at[span((1 - c) * half_rows, half_rows, SUB)], de_out.at[:, sel], dc=1)

    def c_third(half):
        with scope("b_c3"):
            for i in BOTH:
                c_near(half, i).wait_recv()
            at = piece(half, 0)
            acc[half, 0, at] = acc[half, 0, at] + r2[half, 0] + r2[half, 1]
            start_all(out_copies(half))

    step = min(32, hq)

    def dh_body(i, carry):
        sel = span(i * step, step, step)
        row = span(x * quarter + i * step, step, step)
        d_x = part[row]
        h_wide = h_buf[sel].astype(F32)
        inv_rms = lax.rsqrt(jnp.sum(h_wide * h_wide, axis=1, keepdims=True) * (1.0 / width) + NORM_EPS)
        h_norm = h_wide * inv_rms
        g_dir = d_x * gain_ref[0:1]
        mean = jnp.sum(g_dir * h_norm, axis=1, keepdims=True) * (1.0 / width)
        dh_buf[sel] = (inv_rms * (g_dir - h_norm * mean)).astype(BF16)
        prod = d_x * h_norm
        total = prod[0:SUB]
        for j in range(SUB, step, SUB):
            total = total + prod[j:j + SUB]
        dg_acc[...] = dg_acc[...] + total
        return carry

    def h_first(i, j):
        return place.send(("hf", i, j), dh_buf.at[pl.ds(j * hq, hq)], dh_out.at[qrow(0, j * hq)], dx=WAYS[i])

    def h_second(i):
        ref = dh_out.at[qrow(FROM[i], i * hq)]
        return place.send(("hs", i), ref, ref, dx=WAYS[i])

    keep_dh = place.local("dh", dh_buf, dh_out.at[qrow(0, 0, quarter)])
    small = SmallSum(place, ("dc", "dx", "dy", "dz"), slots)
    per_j = hq // step

    def dh_part(j):
        with scope("b_dh"):
            lax.fori_loop(j * per_j, (j + 1) * per_j, dh_body, 0)
            start_all(h_first(i, j) for i in BOTH)
            if j:
                keep_dh.start()

    def h_passes():
        with scope("b_h2"):
            for i in BOTH:
                h_first(i, i).wait_recv()
                h_second(i).start()

    def small_step(k):
        dims_of = small.dims
        with scope("b_s"):
            if k == 1:
                sums = [jnp.sum(part_sum, axis=0, keepdims=True) for part_sum in (dg_acc[...], loss_ref[...])]
                small.start(dims_of[0], jnp.concatenate(sums, axis=1))
            elif k <= len(dims_of):
                small.start(dims_of[k - 1], small.finish(dims_of[k - 2]))
            else:
                total = small.finish(dims_of[-1])
                loss = jnp.sum(total[:, width:], axis=1, keepdims=True) * (1.0 / dims["total"])
                tail_out[...] = jnp.concatenate([total[:, 0:width], jnp.broadcast_to(loss, (1, LANE))], axis=1)

    def dxn(d):
        dxn_chunk(d)
        x_first(d)

    def unit(half, k):
        if k == 0:
            with scope("b_wait_far"):
                for i in BOTH:
                    a_far(half, i).wait_send()
        de_unit(half, k)
        if k == FAR:
            a_first(half)

    families = {
        "CH": dxn, "XS": x_second, "UN": unit, "AS": a_second, "XT": x_third, "AT": a_third, "CF": c_first, "CS": c_second,
        "CT": c_third, "DH": dh_part, "SM": small_step, "HP": h_passes,
    }

    def perform(text):
        for word in text.split():
            families[word[:2]](*(int(digit) for digit in word[2:]))

    with scope("b_load"):
        loads[0].wait()
        dg_acc[...] = jnp.zeros_like(dg_acc)
        load_h.wait()
    loads[1].wait()
    for text in (
        "CH0 CH1 UN02 UN12", "CH2 XS1 UN03 UN01", "XS2 UN11 AS01 AS00", "UN13 AS11 AS10 XS0",
        "CH3 XT10 XT20 CH4", "XS3 UN10 XS4 UN00", "AT10 AT00 XT30 XT00", "XT11 XT01 XT40 DH0",
        "XT41 XT21 XT31 DH1", "AT01 CF0 AT11 CF1", "SM1 CS0 SM2 CS1", "HP SM3 CT0 SM4", "CT1 SM5",
    ):
        perform(text)

    with scope("b_end_x"):
        keep_dh.wait()
        for i in BOTH:
            for d in range(chunks):
                x_far(d, i).wait_send()
                for j in BOTH:
                    x_near(d, i, j).wait_send()
            h_first(i, i).wait_send()
            h_first(i, 1 - i).wait()
            h_second(i).wait()
    with scope("b_end_a"):
        for half in BOTH:
            for i in BOTH:
                for j in BOTH:
                    a_near(half, i, j).wait_send()
                c_far(half, i).wait_send()
                c_near(half, i).wait_send()
            for copy in out_copies(half):
                copy.wait()
    assert (place.n_link, place.n_local) <= dims["back_sems"], (place.n_link, place.n_local)


def back(dims, limit, gain, loss, tokc, dz, dzp, et, xnt, xpar, gt, gpar, h):
    n, tok, vocab, width, tile = (dims[k] for k in ("n", "tok", "vocab", "width", "tile"))
    rows = width // (n * n)
    half_v = vocab // CORES
    lanes = half_v // 2
    quarter = tok // n
    hq = quarter // 2
    tail_w = width + loss.shape[1]
    n_tile, n_half, vt = dz.shape[0], dzp.shape[0], dims["vt"]
    turned = [a.reshape(n, n, rows, tok) for a in (xnt, xpar, gt, gpar)]
    return pl.pallas_call(
        functools.partial(back_kernel, dims),
        name="back",
        out_shape=shapes([
            ((1, width + LANE), F32), ((tok, width), BF16), ((rows // CORES, vocab), F32), ((2, 2, n, rows, lanes), F32),
            ((2, quarter, width), F32),
        ]),
        in_specs=specs(3, 8),
        out_specs=tuple(specs(1, 4)),
        scratch_shapes=scratch([
            ((n_tile, tok, vt), BF16), ((n_half, tok, vt), BF16), ((2, n_tile, tile, vt), BF16), ((tok, width), F32),
            ((2, hq, width), F32), ((2, 3, n, rows, lanes), F32), ((2, 2, 2, rows, lanes), F32),
            ((2, 2, rows // 2, lanes), F32), ((2, 2, rows, lanes), F32), ((2, CORES, n, rows, tok), BF16), ((quarter, width), BF16),
            ((quarter, width), BF16), ((SUB, width), F32), ((3 * n + CORES, 1, tail_w), F32),
        ], dims["back_sems"][0], dims["back_sems"][1]),
        compiler_params=params(1, limit),
    )(gain, loss, tokc, dz, dzp, et.reshape(n_tile, width, vt), *turned, h)[:3]


def finish_kernel(
    n, scale, table_ref, tail_ref, x0_hbm, dh_hbm, de_hbm, dg_out, loss_out, x0_out, dh_out, de_out,
    x0_in, x0_buf, rows_ref, dh_buf, de_buf, sems,
):
    place = Place(n, None, None, sems)
    quarter, cols, width = x0_in.shape[3], x0_in.shape[2], x0_buf.shape[2]

    def step(q):
        rows = span(q * quarter, quarter, quarter)
        return (
            place.local("x0", x0_hbm.at[q], x0_in.at[q], q, n), place.local("x0o", x0_buf.at[q], x0_out.at[rows], q, n),
            place.local("dh", dh_hbm.at[rows], dh_buf.at[q], q, n), place.local("dho", dh_buf.at[q], dh_out.at[rows], q, n),
        )

    moves = [step(q) for q in range(n)]
    de_in, de_put = place.local("de", de_hbm, de_buf, 0), place.local("de", de_buf, de_out, 1)
    for x0_load, _, dh_load, _ in moves:
        x0_load.start()
        dh_load.start()
    de_in.start()
    gain = jnp.broadcast_to(tail_ref[:, 0:width], (SUB, width))
    dg_out[...] = pltpu.roll(gain, width - place.f * cols, axis=1)[0:1, 0:cols]
    loss_out[...] = tail_ref[:, width:width + 1]

    def body(q, carry):
        x0_load, x0_put, dh_load, dh_put = step(q)
        x0_load.wait()
        for zi in range(n):
            for yi in range(n):
                for h in BOTH:
                    dz, dy = (zi - place.z) % n, (yi - place.y) % n
                    k1, k2 = (dy, dz) if h == 0 else (dz, dy)
                    piece = table_ref[(h * n + k1) * n + k2]
                    rows_ref[pl.ds(((zi * n + yi) * CORES + h) * cols, cols)] = x0_in[q, piece]
        x0_buf[q] = (rows_ref[...].T.astype(F32) * scale).astype(BF16)
        x0_put.start()
        dh_load.wait()
        dh_put.start()
        return carry

    lax.fori_loop(0, n, body, 0)
    de_in.wait()
    de_put.start()
    for _, x0_put, _, dh_put in moves:
        x0_put.wait()
        dh_put.wait()
    de_put.wait()


def finish(n, scale, limit, tail, x0, dh, de):
    _, pieces, cols, quarter = x0.shape
    width = pieces * cols
    table = np.zeros((CORES, n, n), np.int32)
    for u, unit in enumerate(UNITS):
        for h in BOTH:
            for i, (k1, k2) in enumerate(unit):
                table[h, k1, k2] = BASE[u] + h * len(unit) + i
    return pl.pallas_call(
        functools.partial(finish_kernel, n, scale),
        name="finish",
        in_specs=[pl.BlockSpec(memory_space=pltpu.SMEM)] + specs(1, 3),
        out_specs=tuple(specs(2, 3)),
        out_shape=shapes([((1, cols), F32), ((1, 1), F32), (dh.shape, BF16), (dh.shape, BF16), (de.shape, F32)]),
        scratch_shapes=[
            pltpu.VMEM(x0.shape, BF16), pltpu.VMEM((n, quarter, width), BF16), pltpu.VMEM((width, quarter), BF16),
            pltpu.VMEM((n, quarter, width), BF16), pltpu.VMEM(de.shape, F32), pltpu.SemaphoreType.DMA((4 * n + 2,)),
        ],
        compiler_params=pltpu.CompilerParams(vmem_limit_bytes=limit),
    )(jnp.asarray(table.reshape(-1)), tail, x0, dh, de)


def solution(mesh):
    return build(mesh, mesh.shape["tp"], 256, digits("12222")[0], 256, 6, 67_000_000)


def build(mesh, n, tile, tiles, vt, n_block, limit):
    fsdp_size = mesh.shape["fsdp"]

    def device_step(emb_shard, tok_ids, lab_ids, h_last, g_embed, norm_w):
        vocab_rows, cols = emb_shard.shape
        batch_loc, seq_len, width = h_last.shape
        tok_count = batch_loc * seq_len
        fsdp_id = lax.axis_index("fsdp")
        scale = float(np.asarray(math.sqrt(width)).astype(jnp.bfloat16))
        dims = {
            "n": n, "tok": tok_count, "vocab": vocab_rows, "width": width, "total": tok_count * fsdp_size, "vt": vt,
            "tile": tile, "tiles": tiles, "scale": scale, "n_block": n_block,
            "stages": digits("020 021 120 121") + digits("030 031 010 011") + digits("110 111 130 131") + digits("100 101 000 001"),
            "front_sems": (110, 42), "back_sems": (68, 22),
        }
        h_flat = h_last.reshape(tok_count, width)
        placed = lax.dynamic_update_slice(jnp.zeros((SUB, width), F32), jnp.broadcast_to(norm_w, (SUB, cols)), (0, fsdp_id * cols))
        ids = [a.reshape(1, tok_count) for a in (tok_ids, lab_ids)]
        table, xn_t, xpar_t, g_t, gpar_t, dz, dzp, x0, _, gain, loss_part, tokc = front(
            dims, limit, emb_shard.T, *ids, norm_w.reshape(1, cols), h_flat, g_embed.reshape(tok_count, width))
        tail, d_hidden, d_cols = back(dims, limit, gain, loss_part, tokc, dz, dzp, table, xn_t, xpar_t, g_t, gpar_t, h_flat)
        d_norm_w, loss, x_emb, d_hidden, d_cols = finish(n, scale, limit, tail, x0, d_hidden, d_cols)
        return (x_emb.reshape(h_last.shape), loss.reshape(()), d_hidden.reshape(h_last.shape), d_norm_w.reshape(cols), d_cols.T)

    spec_tok = P("fsdp", None)
    spec_act = P("fsdp", None, None)
    return jax.shard_map(device_step, mesh=mesh, in_specs=(P("tp", "fsdp"), spec_tok, spec_tok, spec_act, spec_act, P("fsdp")), out_specs=(spec_act, P(), spec_act, P("fsdp"), P("tp", "fsdp")), check_vma=False)
```

```python
import functools
import math
import jax
import numpy as np
import jax.numpy as jnp
from jax import lax
from jax.experimental import pallas as pl
from jax.experimental.pallas import tpu as pltpu
from jax.sharding import PartitionSpec as P

SOFT_CAP = 30.0
NORM_EPS = 1e-6
F32, BF16, I32 = jnp.float32, jnp.bfloat16, jnp.int32
LANE, SUB = 128, 8
BOTH = (0, 1)
FOUR = range(4)
WAYS = (1, 3)
FROM = (3, 1)
FAR = 2
CORES = 2


def span(start, size, unit=LANE):
    return pl.ds(pl.multiple_of(start, unit), size)


class Place:
    def __init__(self, n, sends, recvs, local_sems):
        self.n, self.sends, self.recvs, self.local_sems = n, sends, recvs, local_sems
        self.x = lax.axis_index("tp")
        f = lax.axis_index("fsdp")
        self.f = f
        self.c = f % CORES
        self.y = f // CORES % n
        self.z = f // CORES // n
        self.link_of, self.local_of, self.n_link, self.n_local = {}, {}, 0, 0
        self.size = {"dx": n, "dz": n, "dy": n, "dc": CORES}
        self.me = {"dx": self.x, "dz": self.z, "dy": self.y, "dc": self.c}

    def at(self, dx=0, dz=0, dy=0, dc=0):
        n = self.n
        z, y, c = (self.z + dz) % n, (self.y + dy) % n, (self.c + dc) % CORES
        return ((self.x + dx) % n, (z * n + y) * CORES + c)

    def enter(self):
        barrier = pltpu.get_barrier_semaphore()
        peers = [self.at(**{d: k}) for d in self.size for k in range(1, self.size[d])]
        for peer in peers:
            pl.semaphore_signal(barrier, inc=1, device_id=peer, device_id_type=pl.DeviceIdType.MESH)
        pl.semaphore_wait(barrier, len(peers))

    def link(self, key, count=1):
        if key not in self.link_of:
            self.link_of[key] = self.n_link
            self.n_link += count
        return self.link_of[key]

    def send(self, key, src, dst, **step):
        i = self.link(key)
        return pltpu.make_async_remote_copy(
            src, dst, self.sends.at[i], self.recvs.at[i], device_id=self.at(**step), device_id_type=pl.DeviceIdType.MESH)

    def local(self, key, src, dst, slot=0, count=2):
        if key not in self.local_of:
            self.local_of[key] = self.n_local
            self.n_local += count
        return pltpu.make_async_copy(src, dst, self.local_sems.at[self.local_of[key] + slot])


class SmallSum:
    def __init__(self, place, dims, slots):
        self.place, self.slots, self.dims, self.base = place, slots, dims, {}
        count = 0
        for d in dims:
            self.base[d] = count
            count += place.size[d]

    def copies(self, d):
        slot = self.slots.at[self.base[d] + self.place.me[d]]
        for k in range(1, self.place.size[d]):
            yield self.place.send((self.dims, d, k), slot, slot, **{d: k})

    def start(self, d, value):
        self.slots[self.base[d] + self.place.me[d]] = value
        for copy in self.copies(d):
            copy.start()

    def finish(self, d):
        for copy in self.copies(d):
            copy.wait()
        total = self.slots[self.base[d]]
        for k in range(1, self.place.size[d]):
            total = total + self.slots[self.base[d] + k]
        return total


def scope(name):
    return jax.named_scope(name)


def start_all(copies):
    for copy in copies:
        copy.start()


def digits(text):
    return tuple(tuple(int(d) for d in word) for word in text.split())


UNITS = [digits(u) for u in ("00", "10 30", "01 03 20", "02 11 31", "13 33 21 23", "12 32 22")]
PAIR, ALL = 1, "all"
PIECES = [2 * len(u) for u in UNITS]
EXP_RATE = SOFT_CAP * math.log2(math.e)
BASE = [sum(PIECES[:i]) for i in range(len(UNITS))]


def front_kernel(
    dims,
    shard_ref, tok_ref, lab_ref, w_ref, h_hbm, g_hbm,
    et_out, xnt_out, xpar_out, gt_out, gpar_out, lt_out, dz_out, dzpar_out, x0_out, u_hbm, gain_out, loss_out, tokc_out,
    shard_t, chunk, tokr, hit_t, lhs, xp, xw, xr, xf, xg, xq, etb, xn, gl, z_even, z_odd, dzb,
    acc_e, acc_l, inv_s, labc, w_slots, s_slots, sends, recvs, local_sems,
):
    n, tok, vocab, width, vt = dims["n"], dims["tok"], dims["vocab"], dims["width"], dims["vt"]
    place = Place(n, sends, recvs, local_sems)
    x, z, y, c = place.x, place.z, place.y, place.c
    half_v = vocab // CORES
    n_tile = vocab // vt
    n_half = n_tile // CORES
    hh = n_half // 2
    cols = width // (n * n * CORES)
    quarter = tok // n
    row_start = x * vocab

    def ring1(h, k):
        return {"dy": k} if h == 0 else {"dz": k}

    def ring2(h, k):
        return {"dz": k} if h == 0 else {"dy": k}

    def coord(base, k, paired):
        every = slice(None)
        if k == ALL:
            return every, every
        return every if paired else (base + k) % n // 2, (base + k) % 2

    def loc(h, k1, k2, lo=0, size=n_half, pair1=False, pair2=False):
        first, second = coord((y, z)[h], k1, pair1), coord((z, y)[h], k2, pair2)
        return et_out.at[(pl.ds(c * n_half + lo, size), *((second, first)[h]), *((first, second)[h]), h)]

    with scope("f_enter"):
        place.enter()

    load_g = place.local("g", g_hbm, xn)
    load_g.start()
    with scope("f_cast"):
        for t in range(n_tile):
            shard_t[t] = shard_ref[:, pl.ds(t * vt, vt)].astype(BF16)
        tokr[c] = jnp.broadcast_to(tok_ref[...], (SUB, tok))
        give_tok = place.send("tok", tokr.at[c], tokr.at[c], dc=1)
        give_chunk = place.send("chunk", shard_t.at[pl.ds((1 - c) * n_half, n_half)], chunk.at[c], dc=1)
        give_chunk.start()
        give_tok.start()
        chunk[c] = shard_t[pl.ds(c * n_half, n_half)]
        gain_sum = SmallSum(place, ("dc", "dy", "dz"), w_slots)
        own_w = jnp.concatenate([w_ref[...], jnp.zeros((1, width - cols), F32)], axis=1)
        gain_sum.start("dc", pltpu.roll(jnp.broadcast_to(own_w, (SUB, width)), place.f * cols, axis=1)[0:1])

    def p1_send(h, i):
        return place.send(("p1", h, i), chunk.at[h], loc(h, 0, 0), **ring1(h, WAYS[i]))

    def p1_fwd(h, i):
        ref = loc(h, FROM[i], 0, i * hh, hh)
        return place.send(("p1f", h, i), ref, ref, **ring1(h, WAYS[i]))

    def p2_send(h, k1, i):
        ref = loc(h, k1, 0, pair1=k1 == PAIR)
        return place.send(("p2", h, k1, i), chunk.at[h] if k1 == 0 else ref, ref, **ring2(h, WAYS[i]))

    def p2_fwd(h, k1, i):
        ref = loc(h, k1, FROM[i], i * hh, hh, pair1=k1 == PAIR)
        return place.send(("p2f", h, k1, i), ref, ref, **ring2(h, WAYS[i]))

    def keep(h):
        return place.local("keep", chunk.at[h], loc(h, 0, 0), h)

    def share(h, k2):
        ref = loc(h, ALL, k2, pair2=k2 == PAIR)
        return place.send(("share", h, k2), ref, ref, dc=1)

    def pass_first():
        with scope("f_p1"):
            for h in BOTH:
                for i in BOTH:
                    p1_send(h, i).wait_recv()
                    p1_fwd(h, i).start()
            for h in BOTH:
                start_all(p2_send(h, PAIR, i) for i in BOTH)

    def pass_first_far():
        with scope("f_p1f"):
            for h in BOTH:
                for i in BOTH:
                    p1_fwd(h, i).wait_recv()
                start_all(p2_send(h, FAR, j) for j in BOTH)

    def pass_second(k1):
        with scope("f_p2"):
            for h in BOTH:
                for i in BOTH:
                    p2_send(h, k1, i).wait_recv()
                    p2_fwd(h, k1, i).start()

    def end_second(k1):
        with scope("f_p2f"):
            for h in BOTH:
                for i in BOTH:
                    p2_fwd(h, k1, i).wait_recv()

    def share_group(k2):
        start_all(share(h, k2) for h in BOTH)

    with scope("f_chunk"):
        give_chunk.wait_recv()
        start_all(keep(h) for h in BOTH)
        gain_sum.start("dy", gain_sum.finish("dc"))
        for h in BOTH:
            start_all(p1_send(h, i) for i in BOTH)
        for h in BOTH:
            start_all(p2_send(h, 0, i) for i in BOTH)

    v_step = min(LANE, half_v)

    def hit_body(j, carry):
        off = j * v_step
        ids = lax.broadcasted_iota(I32, (v_step, tok), 0) + (row_start + c * half_v + off)
        for i, core in enumerate((c, 1 - c)):
            hit_t[span(off, v_step, v_step), pl.ds(i * tok, tok)] = jnp.where(ids == tokr[core, 0:1, :], 1.0, 0.0).astype(BF16)
        return carry

    def make_hits():
        with scope("f_hit"):
            give_tok.wait_recv()
            lax.fori_loop(0, half_v // v_step, hit_body, 0)

    n_step = min(512, tok)
    most = max(PIECES)

    def whole(u):
        return pl.ds(BASE[u], PIECES[u])

    def unit_copies(u):
        slot = u % 2
        for p, (h, (k1, k2)) in enumerate((h, k) for h in BOTH for k in UNITS[u]):
            yield place.local("lhs", loc(h, k1, k2), lhs.at[slot, p], slot * most + p, 2 * most)

    def load_unit(u):
        start_all(unit_copies(u))

    def look(u):
        pieces = PIECES[u]
        with scope("f_look"):
            if u > 1:
                x_swap(u - 2).wait_send()
            left = lhs.at[u % 2]
            for copy in unit_copies(u):
                copy.wait()
            per_core = tok // n_step

            def body(j, carry):
                value = jnp.concatenate([left[pl.ds(0, pieces), t].reshape(pieces * cols, vt) for t in range(n_half)], axis=1)
                rows = jnp.dot(value, hit_t[:, span(j * n_step, n_step)], preferred_element_type=F32)
                rows = rows.reshape(pieces, cols, n_step).astype(BF16)
                xw[u % 2, j // per_core, pl.ds(0, pieces), :, span(j % per_core * n_step, n_step)] = rows
                return carry

            lax.fori_loop(0, CORES * per_core, body, 0)
            x_swap(u).start()

    def x_swap(u):
        return place.send(("swap", u), xw.at[u % 2, 1, pl.ds(0, PIECES[u])], xr.at[whole(u)], dc=1)

    def lanes_of(k):
        return span((x + k) % n * quarter, quarter, quarter)

    def side(u, i):
        return pl.ds(BASE[u] + i * len(UNITS[u]), len(UNITS[u]))

    def x_far(u, i):
        return place.send(("xf", u, i), xp.at[side(u, i), :, lanes_of(FAR)], xf.at[side(u, i)], dx=WAYS[i])

    def x_near(u, i):
        return place.send(("xn", u, i), xp.at[whole(u), :, lanes_of(WAYS[i])], xg.at[i, whole(u)], dx=WAYS[i])

    def x_goal(k, sel):
        return x0_out.at[(x + k) % n, sel]

    def x_put(u, i):
        return place.send(("xp", u, i), xq.at[whole(u)], x_goal(0, whole(u)), dx=WAYS[i])

    def x_keep(u):
        return place.local("x0", xq.at[whole(u)], x_goal(0, whole(u)), u, len(UNITS))

    def x_pass(u, i):
        ref = x_goal(FROM[i], side(u, i))
        return place.send(("xs", u, i), ref, ref, dx=WAYS[i])

    def x_first(u):
        with scope("f_x1"):
            x_swap(u).wait_recv()
            def body(p, carry):
                xp[BASE[u] + p] = xw[u % 2, 0, p] + xr[BASE[u] + p]
                return carry

            lax.fori_loop(0, PIECES[u], body, 0)
            start_all(x_far(u, i) for i in BOTH)

    def x_second(u):
        with scope("f_x2"):
            for i in BOTH:
                x_far(u, i).wait_recv()
                sel, lanes = side(u, i), lanes_of(WAYS[i])
                xp[sel, :, lanes] = xp[sel, :, lanes] + xf[sel]
                x_near(u, i).start()

    def x_third(u):
        with scope("f_x3"):
            for i in BOTH:
                x_near(u, i).wait_recv()
            sel = whole(u)
            xq[sel] = xp[sel, :, lanes_of(0)] + xg[0, sel] + xg[1, sel]
            start_all(x_put(u, i) for i in BOTH)
            x_keep(u).start()

    def x_fourth(u):
        with scope("f_x4"):
            for i in BOTH:
                x_put(u, i).wait_recv()
                x_pass(u, i).start()

    n_part = n * n * CORES // 2

    def moves(key, part, whole_t, other):
        sel = pl.ds(part * n_part, n_part)
        yield place.local(key, gl.at[sel], whole_t.at[sel], part)
        yield place.send((key, part), gl.at[sel], other.at[sel], dc=1)

    def move_g(part):
        return moves("g", part, gt_out, gpar_out)

    def move_xn(part):
        return moves("xt", part, xnt_out, xpar_out)

    def transpose_part(part, copies):
        block = width // dims["n_block"]
        first = part * dims["n_block"] // 2
        turned = [xn[:, pl.ds((first + j) * block, block)].T for j in range(dims["n_block"] // 2)]
        gl[pl.ds(part * n_part, n_part)] = jnp.concatenate(turned, axis=0).reshape(n_part, cols, tok)
        start_all(copies)

    def columns(row):
        return jnp.broadcast_to(row.astype(F32), (LANE, tok)).T.astype(I32)

    r_step = min(LANE, tok)

    def xn_body(j, carry):
        sel = span(j * r_step, r_step, r_step)
        h_wide = xn[sel].astype(F32)
        inv_rms = lax.rsqrt(jnp.sum(h_wide * h_wide, axis=1, keepdims=True) * (1.0 / width) + NORM_EPS)
        xn[sel] = (h_wide * inv_rms * gain_out[0:1]).astype(BF16)
        return carry

    e_step = min(LANE, tok)

    def tile_of(j):
        return (c * n_half + j) % n_tile

    def load_tile(j):
        return place.local("et", et_out.at[tile_of(j)], etb.at[j % 4], j % 4, 4)

    def save_u(i, odd):
        return place.local(("u", odd), (z_even, z_odd)[odd].at[i % 2], u_hbm.at[tile_of(2 * i + odd)], i % 2)

    def lane_blocks():
        return [(b, pl.ds(b, LANE)) for b in range(0, vt, LANE)]

    def post_tile(i, odd):
        base = tile_of(2 * i + odd) * vt
        buf, slot = (z_even, z_odd)[odd], i % 2

        def body(e, carry):
            sel = span(e * e_step, e_step, e_step)
            ids = lax.broadcasted_iota(I32, (e_step, LANE), 1) + base
            sum_e, sum_l = acc_e[sel], acc_l[sel]
            for b, lanes in lane_blocks():
                tanh_z = jnp.tanh(buf[slot, sel, lanes] * (1.0 / SOFT_CAP))
                buf[slot, sel, lanes] = tanh_z
                sum_e = sum_e + jnp.exp2(EXP_RATE * tanh_z - EXP_RATE)
                sum_l = sum_l + jnp.where(ids + b == labc[sel], tanh_z, 0.0)
            acc_e[sel] = sum_e
            acc_l[sel] = sum_l
            return carry

        lax.fori_loop(0, tok // e_step, body, 0)

    def dot_pair(i):
        for odd in BOTH:
            value = etb[(2 * i + odd) % 4].reshape(width, vt)
            (z_even, z_odd)[odd][i % 2] = jnp.dot(xn[...], value, preferred_element_type=F32)

    def load_pair(i):
        start_all(load_tile(2 * i + odd) for odd in BOTH)

    def pair(i, carry):
        for odd in BOTH:
            load_tile(2 * i + odd).wait()

        @pl.when(i > 1)
        def _():
            for odd in BOTH:
                save_u(i - 2, odd).wait()

        for odd in BOTH:
            post_tile(i - 1, odd)
            save_u(i - 1, odd).start()
        dot_pair(i)

        @pl.when(i + 2 < n_tile // 2)
        def _():
            load_pair(i + 2)

        for k, work in enumerate(during):
            @pl.when(i == k + 1)
            def _():
                if k == 0:
                    wait_shares()
                perform(work)
        return carry

    def wait_shares():
        with scope("f_share"):
            for h in BOTH:
                for k2 in (0, PAIR, FAR):
                    share(h, k2).wait_recv()

    def logits_first():
        acc_e[...] = jnp.zeros_like(acc_e)
        acc_l[...] = jnp.zeros_like(acc_l)
        with scope("f_logits0"):
            for i in BOTH:
                load_pair(i)
            far_ends(1)
            for odd in BOTH:
                load_tile(odd).wait()
            dot_pair(0)
            if n_tile // 2 > 2:
                load_pair(2)

    def lay_columns():
        with scope("f_cols"):
            labc[...] = columns(lab_ref[...] - row_start)
            for i, core in enumerate((c, 1 - c)):
                tokc_out[i] = columns(tokr[core, 0:1, :])

    def turn_g():
        with scope("f_gt"):
            load_g.wait()
            for part in BOTH:
                transpose_part(part, move_g(part))
            load_h.start()

    def gain_next():
        with scope("f_gain2"):
            gain_sum.start("dz", gain_sum.finish("dy"))

    def normalize():
        with scope("f_xn"):
            gain_out[...] = 1.0 + gain_sum.finish("dz")
            load_h.wait()
            lax.fori_loop(0, tok // r_step, xn_body, 0)

    def turn_xn():
        with scope("f_xt"):
            for part in BOTH:
                transpose_part(part, move_xn(part))

    spare = BASE[3]
    own_rows, their_rows = (pl.ds(spare + i * 2 * n, 2 * n) for i in BOTH)

    def far_loads(h):
        for i, (src, rows) in enumerate(((gt_out, own_rows), (gpar_out, their_rows))):
            if h == 0:
                yield place.local("far", src.at[pl.ds((z + FAR) % n * 2 * n, 2 * n)], xp.at[rows], i * n, 2 * n)
            else:
                for q in range(n):
                    piece = src.at[pl.ds((q * n + (y + FAR) % n) * 2, 2)]
                    yield place.local("far", piece, xp.at[pl.ds(spare + i * 2 * n + 2 * q, 2)], i * n + q)

    def far_load(h):
        if h == 0:
            for part in BOTH:
                for copy in move_g(part):
                    copy.wait()
        start_all(far_loads(h))

    def put_far(h, j):
        rows = pl.ds(0, 2 * n * cols)
        return place.local("lt", z_even.at[j % 2, rows], lt_out.at[h, :, span(j * vt, vt)], j % 2)

    def far_ends(h):
        for j in range(hh - 2, hh):
            put_far(h, j).wait()

    def far_look(h):
        def body(j, carry):
            @pl.when(j > 1)
            def _():
                put_far(h, j - 2).wait()

            left = jnp.concatenate([xp[rows].reshape(2 * n * cols, tok) for rows in (own_rows, their_rows)], axis=1)
            right = hit_t[span((h * hh + j) * vt, vt)]
            value = lax.dot_general(left, right, (((1,), (1,)), ((), ())), preferred_element_type=F32)
            z_even[j % 2, pl.ds(0, 2 * n * cols)] = value * dims["scale"]
            put_far(h, j).start()
            return carry

        with scope("f_far"):
            for copy in far_loads(h):
                copy.wait()
            if h:
                far_ends(0)
            lax.fori_loop(0, hh, body, 0)

    def begin_unit(u):
        if u == 0:
            for h in BOTH:
                keep(h).wait()
        load_unit(u)

    load_h = place.local("h", h_hbm, xn)
    works = {
        "HIT": make_hits, "GT": turn_g, "COL": lay_columns, "G2": gain_next, "XN": normalize, "XT": turn_xn, "L0": logits_first,
        "PF": pass_first, "PFF": pass_first_far,
    }
    groups = {"0": 0, "P": PAIR, "F": FAR}
    families = {"LF": far_load, "FL": far_look, "LU": begin_unit, "LK": look, "X1": x_first, "X2": x_second, "X3": x_third, "X4": x_fourth}
    families_k = {"SH": share_group, "S": pass_second, "E": end_second}

    def perform(text):
        for word in text.split():
            if word in works:
                works[word]()
            elif word[:-1] in families:
                families[word[:-1]](int(word[-1]))
            else:
                families_k[word[:-1]](groups[word[-1]])

    during = (
        "X41 X15 X42",
        "X24 X33",
        "",
        "",
        "X25",
        "",
        "",
    )
    for text in (
        "LU0 GT G2 HIT", "PF LU1 LK0 LF0", "LK1 X10 XN FL0", "X20 XT LF1 S0", "PFF X11 LU2 X30",
        "LK2 X21 FL1 SH0", "SP E0 X40 LU3", "X12 X31 LK3 SF", "LU4 X22 COL SHP", "LK4 EP X13 X32",
        "EF LU5 SHF L0", "X23 LK5 X14",
    ):
        perform(text)
    if n_half < 4:
        wait_shares()
        for text in during:
            perform(text)
        during = ()
    last = n_tile // 2 - 1
    with scope("f_logits"):
        lax.fori_loop(1, last + 1, pair, 0)
        for odd in BOTH:
            post_tile(last, odd)
            save_u(last, odd).start()

    with scope("f_stats"):
        row = lax.broadcasted_iota(I32, (2, tok), 0)
        sum_e = jnp.sum(acc_e[...].T, axis=0, keepdims=True)
        sum_l = SOFT_CAP * jnp.sum(acc_l[...].T, axis=0, keepdims=True)
        stats = SmallSum(place, ("dx",), s_slots)
        stats.start("dx", jnp.where(row == 0, sum_e, sum_l))
    perform("X43 X34 X35")
    with scope("f_stats2"):
        stat = stats.finish("dx")
        all_e, all_l = stat[0:1], stat[1:2]
        inv_s[...] = jnp.broadcast_to((1.0 / dims["total"]) / all_e, (LANE, tok)).T
        s_slots[0, 0:1, :] = jnp.log(all_e) + SOFT_CAP - all_l
        own = s_slots[0, 0:1, lanes_of(0)]
        part_w = min(LANE, quarter)
        folded = own[:, 0:part_w]
        for j in range(part_w, quarter, part_w):
            folded = folded + own[:, j:j + part_w]
        loss_out[...] = jnp.where(lax.broadcasted_iota(I32, (SUB, part_w), 0) == 0, folded, 0.0)

    def dz_tile(j):
        return ((1 - c) * n_half + j) % n_tile

    def load_u(i, odd):
        return place.local(("u", odd), u_hbm.at[dz_tile(2 * i + odd)], (z_even, z_odd)[odd].at[i % 2], i % 2)

    def put_dz(i, odd):
        return place.local(("dz", odd), dzb.at[odd, i % 2], dz_out.at[dz_tile(2 * i + odd)], i % 2)

    def give_dz(part):
        src = dz_out.at[pl.ds((1 - c) * n_half + part * hh, hh)]
        return place.send(("dz", part), src, dzpar_out.at[pl.ds(part * hh, hh)], dc=1)

    d_step = min(256, tok)

    def dz_rows(i, odd):
        base = dz_tile(2 * i + odd) * vt
        buf, slot = (z_even, z_odd)[odd], i % 2

        def body(e, carry):
            sel = span(e * d_step, d_step, d_step)
            ids = lax.broadcasted_iota(I32, (d_step, LANE), 1) + base
            for b, lanes in lane_blocks():
                tanh_z = buf[slot, sel, lanes]
                prob = jnp.exp2(EXP_RATE * tanh_z - EXP_RATE) * inv_s[sel]
                prob = jnp.where(ids + b == labc[sel], prob - 1.0 / dims["total"], prob)
                dzb[odd, slot, sel, lanes] = (prob * (1.0 - tanh_z * tanh_z)).astype(BF16)
            return carry

        lax.fori_loop(0, tok // d_step, body, 0)

    def dz_pair(i, carry):
        for odd in BOTH:
            load_u(i, odd).wait()

            @pl.when(i > hh + 1)
            def _():
                put_dz(i - 2, odd).wait()

            dz_rows(i, odd)
            put_dz(i, odd).start()

            @pl.when(i + 2 < n_tile // 2)
            def _():
                load_u(i + 2, odd).start()

        return carry

    with scope("f_dz"):
        for i in range(n_tile // 2 - 2, n_tile // 2):
            for odd in BOTH:
                save_u(i, odd).wait()
        for i in BOTH:
            start_all(load_u(i, odd) for odd in BOTH)
        for part in BOTH:
            lo, hi = part * hh // 2, (part + 1) * hh // 2
            lax.fori_loop(lo, hi, dz_pair, 0)
            for i in range(max(lo, hi - 2), hi):
                for odd in BOTH:
                    put_dz(i, odd).wait()
            give_dz(part).start()
        lax.fori_loop(hh, n_tile // 2, dz_pair, 0)

    perform("X44 X45")
    with scope("f_end"):
        for part in BOTH:
            give_dz(part).wait()
        for i in range(n_tile // 2 - 2, n_tile // 2):
            for odd in BOTH:
                put_dz(i, odd).wait()
        give_tok.wait_send()
        give_chunk.wait_send()
        for h in BOTH:
            for i in BOTH:
                p1_send(h, i).wait_send()
                p1_fwd(h, i).wait_send()
                for k in (0, PAIR, FAR):
                    p2_send(h, k, i).wait_send()
                    p2_fwd(h, k, i).wait_send()
            for k in (0, PAIR, FAR):
                share(h, k).wait_send()
        for part in BOTH:
            for copy in move_xn(part):
                copy.wait()
        for u in range(len(UNITS)):
            if u > len(UNITS) - 3:
                x_swap(u).wait_send()
            x_keep(u).wait()
            for i in BOTH:
                x_far(u, i).wait_send()
                x_near(u, i).wait_send()
                x_put(u, i).wait_send()
                x_pass(u, i).wait()
    assert (place.n_link, place.n_local) <= dims["front_sems"], (place.n_link, place.n_local)


def specs(n_vmem, n_any):
    return [pl.BlockSpec(memory_space=pltpu.VMEM)] * n_vmem + [pl.BlockSpec(memory_space=pl.ANY)] * n_any


def shapes(items):
    return tuple(jax.ShapeDtypeStruct(*item) for item in items)


def scratch(items, n_link, n_local):
    dma = pltpu.SemaphoreType.DMA
    return [pltpu.VMEM(*item) for item in items] + [dma((n_link,)), dma((n_link,)), dma((n_local,))]


def params(collective_id, limit):
    return pltpu.CompilerParams(collective_id=collective_id, has_side_effects=True, vmem_limit_bytes=limit)


def front(dims, limit, shard, tok_row, lab_row, w, h, g):
    n, tok, vocab, width, vt = dims["n"], dims["tok"], dims["vocab"], dims["width"], dims["vt"]
    cols = shard.shape[0]
    half_v = vocab // CORES
    quarter = tok // n
    n_tile, n_half, most = vocab // vt, half_v // vt, max(PIECES)
    pieces = n * n * CORES
    grid = (n // 2, 2, n // 2, 2)
    return pl.pallas_call(
        functools.partial(front_kernel, dims),
        name="front",
        out_shape=shapes([
            ((n_tile, *grid, CORES, cols, vt), BF16), *[((pieces, cols, tok), BF16)] * 4, ((2, 2 * n * cols, half_v // 2), F32), ((n_tile, tok, vt), BF16),
            ((n_half, tok, vt), BF16), ((n, pieces, cols, quarter), BF16), ((n_tile, tok, vt), F32),
            ((1, width), F32), ((SUB, min(LANE, quarter)), F32), ((CORES, tok, LANE), I32),
        ]),
        in_specs=specs(4, 2),
        out_specs=tuple(specs(0, 10) + specs(3, 0)),
        scratch_shapes=scratch([
            ((n_tile, cols, vt), BF16), ((CORES, n_half, cols, vt), BF16), ((CORES, SUB, tok), I32), ((half_v, CORES * tok), BF16),
            ((2, most, n_half, cols, vt), BF16), ((pieces, cols, tok), BF16), ((2, CORES, most, cols, tok), BF16), ((pieces, cols, tok), BF16),
            ((pieces, cols, quarter), BF16), ((2, pieces, cols, quarter), BF16), ((pieces, cols, quarter), BF16),
            ((4, *grid, CORES, cols, vt), BF16), ((tok, width), BF16), ((pieces, cols, tok), BF16),
            ((2, tok, vt), F32), ((2, tok, vt), F32), ((2, 2, tok, vt), BF16), ((tok, LANE), F32), ((tok, LANE), F32), ((tok, LANE), F32),
            ((tok, LANE), I32), ((2 * n + CORES, 1, width), F32), ((n, 2, tok), F32),
        ], dims["front_sems"][0], dims["front_sems"][1]),
        compiler_params=params(0, limit),
    )(shard, tok_row, lab_row, w, h, g)


def back_kernel(
    dims,
    gain_ref, loss_ref, tokc, lt_hbm, dz_hbm, dzp_hbm, et_hbm, xnt_hbm, xpar_hbm, gt_hbm, gpar_hbm, h_hbm,
    tail_out, dh_out, de_out, ra_hbm, rx_hbm,
    dz_own, dz_par, et_buf, part, fx, acc, fa, f2, r2, xb, h_buf, dh_buf, dg_acc, slots,
    sends, recvs, local_sems,
):
    n, tok, vocab, width, tile, vt = (dims[k] for k in ("n", "tok", "vocab", "width", "tile", "vt"))
    place = Place(n, sends, recvs, local_sems)
    x, z, y, c = place.x, place.z, place.y, place.c
    half_v = vocab // CORES
    n_tile, n_half = vocab // vt, half_v // vt
    lanes = half_v // 2
    rows = width // (n * n)
    half_rows = rows // 2
    quarter = tok // n
    hq = quarter // 2
    tiles = dims["tiles"]
    chunks = len(tiles)
    edges = [sum(tiles[:d]) for d in range(chunks + 1)]
    per_half = n_half // 2

    with scope("b_enter"):
        place.enter()

    load_h = place.local("h", h_hbm.at[span(x * quarter, quarter, quarter)], h_buf)

    def load_et(t, slot):
        return place.local("et", et_hbm.at[:, span(t * tile, tile, tile)], et_buf.at[slot], slot)

    slot_of = {FAR: 0, 1: 1, 3: 2, 0: 0}
    stages = dims["stages"]

    def load_stage(m, i):
        half, k, kind = stages[m]
        src = ((gt_hbm, gpar_hbm), (xnt_hbm, xpar_hbm))[kind][i]
        src = src.at[(z + k) % n] if half == 0 else src.at[:, (y + k) % n]
        return place.local(("xb", i), src, xb.at[m % 2, i], m % 2)

    def start_stage(m):
        if m < len(stages):
            start_all(load_stage(m, i) for i in BOTH)

    loads = [place.local("dz", dz_hbm, dz_own), place.local("dzp", dzp_hbm, dz_par)]
    load_et(0, 0).start()
    start_all(loads)
    fars = [place.local("lt", lt_hbm.at[half], acc.at[half, 0], half) for half in BOTH]
    start_all(fars)
    for m in BOTH:
        start_stage(m)
    load_h.start()

    def columns(d):
        return pl.ds(edges[d] * tile, tiles[d] * tile)

    def dxn_chunk(d):
        def body(t, carry):
            slot = t % 2

            @pl.when(t + 1 < edges[chunks])
            def _():
                load_et(t + 1, 1 - slot).start()

            load_et(t, slot).wait()
            left = jnp.concatenate([dz_own[j] for j in range(n_tile)], axis=1)
            right = jnp.concatenate([et_buf[slot, j] for j in range(n_tile)], axis=1)
            part[:, span(t * tile, tile, tile)] = lax.dot_general(
                left, right, (((1,), (1,)), ((), ())), preferred_element_type=F32)
            return carry

        with scope("b_dxn"):
            lax.fori_loop(edges[d], edges[d + 1], body, 0)

    def qrow(k, lo=0, size=hq):
        return span((x + k) % n * quarter + lo, size, SUB)

    def x_far(d, i):
        return place.send(("xf", d, i), part.at[qrow(FAR, i * hq), columns(d)], fx.at[i, :, columns(d)], dx=WAYS[i])

    def x_near(d, i, j):
        src = part.at[qrow(WAYS[i], j * hq), columns(d)]
        return place.send(("xn", d, i, j), src, rx_hbm.at[i, pl.ds(j * hq, hq), columns(d)], dx=WAYS[i])

    def x_first(d):
        start_all(x_far(d, i) for i in BOTH)

    def x_second(d):
        with scope("b_x2"):
            for i in BOTH:
                x_far(d, i).wait_recv()
                sel = qrow(WAYS[i], i * hq)
                part[sel, columns(d)] = part[sel, columns(d)] + fx[i, :, columns(d)]
                start_all(x_near(d, i, j) for j in BOTH)

    def stage_x(d, j, i):
        return place.local("sx", rx_hbm.at[i, pl.ds(j * hq, hq), columns(d)], fx.at[i, :, columns(d)], i)

    def x_third(d, j):
        with scope("b_x3"):
            for i in BOTH:
                x_near(d, i, j).wait_recv()
                stage_x(d, j, i).start()
            for i in BOTH:
                stage_x(d, j, i).wait()
            sel = qrow(0, j * hq)
            part[sel, columns(d)] = part[sel, columns(d)] + fx[0, :, columns(d)] + fx[1, :, columns(d)]

    def de_stage(half, k, kind):
        m = stages.index((half, k, kind))
        slot = slot_of[k]

        wide = min(2, per_half) if kind and k else 1

        def right(i, t):
            if kind:
                return dz_par[t] if i else dz_own[c * n_half + t]
            ids = lax.broadcasted_iota(I32, (tok, LANE), 1) + (x * vocab + c * half_v + t * vt)
            hits = [jnp.where(tokc[i] == ids + b, dims["scale"], 0.0).astype(BF16) for b in range(0, vt, LANE)]
            return jnp.concatenate(hits, axis=1)

        def body(j, carry):
            t = half * per_half + j * wide
            sel = span(j * wide * vt, wide * vt)
            left = jnp.concatenate([xb[m % 2, i].reshape(n * rows, tok) for i in BOTH], axis=1)
            both_right = [jnp.concatenate([right(i, t + q) for i in BOTH], axis=0) for q in range(wide)]
            total = jnp.dot(left, jnp.concatenate(both_right, axis=1), preferred_element_type=F32)
            total = total.reshape(n, rows, wide * vt)
            acc[half, slot, :, :, sel] = acc[half, slot, :, :, sel] + total if kind else total
            return carry

        with scope("b_de" if kind else "b_look"):
            for i in BOTH:
                load_stage(m, i).wait()
            lax.fori_loop(0, per_half // wide, body, 0)
            start_stage(m + 2)

    def de_unit(half, k):
        if k == FAR:
            fars[half].wait()
        else:
            de_stage(half, k, 0)
        de_stage(half, k, 1)

    def ring(half, k):
        return {"dz": k} if half == 0 else {"dy": k}

    def cross(half, k):
        return {"dy": k} if half == 0 else {"dz": k}

    def a_far(half, i):
        return place.send(("af", half, i), acc.at[half, 0, pl.ds(2 * i, 2)], fa.at[half, i], **ring(half, WAYS[i]))

    def a_near(half, i, j):
        sel = pl.ds(2 * j, 2)
        return place.send(("an", half, i, j), acc.at[half, 1 + i, sel], ra_hbm.at[half, i, sel], **ring(half, WAYS[i]))

    def a_first(half):
        start_all(a_far(half, i) for i in BOTH)

    def a_second(half, i):
        with scope("b_a2"):
            a_far(half, i).wait_recv()
            sel = pl.ds(2 * i, 2)
            acc[half, 1 + i, sel] = acc[half, 1 + i, sel] + fa[half, i]
            start_all(a_near(half, i, j) for j in BOTH)

    def stage_a(half, j, i):
        return place.local(("sa", half), ra_hbm.at[half, i, pl.ds(2 * j, 2)], fa.at[half, i], i)

    def piece(half, k):
        return ((y if half == 0 else z) + k) % n

    def c_far(half, i):
        src = acc.at[half, 0, piece(half, FAR), pl.ds(i * half_rows, half_rows)]
        return place.send(("cf", half, i), src, f2.at[half, i], **cross(half, WAYS[i]))

    def c_near(half, i):
        return place.send(("cn", half, i), acc.at[half, 0, piece(half, WAYS[i])], r2.at[half, i], **cross(half, WAYS[i]))

    def a_third(half, j):
        with scope("b_a3"):
            for i in BOTH:
                a_near(half, i, j).wait_recv()
                stage_a(half, j, i).start()
            for i in BOTH:
                stage_a(half, j, i).wait()
            sel = pl.ds(2 * j, 2)
            acc[half, 0, sel] = acc[half, 0, sel] + fa[half, 0] + fa[half, 1]

    def c_first(half):
        start_all(c_far(half, i) for i in BOTH)

    def c_second(half):
        with scope("b_c2"):
            for i in BOTH:
                c_far(half, i).wait_recv()
                at = piece(half, WAYS[i])
                sel = pl.ds(i * half_rows, half_rows)
                acc[half, 0, at, sel] = acc[half, 0, at, sel] + f2[half, i]
                c_near(half, i).start()

    def out_copies(half):
        sel = span(c * half_v + half * lanes, lanes)
        mine = acc.at[half, 0, piece(half, 0)]
        yield place.local("de", mine.at[span(c * half_rows, half_rows, SUB)], de_out.at[:, sel], half)
        yield place.send(("de", half), mine.at[span((1 - c) * half_rows, half_rows, SUB)], de_out.at[:, sel], dc=1)

    def c_third(half):
        with scope("b_c3"):
            for i in BOTH:
                c_near(half, i).wait_recv()
            at = piece(half, 0)
            acc[half, 0, at] = acc[half, 0, at] + r2[half, 0] + r2[half, 1]
            start_all(out_copies(half))

    step = min(32, hq)

    def dh_body(i, carry):
        sel = span(i * step, step, step)
        row = span(x * quarter + i * step, step, step)
        d_x = part[row]
        h_wide = h_buf[sel].astype(F32)
        inv_rms = lax.rsqrt(jnp.sum(h_wide * h_wide, axis=1, keepdims=True) * (1.0 / width) + NORM_EPS)
        h_norm = h_wide * inv_rms
        g_dir = d_x * gain_ref[0:1]
        mean = jnp.sum(g_dir * h_norm, axis=1, keepdims=True) * (1.0 / width)
        dh_buf[sel] = (inv_rms * (g_dir - h_norm * mean)).astype(BF16)
        prod = d_x * h_norm
        total = prod[0:SUB]
        for j in range(SUB, step, SUB):
            total = total + prod[j:j + SUB]
        dg_acc[...] = dg_acc[...] + total
        return carry

    def h_first(i, j):
        return place.send(("hf", i, j), dh_buf.at[pl.ds(j * hq, hq)], dh_out.at[qrow(0, j * hq)], dx=WAYS[i])

    def h_second(i):
        ref = dh_out.at[qrow(FROM[i], i * hq)]
        return place.send(("hs", i), ref, ref, dx=WAYS[i])

    keep_dh = place.local("dh", dh_buf, dh_out.at[qrow(0, 0, quarter)])
    small = SmallSum(place, ("dc", "dx", "dy", "dz"), slots)
    per_j = hq // step

    def dh_part(j):
        with scope("b_dh"):
            if j == 0:
                load_h.wait()
            lax.fori_loop(j * per_j, (j + 1) * per_j, dh_body, 0)
            start_all(h_first(i, j) for i in BOTH)
            if j:
                keep_dh.start()

    def h_passes():
        with scope("b_h2"):
            for i in BOTH:
                h_first(i, i).wait_recv()
                h_second(i).start()

    def small_step(k):
        dims_of = small.dims
        with scope("b_s"):
            if k == 1:
                sums = [jnp.sum(part_sum, axis=0, keepdims=True) for part_sum in (dg_acc[...], loss_ref[...])]
                small.start(dims_of[0], jnp.concatenate(sums, axis=1))
            elif k <= len(dims_of):
                small.start(dims_of[k - 1], small.finish(dims_of[k - 2]))
            else:
                total = small.finish(dims_of[-1])
                loss = jnp.sum(total[:, width:], axis=1, keepdims=True) * (1.0 / dims["total"])
                tail_out[...] = jnp.concatenate([total[:, 0:width], jnp.broadcast_to(loss, (1, LANE))], axis=1)

    def dxn(d):
        dxn_chunk(d)
        x_first(d)

    def unit(half, k):
        if k == 0:
            with scope("b_wait_far"):
                for i in BOTH:
                    a_far(half, i).wait_send()
        de_unit(half, k)
        if k == FAR:
            a_first(half)

    families = {
        "CH": dxn, "XS": x_second, "UN": unit, "AS": a_second, "XT": x_third, "AT": a_third, "CF": c_first, "CS": c_second,
        "CT": c_third, "DH": dh_part, "SM": small_step, "HP": h_passes,
    }

    def perform(text):
        for word in text.split():
            families[word[:2]](*(int(digit) for digit in word[2:]))

    with scope("b_load"):
        loads[0].wait()
        dg_acc[...] = jnp.zeros_like(dg_acc)
        loads[1].wait()
    for text in (
        "UN02 CH0 UN12 CH1", "CH2 UN03 XS1 UN11", "XS2 UN01 AS01 AS00", "AS10 UN13 AS11 XS0",
        "XT10 CH3 CH4 XS3", "XT20 XS4 UN00 XT30", "XT00 UN10 XT01 XT40", "DH0 XT21 XT11 AT00",
        "XT31 XT41 AT10 AT01", "CF0 DH1 AT11 CF1", "SM1 SM2 CS0 CS1", "SM3 HP SM4 CT0", "CT1 SM5",
    ):
        perform(text)

    with scope("b_end_x"):
        keep_dh.wait()
        for i in BOTH:
            for d in range(chunks):
                x_far(d, i).wait_send()
                for j in BOTH:
                    x_near(d, i, j).wait_send()
            h_first(i, i).wait_send()
            h_first(i, 1 - i).wait()
            h_second(i).wait()
    with scope("b_end_a"):
        for half in BOTH:
            for i in BOTH:
                for j in BOTH:
                    a_near(half, i, j).wait_send()
                c_far(half, i).wait_send()
                c_near(half, i).wait_send()
            for copy in out_copies(half):
                copy.wait()
    assert (place.n_link, place.n_local) <= dims["back_sems"], (place.n_link, place.n_local)


def back(dims, limit, gain, loss, tokc, far, dz, dzp, et, xnt, xpar, gt, gpar, h):
    n, tok, vocab, width, tile = (dims[k] for k in ("n", "tok", "vocab", "width", "tile"))
    rows = width // (n * n)
    half_v = vocab // CORES
    lanes = half_v // 2
    quarter = tok // n
    hq = quarter // 2
    tail_w = width + loss.shape[1]
    n_tile, n_half, vt = dz.shape[0], dzp.shape[0], dims["vt"]
    turned = [a.reshape(n, n, rows, tok) for a in (xnt, xpar, gt, gpar)]
    return pl.pallas_call(
        functools.partial(back_kernel, dims),
        name="back",
        out_shape=shapes([
            ((1, width + LANE), F32), ((tok, width), BF16), ((rows // CORES, vocab), F32), ((2, 2, n, rows, lanes), F32),
            ((2, quarter, width), F32),
        ]),
        in_specs=specs(3, 9),
        out_specs=tuple(specs(1, 4)),
        scratch_shapes=scratch([
            ((n_tile, tok, vt), BF16), ((n_half, tok, vt), BF16), ((2, n_tile, tile, vt), BF16), ((tok, width), F32),
            ((2, hq, width), F32), ((2, 3, n, rows, lanes), F32), ((2, 2, 2, rows, lanes), F32),
            ((2, 2, rows // 2, lanes), F32), ((2, 2, rows, lanes), F32), ((2, CORES, n, rows, tok), BF16), ((quarter, width), BF16),
            ((quarter, width), BF16), ((SUB, width), F32), ((3 * n + CORES, 1, tail_w), F32),
        ], dims["back_sems"][0], dims["back_sems"][1]),
        compiler_params=params(1, limit),
    )(gain, loss, tokc, far.reshape(2, n, rows, lanes), dz, dzp, et.reshape(n_tile, width, vt), *turned, h)[:3]


def finish_kernel(
    n, scale, table_ref, tail_ref, x0_hbm, dh_hbm, de_hbm, dg_out, loss_out, x0_out, dh_out, de_out,
    x0_in, x0_buf, rows_ref, dh_buf, de_buf, sems,
):
    place = Place(n, None, None, sems)
    quarter, cols, width = x0_in.shape[3], x0_in.shape[2], x0_buf.shape[2]

    def step(q):
        rows = span(q * quarter, quarter, quarter)
        return (
            place.local("x0", x0_hbm.at[q], x0_in.at[q], q, n), place.local("x0o", x0_buf.at[q], x0_out.at[rows], q, n),
            place.local("dh", dh_hbm.at[rows], dh_buf.at[q], q, n), place.local("dho", dh_buf.at[q], dh_out.at[rows], q, n),
        )

    moves = [step(q) for q in range(n)]
    de_in, de_put = place.local("de", de_hbm, de_buf, 0), place.local("de", de_buf, de_out, 1)
    for x0_load, _, dh_load, _ in moves:
        x0_load.start()
        dh_load.start()
    de_in.start()
    gain = jnp.broadcast_to(tail_ref[:, 0:width], (SUB, width))
    dg_out[...] = pltpu.roll(gain, width - place.f * cols, axis=1)[0:1, 0:cols]
    loss_out[...] = tail_ref[:, width:width + 1]

    def body(q, carry):
        x0_load, x0_put, dh_load, dh_put = step(q)
        x0_load.wait()
        for zi in range(n):
            for yi in range(n):
                for h in BOTH:
                    dz, dy = (zi - place.z) % n, (yi - place.y) % n
                    k1, k2 = (dy, dz) if h == 0 else (dz, dy)
                    piece = table_ref[(h * n + k1) * n + k2]
                    rows_ref[pl.ds(((zi * n + yi) * CORES + h) * cols, cols)] = x0_in[q, piece]
        x0_buf[q] = (rows_ref[...].T.astype(F32) * scale).astype(BF16)
        x0_put.start()
        dh_load.wait()
        dh_put.start()
        return carry

    lax.fori_loop(0, n, body, 0)
    de_in.wait()
    de_put.start()
    for _, x0_put, _, dh_put in moves:
        x0_put.wait()
        dh_put.wait()
    de_put.wait()


def finish(n, scale, limit, tail, x0, dh, de):
    _, pieces, cols, quarter = x0.shape
    width = pieces * cols
    table = np.zeros((CORES, n, n), np.int32)
    for u, unit in enumerate(UNITS):
        for h in BOTH:
            for i, (k1, k2) in enumerate(unit):
                table[h, k1, k2] = BASE[u] + h * len(unit) + i
    return pl.pallas_call(
        functools.partial(finish_kernel, n, scale),
        name="finish",
        in_specs=[pl.BlockSpec(memory_space=pltpu.SMEM)] + specs(1, 3),
        out_specs=tuple(specs(2, 3)),
        out_shape=shapes([((1, cols), F32), ((1, 1), F32), (dh.shape, BF16), (dh.shape, BF16), (de.shape, F32)]),
        scratch_shapes=[
            pltpu.VMEM(x0.shape, BF16), pltpu.VMEM((n, quarter, width), BF16), pltpu.VMEM((width, quarter), BF16),
            pltpu.VMEM((n, quarter, width), BF16), pltpu.VMEM(de.shape, F32), pltpu.SemaphoreType.DMA((4 * n + 2,)),
        ],
        compiler_params=pltpu.CompilerParams(vmem_limit_bytes=limit),
    )(jnp.asarray(table.reshape(-1)), tail, x0, dh, de)


def solution(mesh):
    return build(mesh, mesh.shape["tp"], 256, digits("12222")[0], 256, 6, 67_000_000)


def build(mesh, n, tile, tiles, vt, n_block, limit):
    fsdp_size = mesh.shape["fsdp"]

    def device_step(emb_shard, tok_ids, lab_ids, h_last, g_embed, norm_w):
        vocab_rows, cols = emb_shard.shape
        batch_loc, seq_len, width = h_last.shape
        tok_count = batch_loc * seq_len
        fsdp_id = lax.axis_index("fsdp")
        scale = float(np.asarray(math.sqrt(width)).astype(jnp.bfloat16))
        dims = {
            "n": n, "tok": tok_count, "vocab": vocab_rows, "width": width, "total": tok_count * fsdp_size, "vt": vt,
            "tile": tile, "tiles": tiles, "scale": scale, "n_block": n_block,
            "stages": digits("021 121 030 031") + digits("110 111 010 011") + digits("130 131 000 001") + digits("100 101"),
            "front_sems": (110, 52), "back_sems": (68, 24),
        }
        h_flat = h_last.reshape(tok_count, width)
        placed = lax.dynamic_update_slice(jnp.zeros((SUB, width), F32), jnp.broadcast_to(norm_w, (SUB, cols)), (0, fsdp_id * cols))
        ids = [a.reshape(1, tok_count) for a in (tok_ids, lab_ids)]
        table, xn_t, xpar_t, g_t, gpar_t, far, dz, dzp, x0, _, gain, loss_part, tokc = front(
            dims, limit, emb_shard.T, *ids, norm_w.reshape(1, cols), h_flat, g_embed.reshape(tok_count, width))
        tail, d_hidden, d_cols = back(dims, limit, gain, loss_part, tokc, far, dz, dzp, table, xn_t, xpar_t, g_t, gpar_t, h_flat)
        d_norm_w, loss, x_emb, d_hidden, d_cols = finish(n, scale, limit, tail, x0, d_hidden, d_cols)
        return (x_emb.reshape(h_last.shape), loss.reshape(()), d_hidden.reshape(h_last.shape), d_norm_w.reshape(cols), d_cols.T)

    spec_tok = P("fsdp", None)
    spec_act = P("fsdp", None, None)
    return jax.shard_map(device_step, mesh=mesh, in_specs=(P("tp", "fsdp"), spec_tok, spec_tok, spec_act, spec_act, P("fsdp")), out_specs=(spec_act, P(), spec_act, P("fsdp"), P("tp", "fsdp")), check_vma=False)
```

```python
import functools
import math
import jax
import numpy as np
import jax.numpy as jnp
from jax import lax
from jax.experimental import pallas as pl
from jax.experimental.pallas import tpu as pltpu
from jax.sharding import PartitionSpec as P

SOFT_CAP = 30.0
NORM_EPS = 1e-6
F32, BF16, I32 = jnp.float32, jnp.bfloat16, jnp.int32
LANE, SUB = 128, 8
BOTH = (0, 1)
FOUR = range(4)
WAYS = (1, 3)
FROM = (3, 1)
FAR = 2
CORES = 2


def span(start, size, unit=LANE):
    return pl.ds(pl.multiple_of(start, unit), size)


class Place:
    def __init__(self, n, sends, recvs, local_sems):
        self.n, self.sends, self.recvs, self.local_sems = n, sends, recvs, local_sems
        self.x = lax.axis_index("tp")
        f = lax.axis_index("fsdp")
        self.f = f
        self.c = f % CORES
        self.y = f // CORES % n
        self.z = f // CORES // n
        self.link_of, self.local_of, self.n_link, self.n_local = {}, {}, 0, 0
        self.size = {"dx": n, "dz": n, "dy": n, "dc": CORES}
        self.me = {"dx": self.x, "dz": self.z, "dy": self.y, "dc": self.c}

    def at(self, dx=0, dz=0, dy=0, dc=0):
        n = self.n
        z, y, c = (self.z + dz) % n, (self.y + dy) % n, (self.c + dc) % CORES
        return ((self.x + dx) % n, (z * n + y) * CORES + c)

    def enter(self):
        barrier = pltpu.get_barrier_semaphore()
        peers = [self.at(**{d: k}) for d in self.size for k in range(1, self.size[d])]
        for peer in peers:
            pl.semaphore_signal(barrier, inc=1, device_id=peer, device_id_type=pl.DeviceIdType.MESH)
        pl.semaphore_wait(barrier, len(peers))

    def link(self, key, count=1):
        if key not in self.link_of:
            self.link_of[key] = self.n_link
            self.n_link += count
        return self.link_of[key]

    def send(self, key, src, dst, **step):
        i = self.link(key)
        return pltpu.make_async_remote_copy(
            src, dst, self.sends.at[i], self.recvs.at[i], device_id=self.at(**step), device_id_type=pl.DeviceIdType.MESH)

    def local(self, key, src, dst, slot=0, count=2):
        if key not in self.local_of:
            self.local_of[key] = self.n_local
            self.n_local += count
        return pltpu.make_async_copy(src, dst, self.local_sems.at[self.local_of[key] + slot])


class SmallSum:
    def __init__(self, place, dims, slots):
        self.place, self.slots, self.dims, self.base = place, slots, dims, {}
        count = 0
        for d in dims:
            self.base[d] = count
            count += place.size[d]

    def copies(self, d):
        slot = self.slots.at[self.base[d] + self.place.me[d]]
        for k in range(1, self.place.size[d]):
            yield self.place.send((self.dims, d, k), slot, slot, **{d: k})

    def start(self, d, value):
        self.slots[self.base[d] + self.place.me[d]] = value
        for copy in self.copies(d):
            copy.start()

    def finish(self, d):
        for copy in self.copies(d):
            copy.wait()
        total = self.slots[self.base[d]]
        for k in range(1, self.place.size[d]):
            total = total + self.slots[self.base[d] + k]
        return total


def scope(name):
    return jax.named_scope(name)


def start_all(copies):
    for copy in copies:
        copy.start()


def digits(text):
    return tuple(tuple(int(d) for d in word) for word in text.split())


UNITS = [digits(u) for u in ("00", "10 30", "01 03 20", "02 11 31", "13 33 21 23", "12 32 22")]
PAIR, ALL = 1, "all"
PIECES = [2 * len(u) for u in UNITS]
EXP_RATE = SOFT_CAP * math.log2(math.e)
BASE = [sum(PIECES[:i]) for i in range(len(UNITS))]


def front_kernel(
    dims,
    shard_ref, tok_ref, lab_ref, w_ref, h_hbm, g_hbm,
    et_out, xnt_out, xpar_out, gt_out, gpar_out, lt_out, dz_out, dzpar_out, x0_out, q5_out, u_hbm, gain_out, loss_out, tokc_out,
    shard_t, chunk, tokr, hit_t, lhs, xp, xw, xr, xf, xg, xq, etb, xn, gl, z_even, z_odd, dzb,
    acc_e, acc_l, inv_s, labc, w_slots, s_slots, sends, recvs, local_sems,
):
    n, tok, vocab, width, vt = dims["n"], dims["tok"], dims["vocab"], dims["width"], dims["vt"]
    place = Place(n, sends, recvs, local_sems)
    x, z, y, c = place.x, place.z, place.y, place.c
    half_v = vocab // CORES
    n_tile = vocab // vt
    n_half = n_tile // CORES
    hh = n_half // 2
    cols = width // (n * n * CORES)
    quarter = tok // n
    row_start = x * vocab

    def ring1(h, k):
        return {"dy": k} if h == 0 else {"dz": k}

    def ring2(h, k):
        return {"dz": k} if h == 0 else {"dy": k}

    def coord(base, k, paired):
        every = slice(None)
        if k == ALL:
            return every, every
        return every if paired else (base + k) % n // 2, (base + k) % 2

    def loc(h, k1, k2, lo=0, size=n_half, pair1=False, pair2=False):
        first, second = coord((y, z)[h], k1, pair1), coord((z, y)[h], k2, pair2)
        return et_out.at[(pl.ds(c * n_half + lo, size), *((second, first)[h]), *((first, second)[h]), h)]

    with scope("f_enter"):
        place.enter()

    load_g = place.local("g", g_hbm, xn)
    load_g.start()
    with scope("f_cast"):
        for t in range(n_tile):
            shard_t[t] = shard_ref[:, pl.ds(t * vt, vt)].astype(BF16)
        tokr[c] = jnp.broadcast_to(tok_ref[...], (SUB, tok))
        give_tok = place.send("tok", tokr.at[c], tokr.at[c], dc=1)
        give_chunk = place.send("chunk", shard_t.at[pl.ds((1 - c) * n_half, n_half)], chunk.at[c], dc=1)
        give_chunk.start()
        give_tok.start()
        chunk[c] = shard_t[pl.ds(c * n_half, n_half)]
        gain_sum = SmallSum(place, ("dc", "dy", "dz"), w_slots)
        own_w = jnp.concatenate([w_ref[...], jnp.zeros((1, width - cols), F32)], axis=1)
        gain_sum.start("dc", pltpu.roll(jnp.broadcast_to(own_w, (SUB, width)), place.f * cols, axis=1)[0:1])

    def p1_send(h, i):
        return place.send(("p1", h, i), chunk.at[h], loc(h, 0, 0), **ring1(h, WAYS[i]))

    def p1_fwd(h, i):
        ref = loc(h, FROM[i], 0, i * hh, hh)
        return place.send(("p1f", h, i), ref, ref, **ring1(h, WAYS[i]))

    def p2_send(h, k1, i):
        ref = loc(h, k1, 0, pair1=k1 == PAIR)
        return place.send(("p2", h, k1, i), chunk.at[h] if k1 == 0 else ref, ref, **ring2(h, WAYS[i]))

    def p2_fwd(h, k1, i):
        ref = loc(h, k1, FROM[i], i * hh, hh, pair1=k1 == PAIR)
        return place.send(("p2f", h, k1, i), ref, ref, **ring2(h, WAYS[i]))

    def keep(h):
        return place.local("keep", chunk.at[h], loc(h, 0, 0), h)

    def share(h, k2):
        ref = loc(h, ALL, k2, pair2=k2 == PAIR)
        return place.send(("share", h, k2), ref, ref, dc=1)

    def pass_first():
        with scope("f_p1"):
            for h in BOTH:
                for i in BOTH:
                    p1_send(h, i).wait_recv()
                    p1_fwd(h, i).start()
            for h in BOTH:
                start_all(p2_send(h, PAIR, i) for i in BOTH)

    def pass_first_far():
        with scope("f_p1f"):
            for h in BOTH:
                for i in BOTH:
                    p1_fwd(h, i).wait_recv()
                start_all(p2_send(h, FAR, j) for j in BOTH)

    def pass_second(k1):
        with scope("f_p2"):
            for h in BOTH:
                for i in BOTH:
                    p2_send(h, k1, i).wait_recv()
                    p2_fwd(h, k1, i).start()

    def end_second(k1):
        with scope("f_p2f"):
            for h in BOTH:
                for i in BOTH:
                    p2_fwd(h, k1, i).wait_recv()

    def share_group(k2):
        start_all(share(h, k2) for h in BOTH)

    with scope("f_chunk"):
        give_chunk.wait_recv()
        start_all(keep(h) for h in BOTH)
        gain_sum.start("dy", gain_sum.finish("dc"))
        for h in BOTH:
            start_all(p1_send(h, i) for i in BOTH)
        for h in BOTH:
            start_all(p2_send(h, 0, i) for i in BOTH)

    v_step = min(LANE, half_v)

    def hit_body(j, carry):
        off = j * v_step
        ids = lax.broadcasted_iota(I32, (v_step, tok), 0) + (row_start + c * half_v + off)
        for i, core in enumerate((c, 1 - c)):
            hit_t[span(off, v_step, v_step), pl.ds(i * tok, tok)] = jnp.where(ids == tokr[core, 0:1, :], 1.0, 0.0).astype(BF16)
        return carry

    def make_hits():
        with scope("f_hit"):
            give_tok.wait_recv()
            lax.fori_loop(0, half_v // v_step, hit_body, 0)

    n_step = min(512, tok)
    most = max(PIECES)

    def whole(u):
        return pl.ds(BASE[u], PIECES[u])

    def unit_copies(u):
        slot = u % 2
        for p, (h, (k1, k2)) in enumerate((h, k) for h in BOTH for k in UNITS[u]):
            yield place.local("lhs", loc(h, k1, k2), lhs.at[slot, p], slot * most + p, 2 * most)

    def load_unit(u):
        start_all(unit_copies(u))

    def look(u):
        pieces = PIECES[u]
        with scope("f_look"):
            if u > 1:
                x_swap(u - 2).wait_send()
            left = lhs.at[u % 2]
            for copy in unit_copies(u):
                copy.wait()
            per_core = tok // n_step

            def body(j, carry):
                value = jnp.concatenate([left[pl.ds(0, pieces), t].reshape(pieces * cols, vt) for t in range(n_half)], axis=1)
                rows = jnp.dot(value, hit_t[:, span(j * n_step, n_step)], preferred_element_type=F32)
                rows = rows.reshape(pieces, cols, n_step).astype(BF16)
                xw[u % 2, j // per_core, pl.ds(0, pieces), :, span(j % per_core * n_step, n_step)] = rows
                return carry

            lax.fori_loop(0, CORES * per_core, body, 0)
            x_swap(u).start()

    def x_swap(u):
        return place.send(("swap", u), xw.at[u % 2, 1, pl.ds(0, PIECES[u])], xr.at[whole(u)], dc=1)

    def lanes_of(k):
        return span((x + k) % n * quarter, quarter, quarter)

    def side(u, i):
        return pl.ds(BASE[u] + i * len(UNITS[u]), len(UNITS[u]))

    def x_far(u, i):
        return place.send(("xf", u, i), xp.at[side(u, i), :, lanes_of(FAR)], xf.at[side(u, i)], dx=WAYS[i])

    def x_near(u, i):
        return place.send(("xn", u, i), xp.at[whole(u), :, lanes_of(WAYS[i])], xg.at[i, whole(u)], dx=WAYS[i])

    def x_goal(k, sel):
        return x0_out.at[(x + k) % n, sel]

    def x_put(u, i):
        return place.send(("xp", u, i), xq.at[whole(u)], x_goal(0, whole(u)), dx=WAYS[i])

    last_unit = len(UNITS) - 1

    def x_keep(u):
        goal = x_goal(0, whole(u)) if u < last_unit else q5_out
        return place.local("x0", xq.at[whole(u)], goal, u, len(UNITS))

    def x_pass(u, i):
        ref = x_goal(FROM[i], side(u, i))
        return place.send(("xs", u, i), ref, ref, dx=WAYS[i])

    def x_first(u):
        with scope("f_x1"):
            x_swap(u).wait_recv()
            def body(p, carry):
                xp[BASE[u] + p] = xw[u % 2, 0, p] + xr[BASE[u] + p]
                return carry

            lax.fori_loop(0, PIECES[u], body, 0)
            start_all(x_far(u, i) for i in BOTH)

    def x_second(u):
        with scope("f_x2"):
            for i in BOTH:
                x_far(u, i).wait_recv()
                sel, lanes = side(u, i), lanes_of(WAYS[i])
                xp[sel, :, lanes] = xp[sel, :, lanes] + xf[sel]
                x_near(u, i).start()

    def x_third(u):
        with scope("f_x3"):
            for i in BOTH:
                x_near(u, i).wait_recv()
            sel = whole(u)
            xq[sel] = xp[sel, :, lanes_of(0)] + xg[0, sel] + xg[1, sel]
            if u < last_unit:
                start_all(x_put(u, i) for i in BOTH)
            x_keep(u).start()

    def x_fourth(u):
        with scope("f_x4"):
            for i in BOTH:
                x_put(u, i).wait_recv()
                x_pass(u, i).start()

    n_part = n * n * CORES // 2

    def moves(key, part, whole_t, other):
        sel = pl.ds(part * n_part, n_part)
        yield place.local(key, gl.at[sel], whole_t.at[sel], part)
        yield place.send((key, part), gl.at[sel], other.at[sel], dc=1)

    def move_g(part):
        return moves("g", part, gt_out, gpar_out)

    def move_xn(part):
        return moves("xt", part, xnt_out, xpar_out)

    def transpose_part(part, copies):
        block = width // dims["n_block"]
        first = part * dims["n_block"] // 2
        turned = [xn[:, pl.ds((first + j) * block, block)].T for j in range(dims["n_block"] // 2)]
        gl[pl.ds(part * n_part, n_part)] = jnp.concatenate(turned, axis=0).reshape(n_part, cols, tok)
        start_all(copies)

    def columns(row):
        return jnp.broadcast_to(row.astype(F32), (LANE, tok)).T.astype(I32)

    r_step = min(LANE, tok)

    def xn_body(j, carry):
        sel = span(j * r_step, r_step, r_step)
        h_wide = xn[sel].astype(F32)
        inv_rms = lax.rsqrt(jnp.sum(h_wide * h_wide, axis=1, keepdims=True) * (1.0 / width) + NORM_EPS)
        xn[sel] = (h_wide * inv_rms * gain_out[0:1]).astype(BF16)
        return carry

    e_step = min(LANE, tok)

    def tile_of(j):
        return (c * n_half + j) % n_tile

    def load_tile(j):
        return place.local("et", et_out.at[tile_of(j)], etb.at[j % 4], j % 4, 4)

    def save_u(i, odd):
        return place.local(("u", odd), (z_even, z_odd)[odd].at[i % 2], u_hbm.at[tile_of(2 * i + odd)], i % 2)

    def lane_blocks():
        return [(b, pl.ds(b, LANE)) for b in range(0, vt, LANE)]

    def post_tile(i, odd):
        base = tile_of(2 * i + odd) * vt
        buf, slot = (z_even, z_odd)[odd], i % 2

        def body(e, carry):
            sel = span(e * e_step, e_step, e_step)
            ids = lax.broadcasted_iota(I32, (e_step, LANE), 1) + base
            sum_e, sum_l = acc_e[sel], acc_l[sel]
            for b, lanes in lane_blocks():
                tanh_z = jnp.tanh(buf[slot, sel, lanes] * (1.0 / SOFT_CAP))
                buf[slot, sel, lanes] = tanh_z
                sum_e = sum_e + jnp.exp2(EXP_RATE * tanh_z - EXP_RATE)
                sum_l = sum_l + jnp.where(ids + b == labc[sel], tanh_z, 0.0)
            acc_e[sel] = sum_e
            acc_l[sel] = sum_l
            return carry

        lax.fori_loop(0, tok // e_step, body, 0)

    def dot_pair(i):
        for odd in BOTH:
            value = etb[(2 * i + odd) % 4].reshape(width, vt)
            (z_even, z_odd)[odd][i % 2] = jnp.dot(xn[...], value, preferred_element_type=F32)

    def load_pair(i):
        start_all(load_tile(2 * i + odd) for odd in BOTH)

    def pair(i, carry):
        for odd in BOTH:
            load_tile(2 * i + odd).wait()

        @pl.when(i > 1)
        def _():
            for odd in BOTH:
                save_u(i - 2, odd).wait()

        for odd in BOTH:
            post_tile(i - 1, odd)
            save_u(i - 1, odd).start()
        dot_pair(i)

        @pl.when(i + 2 < n_tile // 2)
        def _():
            load_pair(i + 2)

        for k, work in enumerate(during):
            @pl.when(i == k + 1)
            def _():
                if k == 0:
                    wait_shares()
                perform(work)
        return carry

    def wait_shares():
        with scope("f_share"):
            for h in BOTH:
                for k2 in (0, PAIR, FAR):
                    share(h, k2).wait_recv()

    def logits_first():
        acc_e[...] = jnp.zeros_like(acc_e)
        acc_l[...] = jnp.zeros_like(acc_l)
        with scope("f_logits0"):
            for i in BOTH:
                load_pair(i)
            far_ends(1)
            for odd in BOTH:
                load_tile(odd).wait()
            dot_pair(0)
            if n_tile // 2 > 2:
                load_pair(2)

    def lay_columns():
        with scope("f_cols"):
            labc[...] = columns(lab_ref[...] - row_start)
            for i, core in enumerate((c, 1 - c)):
                tokc_out[i] = columns(tokr[core, 0:1, :])

    def turn_g():
        with scope("f_gt"):
            load_g.wait()
            for part in BOTH:
                transpose_part(part, move_g(part))
            load_h.start()

    def gain_next():
        with scope("f_gain2"):
            gain_sum.start("dz", gain_sum.finish("dy"))

    def normalize():
        with scope("f_xn"):
            gain_out[...] = 1.0 + gain_sum.finish("dz")
            load_h.wait()
            lax.fori_loop(0, tok // r_step, xn_body, 0)

    def turn_xn():
        with scope("f_xt"):
            for part in BOTH:
                transpose_part(part, move_xn(part))

    spare = BASE[3]
    own_rows, their_rows = (pl.ds(spare + i * 2 * n, 2 * n) for i in BOTH)

    def far_loads(h):
        for i, (src, rows) in enumerate(((gt_out, own_rows), (gpar_out, their_rows))):
            if h == 0:
                yield place.local("far", src.at[pl.ds((z + FAR) % n * 2 * n, 2 * n)], xp.at[rows], i * n, 2 * n)
            else:
                for q in range(n):
                    piece = src.at[pl.ds((q * n + (y + FAR) % n) * 2, 2)]
                    yield place.local("far", piece, xp.at[pl.ds(spare + i * 2 * n + 2 * q, 2)], i * n + q)

    def far_load(h):
        if h == 0:
            for part in BOTH:
                for copy in move_g(part):
                    copy.wait()
        start_all(far_loads(h))

    def put_far(h, j):
        rows = pl.ds(0, 2 * n * cols)
        return place.local("lt", z_even.at[j % 2, rows], lt_out.at[h, :, span(j * vt, vt)], j % 2)

    def far_ends(h):
        for j in range(hh - 2, hh):
            put_far(h, j).wait()

    def far_look(h):
        def body(j, carry):
            @pl.when(j > 1)
            def _():
                put_far(h, j - 2).wait()

            left = jnp.concatenate([xp[rows].reshape(2 * n * cols, tok) for rows in (own_rows, their_rows)], axis=1)
            right = hit_t[span((h * hh + j) * vt, vt)]
            value = lax.dot_general(left, right, (((1,), (1,)), ((), ())), preferred_element_type=F32)
            z_even[j % 2, pl.ds(0, 2 * n * cols)] = value * dims["scale"]
            put_far(h, j).start()
            return carry

        with scope("f_far"):
            for copy in far_loads(h):
                copy.wait()
            if h:
                far_ends(0)
            lax.fori_loop(0, hh, body, 0)

    def begin_unit(u):
        if u == 0:
            for h in BOTH:
                keep(h).wait()
        load_unit(u)

    load_h = place.local("h", h_hbm, xn)
    works = {
        "HIT": make_hits, "GT": turn_g, "COL": lay_columns, "G2": gain_next, "XN": normalize, "XT": turn_xn, "L0": logits_first,
        "PF": pass_first, "PFF": pass_first_far,
    }
    groups = {"0": 0, "P": PAIR, "F": FAR}
    families = {"LF": far_load, "FL": far_look, "LU": begin_unit, "LK": look, "X1": x_first, "X2": x_second, "X3": x_third, "X4": x_fourth}
    families_k = {"SH": share_group, "S": pass_second, "E": end_second}

    def perform(text):
        for word in text.split():
            if word in works:
                works[word]()
            elif word[:-1] in families:
                families[word[:-1]](int(word[-1]))
            else:
                families_k[word[:-1]](groups[word[-1]])

    during = (
        "X24",
        "X15 X33",
        "",
        "X34",
        "",
        "X25",
        "",
    )
    for text in (
        "HIT LU0 COL G2", "LK0 GT PF X10", "LU1 LK1 XN LF0", "S0 X11 XT FL0", "PFF X21 LU2 LF1",
        "LK2 FL1 SP SH0", "E0 LU3 X12 X20", "LK3 SF LU4 X22", "X31 SHP LK4 X13", "EP X30 X32 EF",
        "LU5 SHF L0 X14", "LK5 X23",
    ):
        perform(text)
    if n_half < 4:
        wait_shares()
        for text in during:
            perform(text)
        during = ()
    last = n_tile // 2 - 1
    with scope("f_logits"):
        lax.fori_loop(1, last + 1, pair, 0)
        for odd in BOTH:
            post_tile(last, odd)
            save_u(last, odd).start()

    with scope("f_stats"):
        row = lax.broadcasted_iota(I32, (2, tok), 0)
        sum_e = jnp.sum(acc_e[...].T, axis=0, keepdims=True)
        sum_l = SOFT_CAP * jnp.sum(acc_l[...].T, axis=0, keepdims=True)
        stats = SmallSum(place, ("dx",), s_slots)
        stats.start("dx", jnp.where(row == 0, sum_e, sum_l))
    perform("X43 X42 X35 X40")
    perform("X44 X41")
    with scope("f_stats2"):
        stat = stats.finish("dx")
        all_e, all_l = stat[0:1], stat[1:2]
        inv_s[...] = jnp.broadcast_to((1.0 / dims["total"]) / all_e, (LANE, tok)).T
        s_slots[0, 0:1, :] = jnp.log(all_e) + SOFT_CAP - all_l
        own = s_slots[0, 0:1, lanes_of(0)]
        part_w = min(LANE, quarter)
        folded = own[:, 0:part_w]
        for j in range(part_w, quarter, part_w):
            folded = folded + own[:, j:j + part_w]
        loss_out[...] = jnp.where(lax.broadcasted_iota(I32, (SUB, part_w), 0) == 0, folded, 0.0)

    def dz_tile(j):
        return ((1 - c) * n_half + j) % n_tile

    def load_u(i, odd):
        return place.local(("u", odd), u_hbm.at[dz_tile(2 * i + odd)], (z_even, z_odd)[odd].at[i % 2], i % 2)

    def put_dz(i, odd):
        return place.local(("dz", odd), dzb.at[odd, i % 2], dz_out.at[dz_tile(2 * i + odd)], i % 2)

    def give_dz(part):
        src = dz_out.at[pl.ds((1 - c) * n_half + part * hh, hh)]
        return place.send(("dz", part), src, dzpar_out.at[pl.ds(part * hh, hh)], dc=1)

    d_step = min(256, tok)

    def dz_rows(i, odd):
        base = dz_tile(2 * i + odd) * vt
        buf, slot = (z_even, z_odd)[odd], i % 2

        def body(e, carry):
            sel = span(e * d_step, d_step, d_step)
            ids = lax.broadcasted_iota(I32, (d_step, LANE), 1) + base
            for b, lanes in lane_blocks():
                tanh_z = buf[slot, sel, lanes]
                prob = jnp.exp2(EXP_RATE * tanh_z - EXP_RATE) * inv_s[sel]
                prob = jnp.where(ids + b == labc[sel], prob - 1.0 / dims["total"], prob)
                dzb[odd, slot, sel, lanes] = (prob * (1.0 - tanh_z * tanh_z)).astype(BF16)
            return carry

        lax.fori_loop(0, tok // d_step, body, 0)

    def dz_pair(i, carry):
        for odd in BOTH:
            load_u(i, odd).wait()

            @pl.when(i > hh + 1)
            def _():
                put_dz(i - 2, odd).wait()

            dz_rows(i, odd)
            put_dz(i, odd).start()

            @pl.when(i + 2 < n_tile // 2)
            def _():
                load_u(i + 2, odd).start()

        return carry

    with scope("f_dz"):
        for i in range(n_tile // 2 - 2, n_tile // 2):
            for odd in BOTH:
                save_u(i, odd).wait()
        for i in BOTH:
            start_all(load_u(i, odd) for odd in BOTH)
        for part in BOTH:
            lo, hi = part * hh // 2, (part + 1) * hh // 2
            lax.fori_loop(lo, hi, dz_pair, 0)
            for i in range(max(lo, hi - 2), hi):
                for odd in BOTH:
                    put_dz(i, odd).wait()
            give_dz(part).start()
        lax.fori_loop(hh, n_tile // 2, dz_pair, 0)

    with scope("f_end"):
        for part in BOTH:
            give_dz(part).wait()
        for i in range(n_tile // 2 - 2, n_tile // 2):
            for odd in BOTH:
                put_dz(i, odd).wait()
        give_tok.wait_send()
        give_chunk.wait_send()
        for h in BOTH:
            for i in BOTH:
                p1_send(h, i).wait_send()
                p1_fwd(h, i).wait_send()
                for k in (0, PAIR, FAR):
                    p2_send(h, k, i).wait_send()
                    p2_fwd(h, k, i).wait_send()
            for k in (0, PAIR, FAR):
                share(h, k).wait_send()
        for part in BOTH:
            for copy in move_xn(part):
                copy.wait()
        for u in range(len(UNITS)):
            if u > len(UNITS) - 3:
                x_swap(u).wait_send()
            x_keep(u).wait()
            for i in BOTH:
                x_far(u, i).wait_send()
                x_near(u, i).wait_send()
                if u < last_unit:
                    x_put(u, i).wait_send()
                    x_pass(u, i).wait()
    assert (place.n_link, place.n_local) <= dims["front_sems"], (place.n_link, place.n_local)


def specs(n_vmem, n_any):
    return [pl.BlockSpec(memory_space=pltpu.VMEM)] * n_vmem + [pl.BlockSpec(memory_space=pl.ANY)] * n_any


def shapes(items):
    return tuple(jax.ShapeDtypeStruct(*item) for item in items)


def scratch(items, n_link, n_local):
    dma = pltpu.SemaphoreType.DMA
    return [pltpu.VMEM(*item) for item in items] + [dma((n_link,)), dma((n_link,)), dma((n_local,))]


def params(collective_id, limit):
    return pltpu.CompilerParams(collective_id=collective_id, has_side_effects=True, vmem_limit_bytes=limit)


def front(dims, limit, shard, tok_row, lab_row, w, h, g):
    n, tok, vocab, width, vt = dims["n"], dims["tok"], dims["vocab"], dims["width"], dims["vt"]
    cols = shard.shape[0]
    half_v = vocab // CORES
    quarter = tok // n
    n_tile, n_half, most = vocab // vt, half_v // vt, max(PIECES)
    pieces = n * n * CORES
    grid = (n // 2, 2, n // 2, 2)
    return pl.pallas_call(
        functools.partial(front_kernel, dims),
        name="front",
        out_shape=shapes([
            ((n_tile, *grid, CORES, cols, vt), BF16), *[((pieces, cols, tok), BF16)] * 4, ((2, 2 * n * cols, half_v // 2), F32), ((n_tile, tok, vt), BF16),
            ((n_half, tok, vt), BF16), ((n, BASE[-1], cols, quarter), BF16), ((PIECES[-1], cols, quarter), BF16), ((n_tile, tok, vt), F32),
            ((1, width), F32), ((SUB, min(LANE, quarter)), F32), ((CORES, tok, LANE), I32),
        ]),
        in_specs=specs(4, 2),
        out_specs=tuple(specs(0, 11) + specs(3, 0)),
        scratch_shapes=scratch([
            ((n_tile, cols, vt), BF16), ((CORES, n_half, cols, vt), BF16), ((CORES, SUB, tok), I32), ((half_v, CORES * tok), BF16),
            ((2, most, n_half, cols, vt), BF16), ((pieces, cols, tok), BF16), ((2, CORES, most, cols, tok), BF16), ((pieces, cols, tok), BF16),
            ((pieces, cols, quarter), BF16), ((2, pieces, cols, quarter), BF16), ((pieces, cols, quarter), BF16),
            ((4, *grid, CORES, cols, vt), BF16), ((tok, width), BF16), ((pieces, cols, tok), BF16),
            ((2, tok, vt), F32), ((2, tok, vt), F32), ((2, 2, tok, vt), BF16), ((tok, LANE), F32), ((tok, LANE), F32), ((tok, LANE), F32),
            ((tok, LANE), I32), ((2 * n + CORES, 1, width), F32), ((n, 2, tok), F32),
        ], dims["front_sems"][0], dims["front_sems"][1]),
        compiler_params=params(0, limit),
    )(shard, tok_row, lab_row, w, h, g)


def back_kernel(
    dims,
    gain_ref, loss_ref, tokc, lt_hbm, dz_hbm, dzp_hbm, et_hbm, xnt_hbm, xpar_hbm, gt_hbm, gpar_hbm, h_hbm, q5_hbm,
    tail_out, dh_out, de_out, x0_out, ra_hbm, rx_hbm,
    q5, dz_own, dz_par, et_buf, part, fx, acc, fa, f2, r2, xb, h_buf, dh_buf, dg_acc, slots,
    sends, recvs, local_sems,
):
    n, tok, vocab, width, tile, vt = (dims[k] for k in ("n", "tok", "vocab", "width", "tile", "vt"))
    place = Place(n, sends, recvs, local_sems)
    x, z, y, c = place.x, place.z, place.y, place.c
    half_v = vocab // CORES
    n_tile, n_half = vocab // vt, half_v // vt
    lanes = half_v // 2
    rows = width // (n * n)
    half_rows = rows // 2
    quarter = tok // n
    hq = quarter // 2
    tiles = dims["tiles"]
    chunks = len(tiles)
    edges = [sum(tiles[:d]) for d in range(chunks + 1)]
    per_half = n_half // 2

    with scope("b_enter"):
        place.enter()

    load_q5 = place.local("q5", q5_hbm, q5)
    load_q5.start()
    load_h = place.local("h", h_hbm.at[span(x * quarter, quarter, quarter)], h_buf)

    def load_et(t, slot):
        return place.local("et", et_hbm.at[:, span(t * tile, tile, tile)], et_buf.at[slot], slot)

    slot_of = {FAR: 0, 1: 1, 3: 2, 0: 0}
    stages = dims["stages"]

    def load_stage(m, i):
        half, k, kind = stages[m]
        src = ((gt_hbm, gpar_hbm), (xnt_hbm, xpar_hbm))[kind][i]
        src = src.at[(z + k) % n] if half == 0 else src.at[:, (y + k) % n]
        return place.local(("xb", i), src, xb.at[m % 2, i], m % 2)

    def start_stage(m):
        if m < len(stages):
            start_all(load_stage(m, i) for i in BOTH)

    loads = [place.local("dz", dz_hbm, dz_own), place.local("dzp", dzp_hbm, dz_par)]
    load_et(0, 0).start()
    start_all(loads)
    keep_q5 = place.local("q5", q5, x0_out.at[x], 1)

    def y_put(i):
        return place.send(("yp", i), q5, x0_out.at[x], dx=WAYS[i])

    def y_pass(i):
        size = q5.shape[0] // 2
        ref = x0_out.at[(x + FROM[i]) % n, pl.ds(i * size, size)]
        return place.send(("yq", i), ref, ref, dx=WAYS[i])

    def y_passes():
        for i in BOTH:
            y_put(i).wait_recv()
            y_pass(i).start()

    fars = [place.local("lt", lt_hbm.at[half], acc.at[half, 0], half) for half in BOTH]
    start_all(fars)
    for m in BOTH:
        start_stage(m)
    load_h.start()

    def columns(d):
        return pl.ds(edges[d] * tile, tiles[d] * tile)

    def dxn_chunk(d):
        def body(t, carry):
            slot = t % 2

            @pl.when(t + 1 < edges[chunks])
            def _():
                load_et(t + 1, 1 - slot).start()

            load_et(t, slot).wait()
            left = jnp.concatenate([dz_own[j] for j in range(n_tile)], axis=1)
            right = jnp.concatenate([et_buf[slot, j] for j in range(n_tile)], axis=1)
            part[:, span(t * tile, tile, tile)] = lax.dot_general(
                left, right, (((1,), (1,)), ((), ())), preferred_element_type=F32)
            return carry

        with scope("b_dxn"):
            lax.fori_loop(edges[d], edges[d + 1], body, 0)

    def qrow(k, lo=0, size=hq):
        return span((x + k) % n * quarter + lo, size, SUB)

    def x_far(d, i):
        return place.send(("xf", d, i), part.at[qrow(FAR, i * hq), columns(d)], fx.at[i, :, columns(d)], dx=WAYS[i])

    def x_near(d, i, j):
        src = part.at[qrow(WAYS[i], j * hq), columns(d)]
        return place.send(("xn", d, i, j), src, rx_hbm.at[i, pl.ds(j * hq, hq), columns(d)], dx=WAYS[i])

    def x_first(d):
        start_all(x_far(d, i) for i in BOTH)

    def x_second(d):
        with scope("b_x2"):
            for i in BOTH:
                x_far(d, i).wait_recv()
                sel = qrow(WAYS[i], i * hq)
                part[sel, columns(d)] = part[sel, columns(d)] + fx[i, :, columns(d)]
                start_all(x_near(d, i, j) for j in BOTH)

    def stage_x(d, j, i):
        return place.local("sx", rx_hbm.at[i, pl.ds(j * hq, hq), columns(d)], fx.at[i, :, columns(d)], i)

    def x_third(d, j):
        with scope("b_x3"):
            for i in BOTH:
                x_near(d, i, j).wait_recv()
                stage_x(d, j, i).start()
            for i in BOTH:
                stage_x(d, j, i).wait()
            sel = qrow(0, j * hq)
            part[sel, columns(d)] = part[sel, columns(d)] + fx[0, :, columns(d)] + fx[1, :, columns(d)]

    def de_stage(half, k, kind):
        m = stages.index((half, k, kind))
        slot = slot_of[k]

        wide = min(2, per_half) if kind and k else 1

        def right(i, t):
            if kind:
                return dz_par[t] if i else dz_own[c * n_half + t]
            ids = lax.broadcasted_iota(I32, (tok, LANE), 1) + (x * vocab + c * half_v + t * vt)
            hits = [jnp.where(tokc[i] == ids + b, dims["scale"], 0.0).astype(BF16) for b in range(0, vt, LANE)]
            return jnp.concatenate(hits, axis=1)

        def body(j, carry):
            t = half * per_half + j * wide
            sel = span(j * wide * vt, wide * vt)
            left = jnp.concatenate([xb[m % 2, i].reshape(n * rows, tok) for i in BOTH], axis=1)
            both_right = [jnp.concatenate([right(i, t + q) for i in BOTH], axis=0) for q in range(wide)]
            total = jnp.dot(left, jnp.concatenate(both_right, axis=1), preferred_element_type=F32)
            total = total.reshape(n, rows, wide * vt)
            acc[half, slot, :, :, sel] = acc[half, slot, :, :, sel] + total if kind else total
            return carry

        with scope("b_de" if kind else "b_look"):
            for i in BOTH:
                load_stage(m, i).wait()
            lax.fori_loop(0, per_half // wide, body, 0)
            start_stage(m + 2)

    def de_unit(half, k):
        if k == FAR:
            fars[half].wait()
        else:
            de_stage(half, k, 0)
        de_stage(half, k, 1)

    def ring(half, k):
        return {"dz": k} if half == 0 else {"dy": k}

    def cross(half, k):
        return {"dy": k} if half == 0 else {"dz": k}

    def a_far(half, i):
        return place.send(("af", half, i), acc.at[half, 0, pl.ds(2 * i, 2)], fa.at[half, i], **ring(half, WAYS[i]))

    def a_near(half, i, j):
        sel = pl.ds(2 * j, 2)
        return place.send(("an", half, i, j), acc.at[half, 1 + i, sel], ra_hbm.at[half, i, sel], **ring(half, WAYS[i]))

    def a_first(half):
        start_all(a_far(half, i) for i in BOTH)

    def a_second(half, i):
        with scope("b_a2"):
            a_far(half, i).wait_recv()
            sel = pl.ds(2 * i, 2)
            acc[half, 1 + i, sel] = acc[half, 1 + i, sel] + fa[half, i]
            start_all(a_near(half, i, j) for j in BOTH)

    def stage_a(half, j, i):
        return place.local(("sa", half), ra_hbm.at[half, i, pl.ds(2 * j, 2)], fa.at[half, i], i)

    def piece(half, k):
        return ((y if half == 0 else z) + k) % n

    def c_far(half, i):
        src = acc.at[half, 0, piece(half, FAR), pl.ds(i * half_rows, half_rows)]
        return place.send(("cf", half, i), src, f2.at[half, i], **cross(half, WAYS[i]))

    def c_near(half, i):
        return place.send(("cn", half, i), acc.at[half, 0, piece(half, WAYS[i])], r2.at[half, i], **cross(half, WAYS[i]))

    def a_third(half, j):
        with scope("b_a3"):
            for i in BOTH:
                a_near(half, i, j).wait_recv()
                stage_a(half, j, i).start()
            for i in BOTH:
                stage_a(half, j, i).wait()
            sel = pl.ds(2 * j, 2)
            acc[half, 0, sel] = acc[half, 0, sel] + fa[half, 0] + fa[half, 1]

    def c_first(half):
        start_all(c_far(half, i) for i in BOTH)

    def c_second(half):
        with scope("b_c2"):
            for i in BOTH:
                c_far(half, i).wait_recv()
                at = piece(half, WAYS[i])
                sel = pl.ds(i * half_rows, half_rows)
                acc[half, 0, at, sel] = acc[half, 0, at, sel] + f2[half, i]
                c_near(half, i).start()

    def out_copies(half):
        sel = span(c * half_v + half * lanes, lanes)
        mine = acc.at[half, 0, piece(half, 0)]
        yield place.local("de", mine.at[span(c * half_rows, half_rows, SUB)], de_out.at[:, sel], half)
        yield place.send(("de", half), mine.at[span((1 - c) * half_rows, half_rows, SUB)], de_out.at[:, sel], dc=1)

    def c_third(half):
        with scope("b_c3"):
            for i in BOTH:
                c_near(half, i).wait_recv()
            at = piece(half, 0)
            acc[half, 0, at] = acc[half, 0, at] + r2[half, 0] + r2[half, 1]
            start_all(out_copies(half))

    step = min(32, hq)

    def dh_body(i, carry):
        sel = span(i * step, step, step)
        row = span(x * quarter + i * step, step, step)
        d_x = part[row]
        h_wide = h_buf[sel].astype(F32)
        inv_rms = lax.rsqrt(jnp.sum(h_wide * h_wide, axis=1, keepdims=True) * (1.0 / width) + NORM_EPS)
        h_norm = h_wide * inv_rms
        g_dir = d_x * gain_ref[0:1]
        mean = jnp.sum(g_dir * h_norm, axis=1, keepdims=True) * (1.0 / width)
        dh_buf[sel] = (inv_rms * (g_dir - h_norm * mean)).astype(BF16)
        prod = d_x * h_norm
        total = prod[0:SUB]
        for j in range(SUB, step, SUB):
            total = total + prod[j:j + SUB]
        dg_acc[...] = dg_acc[...] + total
        return carry

    def h_first(i, j):
        return place.send(("hf", i, j), dh_buf.at[pl.ds(j * hq, hq)], dh_out.at[qrow(0, j * hq)], dx=WAYS[i])

    def h_second(i):
        ref = dh_out.at[qrow(FROM[i], i * hq)]
        return place.send(("hs", i), ref, ref, dx=WAYS[i])

    keep_dh = place.local("dh", dh_buf, dh_out.at[qrow(0, 0, quarter)])
    small = SmallSum(place, ("dc", "dx", "dy", "dz"), slots)
    per_j = hq // step

    def dh_part(j):
        with scope("b_dh"):
            if j == 0:
                load_h.wait()
            lax.fori_loop(j * per_j, (j + 1) * per_j, dh_body, 0)
            start_all(h_first(i, j) for i in BOTH)
            if j:
                keep_dh.start()

    def h_pass(i):
        with scope("b_h2"):
            h_first(i, i).wait_recv()
            h_second(i).start()

    def small_step(k):
        dims_of = small.dims
        with scope("b_s"):
            if k == 1:
                sums = [jnp.sum(part_sum, axis=0, keepdims=True) for part_sum in (dg_acc[...], loss_ref[...])]
                small.start(dims_of[0], jnp.concatenate(sums, axis=1))
            elif k <= len(dims_of):
                small.start(dims_of[k - 1], small.finish(dims_of[k - 2]))
            else:
                total = small.finish(dims_of[-1])
                loss = jnp.sum(total[:, width:], axis=1, keepdims=True) * (1.0 / dims["total"])
                tail_out[...] = jnp.concatenate([total[:, 0:width], jnp.broadcast_to(loss, (1, LANE))], axis=1)

    def dxn(d):
        dxn_chunk(d)
        x_first(d)

    def unit(half, k):
        if k == 0:
            with scope("b_wait_far"):
                for i in BOTH:
                    a_far(half, i).wait_send()
        while len(loads) > 1:
            loads.pop().wait()
        de_unit(half, k)
        if k == FAR:
            a_first(half)

    families = {
        "CH": dxn, "XS": x_second, "UN": unit, "AS": a_second, "XT": x_third, "AT": a_third, "CF": c_first, "CS": c_second,
        "CT": c_third, "DH": dh_part, "SM": small_step, "HP": h_pass, "YQ": y_passes,
    }

    def perform(text):
        for word in text.split():
            families[word[:2]](*(int(digit) for digit in word[2:]))

    with scope("b_load"):
        load_q5.wait()
        start_all(y_put(i) for i in BOTH)
        keep_q5.start()
        loads[0].wait()
        dg_acc[...] = jnp.zeros_like(dg_acc)
    for text in (
        "CH0 UN02 YQ CH1", "UN12 CH2 UN03 XS1", "UN01 XS2 UN13 AS01", "AS00 UN11 AS11 AS10",
        "XS0 CH3 XT10 CH4", "UN00 XT00 XS3 XT01", "XS4 UN10 XT20 AT00", "XT30 XT21 XT11 XT40",
        "DH0 XT31 XT41 DH1", "AT01 AT10 CF0 SM1", "AT11 CF1 SM2 HP0", "CS0 CS1 SM3 HP1", "CT0 SM4 CT1 SM5",
    ):
        perform(text)

    with scope("b_end_x"):
        keep_dh.wait()
        keep_q5.wait()
        for i in BOTH:
            y_put(i).wait_send()
            y_pass(i).wait()
            for d in range(chunks):
                x_far(d, i).wait_send()
                for j in BOTH:
                    x_near(d, i, j).wait_send()
            h_first(i, i).wait_send()
            h_first(i, 1 - i).wait()
            h_second(i).wait()
    with scope("b_end_a"):
        for half in BOTH:
            for i in BOTH:
                for j in BOTH:
                    a_near(half, i, j).wait_send()
                c_far(half, i).wait_send()
                c_near(half, i).wait_send()
            for copy in out_copies(half):
                copy.wait()
    assert (place.n_link, place.n_local) <= dims["back_sems"], (place.n_link, place.n_local)


def back(dims, limit, gain, loss, tokc, far, dz, dzp, et, xnt, xpar, gt, gpar, h, q5):
    n, tok, vocab, width, tile = (dims[k] for k in ("n", "tok", "vocab", "width", "tile"))
    rows = width // (n * n)
    half_v = vocab // CORES
    lanes = half_v // 2
    quarter = tok // n
    hq = quarter // 2
    tail_w = width + loss.shape[1]
    n_tile, n_half, vt = dz.shape[0], dzp.shape[0], dims["vt"]
    turned = [a.reshape(n, n, rows, tok) for a in (xnt, xpar, gt, gpar)]
    return pl.pallas_call(
        functools.partial(back_kernel, dims),
        name="back",
        out_shape=shapes([
            ((1, width + LANE), F32), ((tok, width), BF16), ((rows // CORES, vocab), F32), ((n, *q5.shape), BF16),
            ((2, 2, n, rows, lanes), F32),
            ((2, quarter, width), F32),
        ]),
        in_specs=specs(3, 10),
        out_specs=tuple(specs(1, 5)),
        scratch_shapes=scratch([
            (q5.shape, BF16), ((n_tile, tok, vt), BF16), ((n_half, tok, vt), BF16), ((2, n_tile, tile, vt), BF16), ((tok, width), F32),
            ((2, hq, width), F32), ((2, 3, n, rows, lanes), F32), ((2, 2, 2, rows, lanes), F32),
            ((2, 2, rows // 2, lanes), F32), ((2, 2, rows, lanes), F32), ((2, CORES, n, rows, tok), BF16), ((quarter, width), BF16),
            ((quarter, width), BF16), ((SUB, width), F32), ((3 * n + CORES, 1, tail_w), F32),
        ], dims["back_sems"][0], dims["back_sems"][1]),
        compiler_params=params(1, limit),
    )(gain, loss, tokc, far.reshape(2, n, rows, lanes), dz, dzp, et.reshape(n_tile, width, vt), *turned, h, q5)[:4]


def finish_kernel(
    n, scale, table_ref, tail_ref, x0_hbm, x5_hbm, dh_hbm, de_hbm, dg_out, loss_out, x0_out, dh_out, de_out,
    x0_in, x0_buf, rows_ref, dh_buf, de_buf, sems,
):
    place = Place(n, None, None, sems)
    quarter, cols, width = x0_in.shape[3], x0_in.shape[2], x0_buf.shape[2]

    def step(q):
        rows = span(q * quarter, quarter, quarter)
        return (
            place.local("x0", x0_hbm.at[q], x0_in.at[q, pl.ds(0, BASE[-1])], q, n),
            place.local("x5", x5_hbm.at[q], x0_in.at[q, pl.ds(BASE[-1], PIECES[-1])], q, n), place.local("x0o", x0_buf.at[q], x0_out.at[rows], q, n),
            place.local("dh", dh_hbm.at[rows], dh_buf.at[q], q, n), place.local("dho", dh_buf.at[q], dh_out.at[rows], q, n),
        )

    moves = [step(q) for q in range(n)]
    de_in, de_put = place.local("de", de_hbm, de_buf, 0), place.local("de", de_buf, de_out, 1)
    for x0_load, x5_load, _, dh_load, _ in moves:
        start_all((x0_load, x5_load, dh_load))
    de_in.start()
    gain = jnp.broadcast_to(tail_ref[:, 0:width], (SUB, width))
    dg_out[...] = pltpu.roll(gain, width - place.f * cols, axis=1)[0:1, 0:cols]
    loss_out[...] = tail_ref[:, width:width + 1]

    def body(q, carry):
        x0_load, x5_load, x0_put, dh_load, dh_put = step(q)
        x0_load.wait()
        x5_load.wait()
        for zi in range(n):
            for yi in range(n):
                for h in BOTH:
                    dz, dy = (zi - place.z) % n, (yi - place.y) % n
                    k1, k2 = (dy, dz) if h == 0 else (dz, dy)
                    piece = table_ref[(h * n + k1) * n + k2]
                    rows_ref[pl.ds(((zi * n + yi) * CORES + h) * cols, cols)] = x0_in[q, piece]
        x0_buf[q] = (rows_ref[...].T.astype(F32) * scale).astype(BF16)
        x0_put.start()
        dh_load.wait()
        dh_put.start()
        return carry

    lax.fori_loop(0, n, body, 0)
    de_in.wait()
    de_put.start()
    for _, _, x0_put, _, dh_put in moves:
        x0_put.wait()
        dh_put.wait()
    de_put.wait()


def finish(n, scale, limit, tail, x0, x5, dh, de):
    cols, quarter = x0.shape[2:]
    pieces = n * n * CORES
    width = pieces * cols
    table = np.zeros((CORES, n, n), np.int32)
    for u, unit in enumerate(UNITS):
        for h in BOTH:
            for i, (k1, k2) in enumerate(unit):
                table[h, k1, k2] = BASE[u] + h * len(unit) + i
    return pl.pallas_call(
        functools.partial(finish_kernel, n, scale),
        name="finish",
        in_specs=[pl.BlockSpec(memory_space=pltpu.SMEM)] + specs(1, 4),
        out_specs=tuple(specs(2, 3)),
        out_shape=shapes([((1, cols), F32), ((1, 1), F32), (dh.shape, BF16), (dh.shape, BF16), (de.shape, F32)]),
        scratch_shapes=[
            pltpu.VMEM((n, pieces, cols, quarter), BF16), pltpu.VMEM((n, quarter, width), BF16), pltpu.VMEM((width, quarter), BF16),
            pltpu.VMEM((n, quarter, width), BF16), pltpu.VMEM(de.shape, F32), pltpu.SemaphoreType.DMA((5 * n + 2,)),
        ],
        compiler_params=pltpu.CompilerParams(vmem_limit_bytes=limit),
    )(jnp.asarray(table.reshape(-1)), tail, x0, x5, dh, de)


def solution(mesh):
    return build(mesh, mesh.shape["tp"], 256, digits("12222")[0], 256, 6, 67_000_000)


def build(mesh, n, tile, tiles, vt, n_block, limit):
    fsdp_size = mesh.shape["fsdp"]

    def device_step(emb_shard, tok_ids, lab_ids, h_last, g_embed, norm_w):
        vocab_rows, cols = emb_shard.shape
        batch_loc, seq_len, width = h_last.shape
        tok_count = batch_loc * seq_len
        fsdp_id = lax.axis_index("fsdp")
        scale = float(np.asarray(math.sqrt(width)).astype(jnp.bfloat16))
        dims = {
            "n": n, "tok": tok_count, "vocab": vocab_rows, "width": width, "total": tok_count * fsdp_size, "vt": vt,
            "tile": tile, "tiles": tiles, "scale": scale, "n_block": n_block,
            "stages": digits("021 121 030 031") + digits("010 011 130 131") + digits("110 111 000 001") + digits("100 101"),
            "front_sems": (106, 52), "back_sems": (72, 26),
        }
        h_flat = h_last.reshape(tok_count, width)
        placed = lax.dynamic_update_slice(jnp.zeros((SUB, width), F32), jnp.broadcast_to(norm_w, (SUB, cols)), (0, fsdp_id * cols))
        ids = [a.reshape(1, tok_count) for a in (tok_ids, lab_ids)]
        table, xn_t, xpar_t, g_t, gpar_t, far, dz, dzp, x0, q5, _, gain, loss_part, tokc = front(
            dims, limit, emb_shard.T, *ids, norm_w.reshape(1, cols), h_flat, g_embed.reshape(tok_count, width))
        tail, d_hidden, d_cols, x5 = back(dims, limit, gain, loss_part, tokc, far, dz, dzp, table, xn_t, xpar_t, g_t, gpar_t, h_flat, q5)
        d_norm_w, loss, x_emb, d_hidden, d_cols = finish(n, scale, limit, tail, x0, x5, d_hidden, d_cols)
        return (x_emb.reshape(h_last.shape), loss.reshape(()), d_hidden.reshape(h_last.shape), d_norm_w.reshape(cols), d_cols.T)

    spec_tok = P("fsdp", None)
    spec_act = P("fsdp", None, None)
    return jax.shard_map(device_step, mesh=mesh, in_specs=(P("tp", "fsdp"), spec_tok, spec_tok, spec_act, spec_act, P("fsdp")), out_specs=(spec_act, P(), spec_act, P("fsdp"), P("tp", "fsdp")), check_vma=False)
```

```python
import functools
import math
import jax
import numpy as np
import jax.numpy as jnp
from jax import lax
from jax.experimental import pallas as pl
from jax.experimental.pallas import tpu as pltpu
from jax.sharding import PartitionSpec as P

SOFT_CAP = 30.0
NORM_EPS = 1e-6
F32, BF16, I32 = jnp.float32, jnp.bfloat16, jnp.int32
LANE, SUB = 128, 8
BOTH = (0, 1)
FOUR = range(4)
WAYS = (1, 3)
FROM = (3, 1)
FAR = 2
CORES = 2


def span(start, size, unit=LANE):
    return pl.ds(pl.multiple_of(start, unit), size)


class Place:
    def __init__(self, n, sends, recvs, local_sems):
        self.n, self.sends, self.recvs, self.local_sems = n, sends, recvs, local_sems
        self.x = lax.axis_index("tp")
        f = lax.axis_index("fsdp")
        self.f = f
        self.c = f % CORES
        self.y = f // CORES % n
        self.z = f // CORES // n
        self.link_of, self.local_of, self.n_link, self.n_local = {}, {}, 0, 0
        self.size = {"dx": n, "dz": n, "dy": n, "dc": CORES}
        self.me = {"dx": self.x, "dz": self.z, "dy": self.y, "dc": self.c}

    def at(self, dx=0, dz=0, dy=0, dc=0):
        n = self.n
        z, y, c = (self.z + dz) % n, (self.y + dy) % n, (self.c + dc) % CORES
        return ((self.x + dx) % n, (z * n + y) * CORES + c)

    def enter(self):
        barrier = pltpu.get_barrier_semaphore()
        peers = [self.at(**{d: k}) for d in self.size for k in range(1, self.size[d])]
        for peer in peers:
            pl.semaphore_signal(barrier, inc=1, device_id=peer, device_id_type=pl.DeviceIdType.MESH)
        pl.semaphore_wait(barrier, len(peers))

    def link(self, key, count=1):
        if key not in self.link_of:
            self.link_of[key] = self.n_link
            self.n_link += count
        return self.link_of[key]

    def send(self, key, src, dst, **step):
        i = self.link(key)
        return pltpu.make_async_remote_copy(
            src, dst, self.sends.at[i], self.recvs.at[i], device_id=self.at(**step), device_id_type=pl.DeviceIdType.MESH)

    def local(self, key, src, dst, slot=0, count=2):
        if key not in self.local_of:
            self.local_of[key] = self.n_local
            self.n_local += count
        return pltpu.make_async_copy(src, dst, self.local_sems.at[self.local_of[key] + slot])


class SmallSum:
    def __init__(self, place, dims, slots):
        self.place, self.slots, self.dims, self.base = place, slots, dims, {}
        count = 0
        for d in dims:
            self.base[d] = count
            count += place.size[d]

    def copies(self, d):
        slot = self.slots.at[self.base[d] + self.place.me[d]]
        for k in range(1, self.place.size[d]):
            yield self.place.send((self.dims, d, k), slot, slot, **{d: k})

    def start(self, d, value):
        self.slots[self.base[d] + self.place.me[d]] = value
        for copy in self.copies(d):
            copy.start()

    def finish(self, d):
        for copy in self.copies(d):
            copy.wait()
        total = self.slots[self.base[d]]
        for k in range(1, self.place.size[d]):
            total = total + self.slots[self.base[d] + k]
        return total


def scope(name):
    return jax.named_scope(name)


def start_all(copies):
    for copy in copies:
        copy.start()


def digits(text):
    return tuple(tuple(int(d) for d in word) for word in text.split())


UNITS = [digits(u) for u in ("00", "10 30", "01 03 20", "02 11 31", "13 33 21 23", "12 32 22")]
PAIR, ALL = 1, "all"
PIECES = [2 * len(u) for u in UNITS]
EXP_RATE = SOFT_CAP * math.log2(math.e)
BASE = [sum(PIECES[:i]) for i in range(len(UNITS))]


def front_kernel(
    dims,
    shard_ref, tok_ref, lab_ref, w_ref, h_hbm, g_hbm,
    et_out, xnt_out, xpar_out, gt_out, gpar_out, lt_out, dz_out, dzpar_out, x0_out, q5_out, u_hbm, gain_out, loss_out, tokc_out,
    shard_t, chunk, tokr, hit_t, lhs, xp, xw, xr, xf, xg, xq, etb, xn, gl, z_even, z_odd, dzb,
    acc_e, acc_l, inv_s, labc, w_slots, s_slots, sends, recvs, local_sems,
):
    n, tok, vocab, width, vt = dims["n"], dims["tok"], dims["vocab"], dims["width"], dims["vt"]
    place = Place(n, sends, recvs, local_sems)
    x, z, y, c = place.x, place.z, place.y, place.c
    half_v = vocab // CORES
    n_tile = vocab // vt
    n_half = n_tile // CORES
    hh = n_half // 2
    cols = width // (n * n * CORES)
    quarter = tok // n
    row_start = x * vocab

    def ring1(h, k):
        return {"dy": k} if h == 0 else {"dz": k}

    def ring2(h, k):
        return {"dz": k} if h == 0 else {"dy": k}

    def coord(base, k, paired):
        every = slice(None)
        if k == ALL:
            return every, every
        return every if paired else (base + k) % n // 2, (base + k) % 2

    def loc(h, k1, k2, lo=0, size=n_half, pair1=False, pair2=False):
        first, second = coord((y, z)[h], k1, pair1), coord((z, y)[h], k2, pair2)
        return et_out.at[(pl.ds(c * n_half + lo, size), *((second, first)[h]), *((first, second)[h]), h)]

    with scope("f_enter"):
        place.enter()

    load_g = place.local("g", g_hbm, xn)
    load_g.start()
    with scope("f_cast"):
        for t in range(n_tile):
            shard_t[t] = shard_ref[:, pl.ds(t * vt, vt)].astype(BF16)
        tokr[c] = jnp.broadcast_to(tok_ref[...], (SUB, tok))
        give_tok = place.send("tok", tokr.at[c], tokr.at[c], dc=1)
        give_chunk = place.send("chunk", shard_t.at[pl.ds((1 - c) * n_half, n_half)], chunk.at[c], dc=1)
        give_chunk.start()
        give_tok.start()
        chunk[c] = shard_t[pl.ds(c * n_half, n_half)]
        gain_sum = SmallSum(place, ("dc", "dy", "dz"), w_slots)
        own_w = jnp.concatenate([w_ref[...], jnp.zeros((1, width - cols), F32)], axis=1)
        gain_sum.start("dc", pltpu.roll(jnp.broadcast_to(own_w, (SUB, width)), place.f * cols, axis=1)[0:1])

    def p1_send(h, i):
        return place.send(("p1", h, i), chunk.at[h], loc(h, 0, 0), **ring1(h, WAYS[i]))

    def p1_fwd(h, i):
        ref = loc(h, FROM[i], 0, i * hh, hh)
        return place.send(("p1f", h, i), ref, ref, **ring1(h, WAYS[i]))

    def p2_send(h, k1, i):
        ref = loc(h, k1, 0, pair1=k1 == PAIR)
        return place.send(("p2", h, k1, i), chunk.at[h] if k1 == 0 else ref, ref, **ring2(h, WAYS[i]))

    def p2_fwd(h, k1, i):
        ref = loc(h, k1, FROM[i], i * hh, hh, pair1=k1 == PAIR)
        return place.send(("p2f", h, k1, i), ref, ref, **ring2(h, WAYS[i]))

    def keep(h):
        return place.local("keep", chunk.at[h], loc(h, 0, 0), h)

    def share(h, k2):
        ref = loc(h, ALL, k2, pair2=k2 == PAIR)
        return place.send(("share", h, k2), ref, ref, dc=1)

    def pass_first():
        with scope("f_p1"):
            for h in BOTH:
                for i in BOTH:
                    p1_send(h, i).wait_recv()
                    p1_fwd(h, i).start()
            for h in BOTH:
                start_all(p2_send(h, PAIR, i) for i in BOTH)

    def pass_first_far():
        with scope("f_p1f"):
            for h in BOTH:
                for i in BOTH:
                    p1_fwd(h, i).wait_recv()
                start_all(p2_send(h, FAR, j) for j in BOTH)

    def pass_second(k1):
        with scope("f_p2"):
            for h in BOTH:
                for i in BOTH:
                    p2_send(h, k1, i).wait_recv()
                    p2_fwd(h, k1, i).start()

    def end_second(k1):
        with scope("f_p2f"):
            for h in BOTH:
                for i in BOTH:
                    p2_fwd(h, k1, i).wait_recv()

    def share_group(k2):
        start_all(share(h, k2) for h in BOTH)

    with scope("f_chunk"):
        give_chunk.wait_recv()
        start_all(keep(h) for h in BOTH)
        gain_sum.start("dy", gain_sum.finish("dc"))
        for h in BOTH:
            start_all(p1_send(h, i) for i in BOTH)
        for h in BOTH:
            start_all(p2_send(h, 0, i) for i in BOTH)

    v_step = min(LANE, half_v)

    def hit_body(j, carry):
        off = j * v_step
        ids = lax.broadcasted_iota(I32, (v_step, tok), 0) + (row_start + c * half_v + off)
        for i, core in enumerate((c, 1 - c)):
            hit_t[span(off, v_step, v_step), pl.ds(i * tok, tok)] = jnp.where(ids == tokr[core, 0:1, :], 1.0, 0.0).astype(BF16)
        return carry

    def make_hits():
        with scope("f_hit"):
            give_tok.wait_recv()
            lax.fori_loop(0, half_v // v_step, hit_body, 0)

    n_step = min(512, tok)
    most = max(PIECES)

    def whole(u):
        return pl.ds(BASE[u], PIECES[u])

    def unit_copies(u):
        slot = u % 2
        for p, (h, (k1, k2)) in enumerate((h, k) for h in BOTH for k in UNITS[u]):
            yield place.local("lhs", loc(h, k1, k2), lhs.at[slot, p], slot * most + p, 2 * most)

    def load_unit(u):
        start_all(unit_copies(u))

    def look(u):
        pieces = PIECES[u]
        with scope("f_look"):
            if u > 1:
                x_swap(u - 2).wait_send()
            left = lhs.at[u % 2]
            for copy in unit_copies(u):
                copy.wait()
            per_core = tok // n_step

            def body(j, carry):
                value = jnp.concatenate([left[pl.ds(0, pieces), t].reshape(pieces * cols, vt) for t in range(n_half)], axis=1)
                rows = jnp.dot(value, hit_t[:, span(j * n_step, n_step)], preferred_element_type=F32)
                rows = rows.reshape(pieces, cols, n_step).astype(BF16)
                xw[u % 2, j // per_core, pl.ds(0, pieces), :, span(j % per_core * n_step, n_step)] = rows
                return carry

            lax.fori_loop(0, CORES * per_core, body, 0)
            x_swap(u).start()

    def x_swap(u):
        return place.send(("swap", u), xw.at[u % 2, 1, pl.ds(0, PIECES[u])], xr.at[whole(u)], dc=1)

    def lanes_of(k):
        return span((x + k) % n * quarter, quarter, quarter)

    def side(u, i):
        return pl.ds(BASE[u] + i * len(UNITS[u]), len(UNITS[u]))

    def x_far(u, i):
        return place.send(("xf", u, i), xp.at[side(u, i), :, lanes_of(FAR)], xf.at[side(u, i)], dx=WAYS[i])

    def x_near(u, i):
        return place.send(("xn", u, i), xp.at[whole(u), :, lanes_of(WAYS[i])], xg.at[i, whole(u)], dx=WAYS[i])

    def x_goal(k, sel):
        return x0_out.at[(x + k) % n, sel]

    def x_put(u, i):
        return place.send(("xp", u, i), xq.at[whole(u)], x_goal(0, whole(u)), dx=WAYS[i])

    last_unit = len(UNITS) - 1

    def x_keep(u):
        goal = x_goal(0, whole(u)) if u < last_unit else q5_out
        return place.local("x0", xq.at[whole(u)], goal, u, len(UNITS))

    def x_pass(u, i):
        ref = x_goal(FROM[i], side(u, i))
        return place.send(("xs", u, i), ref, ref, dx=WAYS[i])

    def x_first(u):
        with scope("f_x1"):
            x_swap(u).wait_recv()
            def body(p, carry):
                xp[BASE[u] + p] = xw[u % 2, 0, p] + xr[BASE[u] + p]
                return carry

            lax.fori_loop(0, PIECES[u], body, 0)
            start_all(x_far(u, i) for i in BOTH)

    def x_second(u):
        with scope("f_x2"):
            for i in BOTH:
                x_far(u, i).wait_recv()
                sel, lanes = side(u, i), lanes_of(WAYS[i])
                xp[sel, :, lanes] = xp[sel, :, lanes] + xf[sel]
                x_near(u, i).start()

    def x_third(u):
        with scope("f_x3"):
            for i in BOTH:
                x_near(u, i).wait_recv()
            sel = whole(u)
            xq[sel] = xp[sel, :, lanes_of(0)] + xg[0, sel] + xg[1, sel]
            if u < last_unit:
                start_all(x_put(u, i) for i in BOTH)
            x_keep(u).start()

    def x_fourth(u):
        with scope("f_x4"):
            for i in BOTH:
                x_put(u, i).wait_recv()
                x_pass(u, i).start()

    n_part = n * n * CORES // 2

    def moves(key, part, whole_t, other):
        sel = pl.ds(part * n_part, n_part)
        yield place.local(key, gl.at[sel], whole_t.at[sel], part)
        yield place.send((key, part), gl.at[sel], other.at[sel], dc=1)

    def move_g(part):
        return moves("g", part, gt_out, gpar_out)

    def move_xn(part):
        return moves("xt", part, xnt_out, xpar_out)

    def transpose_part(part, copies):
        block = width // dims["n_block"]
        first = part * dims["n_block"] // 2
        turned = [xn[:, pl.ds((first + j) * block, block)].T for j in range(dims["n_block"] // 2)]
        gl[pl.ds(part * n_part, n_part)] = jnp.concatenate(turned, axis=0).reshape(n_part, cols, tok)
        start_all(copies)

    def columns(row):
        return jnp.broadcast_to(row.astype(F32), (LANE, tok)).T.astype(I32)

    r_step = min(LANE, tok)

    def xn_body(j, carry):
        sel = span(j * r_step, r_step, r_step)
        h_wide = xn[sel].astype(F32)
        inv_rms = lax.rsqrt(jnp.sum(h_wide * h_wide, axis=1, keepdims=True) * (1.0 / width) + NORM_EPS)
        xn[sel] = (h_wide * inv_rms * gain_out[0:1]).astype(BF16)
        return carry

    e_step = min(LANE, tok)

    def tile_of(j):
        return (c * n_half + j) % n_tile

    def load_tile(j):
        return place.local("et", et_out.at[tile_of(j)], etb.at[j % 4], j % 4, 4)

    def save_u(i, odd):
        return place.local(("u", odd), (z_even, z_odd)[odd].at[i % 2], u_hbm.at[tile_of(2 * i + odd)], i % 2)

    def lane_blocks():
        return [(b, pl.ds(b, LANE)) for b in range(0, vt, LANE)]

    def post_tile(i, odd):
        base = tile_of(2 * i + odd) * vt
        buf, slot = (z_even, z_odd)[odd], i % 2

        def body(e, carry):
            sel = span(e * e_step, e_step, e_step)
            ids = lax.broadcasted_iota(I32, (e_step, LANE), 1) + base
            sum_e, sum_l = acc_e[sel], acc_l[sel]
            for b, lanes in lane_blocks():
                tanh_z = jnp.tanh(buf[slot, sel, lanes] * (1.0 / SOFT_CAP))
                buf[slot, sel, lanes] = tanh_z
                sum_e = sum_e + jnp.exp2(EXP_RATE * tanh_z - EXP_RATE)
                sum_l = sum_l + jnp.where(ids + b == labc[sel], tanh_z, 0.0)
            acc_e[sel] = sum_e
            acc_l[sel] = sum_l
            return carry

        lax.fori_loop(0, tok // e_step, body, 0)

    def dot_pair(i):
        for odd in BOTH:
            value = etb[(2 * i + odd) % 4].reshape(width, vt)
            (z_even, z_odd)[odd][i % 2] = jnp.dot(xn[...], value, preferred_element_type=F32)

    def load_pair(i):
        start_all(load_tile(2 * i + odd) for odd in BOTH)

    def pair(i, carry):
        for odd in BOTH:
            load_tile(2 * i + odd).wait()

        @pl.when(i > 1)
        def _():
            for odd in BOTH:
                save_u(i - 2, odd).wait()

        for odd in BOTH:
            post_tile(i - 1, odd)

            @pl.when(i < last)
            def _():
                save_u(i - 1, odd).start()

        dot_pair(i)

        @pl.when(i + 2 < n_tile // 2)
        def _():
            load_pair(i + 2)

        for k, work in enumerate(during):
            @pl.when(i == k + 1)
            def _():
                if k == 0:
                    wait_shares()
                perform(work)
        return carry

    def wait_shares():
        with scope("f_share"):
            for h in BOTH:
                for k2 in (0, PAIR, FAR):
                    share(h, k2).wait_recv()

    def logits_first():
        acc_e[...] = jnp.zeros_like(acc_e)
        acc_l[...] = jnp.zeros_like(acc_l)
        with scope("f_logits0"):
            far_ends(1)
            for odd in BOTH:
                load_tile(odd).wait()
            dot_pair(0)
            if n_tile // 2 > 2:
                load_pair(2)

    def load_first():
        for i in BOTH:
            load_pair(i)

    def lay_columns():
        with scope("f_cols"):
            labc[...] = columns(lab_ref[...] - row_start)
            for i, core in enumerate((c, 1 - c)):
                tokc_out[i] = columns(tokr[core, 0:1, :])

    def turn_g():
        with scope("f_gt"):
            load_g.wait()
            for part in BOTH:
                transpose_part(part, move_g(part))
            load_h.start()

    def gain_next():
        with scope("f_gain2"):
            gain_sum.start("dz", gain_sum.finish("dy"))

    def normalize():
        with scope("f_xn"):
            gain_out[...] = 1.0 + gain_sum.finish("dz")
            load_h.wait()
            lax.fori_loop(0, tok // r_step, xn_body, 0)

    def turn_xn():
        with scope("f_xt"):
            for part in BOTH:
                transpose_part(part, move_xn(part))

    spare = BASE[3]
    own_rows, their_rows = (pl.ds(spare + i * 2 * n, 2 * n) for i in BOTH)

    def far_loads(h):
        for i, (src, rows) in enumerate(((gt_out, own_rows), (gpar_out, their_rows))):
            if h == 0:
                yield place.local("far", src.at[pl.ds((z + FAR) % n * 2 * n, 2 * n)], xp.at[rows], i * n, 2 * n)
            else:
                for q in range(n):
                    piece = src.at[pl.ds((q * n + (y + FAR) % n) * 2, 2)]
                    yield place.local("far", piece, xp.at[pl.ds(spare + i * 2 * n + 2 * q, 2)], i * n + q)

    def far_load(h):
        if h == 0:
            for part in BOTH:
                for copy in move_g(part):
                    copy.wait()
        start_all(far_loads(h))

    def put_far(h, j):
        rows = pl.ds(0, 2 * n * cols)
        return place.local("lt", z_even.at[j % 2, rows], lt_out.at[h, :, span(j * vt, vt)], j % 2)

    def far_ends(h):
        for j in range(hh - 2, hh):
            put_far(h, j).wait()

    def far_look(h):
        def body(j, carry):
            @pl.when(j > 1)
            def _():
                put_far(h, j - 2).wait()

            left = jnp.concatenate([xp[rows].reshape(2 * n * cols, tok) for rows in (own_rows, their_rows)], axis=1)
            right = hit_t[span((h * hh + j) * vt, vt)]
            value = lax.dot_general(left, right, (((1,), (1,)), ((), ())), preferred_element_type=F32)
            z_even[j % 2, pl.ds(0, 2 * n * cols)] = value * dims["scale"]
            put_far(h, j).start()
            return carry

        with scope("f_far"):
            for copy in far_loads(h):
                copy.wait()
            if h:
                far_ends(0)
            lax.fori_loop(0, hh, body, 0)

    def begin_unit(u):
        if u == 0:
            for h in BOTH:
                keep(h).wait()
        load_unit(u)

    load_h = place.local("h", h_hbm, xn)
    works = {
        "HIT": make_hits, "GT": turn_g, "COL": lay_columns, "G2": gain_next, "XN": normalize, "XT": turn_xn, "LP": load_first, "L0": logits_first,
        "PF": pass_first, "PFF": pass_first_far,
    }
    groups = {"0": 0, "P": PAIR, "F": FAR}
    families = {"LF": far_load, "FL": far_look, "LU": begin_unit, "LK": look, "X1": x_first, "X2": x_second, "X3": x_third, "X4": x_fourth}
    families_k = {"SH": share_group, "S": pass_second, "E": end_second}

    def perform(text):
        for word in text.split():
            if word in works:
                works[word]()
            elif word[:-1] in families:
                families[word[:-1]](int(word[-1]))
            else:
                families_k[word[:-1]](groups[word[-1]])

    during = (
        "X24",
        "X15 X33",
        "",
        "X34",
        "",
        "X25",
        "",
    )
    for text in (
        "HIT LU0 LK0 G2", "GT PF X10 LU1", "LK1 XN LF0 S0", "X11 FL0 PFF X21", "LU2 LF1 LK2 FL1",
        "SP SH0 E0 LU3", "X12 X20 LK3 SF", "LU4 X22 X31 SHP", "LK4 X13 EP X30", "X32 EF LU5 SHF",
        "LP XT COL L0", "X14 LK5 X23",
    ):
        perform(text)
    if n_half < 4:
        wait_shares()
        for text in during:
            perform(text)
        during = ()
    last = n_tile // 2 - 1
    with scope("f_logits"):
        lax.fori_loop(1, last + 1, pair, 0)
        for odd in BOTH:
            post_tile(last, odd)

    with scope("f_stats"):
        row = lax.broadcasted_iota(I32, (2, tok), 0)
        sum_e = jnp.sum(acc_e[...].T, axis=0, keepdims=True)
        sum_l = SOFT_CAP * jnp.sum(acc_l[...].T, axis=0, keepdims=True)
        stats = SmallSum(place, ("dx",), s_slots)
        stats.start("dx", jnp.where(row == 0, sum_e, sum_l))
    perform("X43 X42 X40 X44")
    perform("X41")
    with scope("f_stats2"):
        stat = stats.finish("dx")
        all_e, all_l = stat[0:1], stat[1:2]
        inv_s[...] = jnp.broadcast_to((1.0 / dims["total"]) / all_e, (LANE, tok)).T
        s_slots[0, 0:1, :] = jnp.log(all_e) + SOFT_CAP - all_l
        own = s_slots[0, 0:1, lanes_of(0)]
        part_w = min(LANE, quarter)
        folded = own[:, 0:part_w]
        for j in range(part_w, quarter, part_w):
            folded = folded + own[:, j:j + part_w]
        loss_out[...] = jnp.where(lax.broadcasted_iota(I32, (SUB, part_w), 0) == 0, folded, 0.0)

    def dz_tile(j):
        return ((1 - c) * n_half + j) % n_tile

    def load_u(i, odd):
        return place.local(("u", odd), u_hbm.at[dz_tile(2 * i + odd)], (z_even, z_odd)[odd].at[i % 2], i % 2)

    def put_dz(i, odd):
        return place.local(("dz", odd), dzb.at[odd, i % 2], dz_out.at[dz_tile(2 * i + odd)], i % 2)

    def give_dz(part):
        src = dz_out.at[pl.ds((1 - c) * n_half + part * hh, hh)]
        return place.send(("dz", part), src, dzpar_out.at[pl.ds(part * hh, hh)], dc=1)

    d_step = min(256, tok)

    def dz_rows(i, odd):
        base = dz_tile(2 * i + odd) * vt
        buf, slot = (z_even, z_odd)[odd], i % 2

        def body(e, carry):
            sel = span(e * d_step, d_step, d_step)
            ids = lax.broadcasted_iota(I32, (d_step, LANE), 1) + base
            for b, lanes in lane_blocks():
                tanh_z = buf[slot, sel, lanes]
                prob = jnp.exp2(EXP_RATE * tanh_z - EXP_RATE) * inv_s[sel]
                prob = jnp.where(ids + b == labc[sel], prob - 1.0 / dims["total"], prob)
                dzb[odd, slot, sel, lanes] = (prob * (1.0 - tanh_z * tanh_z)).astype(BF16)
            return carry

        lax.fori_loop(0, tok // d_step, body, 0)

    def dz_pair(i, loaded, follow):
        for odd in BOTH:
            if loaded:
                load_u(i, odd).wait()

            @pl.when(i > hh + 1)
            def _():
                put_dz(i - 2, odd).wait()

            dz_rows(i, odd)
            put_dz(i, odd).start()

            @pl.when(i + follow < n_tile // 2)
            def _():
                load_u(i + follow, odd).start()

    def dz_run(lo, hi, loaded, follow):
        def body(i, carry):
            dz_pair(i, loaded, follow)
            return carry

        lax.fori_loop(lo, hi, body, 0)

    with scope("f_dz"):
        half = hh // 2
        for part in (1, 0):
            dz_run(part * half, (part + 1) * half, not part, hh if part == 0 else -half)
            for i in range(part * half, (part + 1) * half):
                for odd in BOTH:
                    put_dz(i, odd).wait()
            give_dz(part).start()
        dz_run(hh, n_tile // 2, True, half)

    perform("X35")
    with scope("f_end"):
        for part in BOTH:
            give_dz(part).wait()
        for i in range(n_tile // 2 - 2, n_tile // 2):
            for odd in BOTH:
                put_dz(i, odd).wait()
        give_tok.wait_send()
        give_chunk.wait_send()
        for h in BOTH:
            for i in BOTH:
                p1_send(h, i).wait_send()
                p1_fwd(h, i).wait_send()
                for k in (0, PAIR, FAR):
                    p2_send(h, k, i).wait_send()
                    p2_fwd(h, k, i).wait_send()
            for k in (0, PAIR, FAR):
                share(h, k).wait_send()
        for part in BOTH:
            for copy in move_xn(part):
                copy.wait()
        for u in range(len(UNITS)):
            if u > len(UNITS) - 3:
                x_swap(u).wait_send()
            x_keep(u).wait()
            for i in BOTH:
                x_far(u, i).wait_send()
                x_near(u, i).wait_send()
                if u < last_unit:
                    x_put(u, i).wait_send()
                    x_pass(u, i).wait()
    assert (place.n_link, place.n_local) <= dims["front_sems"], (place.n_link, place.n_local)


def specs(n_vmem, n_any):
    return [pl.BlockSpec(memory_space=pltpu.VMEM)] * n_vmem + [pl.BlockSpec(memory_space=pl.ANY)] * n_any


def shapes(items):
    return tuple(jax.ShapeDtypeStruct(*item) for item in items)


def scratch(items, n_link, n_local):
    dma = pltpu.SemaphoreType.DMA
    return [pltpu.VMEM(*item) for item in items] + [dma((n_link,)), dma((n_link,)), dma((n_local,))]


def params(collective_id, limit):
    return pltpu.CompilerParams(collective_id=collective_id, has_side_effects=True, vmem_limit_bytes=limit)


def front(dims, limit, shard, tok_row, lab_row, w, h, g):
    n, tok, vocab, width, vt = dims["n"], dims["tok"], dims["vocab"], dims["width"], dims["vt"]
    cols = shard.shape[0]
    half_v = vocab // CORES
    quarter = tok // n
    n_tile, n_half, most = vocab // vt, half_v // vt, max(PIECES)
    pieces = n * n * CORES
    grid = (n // 2, 2, n // 2, 2)
    return pl.pallas_call(
        functools.partial(front_kernel, dims),
        name="front",
        out_shape=shapes([
            ((n_tile, *grid, CORES, cols, vt), BF16), *[((pieces, cols, tok), BF16)] * 4, ((2, 2 * n * cols, half_v // 2), F32), ((n_tile, tok, vt), BF16),
            ((n_half, tok, vt), BF16), ((n, BASE[-1], cols, quarter), BF16), ((PIECES[-1], cols, quarter), BF16), ((n_tile, tok, vt), F32),
            ((1, width), F32), ((SUB, min(LANE, quarter)), F32), ((CORES, tok, LANE), I32),
        ]),
        in_specs=specs(4, 2),
        out_specs=tuple(specs(0, 11) + specs(3, 0)),
        scratch_shapes=scratch([
            ((n_tile, cols, vt), BF16), ((CORES, n_half, cols, vt), BF16), ((CORES, SUB, tok), I32), ((half_v, CORES * tok), BF16),
            ((2, most, n_half, cols, vt), BF16), ((pieces, cols, tok), BF16), ((2, CORES, most, cols, tok), BF16), ((pieces, cols, tok), BF16),
            ((pieces, cols, quarter), BF16), ((2, pieces, cols, quarter), BF16), ((pieces, cols, quarter), BF16),
            ((4, *grid, CORES, cols, vt), BF16), ((tok, width), BF16), ((pieces, cols, tok), BF16),
            ((2, tok, vt), F32), ((2, tok, vt), F32), ((2, 2, tok, vt), BF16), ((tok, LANE), F32), ((tok, LANE), F32), ((tok, LANE), F32),
            ((tok, LANE), I32), ((2 * n + CORES, 1, width), F32), ((n, 2, tok), F32),
        ], dims["front_sems"][0], dims["front_sems"][1]),
        compiler_params=params(0, limit),
    )(shard, tok_row, lab_row, w, h, g)


def back_kernel(
    dims,
    gain_ref, loss_ref, tokc, lt_hbm, dz_hbm, dzp_hbm, et_hbm, xnt_hbm, xpar_hbm, gt_hbm, gpar_hbm, h_hbm, q5_hbm,
    tail_out, dh_out, de_out, x0_out, ra_hbm, rx_hbm,
    q5, dz_own, dz_par, et_buf, part, fx, acc, fa, f2, r2, xb, h_buf, dh_buf, dg_acc, slots,
    sends, recvs, local_sems,
):
    n, tok, vocab, width, tile, vt = (dims[k] for k in ("n", "tok", "vocab", "width", "tile", "vt"))
    place = Place(n, sends, recvs, local_sems)
    x, z, y, c = place.x, place.z, place.y, place.c
    half_v = vocab // CORES
    n_tile, n_half = vocab // vt, half_v // vt
    lanes = half_v // 2
    rows = width // (n * n)
    half_rows = rows // 2
    quarter = tok // n
    hq = quarter // 2
    tiles = dims["tiles"]
    chunks = len(tiles)
    edges = [sum(tiles[:d]) for d in range(chunks + 1)]
    per_half = n_half // 2

    with scope("b_enter"):
        place.enter()

    load_q5 = place.local("q5", q5_hbm, q5)
    load_q5.start()
    load_h = place.local("h", h_hbm.at[span(x * quarter, quarter, quarter)], h_buf)

    def load_et(t, slot):
        return place.local("et", et_hbm.at[:, span(t * tile, tile, tile)], et_buf.at[slot], slot)

    slot_of = {FAR: 0, 1: 1, 3: 2, 0: 0}
    stages = dims["stages"]

    def load_stage(m, i):
        half, k, kind = stages[m]
        src = ((gt_hbm, gpar_hbm), (xnt_hbm, xpar_hbm))[kind][i]
        src = src.at[(z + k) % n] if half == 0 else src.at[:, (y + k) % n]
        return place.local(("xb", i), src, xb.at[m % 2, i], m % 2)

    def start_stage(m):
        if m < len(stages):
            start_all(load_stage(m, i) for i in BOTH)

    loads = [place.local("dz", dz_hbm, dz_own), place.local("dzp", dzp_hbm, dz_par)]
    load_et(0, 0).start()
    start_all(loads)
    keep_q5 = place.local("q5", q5, x0_out.at[x], 1)

    def y_put(i):
        return place.send(("yp", i), q5, x0_out.at[x], dx=WAYS[i])

    def y_pass(i):
        size = q5.shape[0] // 2
        ref = x0_out.at[(x + FROM[i]) % n, pl.ds(i * size, size)]
        return place.send(("yq", i), ref, ref, dx=WAYS[i])

    def y_passes():
        for i in BOTH:
            y_put(i).wait_recv()
            y_pass(i).start()

    fars = [place.local("lt", lt_hbm.at[half], acc.at[half, 0], half) for half in BOTH]
    start_all(fars)
    for m in BOTH:
        start_stage(m)
    load_h.start()

    def columns(d):
        return pl.ds(edges[d] * tile, tiles[d] * tile)

    def dxn_chunk(d):
        def body(t, carry):
            slot = t % 2

            @pl.when(t + 1 < edges[chunks])
            def _():
                load_et(t + 1, 1 - slot).start()

            load_et(t, slot).wait()
            left = jnp.concatenate([dz_own[j] for j in range(n_tile)], axis=1)
            right = jnp.concatenate([et_buf[slot, j] for j in range(n_tile)], axis=1)
            part[:, span(t * tile, tile, tile)] = lax.dot_general(
                left, right, (((1,), (1,)), ((), ())), preferred_element_type=F32)
            return carry

        with scope("b_dxn"):
            lax.fori_loop(edges[d], edges[d + 1], body, 0)

    def qrow(k, lo=0, size=hq):
        return span((x + k) % n * quarter + lo, size, SUB)

    def x_far(d, i):
        return place.send(("xf", d, i), part.at[qrow(FAR, i * hq), columns(d)], fx.at[i, :, columns(d)], dx=WAYS[i])

    def x_near(d, i, j):
        src = part.at[qrow(WAYS[i], j * hq), columns(d)]
        return place.send(("xn", d, i, j), src, rx_hbm.at[i, pl.ds(j * hq, hq), columns(d)], dx=WAYS[i])

    def x_first(d):
        start_all(x_far(d, i) for i in BOTH)

    def x_second(d):
        with scope("b_x2"):
            for i in BOTH:
                x_far(d, i).wait_recv()
                sel = qrow(WAYS[i], i * hq)
                part[sel, columns(d)] = part[sel, columns(d)] + fx[i, :, columns(d)]
                start_all(x_near(d, i, j) for j in BOTH)

    def stage_x(d, j, i):
        return place.local("sx", rx_hbm.at[i, pl.ds(j * hq, hq), columns(d)], fx.at[i, :, columns(d)], i)

    def x_third(d, j):
        with scope("b_x3"):
            for i in BOTH:
                x_near(d, i, j).wait_recv()
                stage_x(d, j, i).start()
            for i in BOTH:
                stage_x(d, j, i).wait()
            sel = qrow(0, j * hq)
            part[sel, columns(d)] = part[sel, columns(d)] + fx[0, :, columns(d)] + fx[1, :, columns(d)]

    def de_stage(half, k, kind):
        m = stages.index((half, k, kind))
        slot = slot_of[k]

        wide = min(2, per_half) if kind and k else 1

        def right(i, t):
            if kind:
                return dz_par[t] if i else dz_own[c * n_half + t]
            ids = lax.broadcasted_iota(I32, (tok, LANE), 1) + (x * vocab + c * half_v + t * vt)
            hits = [jnp.where(tokc[i] == ids + b, dims["scale"], 0.0).astype(BF16) for b in range(0, vt, LANE)]
            return jnp.concatenate(hits, axis=1)

        def body(j, carry):
            t = half * per_half + j * wide
            sel = span(j * wide * vt, wide * vt)
            left = jnp.concatenate([xb[m % 2, i].reshape(n * rows, tok) for i in BOTH], axis=1)
            both_right = [jnp.concatenate([right(i, t + q) for i in BOTH], axis=0) for q in range(wide)]
            total = jnp.dot(left, jnp.concatenate(both_right, axis=1), preferred_element_type=F32)
            total = total.reshape(n, rows, wide * vt)
            acc[half, slot, :, :, sel] = acc[half, slot, :, :, sel] + total if kind else total
            return carry

        with scope("b_de" if kind else "b_look"):
            for i in BOTH:
                load_stage(m, i).wait()
            lax.fori_loop(0, per_half // wide, body, 0)
            start_stage(m + 2)

    def de_unit(half, k):
        if k == FAR:
            fars[half].wait()
        else:
            de_stage(half, k, 0)
        de_stage(half, k, 1)

    def ring(half, k):
        return {"dz": k} if half == 0 else {"dy": k}

    def cross(half, k):
        return {"dy": k} if half == 0 else {"dz": k}

    def a_far(half, i):
        return place.send(("af", half, i), acc.at[half, 0, pl.ds(2 * i, 2)], fa.at[half, i], **ring(half, WAYS[i]))

    def a_near(half, i, j):
        sel = pl.ds(2 * j, 2)
        return place.send(("an", half, i, j), acc.at[half, 1 + i, sel], ra_hbm.at[half, i, sel], **ring(half, WAYS[i]))

    def a_first(half):
        start_all(a_far(half, i) for i in BOTH)

    def a_second(half, i):
        with scope("b_a2"):
            a_far(half, i).wait_recv()
            sel = pl.ds(2 * i, 2)
            acc[half, 1 + i, sel] = acc[half, 1 + i, sel] + fa[half, i]
            start_all(a_near(half, i, j) for j in BOTH)

    def stage_a(half, j, i):
        return place.local(("sa", half), ra_hbm.at[half, i, pl.ds(2 * j, 2)], fa.at[half, i], i)

    def piece(half, k):
        return ((y if half == 0 else z) + k) % n

    def c_far(half, i):
        src = acc.at[half, 0, piece(half, FAR), pl.ds(i * half_rows, half_rows)]
        return place.send(("cf", half, i), src, f2.at[half, i], **cross(half, WAYS[i]))

    def c_near(half, i):
        return place.send(("cn", half, i), acc.at[half, 0, piece(half, WAYS[i])], r2.at[half, i], **cross(half, WAYS[i]))

    def a_third(half, j):
        with scope("b_a3"):
            for i in BOTH:
                a_near(half, i, j).wait_recv()
                stage_a(half, j, i).start()
            for i in BOTH:
                stage_a(half, j, i).wait()
            sel = pl.ds(2 * j, 2)
            acc[half, 0, sel] = acc[half, 0, sel] + fa[half, 0] + fa[half, 1]

    def c_first(half):
        start_all(c_far(half, i) for i in BOTH)

    def c_second(half):
        with scope("b_c2"):
            for i in BOTH:
                c_far(half, i).wait_recv()
                at = piece(half, WAYS[i])
                sel = pl.ds(i * half_rows, half_rows)
                acc[half, 0, at, sel] = acc[half, 0, at, sel] + f2[half, i]
                c_near(half, i).start()

    def out_copies(half):
        sel = span(c * half_v + half * lanes, lanes)
        mine = acc.at[half, 0, piece(half, 0)]
        yield place.local("de", mine.at[span(c * half_rows, half_rows, SUB)], de_out.at[:, sel], half)
        yield place.send(("de", half), mine.at[span((1 - c) * half_rows, half_rows, SUB)], de_out.at[:, sel], dc=1)

    def c_third(half):
        with scope("b_c3"):
            for i in BOTH:
                c_near(half, i).wait_recv()
            at = piece(half, 0)
            acc[half, 0, at] = acc[half, 0, at] + r2[half, 0] + r2[half, 1]
            start_all(out_copies(half))

    step = min(32, hq)

    def dh_body(i, carry):
        sel = span(i * step, step, step)
        row = span(x * quarter + i * step, step, step)
        d_x = part[row]
        h_wide = h_buf[sel].astype(F32)
        inv_rms = lax.rsqrt(jnp.sum(h_wide * h_wide, axis=1, keepdims=True) * (1.0 / width) + NORM_EPS)
        h_norm = h_wide * inv_rms
        g_dir = d_x * gain_ref[0:1]
        mean = jnp.sum(g_dir * h_norm, axis=1, keepdims=True) * (1.0 / width)
        dh_buf[sel] = (inv_rms * (g_dir - h_norm * mean)).astype(BF16)
        prod = d_x * h_norm
        total = prod[0:SUB]
        for j in range(SUB, step, SUB):
            total = total + prod[j:j + SUB]
        dg_acc[...] = dg_acc[...] + total
        return carry

    def h_first(i, j):
        return place.send(("hf", i, j), dh_buf.at[pl.ds(j * hq, hq)], dh_out.at[qrow(0, j * hq)], dx=WAYS[i])

    def h_second(i):
        ref = dh_out.at[qrow(FROM[i], i * hq)]
        return place.send(("hs", i), ref, ref, dx=WAYS[i])

    keep_dh = place.local("dh", dh_buf, dh_out.at[qrow(0, 0, quarter)])
    small = SmallSum(place, ("dc", "dx", "dy", "dz"), slots)
    per_j = hq // step

    def dh_part(j):
        with scope("b_dh"):
            if j == 0:
                load_h.wait()
            lax.fori_loop(j * per_j, (j + 1) * per_j, dh_body, 0)
            start_all(h_first(i, j) for i in BOTH)
            if j:
                keep_dh.start()

    def h_pass(i):
        with scope("b_h2"):
            h_first(i, i).wait_recv()
            h_second(i).start()

    def small_step(k):
        dims_of = small.dims
        with scope("b_s"):
            if k == 1:
                sums = [jnp.sum(part_sum, axis=0, keepdims=True) for part_sum in (dg_acc[...], loss_ref[...])]
                small.start(dims_of[0], jnp.concatenate(sums, axis=1))
            elif k <= len(dims_of):
                small.start(dims_of[k - 1], small.finish(dims_of[k - 2]))
            else:
                total = small.finish(dims_of[-1])
                loss = jnp.sum(total[:, width:], axis=1, keepdims=True) * (1.0 / dims["total"])
                tail_out[...] = jnp.concatenate([total[:, 0:width], jnp.broadcast_to(loss, (1, LANE))], axis=1)

    def dxn(d):
        dxn_chunk(d)
        x_first(d)

    def unit(half, k):
        if k == 0:
            with scope("b_wait_far"):
                for i in BOTH:
                    a_far(half, i).wait_send()
        while len(loads) > 1:
            loads.pop().wait()
        de_unit(half, k)
        if k == FAR:
            a_first(half)

    families = {
        "CH": dxn, "XS": x_second, "UN": unit, "AS": a_second, "XT": x_third, "AT": a_third, "CF": c_first, "CS": c_second,
        "CT": c_third, "DH": dh_part, "SM": small_step, "HP": h_pass, "YQ": y_passes,
    }

    def perform(text):
        for word in text.split():
            families[word[:2]](*(int(digit) for digit in word[2:]))

    with scope("b_load"):
        load_q5.wait()
        start_all(y_put(i) for i in BOTH)
        keep_q5.start()
        loads[0].wait()
        dg_acc[...] = jnp.zeros_like(dg_acc)
    for text in (
        "CH0 UN02 YQ CH1", "UN12 CH2 UN03 XS1", "UN01 XS2 UN13 AS01", "AS00 UN11 AS11 AS10",
        "XS0 CH3 XT10 CH4", "UN00 XT00 XS3 XT01", "XS4 UN10 XT20 AT00", "XT30 XT21 XT11 XT40",
        "DH0 XT31 XT41 DH1", "AT01 AT10 CF0 SM1", "AT11 CF1 SM2 HP0", "CS0 CS1 SM3 HP1", "CT0 SM4 CT1 SM5",
    ):
        perform(text)

    with scope("b_end_x"):
        keep_dh.wait()
        keep_q5.wait()
        for i in BOTH:
            y_put(i).wait_send()
            y_pass(i).wait()
            for d in range(chunks):
                x_far(d, i).wait_send()
                for j in BOTH:
                    x_near(d, i, j).wait_send()
            h_first(i, i).wait_send()
            h_first(i, 1 - i).wait()
            h_second(i).wait()
    with scope("b_end_a"):
        for half in BOTH:
            for i in BOTH:
                for j in BOTH:
                    a_near(half, i, j).wait_send()
                c_far(half, i).wait_send()
                c_near(half, i).wait_send()
            for copy in out_copies(half):
                copy.wait()
    assert (place.n_link, place.n_local) <= dims["back_sems"], (place.n_link, place.n_local)


def back(dims, limit, gain, loss, tokc, far, dz, dzp, et, xnt, xpar, gt, gpar, h, q5):
    n, tok, vocab, width, tile = (dims[k] for k in ("n", "tok", "vocab", "width", "tile"))
    rows = width // (n * n)
    half_v = vocab // CORES
    lanes = half_v // 2
    quarter = tok // n
    hq = quarter // 2
    tail_w = width + loss.shape[1]
    n_tile, n_half, vt = dz.shape[0], dzp.shape[0], dims["vt"]
    turned = [a.reshape(n, n, rows, tok) for a in (xnt, xpar, gt, gpar)]
    return pl.pallas_call(
        functools.partial(back_kernel, dims),
        name="back",
        out_shape=shapes([
            ((1, width + LANE), F32), ((tok, width), BF16), ((rows // CORES, vocab), F32), ((n, *q5.shape), BF16),
            ((2, 2, n, rows, lanes), F32),
            ((2, quarter, width), F32),
        ]),
        in_specs=specs(3, 10),
        out_specs=tuple(specs(1, 5)),
        scratch_shapes=scratch([
            (q5.shape, BF16), ((n_tile, tok, vt), BF16), ((n_half, tok, vt), BF16), ((2, n_tile, tile, vt), BF16), ((tok, width), F32),
            ((2, hq, width), F32), ((2, 3, n, rows, lanes), F32), ((2, 2, 2, rows, lanes), F32),
            ((2, 2, rows // 2, lanes), F32), ((2, 2, rows, lanes), F32), ((2, CORES, n, rows, tok), BF16), ((quarter, width), BF16),
            ((quarter, width), BF16), ((SUB, width), F32), ((3 * n + CORES, 1, tail_w), F32),
        ], dims["back_sems"][0], dims["back_sems"][1]),
        compiler_params=params(1, limit),
    )(gain, loss, tokc, far.reshape(2, n, rows, lanes), dz, dzp, et.reshape(n_tile, width, vt), *turned, h, q5)[:4]


def finish_kernel(
    n, scale, table_ref, tail_ref, x0_hbm, x5_hbm, dh_hbm, de_hbm, dg_out, loss_out, x0_out, dh_out, de_out,
    x0_in, x0_buf, rows_ref, dh_buf, de_buf, sems,
):
    place = Place(n, None, None, sems)
    quarter, cols, width = x0_in.shape[3], x0_in.shape[2], x0_buf.shape[2]

    def step(q):
        rows = span(q * quarter, quarter, quarter)
        return (
            place.local("x0", x0_hbm.at[q], x0_in.at[q, pl.ds(0, BASE[-1])], q, n),
            place.local("x5", x5_hbm.at[q], x0_in.at[q, pl.ds(BASE[-1], PIECES[-1])], q, n), place.local("x0o", x0_buf.at[q], x0_out.at[rows], q, n),
            place.local("dh", dh_hbm.at[rows], dh_buf.at[q], q, n), place.local("dho", dh_buf.at[q], dh_out.at[rows], q, n),
        )

    moves = [step(q) for q in range(n)]
    de_in, de_put = place.local("de", de_hbm, de_buf, 0), place.local("de", de_buf, de_out, 1)
    for x0_load, x5_load, _, dh_load, _ in moves:
        start_all((x0_load, x5_load, dh_load))
    de_in.start()
    gain = jnp.broadcast_to(tail_ref[:, 0:width], (SUB, width))
    dg_out[...] = pltpu.roll(gain, width - place.f * cols, axis=1)[0:1, 0:cols]
    loss_out[...] = tail_ref[:, width:width + 1]

    def body(q, carry):
        x0_load, x5_load, x0_put, dh_load, dh_put = step(q)
        x0_load.wait()
        x5_load.wait()
        for zi in range(n):
            for yi in range(n):
                for h in BOTH:
                    dz, dy = (zi - place.z) % n, (yi - place.y) % n
                    k1, k2 = (dy, dz) if h == 0 else (dz, dy)
                    piece = table_ref[(h * n + k1) * n + k2]
                    rows_ref[pl.ds(((zi * n + yi) * CORES + h) * cols, cols)] = x0_in[q, piece]
        x0_buf[q] = (rows_ref[...].T.astype(F32) * scale).astype(BF16)
        x0_put.start()
        dh_load.wait()
        dh_put.start()
        return carry

    lax.fori_loop(0, n, body, 0)
    de_in.wait()
    de_put.start()
    for _, _, x0_put, _, dh_put in moves:
        x0_put.wait()
        dh_put.wait()
    de_put.wait()


def finish(n, scale, limit, tail, x0, x5, dh, de):
    cols, quarter = x0.shape[2:]
    pieces = n * n * CORES
    width = pieces * cols
    table = np.zeros((CORES, n, n), np.int32)
    for u, unit in enumerate(UNITS):
        for h in BOTH:
            for i, (k1, k2) in enumerate(unit):
                table[h, k1, k2] = BASE[u] + h * len(unit) + i
    return pl.pallas_call(
        functools.partial(finish_kernel, n, scale),
        name="finish",
        in_specs=[pl.BlockSpec(memory_space=pltpu.SMEM)] + specs(1, 4),
        out_specs=tuple(specs(2, 3)),
        out_shape=shapes([((1, cols), F32), ((1, 1), F32), (dh.shape, BF16), (dh.shape, BF16), (de.shape, F32)]),
        scratch_shapes=[
            pltpu.VMEM((n, pieces, cols, quarter), BF16), pltpu.VMEM((n, quarter, width), BF16), pltpu.VMEM((width, quarter), BF16),
            pltpu.VMEM((n, quarter, width), BF16), pltpu.VMEM(de.shape, F32), pltpu.SemaphoreType.DMA((5 * n + 2,)),
        ],
        compiler_params=pltpu.CompilerParams(vmem_limit_bytes=limit),
    )(jnp.asarray(table.reshape(-1)), tail, x0, x5, dh, de)


def solution(mesh):
    return build(mesh, mesh.shape["tp"], 256, digits("12222")[0], 256, 6, 67_000_000)


def build(mesh, n, tile, tiles, vt, n_block, limit):
    fsdp_size = mesh.shape["fsdp"]

    def device_step(emb_shard, tok_ids, lab_ids, h_last, g_embed, norm_w):
        vocab_rows, cols = emb_shard.shape
        batch_loc, seq_len, width = h_last.shape
        tok_count = batch_loc * seq_len
        fsdp_id = lax.axis_index("fsdp")
        scale = float(np.asarray(math.sqrt(width)).astype(jnp.bfloat16))
        dims = {
            "n": n, "tok": tok_count, "vocab": vocab_rows, "width": width, "total": tok_count * fsdp_size, "vt": vt,
            "tile": tile, "tiles": tiles, "scale": scale, "n_block": n_block,
            "stages": digits("021 121 030 031") + digits("010 011 130 131") + digits("110 111 000 001") + digits("100 101"),
            "front_sems": (106, 52), "back_sems": (72, 26),
        }
        h_flat = h_last.reshape(tok_count, width)
        placed = lax.dynamic_update_slice(jnp.zeros((SUB, width), F32), jnp.broadcast_to(norm_w, (SUB, cols)), (0, fsdp_id * cols))
        ids = [a.reshape(1, tok_count) for a in (tok_ids, lab_ids)]
        table, xn_t, xpar_t, g_t, gpar_t, far, dz, dzp, x0, q5, _, gain, loss_part, tokc = front(
            dims, limit, emb_shard.T, *ids, norm_w.reshape(1, cols), h_flat, g_embed.reshape(tok_count, width))
        tail, d_hidden, d_cols, x5 = back(dims, limit, gain, loss_part, tokc, far, dz, dzp, table, xn_t, xpar_t, g_t, gpar_t, h_flat, q5)
        d_norm_w, loss, x_emb, d_hidden, d_cols = finish(n, scale, limit, tail, x0, x5, d_hidden, d_cols)
        return (x_emb.reshape(h_last.shape), loss.reshape(()), d_hidden.reshape(h_last.shape), d_norm_w.reshape(cols), d_cols.T)

    spec_tok = P("fsdp", None)
    spec_act = P("fsdp", None, None)
    return jax.shard_map(device_step, mesh=mesh, in_specs=(P("tp", "fsdp"), spec_tok, spec_tok, spec_act, spec_act, P("fsdp")), out_specs=(spec_act, P(), spec_act, P("fsdp"), P("tp", "fsdp")), check_vma=False)
```

```python
import functools
import math
import jax
import numpy as np
import jax.numpy as jnp
from jax import lax
from jax.experimental import pallas as pl
from jax.experimental.pallas import tpu as pltpu
from jax.sharding import PartitionSpec as P

SOFT_CAP = 30.0
NORM_EPS = 1e-6
F32, BF16, I32 = jnp.float32, jnp.bfloat16, jnp.int32
LANE, SUB = 128, 8
BOTH = (0, 1)
FOUR = range(4)
WAYS = (1, 3)
FROM = (3, 1)
FAR = 2
CORES = 2


def span(start, size, unit=LANE):
    return pl.ds(pl.multiple_of(start, unit), size)


class Place:
    def __init__(self, n, sends, recvs, local_sems):
        self.n, self.sends, self.recvs, self.local_sems = n, sends, recvs, local_sems
        self.x = lax.axis_index("tp")
        f = lax.axis_index("fsdp")
        self.f = f
        self.c = f % CORES
        self.y = f // CORES % n
        self.z = f // CORES // n
        self.link_of, self.local_of, self.n_link, self.n_local = {}, {}, 0, 0
        self.size = {"dx": n, "dz": n, "dy": n, "dc": CORES}
        self.me = {"dx": self.x, "dz": self.z, "dy": self.y, "dc": self.c}

    def at(self, dx=0, dz=0, dy=0, dc=0):
        n = self.n
        z, y, c = (self.z + dz) % n, (self.y + dy) % n, (self.c + dc) % CORES
        return ((self.x + dx) % n, (z * n + y) * CORES + c)

    def knock(self):
        peers = [self.at(**{d: k}) for d in self.size for k in range(1, self.size[d])]
        for peer in peers:
            pl.semaphore_signal(pltpu.get_barrier_semaphore(), inc=1, device_id=peer, device_id_type=pl.DeviceIdType.MESH)
        return len(peers)

    def enter(self, knocks):
        pl.semaphore_wait(pltpu.get_barrier_semaphore(), knocks)

    def link(self, key, count=1):
        if key not in self.link_of:
            self.link_of[key] = self.n_link
            self.n_link += count
        return self.link_of[key]

    def send(self, key, src, dst, **step):
        i = self.link(key)
        return pltpu.make_async_remote_copy(
            src, dst, self.sends.at[i], self.recvs.at[i], device_id=self.at(**step), device_id_type=pl.DeviceIdType.MESH)

    def local(self, key, src, dst, slot=0, count=2):
        if key not in self.local_of:
            self.local_of[key] = self.n_local
            self.n_local += count
        return pltpu.make_async_copy(src, dst, self.local_sems.at[self.local_of[key] + slot])


class SmallSum:
    def __init__(self, place, dims, slots):
        self.place, self.slots, self.dims, self.base = place, slots, dims, {}
        count = 0
        for d in dims:
            self.base[d] = count
            count += place.size[d]

    def copies(self, d):
        slot = self.slots.at[self.base[d] + self.place.me[d]]
        for k in range(1, self.place.size[d]):
            yield self.place.send((self.dims, d, k), slot, slot, **{d: k})

    def start(self, d, value):
        self.slots[self.base[d] + self.place.me[d]] = value
        for copy in self.copies(d):
            copy.start()

    def finish(self, d):
        for copy in self.copies(d):
            copy.wait()
        total = self.slots[self.base[d]]
        for k in range(1, self.place.size[d]):
            total = total + self.slots[self.base[d] + k]
        return total


def scope(name):
    return jax.named_scope(name)


def start_all(copies):
    for copy in copies:
        copy.start()


def digits(text):
    return tuple(tuple(int(d) for d in word) for word in text.split())


UNITS = [digits(u) for u in ("00", "10 30", "01 03 20", "02 11 31", "13 33 21 23", "12 32 22")]
PAIR, ALL = 1, "all"
PIECES = [2 * len(u) for u in UNITS]
EXP_RATE = SOFT_CAP * math.log2(math.e)
BASE = [sum(PIECES[:i]) for i in range(len(UNITS))]


def front_kernel(
    dims,
    shard_hbm, tok_hbm, lab_hbm, w_hbm, h_hbm, g_hbm,
    et_out, xnt_out, xpar_out, gt_out, gpar_out, lt_out, dz_out, dzpar_out, x0_out, q5_out, u_hbm, gain_hbm, loss_hbm, tokc_hbm,
    shard_ref, tok_ref, lab_ref, w_ref, gain_out, loss_out, tokc_out, shard_t, chunk, tokr, hit_t, lhs, xp, xw, xr, xf, xg, xq, etb, xn, gl, z_even, z_odd, dzb,
    acc_e, acc_l, inv_s, labc, w_slots, s_slots, sends, recvs, local_sems,
):
    n, tok, vocab, width, vt = dims["n"], dims["tok"], dims["vocab"], dims["width"], dims["vt"]
    place = Place(n, sends, recvs, local_sems)
    x, z, y, c = place.x, place.z, place.y, place.c
    half_v = vocab // CORES
    n_tile = vocab // vt
    n_half = n_tile // CORES
    hh = n_half // 2
    cols = width // (n * n * CORES)
    quarter = tok // n
    row_start = x * vocab

    def ring1(h, k):
        return {"dy": k} if h == 0 else {"dz": k}

    def ring2(h, k):
        return {"dz": k} if h == 0 else {"dy": k}

    def coord(base, k, paired):
        every = slice(None)
        if k == ALL:
            return every, every
        return every if paired else (base + k) % n // 2, (base + k) % 2

    def loc(h, k1, k2, lo=0, size=n_half, pair1=False, pair2=False):
        first, second = coord((y, z)[h], k1, pair1), coord((z, y)[h], k2, pair2)
        return et_out.at[(pl.ds(c * n_half + lo, size), *((second, first)[h]), *((first, second)[h]), h)]

    knocks = place.knock()
    early_loads = [
        place.local(("in", i), src, dst, 0, 1)
        for i, (src, dst) in enumerate(((shard_hbm, shard_ref), (tok_hbm, tok_ref), (lab_hbm, lab_ref), (w_hbm, w_ref)))
    ]
    start_all(early_loads)
    load_g = place.local("g", g_hbm, xn)
    load_g.start()
    with scope("f_cast"):
        for copy in early_loads:
            copy.wait()
        for t in range(n_tile):
            shard_t[t] = shard_ref[:, pl.ds(t * vt, vt)].astype(BF16)
    with scope("f_enter"):
        place.enter(knocks)
    with scope("f_swap"):
        tokr[c] = jnp.broadcast_to(tok_ref[...], (SUB, tok))
        give_tok = place.send("tok", tokr.at[c], tokr.at[c], dc=1)
        give_chunk = place.send("chunk", shard_t.at[pl.ds((1 - c) * n_half, n_half)], chunk.at[c], dc=1)
        give_chunk.start()
        give_tok.start()
        chunk[c] = shard_t[pl.ds(c * n_half, n_half)]
        gain_sum = SmallSum(place, ("dc", "dy", "dz"), w_slots)
        own_w = jnp.concatenate([w_ref[...], jnp.zeros((1, width - cols), F32)], axis=1)
        gain_sum.start("dc", pltpu.roll(jnp.broadcast_to(own_w, (SUB, width)), place.f * cols, axis=1)[0:1])

    def p1_send(h, i):
        return place.send(("p1", h, i), chunk.at[h], loc(h, 0, 0), **ring1(h, WAYS[i]))

    def p1_fwd(h, i):
        ref = loc(h, FROM[i], 0, i * hh, hh)
        return place.send(("p1f", h, i), ref, ref, **ring1(h, WAYS[i]))

    def p2_send(h, k1, i):
        ref = loc(h, k1, 0, pair1=k1 == PAIR)
        return place.send(("p2", h, k1, i), chunk.at[h] if k1 == 0 else ref, ref, **ring2(h, WAYS[i]))

    def p2_fwd(h, k1, i):
        ref = loc(h, k1, FROM[i], i * hh, hh, pair1=k1 == PAIR)
        return place.send(("p2f", h, k1, i), ref, ref, **ring2(h, WAYS[i]))

    def keep(h):
        return place.local("keep", chunk.at[h], loc(h, 0, 0), h)

    def share(h, k2):
        ref = loc(h, ALL, k2, pair2=k2 == PAIR)
        return place.send(("share", h, k2), ref, ref, dc=1)

    def pass_first():
        with scope("f_p1"):
            for h in BOTH:
                for i in BOTH:
                    p1_send(h, i).wait_recv()
                    p1_fwd(h, i).start()
            for h in BOTH:
                start_all(p2_send(h, PAIR, i) for i in BOTH)

    def pass_first_far():
        with scope("f_p1f"):
            for h in BOTH:
                for i in BOTH:
                    p1_fwd(h, i).wait_recv()
                start_all(p2_send(h, FAR, j) for j in BOTH)

    def pass_second(k1):
        with scope("f_p2"):
            for h in BOTH:
                for i in BOTH:
                    p2_send(h, k1, i).wait_recv()
                    p2_fwd(h, k1, i).start()

    def end_second(k1):
        with scope("f_p2f"):
            for h in BOTH:
                for i in BOTH:
                    p2_fwd(h, k1, i).wait_recv()

    def share_group(k2):
        start_all(share(h, k2) for h in BOTH)

    with scope("f_chunk"):
        give_chunk.wait_recv()
        start_all(keep(h) for h in BOTH)
        gain_sum.start("dy", gain_sum.finish("dc"))
        for h in BOTH:
            start_all(p1_send(h, i) for i in BOTH)
        for h in BOTH:
            start_all(p2_send(h, 0, i) for i in BOTH)

    v_step = min(LANE, half_v)

    def hit_body(j, carry):
        off = j * v_step
        ids = lax.broadcasted_iota(I32, (v_step, tok), 0) + (row_start + c * half_v + off)
        for i, core in enumerate((c, 1 - c)):
            hit_t[span(off, v_step, v_step), pl.ds(i * tok, tok)] = jnp.where(ids == tokr[core, 0:1, :], 1.0, 0.0).astype(BF16)
        return carry

    def make_hits():
        with scope("f_hit"):
            give_tok.wait_recv()
            lax.fori_loop(0, half_v // v_step, hit_body, 0)

    n_step = min(512, tok)
    most = max(PIECES)

    def whole(u):
        return pl.ds(BASE[u], PIECES[u])

    def unit_copies(u):
        slot = u % 2
        for p, (h, (k1, k2)) in enumerate((h, k) for h in BOTH for k in UNITS[u]):
            yield place.local("lhs", loc(h, k1, k2), lhs.at[slot, p], slot * most + p, 2 * most)

    def load_unit(u):
        start_all(unit_copies(u))

    def look(u):
        pieces = PIECES[u]
        with scope("f_look"):
            if u > 1:
                x_swap(u - 2).wait_send()
            left = lhs.at[u % 2]
            for copy in unit_copies(u):
                copy.wait()
            per_core = tok // n_step

            def body(j, carry):
                value = jnp.concatenate([left[pl.ds(0, pieces), t].reshape(pieces * cols, vt) for t in range(n_half)], axis=1)
                rows = jnp.dot(value, hit_t[:, span(j * n_step, n_step)], preferred_element_type=F32)
                rows = rows.reshape(pieces, cols, n_step).astype(BF16)
                xw[u % 2, j // per_core, pl.ds(0, pieces), :, span(j % per_core * n_step, n_step)] = rows
                return carry

            lax.fori_loop(0, CORES * per_core, body, 0)
            x_swap(u).start()

    def x_swap(u):
        return place.send(("swap", u), xw.at[u % 2, 1, pl.ds(0, PIECES[u])], xr.at[whole(u)], dc=1)

    def lanes_of(k):
        return span((x + k) % n * quarter, quarter, quarter)

    def side(u, i):
        return pl.ds(BASE[u] + i * len(UNITS[u]), len(UNITS[u]))

    def x_far(u, i):
        return place.send(("xf", u, i), xp.at[side(u, i), :, lanes_of(FAR)], xf.at[side(u, i)], dx=WAYS[i])

    def x_near(u, i):
        return place.send(("xn", u, i), xp.at[whole(u), :, lanes_of(WAYS[i])], xg.at[i, whole(u)], dx=WAYS[i])

    def x_goal(k, sel):
        return x0_out.at[(x + k) % n, sel]

    def x_put(u, i):
        return place.send(("xp", u, i), xq.at[whole(u)], x_goal(0, whole(u)), dx=WAYS[i])

    last_unit = len(UNITS) - 1

    def x_keep(u):
        goal = x_goal(0, whole(u)) if u < last_unit else q5_out
        return place.local("x0", xq.at[whole(u)], goal, u, len(UNITS))

    def x_pass(u, i):
        ref = x_goal(FROM[i], side(u, i))
        return place.send(("xs", u, i), ref, ref, dx=WAYS[i])

    def x_first(u):
        with scope("f_x1"):
            x_swap(u).wait_recv()
            def body(p, carry):
                xp[BASE[u] + p] = xw[u % 2, 0, p] + xr[BASE[u] + p]
                return carry

            lax.fori_loop(0, PIECES[u], body, 0)
            start_all(x_far(u, i) for i in BOTH)

    def x_second(u):
        with scope("f_x2"):
            for i in BOTH:
                x_far(u, i).wait_recv()
                sel, lanes = side(u, i), lanes_of(WAYS[i])
                xp[sel, :, lanes] = xp[sel, :, lanes] + xf[sel]
                x_near(u, i).start()

    def x_third(u):
        with scope("f_x3"):
            for i in BOTH:
                x_near(u, i).wait_recv()
            sel = whole(u)
            xq[sel] = xp[sel, :, lanes_of(0)] + xg[0, sel] + xg[1, sel]
            if u < last_unit:
                start_all(x_put(u, i) for i in BOTH)
            x_keep(u).start()

    def x_fourth(u):
        with scope("f_x4"):
            for i in BOTH:
                x_put(u, i).wait_recv()
                x_pass(u, i).start()

    n_part = n * n * CORES // 2

    def moves(key, part, whole_t, other):
        sel = pl.ds(part * n_part, n_part)
        yield place.local(key, gl.at[sel], whole_t.at[sel], part)
        yield place.send((key, part), gl.at[sel], other.at[sel], dc=1)

    def move_g(part):
        return moves("g", part, gt_out, gpar_out)

    def move_xn(part):
        return moves("xt", part, xnt_out, xpar_out)

    def transpose_part(part, copies):
        block = width // dims["n_block"]
        first = part * dims["n_block"] // 2
        turned = [xn[:, pl.ds((first + j) * block, block)].T for j in range(dims["n_block"] // 2)]
        gl[pl.ds(part * n_part, n_part)] = jnp.concatenate(turned, axis=0).reshape(n_part, cols, tok)
        start_all(copies)

    def columns(row):
        return jnp.broadcast_to(row.astype(F32), (LANE, tok)).T.astype(I32)

    r_step = min(LANE, tok)

    def xn_body(j, carry):
        sel = span(j * r_step, r_step, r_step)
        h_wide = xn[sel].astype(F32)
        inv_rms = lax.rsqrt(jnp.sum(h_wide * h_wide, axis=1, keepdims=True) * (1.0 / width) + NORM_EPS)
        xn[sel] = (h_wide * inv_rms * gain_out[0:1]).astype(BF16)
        return carry

    e_step = min(LANE, tok)

    def tile_of(j):
        return (c * n_half + j) % n_tile

    def load_tile(j):
        return place.local("et", et_out.at[tile_of(j)], etb.at[j % 4], j % 4, 4)

    def save_u(i, odd):
        return place.local(("u", odd), (z_even, z_odd)[odd].at[i % 2], u_hbm.at[tile_of(2 * i + odd)], i % 2)

    def lane_blocks():
        return [(b, pl.ds(b, LANE)) for b in range(0, vt, LANE)]

    def post_tile(i, odd):
        base = tile_of(2 * i + odd) * vt
        buf, slot = (z_even, z_odd)[odd], i % 2

        def body(e, carry):
            sel = span(e * e_step, e_step, e_step)
            ids = lax.broadcasted_iota(I32, (e_step, LANE), 1) + base
            sum_e, sum_l = acc_e[sel], acc_l[sel]
            for b, lanes in lane_blocks():
                tanh_z = jnp.tanh(buf[slot, sel, lanes] * (1.0 / SOFT_CAP))
                buf[slot, sel, lanes] = tanh_z
                sum_e = sum_e + jnp.exp2(EXP_RATE * tanh_z - EXP_RATE)
                sum_l = sum_l + jnp.where(ids + b == labc[sel], tanh_z, 0.0)
            acc_e[sel] = sum_e
            acc_l[sel] = sum_l
            return carry

        lax.fori_loop(0, tok // e_step, body, 0)

    def dot_pair(i):
        for odd in BOTH:
            value = etb[(2 * i + odd) % 4].reshape(width, vt)
            (z_even, z_odd)[odd][i % 2] = jnp.dot(xn[...], value, preferred_element_type=F32)

    def load_pair(i):
        start_all(load_tile(2 * i + odd) for odd in BOTH)

    def pair(i, carry):
        for odd in BOTH:
            load_tile(2 * i + odd).wait()

        @pl.when(i > 1)
        def _():
            for odd in BOTH:
                save_u(i - 2, odd).wait()

        for odd in BOTH:
            post_tile(i - 1, odd)

            @pl.when(i < last)
            def _():
                save_u(i - 1, odd).start()

        dot_pair(i)

        @pl.when(i + 2 < n_tile // 2)
        def _():
            load_pair(i + 2)

        for k, work in enumerate(during):
            @pl.when(i == k + 1)
            def _():
                if k == 0:
                    wait_shares()
                perform(work)
        return carry

    def wait_shares():
        with scope("f_share"):
            for h in BOTH:
                for k2 in (0, PAIR, FAR):
                    share(h, k2).wait_recv()

    def logits_first():
        acc_e[...] = jnp.zeros_like(acc_e)
        acc_l[...] = jnp.zeros_like(acc_l)
        with scope("f_logits0"):
            far_ends(1)
            for odd in BOTH:
                load_tile(odd).wait()
            dot_pair(0)
            if n_tile // 2 > 2:
                load_pair(2)

    def load_first():
        for i in BOTH:
            load_pair(i)

    def put_small(i):
        src, dst = ((gain_out, gain_hbm), (loss_out, loss_hbm), (tokc_out, tokc_hbm))[i]
        return place.local(("out", i), src, dst, 0, 1)

    def lay_columns():
        with scope("f_cols"):
            labc[...] = columns(lab_ref[...] - row_start)
            for i, core in enumerate((c, 1 - c)):
                tokc_out[i] = columns(tokr[core, 0:1, :])
            put_small(2).start()

    def turn_g():
        with scope("f_gt"):
            load_g.wait()
            for part in BOTH:
                transpose_part(part, move_g(part))
            load_h.start()

    def gain_next():
        with scope("f_gain2"):
            gain_sum.start("dz", gain_sum.finish("dy"))

    def normalize():
        with scope("f_xn"):
            gain_out[...] = 1.0 + gain_sum.finish("dz")
            put_small(0).start()
            load_h.wait()
            lax.fori_loop(0, tok // r_step, xn_body, 0)

    def turn_xn():
        with scope("f_xt"):
            for part in BOTH:
                transpose_part(part, move_xn(part))

    spare = BASE[3]
    own_rows, their_rows = (pl.ds(spare + i * 2 * n, 2 * n) for i in BOTH)

    def far_loads(h):
        for i, (src, rows) in enumerate(((gt_out, own_rows), (gpar_out, their_rows))):
            if h == 0:
                yield place.local("far", src.at[pl.ds((z + FAR) % n * 2 * n, 2 * n)], xp.at[rows], i * n, 2 * n)
            else:
                for q in range(n):
                    piece = src.at[pl.ds((q * n + (y + FAR) % n) * 2, 2)]
                    yield place.local("far", piece, xp.at[pl.ds(spare + i * 2 * n + 2 * q, 2)], i * n + q)

    def far_load(h):
        if h == 0:
            for part in BOTH:
                for copy in move_g(part):
                    copy.wait()
        start_all(far_loads(h))

    def put_far(h, j):
        rows = pl.ds(0, 2 * n * cols)
        return place.local("lt", z_even.at[j % 2, rows], lt_out.at[h, :, span(j * vt, vt)], j % 2)

    def far_ends(h):
        for j in range(hh - 2, hh):
            put_far(h, j).wait()

    def far_look(h):
        def body(j, carry):
            @pl.when(j > 1)
            def _():
                put_far(h, j - 2).wait()

            left = jnp.concatenate([xp[rows].reshape(2 * n * cols, tok) for rows in (own_rows, their_rows)], axis=1)
            right = hit_t[span((h * hh + j) * vt, vt)]
            value = lax.dot_general(left, right, (((1,), (1,)), ((), ())), preferred_element_type=F32)
            z_even[j % 2, pl.ds(0, 2 * n * cols)] = value * dims["scale"]
            put_far(h, j).start()
            return carry

        with scope("f_far"):
            for copy in far_loads(h):
                copy.wait()
            if h:
                far_ends(0)
            lax.fori_loop(0, hh, body, 0)

    def begin_unit(u):
        if u == 0:
            for h in BOTH:
                keep(h).wait()
        load_unit(u)

    load_h = place.local("h", h_hbm, xn)
    works = {
        "HIT": make_hits, "GT": turn_g, "COL": lay_columns, "G2": gain_next, "XN": normalize, "XT": turn_xn, "LP": load_first, "L0": logits_first,
        "PF": pass_first, "PFF": pass_first_far,
    }
    groups = {"0": 0, "P": PAIR, "F": FAR}
    families = {"LF": far_load, "FL": far_look, "LU": begin_unit, "LK": look, "X1": x_first, "X2": x_second, "X3": x_third, "X4": x_fourth}
    families_k = {"SH": share_group, "S": pass_second, "E": end_second}

    def perform(text):
        for word in text.split():
            if word in works:
                works[word]()
            elif word[:-1] in families:
                families[word[:-1]](int(word[-1]))
            else:
                families_k[word[:-1]](groups[word[-1]])

    during = (
        "X24",
        "X15 X33",
        "",
        "X34",
        "X42",
        "X43",
        "",
    )
    for text in (
        "HIT LU0 LK0 G2", "GT X10 PF LU1", "LK1 LF0 S0 X20", "X11 FL0 PFF X21", "LU2 LF1 X30 LK2",
        "FL1 XN SP SH0", "E0 LU3 X12 X31", "LK3 SF LU4 X22", "X40 SHP LK4 X13", "EP X32 X41 EF",
        "LU5 SHF LP XT", "COL L0 X14 LK5", "X23",
    ):
        perform(text)
    if n_half < 4:
        wait_shares()
        for text in during:
            perform(text)
        during = ()
    last = n_tile // 2 - 1
    with scope("f_logits"):
        lax.fori_loop(1, last + 1, pair, 0)
        for odd in BOTH:
            post_tile(last, odd)

    with scope("f_stats"):
        row = lax.broadcasted_iota(I32, (2, tok), 0)
        sum_e = jnp.sum(acc_e[...].T, axis=0, keepdims=True)
        sum_l = SOFT_CAP * jnp.sum(acc_l[...].T, axis=0, keepdims=True)
        stats = SmallSum(place, ("dx",), s_slots)
        stats.start("dx", jnp.where(row == 0, sum_e, sum_l))
    perform("X25 X44")
    with scope("f_stats2"):
        stat = stats.finish("dx")
        all_e, all_l = stat[0:1], stat[1:2]
        inv_s[...] = jnp.broadcast_to((1.0 / dims["total"]) / all_e, (LANE, tok)).T
        s_slots[0, 0:1, :] = jnp.log(all_e) + SOFT_CAP - all_l
        own = s_slots[0, 0:1, lanes_of(0)]
        part_w = min(LANE, quarter)
        folded = own[:, 0:part_w]
        for j in range(part_w, quarter, part_w):
            folded = folded + own[:, j:j + part_w]
        loss_out[...] = jnp.where(lax.broadcasted_iota(I32, (SUB, part_w), 0) == 0, folded, 0.0)
        put_small(1).start()

    def dz_tile(j):
        return ((1 - c) * n_half + j) % n_tile

    def load_u(i, odd):
        return place.local(("u", odd), u_hbm.at[dz_tile(2 * i + odd)], (z_even, z_odd)[odd].at[i % 2], i % 2)

    def put_dz(i, odd):
        return place.local(("dz", odd), dzb.at[odd, i % 2], dz_out.at[dz_tile(2 * i + odd)], i % 2)

    def give_dz(part):
        src = dz_out.at[pl.ds((1 - c) * n_half + part * hh, hh)]
        return place.send(("dz", part), src, dzpar_out.at[pl.ds(part * hh, hh)], dc=1)

    d_step = min(256, tok)

    def dz_rows(i, odd):
        base = dz_tile(2 * i + odd) * vt
        buf, slot = (z_even, z_odd)[odd], i % 2

        def body(e, carry):
            sel = span(e * d_step, d_step, d_step)
            ids = lax.broadcasted_iota(I32, (d_step, LANE), 1) + base
            for b, lanes in lane_blocks():
                tanh_z = buf[slot, sel, lanes]
                prob = jnp.exp2(EXP_RATE * tanh_z - EXP_RATE) * inv_s[sel]
                prob = jnp.where(ids + b == labc[sel], prob - 1.0 / dims["total"], prob)
                dzb[odd, slot, sel, lanes] = (prob * (1.0 - tanh_z * tanh_z)).astype(BF16)
            return carry

        lax.fori_loop(0, tok // d_step, body, 0)

    def dz_pair(i, loaded, follow):
        for odd in BOTH:
            if loaded:
                load_u(i, odd).wait()

            @pl.when(i > hh + 1)
            def _():
                put_dz(i - 2, odd).wait()

            dz_rows(i, odd)
            put_dz(i, odd).start()

            @pl.when(i + follow < n_tile // 2)
            def _():
                load_u(i + follow, odd).start()

    def dz_run(lo, hi, loaded, follow):
        def body(i, carry):
            dz_pair(i, loaded, follow)
            return carry

        lax.fori_loop(lo, hi, body, 0)

    with scope("f_dz"):
        half = hh // 2
        for part in (1, 0):
            dz_run(part * half, (part + 1) * half, not part, hh if part == 0 else -half)
            for i in range(part * half, (part + 1) * half):
                for odd in BOTH:
                    put_dz(i, odd).wait()
            give_dz(part).start()
        dz_run(hh, n_tile // 2, True, half)

    perform("X35")
    with scope("f_end"):
        for i in range(3):
            put_small(i).wait()
        for part in BOTH:
            give_dz(part).wait()
        for i in range(n_tile // 2 - 2, n_tile // 2):
            for odd in BOTH:
                put_dz(i, odd).wait()
        give_tok.wait_send()
        give_chunk.wait_send()
        for h in BOTH:
            for i in BOTH:
                p1_send(h, i).wait_send()
                p1_fwd(h, i).wait_send()
                for k in (0, PAIR, FAR):
                    p2_send(h, k, i).wait_send()
                    p2_fwd(h, k, i).wait_send()
            for k in (0, PAIR, FAR):
                share(h, k).wait_send()
        for part in BOTH:
            for copy in move_xn(part):
                copy.wait()
        for u in range(len(UNITS)):
            if u > len(UNITS) - 3:
                x_swap(u).wait_send()
            x_keep(u).wait()
            for i in BOTH:
                x_far(u, i).wait_send()
                x_near(u, i).wait_send()
                if u < last_unit:
                    x_put(u, i).wait_send()
                    x_pass(u, i).wait()
    assert (place.n_link, place.n_local) <= dims["front_sems"], (place.n_link, place.n_local)


def specs(n_vmem, n_any):
    return [pl.BlockSpec(memory_space=pltpu.VMEM)] * n_vmem + [pl.BlockSpec(memory_space=pl.ANY)] * n_any


def shapes(items):
    return tuple(jax.ShapeDtypeStruct(*item) for item in items)


def scratch(items, n_link, n_local):
    dma = pltpu.SemaphoreType.DMA
    return [pltpu.VMEM(*item) for item in items] + [dma((n_link,)), dma((n_link,)), dma((n_local,))]


def params(collective_id, limit):
    return pltpu.CompilerParams(collective_id=collective_id, has_side_effects=True, vmem_limit_bytes=limit)


def front(dims, limit, shard, tok_row, lab_row, w, h, g):
    n, tok, vocab, width, vt = dims["n"], dims["tok"], dims["vocab"], dims["width"], dims["vt"]
    cols = shard.shape[0]
    half_v = vocab // CORES
    quarter = tok // n
    n_tile, n_half, most = vocab // vt, half_v // vt, max(PIECES)
    pieces = n * n * CORES
    grid = (n // 2, 2, n // 2, 2)
    return pl.pallas_call(
        functools.partial(front_kernel, dims),
        name="front",
        out_shape=shapes([
            ((n_tile, *grid, CORES, cols, vt), BF16), *[((pieces, cols, tok), BF16)] * 4, ((2, 2 * n * cols, half_v // 2), F32), ((n_tile, tok, vt), BF16),
            ((n_half, tok, vt), BF16), ((n, BASE[-1], cols, quarter), BF16), ((PIECES[-1], cols, quarter), BF16), ((n_tile, tok, vt), F32),
            ((1, width), F32), ((SUB, min(LANE, quarter)), F32), ((CORES, tok, LANE), I32),
        ]),
        in_specs=specs(0, 6),
        out_specs=tuple(specs(0, 14)),
        scratch_shapes=scratch([
            (shard.shape, F32), (tok_row.shape, I32), (lab_row.shape, I32), (w.shape, F32), ((1, width), F32),
            ((SUB, min(LANE, quarter)), F32), ((CORES, tok, LANE), I32),
            ((n_tile, cols, vt), BF16), ((CORES, n_half, cols, vt), BF16), ((CORES, SUB, tok), I32), ((half_v, CORES * tok), BF16),
            ((2, most, n_half, cols, vt), BF16), ((pieces, cols, tok), BF16), ((2, CORES, most, cols, tok), BF16), ((pieces, cols, tok), BF16),
            ((pieces, cols, quarter), BF16), ((2, pieces, cols, quarter), BF16), ((pieces, cols, quarter), BF16),
            ((4, *grid, CORES, cols, vt), BF16), ((tok, width), BF16), ((pieces, cols, tok), BF16),
            ((2, tok, vt), F32), ((2, tok, vt), F32), ((2, 2, tok, vt), BF16), ((tok, LANE), F32), ((tok, LANE), F32), ((tok, LANE), F32),
            ((tok, LANE), I32), ((2 * n + CORES, 1, width), F32), ((n, 2, tok), F32),
        ], dims["front_sems"][0], dims["front_sems"][1]),
        compiler_params=params(0, limit),
    )(shard, tok_row, lab_row, w, h, g)


def back_kernel(
    dims,
    gain_hbm, loss_hbm, tokc_hbm, lt_hbm, dz_hbm, dzp_hbm, et_hbm, xnt_hbm, xpar_hbm, gt_hbm, gpar_hbm, h_hbm, q5_hbm,
    tail_hbm, dh_out, de_out, x0_out, ra_hbm, rx_hbm,
    gain_ref, loss_ref, tokc, tail_out, q5, dz_own, dz_par, et_buf, part, fx, acc, fa, f2, r2, xb, h_buf, dh_buf, dg_acc, slots,
    sends, recvs, local_sems,
):
    n, tok, vocab, width, tile, vt = (dims[k] for k in ("n", "tok", "vocab", "width", "tile", "vt"))
    place = Place(n, sends, recvs, local_sems)
    x, z, y, c = place.x, place.z, place.y, place.c
    half_v = vocab // CORES
    n_tile, n_half = vocab // vt, half_v // vt
    lanes = half_v // 2
    rows = width // (n * n)
    half_rows = rows // 2
    quarter = tok // n
    hq = quarter // 2
    tiles = dims["tiles"]
    chunks = len(tiles)
    edges = [sum(tiles[:d]) for d in range(chunks + 1)]
    per_half = n_half // 2

    knocks = place.knock()
    load_q5 = place.local("q5", q5_hbm, q5)
    load_q5.start()
    load_h = place.local("h", h_hbm.at[span(x * quarter, quarter, quarter)], h_buf)

    def load_et(t, slot):
        return place.local("et", et_hbm.at[:, span(t * tile, tile, tile)], et_buf.at[slot], slot)

    slot_of = {FAR: 0, 1: 1, 3: 2, 0: 0}
    stages = dims["stages"]

    def load_stage(m, i):
        half, k, kind = stages[m]
        src = ((gt_hbm, gpar_hbm), (xnt_hbm, xpar_hbm))[kind][i]
        src = src.at[(z + k) % n] if half == 0 else src.at[:, (y + k) % n]
        return place.local(("xb", i), src, xb.at[m % 2, i], m % 2)

    def start_stage(m):
        if m < len(stages):
            start_all(load_stage(m, i) for i in BOTH)

    loads = [place.local("dz", dz_hbm, dz_own), place.local("dzp", dzp_hbm, dz_par)]
    load_et(0, 0).start()
    start_all(loads)
    keep_q5 = place.local("q5", q5, x0_out.at[x], 1)

    def y_put(i):
        return place.send(("yp", i), q5, x0_out.at[x], dx=WAYS[i])

    def y_pass(i):
        size = q5.shape[0] // 2
        ref = x0_out.at[(x + FROM[i]) % n, pl.ds(i * size, size)]
        return place.send(("yq", i), ref, ref, dx=WAYS[i])

    def y_passes():
        for i in BOTH:
            y_put(i).wait_recv()
            y_pass(i).start()

    small_loads = [
        place.local(("in", i), src, dst, 0, 1)
        for i, (src, dst) in enumerate(((tokc_hbm, tokc), (gain_hbm, gain_ref), (loss_hbm, loss_ref)))
    ]
    fars = [place.local("lt", lt_hbm.at[half], acc.at[half, 0], half) for half in BOTH]
    start_all(fars + small_loads)
    for m in BOTH:
        start_stage(m)
    load_h.start()

    def columns(d):
        return pl.ds(edges[d] * tile, tiles[d] * tile)

    def dxn_chunk(d):
        def body(t, carry):
            slot = t % 2

            @pl.when(t + 1 < edges[chunks])
            def _():
                load_et(t + 1, 1 - slot).start()

            load_et(t, slot).wait()
            left = jnp.concatenate([dz_own[j] for j in range(n_tile)], axis=1)
            right = jnp.concatenate([et_buf[slot, j] for j in range(n_tile)], axis=1)
            part[:, span(t * tile, tile, tile)] = lax.dot_general(
                left, right, (((1,), (1,)), ((), ())), preferred_element_type=F32)
            return carry

        with scope("b_dxn"):
            lax.fori_loop(edges[d], edges[d + 1], body, 0)

    def qrow(k, lo=0, size=hq):
        return span((x + k) % n * quarter + lo, size, SUB)

    def x_far(d, i):
        return place.send(("xf", d, i), part.at[qrow(FAR, i * hq), columns(d)], fx.at[i, :, columns(d)], dx=WAYS[i])

    def x_near(d, i, j):
        src = part.at[qrow(WAYS[i], j * hq), columns(d)]
        return place.send(("xn", d, i, j), src, rx_hbm.at[i, pl.ds(j * hq, hq), columns(d)], dx=WAYS[i])

    def x_first(d):
        start_all(x_far(d, i) for i in BOTH)

    def x_second(d):
        with scope("b_x2"):
            for i in BOTH:
                x_far(d, i).wait_recv()
                sel = qrow(WAYS[i], i * hq)
                part[sel, columns(d)] = part[sel, columns(d)] + fx[i, :, columns(d)]
                start_all(x_near(d, i, j) for j in BOTH)

    def stage_x(d, j, i):
        return place.local("sx", rx_hbm.at[i, pl.ds(j * hq, hq), columns(d)], fx.at[i, :, columns(d)], i)

    def x_third(d, j):
        with scope("b_x3"):
            for i in BOTH:
                x_near(d, i, j).wait_recv()
                stage_x(d, j, i).start()
            for i in BOTH:
                stage_x(d, j, i).wait()
            sel = qrow(0, j * hq)
            part[sel, columns(d)] = part[sel, columns(d)] + fx[0, :, columns(d)] + fx[1, :, columns(d)]

    def de_stage(half, k, kind):
        m = stages.index((half, k, kind))
        slot = slot_of[k]

        wide = min(2, per_half) if kind and k else 1

        def right(i, t):
            if kind:
                return dz_par[t] if i else dz_own[c * n_half + t]
            ids = lax.broadcasted_iota(I32, (tok, LANE), 1) + (x * vocab + c * half_v + t * vt)
            hits = [jnp.where(tokc[i] == ids + b, dims["scale"], 0.0).astype(BF16) for b in range(0, vt, LANE)]
            return jnp.concatenate(hits, axis=1)

        def body(j, carry):
            t = half * per_half + j * wide
            sel = span(j * wide * vt, wide * vt)
            left = jnp.concatenate([xb[m % 2, i].reshape(n * rows, tok) for i in BOTH], axis=1)
            both_right = [jnp.concatenate([right(i, t + q) for i in BOTH], axis=0) for q in range(wide)]
            total = jnp.dot(left, jnp.concatenate(both_right, axis=1), preferred_element_type=F32)
            total = total.reshape(n, rows, wide * vt)
            acc[half, slot, :, :, sel] = acc[half, slot, :, :, sel] + total if kind else total
            return carry

        with scope("b_de" if kind else "b_look"):
            for i in BOTH:
                load_stage(m, i).wait()
            lax.fori_loop(0, per_half // wide, body, 0)
            start_stage(m + 2)

    def de_unit(half, k):
        if k == FAR:
            fars[half].wait()
        else:
            de_stage(half, k, 0)
        de_stage(half, k, 1)

    def ring(half, k):
        return {"dz": k} if half == 0 else {"dy": k}

    def cross(half, k):
        return {"dy": k} if half == 0 else {"dz": k}

    def a_far(half, i):
        return place.send(("af", half, i), acc.at[half, 0, pl.ds(2 * i, 2)], fa.at[half, i], **ring(half, WAYS[i]))

    def a_near(half, i, j):
        sel = pl.ds(2 * j, 2)
        return place.send(("an", half, i, j), acc.at[half, 1 + i, sel], ra_hbm.at[half, i, sel], **ring(half, WAYS[i]))

    def a_first(half):
        start_all(a_far(half, i) for i in BOTH)

    def a_second(half, i):
        with scope("b_a2"):
            a_far(half, i).wait_recv()
            sel = pl.ds(2 * i, 2)
            acc[half, 1 + i, sel] = acc[half, 1 + i, sel] + fa[half, i]
            start_all(a_near(half, i, j) for j in BOTH)

    def stage_a(half, j, i):
        return place.local(("sa", half), ra_hbm.at[half, i, pl.ds(2 * j, 2)], fa.at[half, i], i)

    def piece(half, k):
        return ((y if half == 0 else z) + k) % n

    def c_far(half, i):
        src = acc.at[half, 0, piece(half, FAR), pl.ds(i * half_rows, half_rows)]
        return place.send(("cf", half, i), src, f2.at[half, i], **cross(half, WAYS[i]))

    def c_near(half, i):
        return place.send(("cn", half, i), acc.at[half, 0, piece(half, WAYS[i])], r2.at[half, i], **cross(half, WAYS[i]))

    def a_third(half, j):
        with scope("b_a3"):
            for i in BOTH:
                a_near(half, i, j).wait_recv()
                stage_a(half, j, i).start()
            for i in BOTH:
                stage_a(half, j, i).wait()
            sel = pl.ds(2 * j, 2)
            acc[half, 0, sel] = acc[half, 0, sel] + fa[half, 0] + fa[half, 1]

    def c_first(half):
        start_all(c_far(half, i) for i in BOTH)

    def c_second(half):
        with scope("b_c2"):
            for i in BOTH:
                c_far(half, i).wait_recv()
                at = piece(half, WAYS[i])
                sel = pl.ds(i * half_rows, half_rows)
                acc[half, 0, at, sel] = acc[half, 0, at, sel] + f2[half, i]
                c_near(half, i).start()

    def out_copies(half):
        sel = span(c * half_v + half * lanes, lanes)
        mine = acc.at[half, 0, piece(half, 0)]
        yield place.local("de", mine.at[span(c * half_rows, half_rows, SUB)], de_out.at[:, sel], half)
        yield place.send(("de", half), mine.at[span((1 - c) * half_rows, half_rows, SUB)], de_out.at[:, sel], dc=1)

    def c_third(half):
        with scope("b_c3"):
            for i in BOTH:
                c_near(half, i).wait_recv()
            at = piece(half, 0)
            acc[half, 0, at] = acc[half, 0, at] + r2[half, 0] + r2[half, 1]
            start_all(out_copies(half))

    step = min(32, hq)

    def dh_body(i, carry):
        sel = span(i * step, step, step)
        row = span(x * quarter + i * step, step, step)
        d_x = part[row]
        h_wide = h_buf[sel].astype(F32)
        inv_rms = lax.rsqrt(jnp.sum(h_wide * h_wide, axis=1, keepdims=True) * (1.0 / width) + NORM_EPS)
        h_norm = h_wide * inv_rms
        g_dir = d_x * gain_ref[0:1]
        mean = jnp.sum(g_dir * h_norm, axis=1, keepdims=True) * (1.0 / width)
        dh_buf[sel] = (inv_rms * (g_dir - h_norm * mean)).astype(BF16)
        prod = d_x * h_norm
        total = prod[0:SUB]
        for j in range(SUB, step, SUB):
            total = total + prod[j:j + SUB]
        dg_acc[...] = dg_acc[...] + total
        return carry

    def h_first(i, j):
        return place.send(("hf", i, j), dh_buf.at[pl.ds(j * hq, hq)], dh_out.at[qrow(0, j * hq)], dx=WAYS[i])

    def h_second(i):
        ref = dh_out.at[qrow(FROM[i], i * hq)]
        return place.send(("hs", i), ref, ref, dx=WAYS[i])

    keep_dh = place.local("dh", dh_buf, dh_out.at[qrow(0, 0, quarter)])
    small = SmallSum(place, ("dc", "dx", "dy", "dz"), slots)
    per_j = hq // step

    def dh_part(j):
        with scope("b_dh"):
            if j == 0:
                load_h.wait()
            lax.fori_loop(j * per_j, (j + 1) * per_j, dh_body, 0)
            start_all(h_first(i, j) for i in BOTH)
            if j:
                keep_dh.start()

    def h_pass(i):
        with scope("b_h2"):
            h_first(i, i).wait_recv()
            h_second(i).start()

    put_tail = place.local("tail", tail_out, tail_hbm, 0, 1)

    def small_step(k):
        dims_of = small.dims
        with scope("b_s"):
            if k == 1:
                sums = [jnp.sum(part_sum, axis=0, keepdims=True) for part_sum in (dg_acc[...], loss_ref[...])]
                small.start(dims_of[0], jnp.concatenate(sums, axis=1))
            elif k <= len(dims_of):
                small.start(dims_of[k - 1], small.finish(dims_of[k - 2]))
            else:
                total = small.finish(dims_of[-1])
                loss = jnp.sum(total[:, width:], axis=1, keepdims=True) * (1.0 / dims["total"])
                tail_out[...] = jnp.concatenate([total[:, 0:width], jnp.broadcast_to(loss, (1, LANE))], axis=1)
                put_tail.start()

    def dxn(d):
        dxn_chunk(d)
        x_first(d)

    def unit(half, k):
        if k == 0:
            with scope("b_wait_far"):
                for i in BOTH:
                    a_far(half, i).wait_send()
        while len(loads) > 1:
            loads.pop().wait()
            for copy in small_loads:
                copy.wait()
        de_unit(half, k)
        if k == FAR:
            a_first(half)

    families = {
        "CH": dxn, "XS": x_second, "UN": unit, "AS": a_second, "XT": x_third, "AT": a_third, "CF": c_first, "CS": c_second,
        "CT": c_third, "DH": dh_part, "SM": small_step, "HP": h_pass, "YQ": y_passes,
    }

    def perform(text):
        for word in text.split():
            families[word[:2]](*(int(digit) for digit in word[2:]))

    with scope("b_enter"):
        place.enter(knocks)
    with scope("b_load"):
        load_q5.wait()
        start_all(y_put(i) for i in BOTH)
        keep_q5.start()
        loads[0].wait()
        dg_acc[...] = jnp.zeros_like(dg_acc)
    for text in (
        "CH0 UN02 YQ CH1", "UN12 CH2 UN03 XS1", "UN01 XS2 UN13 AS01", "AS00 UN11 AS11 AS10",
        "XS0 CH3 XT10 CH4", "UN00 XT00 XS3 XT01", "XS4 UN10 XT20 AT00", "XT30 XT21 XT11 XT40",
        "DH0 XT31 XT41 DH1", "AT01 AT10 CF0 SM1", "AT11 CF1 SM2 HP0", "CS0 CS1 SM3 HP1", "CT0 SM4 CT1 SM5",
    ):
        perform(text)

    with scope("b_end_x"):
        put_tail.wait()
        keep_dh.wait()
        keep_q5.wait()
        for i in BOTH:
            y_put(i).wait_send()
            y_pass(i).wait()
            for d in range(chunks):
                x_far(d, i).wait_send()
                for j in BOTH:
                    x_near(d, i, j).wait_send()
            h_first(i, i).wait_send()
            h_first(i, 1 - i).wait()
            h_second(i).wait()
    with scope("b_end_a"):
        for half in BOTH:
            for i in BOTH:
                for j in BOTH:
                    a_near(half, i, j).wait_send()
                c_far(half, i).wait_send()
                c_near(half, i).wait_send()
            for copy in out_copies(half):
                copy.wait()
    assert (place.n_link, place.n_local) <= dims["back_sems"], (place.n_link, place.n_local)


def back(dims, limit, gain, loss, tokc, far, dz, dzp, et, xnt, xpar, gt, gpar, h, q5):
    n, tok, vocab, width, tile = (dims[k] for k in ("n", "tok", "vocab", "width", "tile"))
    rows = width // (n * n)
    half_v = vocab // CORES
    lanes = half_v // 2
    quarter = tok // n
    hq = quarter // 2
    tail_w = width + loss.shape[1]
    n_tile, n_half, vt = dz.shape[0], dzp.shape[0], dims["vt"]
    turned = [a.reshape(n, n, rows, tok) for a in (xnt, xpar, gt, gpar)]
    return pl.pallas_call(
        functools.partial(back_kernel, dims),
        name="back",
        out_shape=shapes([
            ((1, width + LANE), F32), ((tok, width), BF16), ((rows // CORES, vocab), F32), ((n, *q5.shape), BF16),
            ((2, 2, n, rows, lanes), F32),
            ((2, quarter, width), F32),
        ]),
        in_specs=specs(0, 13),
        out_specs=tuple(specs(0, 6)),
        scratch_shapes=scratch([
            (gain.shape, F32), (loss.shape, F32), (tokc.shape, I32), ((1, width + LANE), F32),
            (q5.shape, BF16), ((n_tile, tok, vt), BF16), ((n_half, tok, vt), BF16), ((2, n_tile, tile, vt), BF16), ((tok, width), F32),
            ((2, hq, width), F32), ((2, 3, n, rows, lanes), F32), ((2, 2, 2, rows, lanes), F32),
            ((2, 2, rows // 2, lanes), F32), ((2, 2, rows, lanes), F32), ((2, CORES, n, rows, tok), BF16), ((quarter, width), BF16),
            ((quarter, width), BF16), ((SUB, width), F32), ((3 * n + CORES, 1, tail_w), F32),
        ], dims["back_sems"][0], dims["back_sems"][1]),
        compiler_params=params(1, limit),
    )(gain, loss, tokc, far.reshape(2, n, rows, lanes), dz, dzp, et.reshape(n_tile, width, vt), *turned, h, q5)[:4]


def finish_kernel(
    n, scale, table_ref, tail_ref, x0_hbm, x5_hbm, dh_hbm, de_hbm, dg_out, loss_out, x0_out, dh_out, de_out,
    x0_in, x0_buf, rows_ref, dh_buf, de_buf, sems,
):
    place = Place(n, None, None, sems)
    quarter, cols, width = x0_in.shape[3], x0_in.shape[2], x0_buf.shape[2]

    def step(q):
        rows = span(q * quarter, quarter, quarter)
        return (
            place.local("x0", x0_hbm.at[q], x0_in.at[q, pl.ds(0, BASE[-1])], q, n),
            place.local("x5", x5_hbm.at[q], x0_in.at[q, pl.ds(BASE[-1], PIECES[-1])], q, n), place.local("x0o", x0_buf.at[q], x0_out.at[rows], q, n),
            place.local("dh", dh_hbm.at[rows], dh_buf.at[q], q, n), place.local("dho", dh_buf.at[q], dh_out.at[rows], q, n),
        )

    moves = [step(q) for q in range(n)]
    de_in, de_put = place.local("de", de_hbm, de_buf, 0), place.local("de", de_buf, de_out, 1)
    for x0_load, x5_load, _, dh_load, _ in moves:
        start_all((x0_load, x5_load, dh_load))
    de_in.start()
    gain = jnp.broadcast_to(tail_ref[:, 0:width], (SUB, width))
    dg_out[...] = pltpu.roll(gain, width - place.f * cols, axis=1)[0:1, 0:cols]
    loss_out[...] = tail_ref[:, width:width + 1]

    def body(q, carry):
        x0_load, x5_load, x0_put, dh_load, dh_put = step(q)
        x0_load.wait()
        x5_load.wait()
        for zi in range(n):
            for yi in range(n):
                for h in BOTH:
                    dz, dy = (zi - place.z) % n, (yi - place.y) % n
                    k1, k2 = (dy, dz) if h == 0 else (dz, dy)
                    piece = table_ref[(h * n + k1) * n + k2]
                    rows_ref[pl.ds(((zi * n + yi) * CORES + h) * cols, cols)] = x0_in[q, piece]
        x0_buf[q] = (rows_ref[...].T.astype(F32) * scale).astype(BF16)
        x0_put.start()
        dh_load.wait()
        dh_put.start()
        return carry

    lax.fori_loop(0, n, body, 0)
    de_in.wait()
    de_put.start()
    for _, _, x0_put, _, dh_put in moves:
        x0_put.wait()
        dh_put.wait()
    de_put.wait()


def finish(n, scale, limit, tail, x0, x5, dh, de):
    cols, quarter = x0.shape[2:]
    pieces = n * n * CORES
    width = pieces * cols
    table = np.zeros((CORES, n, n), np.int32)
    for u, unit in enumerate(UNITS):
        for h in BOTH:
            for i, (k1, k2) in enumerate(unit):
                table[h, k1, k2] = BASE[u] + h * len(unit) + i
    return pl.pallas_call(
        functools.partial(finish_kernel, n, scale),
        name="finish",
        in_specs=[pl.BlockSpec(memory_space=pltpu.SMEM)] + specs(1, 4),
        out_specs=tuple(specs(2, 3)),
        out_shape=shapes([((1, cols), F32), ((1, 1), F32), (dh.shape, BF16), (dh.shape, BF16), (de.shape, F32)]),
        scratch_shapes=[
            pltpu.VMEM((n, pieces, cols, quarter), BF16), pltpu.VMEM((n, quarter, width), BF16), pltpu.VMEM((width, quarter), BF16),
            pltpu.VMEM((n, quarter, width), BF16), pltpu.VMEM(de.shape, F32), pltpu.SemaphoreType.DMA((5 * n + 2,)),
        ],
        compiler_params=pltpu.CompilerParams(vmem_limit_bytes=limit),
    )(jnp.asarray(table.reshape(-1)), tail, x0, x5, dh, de)


def solution(mesh):
    return build(mesh, mesh.shape["tp"], 256, digits("12222")[0], 256, 6, 67_000_000)


def build(mesh, n, tile, tiles, vt, n_block, limit):
    fsdp_size = mesh.shape["fsdp"]

    def device_step(emb_shard, tok_ids, lab_ids, h_last, g_embed, norm_w):
        vocab_rows, cols = emb_shard.shape
        batch_loc, seq_len, width = h_last.shape
        tok_count = batch_loc * seq_len
        fsdp_id = lax.axis_index("fsdp")
        scale = float(np.asarray(math.sqrt(width)).astype(jnp.bfloat16))
        dims = {
            "n": n, "tok": tok_count, "vocab": vocab_rows, "width": width, "total": tok_count * fsdp_size, "vt": vt,
            "tile": tile, "tiles": tiles, "scale": scale, "n_block": n_block,
            "stages": digits("021 121 030 031") + digits("010 011 130 131") + digits("110 111 000 001") + digits("100 101"),
            "front_sems": (106, 59), "back_sems": (72, 30),
        }
        h_flat = h_last.reshape(tok_count, width)
        placed = lax.dynamic_update_slice(jnp.zeros((SUB, width), F32), jnp.broadcast_to(norm_w, (SUB, cols)), (0, fsdp_id * cols))
        ids = [a.reshape(1, tok_count) for a in (tok_ids, lab_ids)]
        table, xn_t, xpar_t, g_t, gpar_t, far, dz, dzp, x0, q5, _, gain, loss_part, tokc = front(
            dims, limit, emb_shard.T, *ids, norm_w.reshape(1, cols), h_flat, g_embed.reshape(tok_count, width))
        tail, d_hidden, d_cols, x5 = back(dims, limit, gain, loss_part, tokc, far, dz, dzp, table, xn_t, xpar_t, g_t, gpar_t, h_flat, q5)
        d_norm_w, loss, x_emb, d_hidden, d_cols = finish(n, scale, limit, tail, x0, x5, d_hidden, d_cols)
        return (x_emb.reshape(h_last.shape), loss.reshape(()), d_hidden.reshape(h_last.shape), d_norm_w.reshape(cols), d_cols.T)

    spec_tok = P("fsdp", None)
    spec_act = P("fsdp", None, None)
    return jax.shard_map(device_step, mesh=mesh, in_specs=(P("tp", "fsdp"), spec_tok, spec_tok, spec_act, spec_act, P("fsdp")), out_specs=(spec_act, P(), spec_act, P("fsdp"), P("tp", "fsdp")), check_vma=False)
```

```python
import functools
import math
import jax
import numpy as np
import jax.numpy as jnp
from jax import lax
from jax.experimental import pallas as pl
from jax.experimental.pallas import tpu as pltpu
from jax.sharding import PartitionSpec as P

SOFT_CAP = 30.0
NORM_EPS = 1e-6
F32, BF16, I32 = jnp.float32, jnp.bfloat16, jnp.int32
LANE, SUB = 128, 8
BOTH = (0, 1)
FOUR = range(4)
WAYS = (1, 3)
FROM = (3, 1)
FAR = 2
CORES = 2


def span(start, size, unit=LANE):
    return pl.ds(pl.multiple_of(start, unit), size)


class Place:
    def __init__(self, n, sends, recvs, local_sems):
        self.n, self.sends, self.recvs, self.local_sems = n, sends, recvs, local_sems
        self.x = lax.axis_index("tp")
        f = lax.axis_index("fsdp")
        self.f = f
        self.c = f % CORES
        self.y = f // CORES % n
        self.z = f // CORES // n
        self.link_of, self.local_of, self.n_link, self.n_local = {}, {}, 0, 0
        self.size = {"dx": n, "dz": n, "dy": n, "dc": CORES}
        self.me = {"dx": self.x, "dz": self.z, "dy": self.y, "dc": self.c}

    def at(self, dx=0, dz=0, dy=0, dc=0):
        n = self.n
        z, y, c = (self.z + dz) % n, (self.y + dy) % n, (self.c + dc) % CORES
        return ((self.x + dx) % n, (z * n + y) * CORES + c)

    def knock(self):
        peers = [self.at(**{d: k}) for d in self.size for k in range(1, self.size[d])]
        for peer in peers:
            pl.semaphore_signal(pltpu.get_barrier_semaphore(), inc=1, device_id=peer, device_id_type=pl.DeviceIdType.MESH)
        return len(peers)

    def enter(self, knocks):
        pl.semaphore_wait(pltpu.get_barrier_semaphore(), knocks)

    def link(self, key, count=1):
        if key not in self.link_of:
            self.link_of[key] = self.n_link
            self.n_link += count
        return self.link_of[key]

    def send(self, key, src, dst, **step):
        i = self.link(key)
        return pltpu.make_async_remote_copy(
            src, dst, self.sends.at[i], self.recvs.at[i], device_id=self.at(**step), device_id_type=pl.DeviceIdType.MESH)

    def local(self, key, src, dst, slot=0, count=2):
        if key not in self.local_of:
            self.local_of[key] = self.n_local
            self.n_local += count
        return pltpu.make_async_copy(src, dst, self.local_sems.at[self.local_of[key] + slot])


class SmallSum:
    def __init__(self, place, dims, slots):
        self.place, self.slots, self.dims, self.base = place, slots, dims, {}
        count = 0
        for d in dims:
            self.base[d] = count
            count += place.size[d]

    def copies(self, d):
        slot = self.slots.at[self.base[d] + self.place.me[d]]
        for k in range(1, self.place.size[d]):
            yield self.place.send((self.dims, d, k), slot, slot, **{d: k})

    def start(self, d, value):
        self.slots[self.base[d] + self.place.me[d]] = value
        for copy in self.copies(d):
            copy.start()

    def finish(self, d):
        for copy in self.copies(d):
            copy.wait()
        total = self.slots[self.base[d]]
        for k in range(1, self.place.size[d]):
            total = total + self.slots[self.base[d] + k]
        return total


def scope(name):
    return jax.named_scope(name)


def start_all(copies):
    for copy in copies:
        copy.start()


def digits(text):
    return tuple(tuple(int(d) for d in word) for word in text.split())


UNITS = [digits(u) for u in ("00", "10 30", "01 03 20", "02 11 31", "13 33 21 23", "12 32 22")]
PAIR, ALL = 1, "all"
PIECES = [2 * len(u) for u in UNITS]
EXP_RATE = SOFT_CAP * math.log2(math.e)
BASE = [sum(PIECES[:i]) for i in range(len(UNITS))]


def front_kernel(
    dims,
    shard_hbm, tok_hbm, lab_hbm, w_hbm, h_hbm, g_hbm,
    et_out, xnt_out, xpar_out, gt_out, gpar_out, lt_out, dz_out, dzpar_out, x0_out, q5_out, u_hbm, gain_hbm, loss_hbm, tokc_hbm,
    shard_ref, tok_ref, lab_ref, w_ref, gain_out, loss_out, tokc_out, shard_t, chunk, tokr, hit_t, lhs, xp, xw, xr, xf, xg, xq, etb, xn, gl, z_even, z_odd, dzb,
    acc_e, acc_l, inv_s, labc, w_slots, s_slots, sends, recvs, local_sems,
):
    n, tok, vocab, width, vt = dims["n"], dims["tok"], dims["vocab"], dims["width"], dims["vt"]
    place = Place(n, sends, recvs, local_sems)
    x, z, y, c = place.x, place.z, place.y, place.c
    half_v = vocab // CORES
    n_tile = vocab // vt
    n_half = n_tile // CORES
    hh = n_half // 2
    cols = width // (n * n * CORES)
    quarter = tok // n
    row_start = x * vocab

    def ring1(h, k):
        return {"dy": k} if h == 0 else {"dz": k}

    def ring2(h, k):
        return {"dz": k} if h == 0 else {"dy": k}

    def coord(base, k, paired):
        every = slice(None)
        if k == ALL:
            return every, every
        return every if paired else (base + k) % n // 2, (base + k) % 2

    def loc(h, k1, k2, lo=0, size=n_half, pair1=False, pair2=False):
        first, second = coord((y, z)[h], k1, pair1), coord((z, y)[h], k2, pair2)
        return et_out.at[(pl.ds(c * n_half + lo, size), *((second, first)[h]), *((first, second)[h]), h)]

    knocks = place.knock()
    early_loads = [
        place.local(("in", i), src, dst, 0, 1)
        for i, (src, dst) in enumerate(((shard_hbm, shard_ref), (tok_hbm, tok_ref), (lab_hbm, lab_ref), (w_hbm, w_ref)))
    ]
    start_all(early_loads)
    load_g = place.local("g", g_hbm, xn)
    load_g.start()
    with scope("f_cast"):
        for copy in early_loads:
            copy.wait()
        for t in range(n_tile):
            shard_t[t] = shard_ref[:, pl.ds(t * vt, vt)].astype(BF16)
    with scope("f_enter"):
        place.enter(knocks)
    with scope("f_swap"):
        tokr[c] = jnp.broadcast_to(tok_ref[...], (SUB, tok))
        give_tok = place.send("tok", tokr.at[c], tokr.at[c], dc=1)
        give_chunk = place.send("chunk", shard_t.at[pl.ds((1 - c) * n_half, n_half)], chunk.at[c], dc=1)
        give_chunk.start()
        give_tok.start()
        chunk[c] = shard_t[pl.ds(c * n_half, n_half)]
        gain_sum = SmallSum(place, ("dc", "dy", "dz"), w_slots)
        own_w = jnp.concatenate([w_ref[...], jnp.zeros((1, width - cols), F32)], axis=1)
        gain_sum.start("dc", pltpu.roll(jnp.broadcast_to(own_w, (SUB, width)), place.f * cols, axis=1)[0:1])

    def p1_send(h, i):
        return place.send(("p1", h, i), chunk.at[h], loc(h, 0, 0), **ring1(h, WAYS[i]))

    def p1_fwd(h, i):
        ref = loc(h, FROM[i], 0, i * hh, hh)
        return place.send(("p1f", h, i), ref, ref, **ring1(h, WAYS[i]))

    def p2_send(h, k1, i):
        ref = loc(h, k1, 0, pair1=k1 == PAIR)
        return place.send(("p2", h, k1, i), chunk.at[h] if k1 == 0 else ref, ref, **ring2(h, WAYS[i]))

    def p2_fwd(h, k1, i):
        ref = loc(h, k1, FROM[i], i * hh, hh, pair1=k1 == PAIR)
        return place.send(("p2f", h, k1, i), ref, ref, **ring2(h, WAYS[i]))

    def keep(h):
        return place.local("keep", chunk.at[h], loc(h, 0, 0), h)

    def share(h, k2):
        ref = loc(h, ALL, k2, pair2=k2 == PAIR)
        return place.send(("share", h, k2), ref, ref, dc=1)

    def pass_first():
        with scope("f_p1"):
            for h in BOTH:
                for i in BOTH:
                    p1_send(h, i).wait_recv()
                    p1_fwd(h, i).start()
            for h in BOTH:
                start_all(p2_send(h, PAIR, i) for i in BOTH)

    def pass_first_far():
        with scope("f_p1f"):
            for h in BOTH:
                for i in BOTH:
                    p1_fwd(h, i).wait_recv()
                start_all(p2_send(h, FAR, j) for j in BOTH)

    def pass_second(k1):
        with scope("f_p2"):
            for h in BOTH:
                for i in BOTH:
                    p2_send(h, k1, i).wait_recv()
                    p2_fwd(h, k1, i).start()

    def end_second(k1):
        with scope("f_p2f"):
            for h in BOTH:
                for i in BOTH:
                    p2_fwd(h, k1, i).wait_recv()

    def share_group(k2):
        start_all(share(h, k2) for h in BOTH)

    with scope("f_chunk"):
        give_chunk.wait_recv()
        start_all(keep(h) for h in BOTH)
        gain_sum.start("dy", gain_sum.finish("dc"))
        for h in BOTH:
            start_all(p1_send(h, i) for i in BOTH)
        for h in BOTH:
            start_all(p2_send(h, 0, i) for i in BOTH)

    v_step = min(LANE, half_v)

    def hit_body(j, carry):
        off = j * v_step
        ids = lax.broadcasted_iota(I32, (v_step, tok), 0) + (row_start + c * half_v + off)
        for i, core in enumerate((c, 1 - c)):
            hit_t[span(off, v_step, v_step), pl.ds(i * tok, tok)] = jnp.where(ids == tokr[core, 0:1, :], 1.0, 0.0).astype(BF16)
        return carry

    def make_hits():
        with scope("f_hit"):
            give_tok.wait_recv()
            lax.fori_loop(0, half_v // v_step, hit_body, 0)

    n_step = min(512, tok)
    most = max(PIECES)

    def whole(u):
        return pl.ds(BASE[u], PIECES[u])

    def unit_copies(u):
        slot = u % 2
        for p, (h, (k1, k2)) in enumerate((h, k) for h in BOTH for k in UNITS[u]):
            yield place.local("lhs", loc(h, k1, k2), lhs.at[slot, p], slot * most + p, 2 * most)

    def load_unit(u):
        start_all(unit_copies(u))

    def look(u):
        pieces = PIECES[u]
        with scope("f_look"):
            if u > 1:
                x_swap(u - 2).wait_send()
            left = lhs.at[u % 2]
            for copy in unit_copies(u):
                copy.wait()
            per_core = tok // n_step

            def body(j, carry):
                value = jnp.concatenate([left[pl.ds(0, pieces), t].reshape(pieces * cols, vt) for t in range(n_half)], axis=1)
                rows = jnp.dot(value, hit_t[:, span(j * n_step, n_step)], preferred_element_type=F32)
                rows = rows.reshape(pieces, cols, n_step).astype(BF16)
                xw[u % 2, j // per_core, pl.ds(0, pieces), :, span(j % per_core * n_step, n_step)] = rows
                return carry

            lax.fori_loop(0, CORES * per_core, body, 0)
            x_swap(u).start()

    def x_swap(u):
        return place.send(("swap", u), xw.at[u % 2, 1, pl.ds(0, PIECES[u])], xr.at[whole(u)], dc=1)

    def lanes_of(k):
        return span((x + k) % n * quarter, quarter, quarter)

    def side(u, i):
        return pl.ds(BASE[u] + i * len(UNITS[u]), len(UNITS[u]))

    def x_far(u, i):
        return place.send(("xf", u, i), xp.at[side(u, i), :, lanes_of(FAR)], xf.at[side(u, i)], dx=WAYS[i])

    def x_near(u, i):
        return place.send(("xn", u, i), xp.at[whole(u), :, lanes_of(WAYS[i])], xg.at[i, whole(u)], dx=WAYS[i])

    def x_goal(k, sel):
        return x0_out.at[(x + k) % n, sel]

    def x_put(u, i):
        return place.send(("xp", u, i), xq.at[whole(u)], x_goal(0, whole(u)), dx=WAYS[i])

    last_unit = len(UNITS) - 1

    def x_keep(u):
        goal = x_goal(0, whole(u)) if u < last_unit else q5_out
        return place.local("x0", xq.at[whole(u)], goal, u, len(UNITS))

    def x_pass(u, i):
        ref = x_goal(FROM[i], side(u, i))
        return place.send(("xs", u, i), ref, ref, dx=WAYS[i])

    def x_first(u):
        with scope("f_x1"):
            x_swap(u).wait_recv()
            def body(p, carry):
                xp[BASE[u] + p] = xw[u % 2, 0, p] + xr[BASE[u] + p]
                return carry

            lax.fori_loop(0, PIECES[u], body, 0)
            start_all(x_far(u, i) for i in BOTH)

    def x_second(u):
        with scope("f_x2"):
            for i in BOTH:
                x_far(u, i).wait_recv()
                sel, lanes = side(u, i), lanes_of(WAYS[i])
                xp[sel, :, lanes] = xp[sel, :, lanes] + xf[sel]
                x_near(u, i).start()

    def x_third(u):
        with scope("f_x3"):
            for i in BOTH:
                x_near(u, i).wait_recv()
            sel = whole(u)
            xq[sel] = xp[sel, :, lanes_of(0)] + xg[0, sel] + xg[1, sel]
            if u < last_unit:
                start_all(x_put(u, i) for i in BOTH)
            x_keep(u).start()

    def x_fourth(u):
        with scope("f_x4"):
            for i in BOTH:
                x_put(u, i).wait_recv()
                x_pass(u, i).start()

    n_part = n * n * CORES // 2

    def moves(key, part, whole_t, other):
        sel = pl.ds(part * n_part, n_part)
        yield place.local(key, gl.at[sel], whole_t.at[sel], part)
        yield place.send((key, part), gl.at[sel], other.at[sel], dc=1)

    def move_g(part):
        return moves("g", part, gt_out, gpar_out)

    def move_xn(part):
        return moves("xt", part, xnt_out, xpar_out)

    def transpose_part(part, copies):
        block = width // dims["n_block"]
        first = part * dims["n_block"] // 2
        turned = [xn[:, pl.ds((first + j) * block, block)].T for j in range(dims["n_block"] // 2)]
        gl[pl.ds(part * n_part, n_part)] = jnp.concatenate(turned, axis=0).reshape(n_part, cols, tok)
        start_all(copies)

    def columns(row):
        return jnp.broadcast_to(row.astype(F32), (LANE, tok)).T.astype(I32)

    r_step = min(LANE, tok)

    def xn_body(j, carry):
        sel = span(j * r_step, r_step, r_step)
        h_wide = xn[sel].astype(F32)
        inv_rms = lax.rsqrt(jnp.sum(h_wide * h_wide, axis=1, keepdims=True) * (1.0 / width) + NORM_EPS)
        xn[sel] = (h_wide * inv_rms * gain_out[0:1]).astype(BF16)
        return carry

    e_step = min(LANE, tok)

    def tile_of(j):
        return (c * n_half + j) % n_tile

    def load_tile(j):
        return place.local("et", et_out.at[tile_of(j)], etb.at[j % 4], j % 4, 4)

    def save_u(i, odd):
        return place.local(("u", odd), (z_even, z_odd)[odd].at[i % 2], u_hbm.at[tile_of(2 * i + odd)], i % 2)

    def lane_blocks():
        return [(b, pl.ds(b, LANE)) for b in range(0, vt, LANE)]

    def post_tile(i, odd):
        base = tile_of(2 * i + odd) * vt
        buf, slot = (z_even, z_odd)[odd], i % 2

        def body(e, carry):
            sel = span(e * e_step, e_step, e_step)
            ids = lax.broadcasted_iota(I32, (e_step, LANE), 1) + base
            sum_e, sum_l = acc_e[sel], acc_l[sel]
            for b, lanes in lane_blocks():
                tanh_z = jnp.tanh(buf[slot, sel, lanes] * (1.0 / SOFT_CAP))
                buf[slot, sel, lanes] = tanh_z
                sum_e = sum_e + jnp.exp2(EXP_RATE * tanh_z - EXP_RATE)
                sum_l = sum_l + jnp.where(ids + b == labc[sel], tanh_z, 0.0)
            acc_e[sel] = sum_e
            acc_l[sel] = sum_l
            return carry

        lax.fori_loop(0, tok // e_step, body, 0)

    def dot_pair(i):
        for odd in BOTH:
            value = etb[(2 * i + odd) % 4].reshape(width, vt)
            (z_even, z_odd)[odd][i % 2] = jnp.dot(xn[...], value, preferred_element_type=F32)

    def load_pair(i):
        start_all(load_tile(2 * i + odd) for odd in BOTH)

    def pair(i, carry):
        for odd in BOTH:
            load_tile(2 * i + odd).wait()

        @pl.when(i > 1)
        def _():
            for odd in BOTH:
                save_u(i - 2, odd).wait()

        for odd in BOTH:
            post_tile(i - 1, odd)

            @pl.when(i < last)
            def _():
                save_u(i - 1, odd).start()

        dot_pair(i)

        @pl.when(i + 2 < n_tile // 2)
        def _():
            load_pair(i + 2)

        for k, work in enumerate(during):
            @pl.when(i == k + 1)
            def _():
                if k == 0:
                    wait_shares()
                perform(work)
        return carry

    def wait_shares():
        with scope("f_share"):
            for h in BOTH:
                for k2 in (0, PAIR, FAR):
                    share(h, k2).wait_recv()

    def logits_first():
        acc_e[...] = jnp.zeros_like(acc_e)
        acc_l[...] = jnp.zeros_like(acc_l)
        with scope("f_logits0"):
            far_ends(1)
            for odd in BOTH:
                load_tile(odd).wait()
            dot_pair(0)
            if n_tile // 2 > 2:
                load_pair(2)

    def load_first():
        for i in BOTH:
            load_pair(i)

    def put_small(i):
        src, dst = ((gain_out, gain_hbm), (loss_out, loss_hbm), (tokc_out, tokc_hbm))[i]
        return place.local(("out", i), src, dst, 0, 1)

    def lay_columns():
        with scope("f_cols"):
            labc[...] = columns(lab_ref[...] - row_start)
            for i, core in enumerate((c, 1 - c)):
                tokc_out[i] = columns(tokr[core, 0:1, :])
            put_small(2).start()

    def turn_g():
        with scope("f_gt"):
            load_g.wait()
            for part in BOTH:
                transpose_part(part, move_g(part))
            load_h.start()

    def gain_next():
        with scope("f_gain2"):
            gain_sum.start("dz", gain_sum.finish("dy"))

    def normalize():
        with scope("f_xn"):
            gain_out[...] = 1.0 + gain_sum.finish("dz")
            put_small(0).start()
            load_h.wait()
            lax.fori_loop(0, tok // r_step, xn_body, 0)

    def turn_xn():
        with scope("f_xt"):
            for part in BOTH:
                transpose_part(part, move_xn(part))

    spare = BASE[3]
    own_rows, their_rows = (pl.ds(spare + i * 2 * n, 2 * n) for i in BOTH)

    def far_loads(h):
        for i, (src, rows) in enumerate(((gt_out, own_rows), (gpar_out, their_rows))):
            if h == 0:
                yield place.local("far", src.at[pl.ds((z + FAR) % n * 2 * n, 2 * n)], xp.at[rows], i * n, 2 * n)
            else:
                for q in range(n):
                    piece = src.at[pl.ds((q * n + (y + FAR) % n) * 2, 2)]
                    yield place.local("far", piece, xp.at[pl.ds(spare + i * 2 * n + 2 * q, 2)], i * n + q)

    def far_load(h):
        if h == 0:
            for part in BOTH:
                for copy in move_g(part):
                    copy.wait()
        start_all(far_loads(h))

    def put_far(h, j):
        rows = pl.ds(0, 2 * n * cols)
        return place.local("lt", z_even.at[j % 2, rows], lt_out.at[h, :, span(j * vt, vt)], j % 2)

    def far_ends(h):
        for j in range(hh - 2, hh):
            put_far(h, j).wait()

    def far_look(h):
        def body(j, carry):
            @pl.when(j > 1)
            def _():
                put_far(h, j - 2).wait()

            left = jnp.concatenate([xp[rows].reshape(2 * n * cols, tok) for rows in (own_rows, their_rows)], axis=1)
            right = hit_t[span((h * hh + j) * vt, vt)]
            value = lax.dot_general(left, right, (((1,), (1,)), ((), ())), preferred_element_type=F32)
            z_even[j % 2, pl.ds(0, 2 * n * cols)] = value * dims["scale"]
            put_far(h, j).start()
            return carry

        with scope("f_far"):
            for copy in far_loads(h):
                copy.wait()
            if h:
                far_ends(0)
            lax.fori_loop(0, hh, body, 0)

    def begin_unit(u):
        if u == 0:
            for h in BOTH:
                keep(h).wait()
        load_unit(u)

    load_h = place.local("h", h_hbm, xn)
    works = {
        "HIT": make_hits, "GT": turn_g, "COL": lay_columns, "G2": gain_next, "XN": normalize, "XT": turn_xn, "LP": load_first, "L0": logits_first,
        "PF": pass_first, "PFF": pass_first_far,
    }
    groups = {"0": 0, "P": PAIR, "F": FAR}
    families = {"LF": far_load, "FL": far_look, "LU": begin_unit, "LK": look, "X1": x_first, "X2": x_second, "X3": x_third, "X4": x_fourth}
    families_k = {"SH": share_group, "S": pass_second, "E": end_second}

    def perform(text):
        for word in text.split():
            if word in works:
                works[word]()
            elif word[:-1] in families:
                families[word[:-1]](int(word[-1]))
            else:
                families_k[word[:-1]](groups[word[-1]])

    during = (
        "X24",
        "X15 X33",
        "",
        "X34",
        "X42",
        "X43",
        "",
    )
    for text in (
        "HIT LU0 LK0 G2", "GT X10 PF LU1", "LK1 LF0 S0 X20", "X11 FL0 PFF X21", "LU2 LF1 X30 LK2",
        "FL1 XN SP SH0", "E0 LU3 X12 X31", "LK3 SF LU4 X22", "X40 SHP LK4 X13", "EP X32 X41 EF",
        "LU5 SHF LP XT", "COL L0 X14 LK5", "X23",
    ):
        perform(text)
    if n_half < 4:
        wait_shares()
        for text in during:
            perform(text)
        during = ()
    last = n_tile // 2 - 1
    with scope("f_logits"):
        lax.fori_loop(1, last + 1, pair, 0)
        for odd in BOTH:
            post_tile(last, odd)

    with scope("f_stats"):
        row = lax.broadcasted_iota(I32, (2, tok), 0)
        sum_e = jnp.sum(acc_e[...].T, axis=0, keepdims=True)
        sum_l = SOFT_CAP * jnp.sum(acc_l[...].T, axis=0, keepdims=True)
        stats = SmallSum(place, ("dx",), s_slots)
        stats.start("dx", jnp.where(row == 0, sum_e, sum_l))
    perform("X25 X44")
    with scope("f_stats2"):
        stat = stats.finish("dx")
        all_e, all_l = stat[0:1], stat[1:2]
        inv_s[...] = jnp.broadcast_to((1.0 / dims["total"]) / all_e, (LANE, tok)).T
        s_slots[0, 0:1, :] = jnp.log(all_e) + SOFT_CAP - all_l
        own = s_slots[0, 0:1, lanes_of(0)]
        part_w = min(LANE, quarter)
        folded = own[:, 0:part_w]
        for j in range(part_w, quarter, part_w):
            folded = folded + own[:, j:j + part_w]
        loss_out[...] = jnp.where(lax.broadcasted_iota(I32, (SUB, part_w), 0) == 0, folded, 0.0)
        put_small(1).start()

    def dz_tile(j):
        return ((1 - c) * n_half + j) % n_tile

    def load_u(i, odd):
        return place.local(("u", odd), u_hbm.at[dz_tile(2 * i + odd)], (z_even, z_odd)[odd].at[i % 2], i % 2)

    def put_dz(i, odd):
        return place.local(("dz", odd), dzb.at[odd, i % 2], dz_out.at[dz_tile(2 * i + odd)], i % 2)

    def give_dz(part):
        src = dz_out.at[pl.ds((1 - c) * n_half + part * hh, hh)]
        return place.send(("dz", part), src, dzpar_out.at[pl.ds(part * hh, hh)], dc=1)

    d_step = min(256, tok)

    def dz_rows(i, odd):
        base = dz_tile(2 * i + odd) * vt
        buf, slot = (z_even, z_odd)[odd], i % 2

        def body(e, carry):
            sel = span(e * d_step, d_step, d_step)
            ids = lax.broadcasted_iota(I32, (d_step, LANE), 1) + base
            for b, lanes in lane_blocks():
                tanh_z = buf[slot, sel, lanes]
                prob = jnp.exp2(EXP_RATE * tanh_z - EXP_RATE) * inv_s[sel]
                prob = jnp.where(ids + b == labc[sel], prob - 1.0 / dims["total"], prob)
                dzb[odd, slot, sel, lanes] = (prob * (1.0 - tanh_z * tanh_z)).astype(BF16)
            return carry

        lax.fori_loop(0, tok // d_step, body, 0)

    def dz_pair(i, loaded, follow):
        for odd in BOTH:
            if loaded:
                load_u(i, odd).wait()

            @pl.when(i > hh + 1)
            def _():
                put_dz(i - 2, odd).wait()

            dz_rows(i, odd)
            put_dz(i, odd).start()

            @pl.when(i + follow < n_tile // 2)
            def _():
                load_u(i + follow, odd).start()

    def dz_run(lo, hi, loaded, follow):
        def body(i, carry):
            dz_pair(i, loaded, follow)
            return carry

        lax.fori_loop(lo, hi, body, 0)

    with scope("f_dz"):
        half = hh // 2
        for part in (1, 0):
            dz_run(part * half, (part + 1) * half, not part, hh if part == 0 else -half)
            for i in range(part * half, (part + 1) * half):
                for odd in BOTH:
                    put_dz(i, odd).wait()
            give_dz(part).start()
        dz_run(hh, n_tile // 2, True, half)

    perform("X35")
    with scope("f_end"):
        for i in range(3):
            put_small(i).wait()
        for part in BOTH:
            give_dz(part).wait()
        for i in range(n_tile // 2 - 2, n_tile // 2):
            for odd in BOTH:
                put_dz(i, odd).wait()
        give_tok.wait_send()
        give_chunk.wait_send()
        for h in BOTH:
            for i in BOTH:
                p1_send(h, i).wait_send()
                p1_fwd(h, i).wait_send()
                for k in (0, PAIR, FAR):
                    p2_send(h, k, i).wait_send()
                    p2_fwd(h, k, i).wait_send()
            for k in (0, PAIR, FAR):
                share(h, k).wait_send()
        for part in BOTH:
            for copy in move_xn(part):
                copy.wait()
        for u in range(len(UNITS)):
            if u > len(UNITS) - 3:
                x_swap(u).wait_send()
            x_keep(u).wait()
            for i in BOTH:
                x_far(u, i).wait_send()
                x_near(u, i).wait_send()
                if u < last_unit:
                    x_put(u, i).wait_send()
                    x_pass(u, i).wait()
    assert (place.n_link, place.n_local) <= dims["front_sems"], (place.n_link, place.n_local)


def specs(n_vmem, n_any):
    return [pl.BlockSpec(memory_space=pltpu.VMEM)] * n_vmem + [pl.BlockSpec(memory_space=pl.ANY)] * n_any


def shapes(items):
    return tuple(jax.ShapeDtypeStruct(*item) for item in items)


def scratch(items, n_link, n_local):
    dma = pltpu.SemaphoreType.DMA
    return [pltpu.VMEM(*item) for item in items] + [dma((n_link,)), dma((n_link,)), dma((n_local,))]


def params(collective_id, limit):
    return pltpu.CompilerParams(collective_id=collective_id, has_side_effects=True, vmem_limit_bytes=limit)


def front(dims, limit, shard, tok_row, lab_row, w, h, g):
    n, tok, vocab, width, vt = dims["n"], dims["tok"], dims["vocab"], dims["width"], dims["vt"]
    cols = shard.shape[0]
    half_v = vocab // CORES
    quarter = tok // n
    n_tile, n_half, most = vocab // vt, half_v // vt, max(PIECES)
    pieces = n * n * CORES
    grid = (n // 2, 2, n // 2, 2)
    return pl.pallas_call(
        functools.partial(front_kernel, dims),
        name="front",
        out_shape=shapes([
            ((n_tile, *grid, CORES, cols, vt), BF16), *[((pieces, cols, tok), BF16)] * 4, ((2, 2 * n * cols, half_v // 2), F32), ((n_tile, tok, vt), BF16),
            ((n_half, tok, vt), BF16), ((n, BASE[-1], cols, quarter), BF16), ((PIECES[-1], cols, quarter), BF16), ((n_tile, tok, vt), F32),
            ((1, width), F32), ((SUB, min(LANE, quarter)), F32), ((CORES, tok, LANE), I32),
        ]),
        in_specs=specs(0, 6),
        out_specs=tuple(specs(0, 14)),
        scratch_shapes=scratch([
            (shard.shape, F32), (tok_row.shape, I32), (lab_row.shape, I32), (w.shape, F32), ((1, width), F32),
            ((SUB, min(LANE, quarter)), F32), ((CORES, tok, LANE), I32),
            ((n_tile, cols, vt), BF16), ((CORES, n_half, cols, vt), BF16), ((CORES, SUB, tok), I32), ((half_v, CORES * tok), BF16),
            ((2, most, n_half, cols, vt), BF16), ((pieces, cols, tok), BF16), ((2, CORES, most, cols, tok), BF16), ((pieces, cols, tok), BF16),
            ((pieces, cols, quarter), BF16), ((2, pieces, cols, quarter), BF16), ((pieces, cols, quarter), BF16),
            ((4, *grid, CORES, cols, vt), BF16), ((tok, width), BF16), ((pieces, cols, tok), BF16),
            ((2, tok, vt), F32), ((2, tok, vt), F32), ((2, 2, tok, vt), BF16), ((tok, LANE), F32), ((tok, LANE), F32), ((tok, LANE), F32),
            ((tok, LANE), I32), ((2 * n + CORES, 1, width), F32), ((n, 2, tok), F32),
        ], dims["front_sems"][0], dims["front_sems"][1]),
        compiler_params=params(0, limit),
    )(shard, tok_row, lab_row, w, h, g)


def back_kernel(
    dims,
    gain_hbm, loss_hbm, tokc_hbm, lt_hbm, dz_hbm, dzp_hbm, et_hbm, xnt_hbm, xpar_hbm, gt_hbm, gpar_hbm, h_hbm, q5_hbm,
    tail_hbm, dh_out, de_out, x0_out, ra_hbm, rx_hbm,
    gain_ref, loss_ref, tokc, tail_out, q5, dz_own, dz_par, et_buf, part, fx, acc, fa, f2, r2, xb, h_buf, dh_buf, dg_acc, slots,
    sends, recvs, local_sems,
):
    n, tok, vocab, width, tile, vt = (dims[k] for k in ("n", "tok", "vocab", "width", "tile", "vt"))
    place = Place(n, sends, recvs, local_sems)
    x, z, y, c = place.x, place.z, place.y, place.c
    half_v = vocab // CORES
    n_tile, n_half = vocab // vt, half_v // vt
    lanes = half_v // 2
    rows = width // (n * n)
    half_rows = rows // 2
    quarter = tok // n
    hq = quarter // 2
    tiles = dims["tiles"]
    chunks = len(tiles)
    edges = [sum(tiles[:d]) for d in range(chunks + 1)]
    per_half = n_half // 2

    knocks = place.knock()
    load_q5 = place.local("q5", q5_hbm, q5)
    load_q5.start()
    load_h = place.local("h", h_hbm.at[span(x * quarter, quarter, quarter)], h_buf)

    def load_et(t, slot):
        return place.local("et", et_hbm.at[:, span(t * tile, tile, tile)], et_buf.at[slot], slot)

    slot_of = {FAR: 0, 1: 1, 3: 2, 0: 0}
    stages = dims["stages"]

    def load_stage(m, i):
        half, k, kind = stages[m]
        src = ((gt_hbm, gpar_hbm), (xnt_hbm, xpar_hbm))[kind][i]
        src = src.at[(z + k) % n] if half == 0 else src.at[:, (y + k) % n]
        return place.local(("xb", i), src, xb.at[m % 2, i], m % 2)

    def start_stage(m):
        if m < len(stages):
            start_all(load_stage(m, i) for i in BOTH)

    loads = [place.local("dz", dz_hbm, dz_own), place.local("dzp", dzp_hbm, dz_par)]
    load_et(0, 0).start()
    start_all(loads)
    keep_q5 = place.local("q5", q5, x0_out.at[x], 1)

    def y_put(i):
        return place.send(("yp", i), q5, x0_out.at[x], dx=WAYS[i])

    def y_pass(i):
        size = q5.shape[0] // 2
        ref = x0_out.at[(x + FROM[i]) % n, pl.ds(i * size, size)]
        return place.send(("yq", i), ref, ref, dx=WAYS[i])

    def y_passes():
        for i in BOTH:
            y_put(i).wait_recv()
            y_pass(i).start()

    small_loads = [
        place.local(("in", i), src, dst, 0, 1)
        for i, (src, dst) in enumerate(((tokc_hbm, tokc), (gain_hbm, gain_ref), (loss_hbm, loss_ref)))
    ]
    fars = [place.local("lt", lt_hbm.at[half], acc.at[half, 0], half) for half in BOTH]
    start_all(fars + small_loads)
    for m in BOTH:
        start_stage(m)
    load_h.start()

    def columns(d):
        return pl.ds(edges[d] * tile, tiles[d] * tile)

    def dxn_chunk(d):
        def body(t, carry):
            slot = t % 2

            @pl.when(t + 1 < edges[chunks])
            def _():
                load_et(t + 1, 1 - slot).start()

            load_et(t, slot).wait()
            left = jnp.concatenate([dz_own[j] for j in range(n_tile)], axis=1)
            right = jnp.concatenate([et_buf[slot, j] for j in range(n_tile)], axis=1)
            part[:, span(t * tile, tile, tile)] = lax.dot_general(
                left, right, (((1,), (1,)), ((), ())), preferred_element_type=F32)
            return carry

        with scope("b_dxn"):
            lax.fori_loop(edges[d], edges[d + 1], body, 0)

    def qrow(k, lo=0, size=hq):
        return span((x + k) % n * quarter + lo, size, SUB)

    def x_far(d, i):
        return place.send(("xf", d, i), part.at[qrow(FAR, i * hq), columns(d)], fx.at[i, :, columns(d)], dx=WAYS[i])

    def x_near(d, i, j):
        src = part.at[qrow(WAYS[i], j * hq), columns(d)]
        return place.send(("xn", d, i, j), src, rx_hbm.at[i, pl.ds(j * hq, hq), columns(d)], dx=WAYS[i])

    def x_first(d):
        start_all(x_far(d, i) for i in BOTH)

    def x_second(d):
        with scope("b_x2"):
            for i in BOTH:
                x_far(d, i).wait_recv()
                sel = qrow(WAYS[i], i * hq)
                part[sel, columns(d)] = part[sel, columns(d)] + fx[i, :, columns(d)]
                start_all(x_near(d, i, j) for j in BOTH)

    def stage_x(d, j, i):
        return place.local("sx", rx_hbm.at[i, pl.ds(j * hq, hq), columns(d)], fx.at[i, :, columns(d)], i)

    def x_third(d, j):
        with scope("b_x3"):
            for i in BOTH:
                x_near(d, i, j).wait_recv()
                stage_x(d, j, i).start()
            for i in BOTH:
                stage_x(d, j, i).wait()
            sel = qrow(0, j * hq)
            part[sel, columns(d)] = part[sel, columns(d)] + fx[0, :, columns(d)] + fx[1, :, columns(d)]

    def de_stage(half, k, kind):
        m = stages.index((half, k, kind))
        slot = slot_of[k]

        wide = min(2, per_half) if kind and k else 1

        def right(i, t):
            if kind:
                return dz_par[t] if i else dz_own[c * n_half + t]
            ids = lax.broadcasted_iota(I32, (tok, LANE), 1) + (x * vocab + c * half_v + t * vt)
            hits = [jnp.where(tokc[i] == ids + b, dims["scale"], 0.0).astype(BF16) for b in range(0, vt, LANE)]
            return jnp.concatenate(hits, axis=1)

        def body(j, carry):
            t = half * per_half + j * wide
            sel = span(j * wide * vt, wide * vt)
            left = jnp.concatenate([xb[m % 2, i].reshape(n * rows, tok) for i in BOTH], axis=1)
            both_right = [jnp.concatenate([right(i, t + q) for i in BOTH], axis=0) for q in range(wide)]
            total = jnp.dot(left, jnp.concatenate(both_right, axis=1), preferred_element_type=F32)
            total = total.reshape(n, rows, wide * vt)
            acc[half, slot, :, :, sel] = acc[half, slot, :, :, sel] + total if kind else total
            return carry

        with scope("b_de" if kind else "b_look"):
            for i in BOTH:
                load_stage(m, i).wait()
            lax.fori_loop(0, per_half // wide, body, 0)
            start_stage(m + 2)

    def de_unit(half, k):
        if k == FAR:
            fars[half].wait()
        else:
            de_stage(half, k, 0)
        de_stage(half, k, 1)

    def ring(half, k):
        return {"dz": k} if half == 0 else {"dy": k}

    def cross(half, k):
        return {"dy": k} if half == 0 else {"dz": k}

    def a_far(half, i):
        return place.send(("af", half, i), acc.at[half, 0, pl.ds(2 * i, 2)], fa.at[half, i], **ring(half, WAYS[i]))

    def a_near(half, i, j):
        sel = pl.ds(2 * j, 2)
        return place.send(("an", half, i, j), acc.at[half, 1 + i, sel], ra_hbm.at[half, i, sel], **ring(half, WAYS[i]))

    def a_first(half):
        start_all(a_far(half, i) for i in BOTH)

    def a_second(half, i):
        with scope("b_a2"):
            a_far(half, i).wait_recv()
            sel = pl.ds(2 * i, 2)
            acc[half, 1 + i, sel] = acc[half, 1 + i, sel] + fa[half, i]
            start_all(a_near(half, i, j) for j in BOTH)

    def stage_a(half, j, i):
        return place.local(("sa", half), ra_hbm.at[half, i, pl.ds(2 * j, 2)], fa.at[half, i], i)

    def piece(half, k):
        return ((y if half == 0 else z) + k) % n

    def c_far(half, i):
        src = acc.at[half, 0, piece(half, FAR), pl.ds(i * half_rows, half_rows)]
        return place.send(("cf", half, i), src, f2.at[half, i], **cross(half, WAYS[i]))

    def c_near(half, i):
        return place.send(("cn", half, i), acc.at[half, 0, piece(half, WAYS[i])], r2.at[half, i], **cross(half, WAYS[i]))

    def a_third(half, j):
        with scope("b_a3"):
            for i in BOTH:
                a_near(half, i, j).wait_recv()
                stage_a(half, j, i).start()
            for i in BOTH:
                stage_a(half, j, i).wait()
            sel = pl.ds(2 * j, 2)
            acc[half, 0, sel] = acc[half, 0, sel] + fa[half, 0] + fa[half, 1]

    def c_first(half):
        start_all(c_far(half, i) for i in BOTH)

    def c_second(half):
        with scope("b_c2"):
            for i in BOTH:
                c_far(half, i).wait_recv()
                at = piece(half, WAYS[i])
                sel = pl.ds(i * half_rows, half_rows)
                acc[half, 0, at, sel] = acc[half, 0, at, sel] + f2[half, i]
                c_near(half, i).start()

    def out_copies(half):
        sel = span(c * half_v + half * lanes, lanes)
        mine = acc.at[half, 0, piece(half, 0)]
        yield place.local("de", mine.at[span(c * half_rows, half_rows, SUB)], de_out.at[:, sel], half)
        yield place.send(("de", half), mine.at[span((1 - c) * half_rows, half_rows, SUB)], de_out.at[:, sel], dc=1)

    def c_third(half):
        with scope("b_c3"):
            for i in BOTH:
                c_near(half, i).wait_recv()
            at = piece(half, 0)
            acc[half, 0, at] = acc[half, 0, at] + r2[half, 0] + r2[half, 1]
            start_all(out_copies(half))

    step = min(32, hq)

    def dh_body(i, carry):
        sel = span(i * step, step, step)
        row = span(x * quarter + i * step, step, step)
        d_x = part[row]
        h_wide = h_buf[sel].astype(F32)
        inv_rms = lax.rsqrt(jnp.sum(h_wide * h_wide, axis=1, keepdims=True) * (1.0 / width) + NORM_EPS)
        h_norm = h_wide * inv_rms
        g_dir = d_x * gain_ref[0:1]
        mean = jnp.sum(g_dir * h_norm, axis=1, keepdims=True) * (1.0 / width)
        dh_buf[sel] = (inv_rms * (g_dir - h_norm * mean)).astype(BF16)
        prod = d_x * h_norm
        total = prod[0:SUB]
        for j in range(SUB, step, SUB):
            total = total + prod[j:j + SUB]
        dg_acc[...] = dg_acc[...] + total
        return carry

    def h_first(i, j):
        return place.send(("hf", i, j), dh_buf.at[pl.ds(j * hq, hq)], dh_out.at[qrow(0, j * hq)], dx=WAYS[i])

    def h_second(i):
        ref = dh_out.at[qrow(FROM[i], i * hq)]
        return place.send(("hs", i), ref, ref, dx=WAYS[i])

    keep_dh = place.local("dh", dh_buf, dh_out.at[qrow(0, 0, quarter)])
    small = SmallSum(place, ("dc", "dx", "dy", "dz"), slots)
    per_j = hq // step

    def dh_part(j):
        with scope("b_dh"):
            if j == 0:
                load_h.wait()
            lax.fori_loop(j * per_j, (j + 1) * per_j, dh_body, 0)
            start_all(h_first(i, j) for i in BOTH)
            if j:
                keep_dh.start()

    def h_pass(i):
        with scope("b_h2"):
            h_first(i, i).wait_recv()
            h_second(i).start()

    put_tail = place.local("tail", tail_out, tail_hbm, 0, 1)

    def small_step(k):
        dims_of = small.dims
        with scope("b_s"):
            if k == 1:
                sums = [jnp.sum(part_sum, axis=0, keepdims=True) for part_sum in (dg_acc[...], loss_ref[...])]
                small.start(dims_of[0], jnp.concatenate(sums, axis=1))
            elif k <= len(dims_of):
                small.start(dims_of[k - 1], small.finish(dims_of[k - 2]))
            else:
                total = small.finish(dims_of[-1])
                loss = jnp.sum(total[:, width:], axis=1, keepdims=True) * (1.0 / dims["total"])
                tail_out[...] = jnp.concatenate([total[:, 0:width], jnp.broadcast_to(loss, (1, LANE))], axis=1)
                put_tail.start()

    def dxn(d):
        dxn_chunk(d)
        x_first(d)

    def unit(half, k):
        if k == 0:
            with scope("b_wait_far"):
                for i in BOTH:
                    a_far(half, i).wait_send()
        while len(loads) > 1:
            loads.pop().wait()
            for copy in small_loads:
                copy.wait()
        de_unit(half, k)
        if k == FAR:
            a_first(half)

    families = {
        "CH": dxn, "XS": x_second, "UN": unit, "AS": a_second, "XT": x_third, "AT": a_third, "CF": c_first, "CS": c_second,
        "CT": c_third, "DH": dh_part, "SM": small_step, "HP": h_pass, "YQ": y_passes,
    }

    def perform(text):
        for word in text.split():
            families[word[:2]](*(int(digit) for digit in word[2:]))

    with scope("b_enter"):
        place.enter(knocks)
    with scope("b_load"):
        load_q5.wait()
        start_all(y_put(i) for i in BOTH)
        keep_q5.start()
        loads[0].wait()
        dg_acc[...] = jnp.zeros_like(dg_acc)
    for text in (
        "CH0 UN02 YQ CH1", "UN12 CH2 UN03 XS1", "UN01 XS2 UN13 AS01", "AS00 UN11 AS11 AS10",
        "XS0 CH3 XT10 CH4", "UN00 XT00 XS3 XT01", "XS4 UN10 XT20 AT00", "XT30 XT21 XT11 XT40",
        "DH0 XT31 XT41 DH1", "AT01 AT10 CF0 SM1", "AT11 CF1 SM2 HP0", "CS0 CS1 SM3 HP1", "CT0 SM4 CT1 SM5",
    ):
        perform(text)

    with scope("b_end_x"):
        put_tail.wait()
        keep_dh.wait()
        keep_q5.wait()
        for i in BOTH:
            y_put(i).wait_send()
            y_pass(i).wait()
            for d in range(chunks):
                x_far(d, i).wait_send()
                for j in BOTH:
                    x_near(d, i, j).wait_send()
            h_first(i, i).wait_send()
            h_first(i, 1 - i).wait()
            h_second(i).wait()
    with scope("b_end_a"):
        for half in BOTH:
            for i in BOTH:
                for j in BOTH:
                    a_near(half, i, j).wait_send()
                c_far(half, i).wait_send()
                c_near(half, i).wait_send()
            for copy in out_copies(half):
                copy.wait()
    assert (place.n_link, place.n_local) <= dims["back_sems"], (place.n_link, place.n_local)


def back(dims, limit, gain, loss, tokc, far, dz, dzp, et, xnt, xpar, gt, gpar, h, q5):
    n, tok, vocab, width, tile = (dims[k] for k in ("n", "tok", "vocab", "width", "tile"))
    rows = width // (n * n)
    half_v = vocab // CORES
    lanes = half_v // 2
    quarter = tok // n
    hq = quarter // 2
    tail_w = width + loss.shape[1]
    n_tile, n_half, vt = dz.shape[0], dzp.shape[0], dims["vt"]
    turned = [a.reshape(n, n, rows, tok) for a in (xnt, xpar, gt, gpar)]
    return pl.pallas_call(
        functools.partial(back_kernel, dims),
        name="back",
        out_shape=shapes([
            ((1, width + LANE), F32), ((tok, width), BF16), ((rows // CORES, vocab), F32), ((n, *q5.shape), BF16),
            ((2, 2, n, rows, lanes), F32),
            ((2, quarter, width), F32),
        ]),
        in_specs=specs(0, 13),
        out_specs=tuple(specs(0, 6)),
        scratch_shapes=scratch([
            (gain.shape, F32), (loss.shape, F32), (tokc.shape, I32), ((1, width + LANE), F32),
            (q5.shape, BF16), ((n_tile, tok, vt), BF16), ((n_half, tok, vt), BF16), ((2, n_tile, tile, vt), BF16), ((tok, width), F32),
            ((2, hq, width), F32), ((2, 3, n, rows, lanes), F32), ((2, 2, 2, rows, lanes), F32),
            ((2, 2, rows // 2, lanes), F32), ((2, 2, rows, lanes), F32), ((2, CORES, n, rows, tok), BF16), ((quarter, width), BF16),
            ((quarter, width), BF16), ((SUB, width), F32), ((3 * n + CORES, 1, tail_w), F32),
        ], dims["back_sems"][0], dims["back_sems"][1]),
        compiler_params=params(1, limit),
    )(gain, loss, tokc, far.reshape(2, n, rows, lanes), dz, dzp, et.reshape(n_tile, width, vt), *turned, h, q5)[:4]


def finish_kernel(
    n, scale, table_ref, tail_hbm, x0_hbm, x5_hbm, dh_hbm, de_hbm, dg_hbm, loss_hbm, x0_out, dh_out, de_out,
    tail_ref, dg_out, loss_out, x0_in, x0_buf, rows_ref, dh_buf, de_buf, sems,
):
    place = Place(n, None, None, sems)
    quarter, cols, width = x0_in.shape[3], x0_in.shape[2], x0_buf.shape[2]

    def step(q):
        rows = span(q * quarter, quarter, quarter)
        return (
            place.local("x0", x0_hbm.at[q], x0_in.at[q, pl.ds(0, BASE[-1])], q, n),
            place.local("x5", x5_hbm.at[q], x0_in.at[q, pl.ds(BASE[-1], PIECES[-1])], q, n), place.local("x0o", x0_buf.at[q], x0_out.at[rows], q, n),
            place.local("dh", dh_hbm.at[rows], dh_buf.at[q], q, n), place.local("dho", dh_buf.at[q], dh_out.at[rows], q, n),
        )

    moves = [step(q) for q in range(n)]
    de_in, de_put = place.local("de", de_hbm, de_buf, 0), place.local("de", de_buf, de_out, 1)
    for x0_load, x5_load, _, dh_load, _ in moves:
        start_all((x0_load, x5_load, dh_load))
    de_in.start()
    tail_in = place.local("tail", tail_hbm, tail_ref)
    small_puts = [place.local("dg", dg_out, dg_hbm), place.local("loss", loss_out, loss_hbm)]
    tail_in.start()
    tail_in.wait()
    gain = jnp.broadcast_to(tail_ref[:, 0:width], (SUB, width))
    dg_out[...] = pltpu.roll(gain, width - place.f * cols, axis=1)[0:1, 0:cols]
    loss_out[...] = tail_ref[:, width:width + 1]
    start_all(small_puts)

    def body(q, carry):
        x0_load, x5_load, x0_put, dh_load, dh_put = step(q)
        x0_load.wait()
        x5_load.wait()
        for zi in range(n):
            for yi in range(n):
                for h in BOTH:
                    dz, dy = (zi - place.z) % n, (yi - place.y) % n
                    k1, k2 = (dy, dz) if h == 0 else (dz, dy)
                    piece = table_ref[(h * n + k1) * n + k2]
                    rows_ref[pl.ds(((zi * n + yi) * CORES + h) * cols, cols)] = x0_in[q, piece]
        x0_buf[q] = (rows_ref[...].T.astype(F32) * scale).astype(BF16)
        x0_put.start()
        dh_load.wait()
        dh_put.start()
        return carry

    lax.fori_loop(0, n, body, 0)
    de_in.wait()
    de_put.start()
    for _, _, x0_put, _, dh_put in moves:
        x0_put.wait()
        dh_put.wait()
    de_put.wait()
    for copy in small_puts:
        copy.wait()


def finish(n, scale, limit, tail, x0, x5, dh, de):
    cols, quarter = x0.shape[2:]
    pieces = n * n * CORES
    width = pieces * cols
    table = np.zeros((CORES, n, n), np.int32)
    for u, unit in enumerate(UNITS):
        for h in BOTH:
            for i, (k1, k2) in enumerate(unit):
                table[h, k1, k2] = BASE[u] + h * len(unit) + i
    return pl.pallas_call(
        functools.partial(finish_kernel, n, scale),
        name="finish",
        in_specs=[pl.BlockSpec(memory_space=pltpu.SMEM)] + specs(0, 5),
        out_specs=tuple(specs(0, 5)),
        out_shape=shapes([((1, cols), F32), ((1, 1), F32), (dh.shape, BF16), (dh.shape, BF16), (de.shape, F32)]),
        scratch_shapes=[
            pltpu.VMEM(tail.shape, F32), pltpu.VMEM((1, cols), F32), pltpu.VMEM((1, 1), F32),
            pltpu.VMEM((n, pieces, cols, quarter), BF16), pltpu.VMEM((n, quarter, width), BF16), pltpu.VMEM((width, quarter), BF16),
            pltpu.VMEM((n, quarter, width), BF16), pltpu.VMEM(de.shape, F32), pltpu.SemaphoreType.DMA((7 * n,)),
        ],
        compiler_params=pltpu.CompilerParams(vmem_limit_bytes=limit),
    )(jnp.asarray(table.reshape(-1)), tail, x0, x5, dh, de)


def solution(mesh):
    return build(mesh, mesh.shape["tp"], 256, digits("12222")[0], 256, 6, 67_000_000)


def build(mesh, n, tile, tiles, vt, n_block, limit):
    fsdp_size = mesh.shape["fsdp"]

    def device_step(emb_shard, tok_ids, lab_ids, h_last, g_embed, norm_w):
        vocab_rows, cols = emb_shard.shape
        batch_loc, seq_len, width = h_last.shape
        tok_count = batch_loc * seq_len
        fsdp_id = lax.axis_index("fsdp")
        scale = float(np.asarray(math.sqrt(width)).astype(jnp.bfloat16))
        dims = {
            "n": n, "tok": tok_count, "vocab": vocab_rows, "width": width, "total": tok_count * fsdp_size, "vt": vt,
            "tile": tile, "tiles": tiles, "scale": scale, "n_block": n_block,
            "stages": digits("021 121 030 031") + digits("010 011 130 131") + digits("110 111 000 001") + digits("100 101"),
            "front_sems": (106, 59), "back_sems": (72, 30),
        }
        h_flat = h_last.reshape(tok_count, width)
        placed = lax.dynamic_update_slice(jnp.zeros((SUB, width), F32), jnp.broadcast_to(norm_w, (SUB, cols)), (0, fsdp_id * cols))
        ids = [a.reshape(1, tok_count) for a in (tok_ids, lab_ids)]
        table, xn_t, xpar_t, g_t, gpar_t, far, dz, dzp, x0, q5, _, gain, loss_part, tokc = front(
            dims, limit, emb_shard.T, *ids, norm_w.reshape(1, cols), h_flat, g_embed.reshape(tok_count, width))
        tail, d_hidden, d_cols, x5 = back(dims, limit, gain, loss_part, tokc, far, dz, dzp, table, xn_t, xpar_t, g_t, gpar_t, h_flat, q5)
        d_norm_w, loss, x_emb, d_hidden, d_cols = finish(n, scale, limit, tail, x0, x5, d_hidden, d_cols)
        return (x_emb.reshape(h_last.shape), loss.reshape(()), d_hidden.reshape(h_last.shape), d_norm_w.reshape(cols), d_cols.T)

    spec_tok = P("fsdp", None)
    spec_act = P("fsdp", None, None)
    return jax.shard_map(device_step, mesh=mesh, in_specs=(P("tp", "fsdp"), spec_tok, spec_tok, spec_act, spec_act, P("fsdp")), out_specs=(spec_act, P(), spec_act, P("fsdp"), P("tp", "fsdp")), check_vma=False)
```

```python
import functools
import math
import jax
import numpy as np
import jax.numpy as jnp
from jax import lax
from jax.experimental import pallas as pl
from jax.experimental.pallas import tpu as pltpu
from jax.sharding import PartitionSpec as P

SOFT_CAP = 30.0
NORM_EPS = 1e-6
F32, BF16, I32 = jnp.float32, jnp.bfloat16, jnp.int32
LANE, SUB = 128, 8
BOTH = (0, 1)
FOUR = range(4)
WAYS = (1, 3)
FROM = (3, 1)
FAR = 2
CORES = 2


def span(start, size, unit=LANE):
    return pl.ds(pl.multiple_of(start, unit), size)


class Place:
    def __init__(self, n, sends, recvs, local_sems):
        self.n, self.sends, self.recvs, self.local_sems = n, sends, recvs, local_sems
        self.x = lax.axis_index("tp")
        f = lax.axis_index("fsdp")
        self.f = f
        self.c = f % CORES
        self.y = f // CORES % n
        self.z = f // CORES // n
        self.link_of, self.local_of, self.n_link, self.n_local = {}, {}, 0, 0
        self.size = {"dx": n, "dz": n, "dy": n, "dc": CORES}
        self.me = {"dx": self.x, "dz": self.z, "dy": self.y, "dc": self.c}

    def at(self, dx=0, dz=0, dy=0, dc=0):
        n = self.n
        z, y, c = (self.z + dz) % n, (self.y + dy) % n, (self.c + dc) % CORES
        return ((self.x + dx) % n, (z * n + y) * CORES + c)

    def knock(self):
        peers = [self.at(**{d: k}) for d in self.size for k in range(1, self.size[d])]
        for peer in peers:
            pl.semaphore_signal(pltpu.get_barrier_semaphore(), inc=1, device_id=peer, device_id_type=pl.DeviceIdType.MESH)
        return len(peers)

    def enter(self, knocks):
        pl.semaphore_wait(pltpu.get_barrier_semaphore(), knocks)

    def link(self, key, count=1):
        if key not in self.link_of:
            self.link_of[key] = self.n_link
            self.n_link += count
        return self.link_of[key]

    def send(self, key, src, dst, **step):
        i = self.link(key)
        return pltpu.make_async_remote_copy(
            src, dst, self.sends.at[i], self.recvs.at[i], device_id=self.at(**step), device_id_type=pl.DeviceIdType.MESH)

    def local(self, key, src, dst, slot=0, count=2):
        if key not in self.local_of:
            self.local_of[key] = self.n_local
            self.n_local += count
        return pltpu.make_async_copy(src, dst, self.local_sems.at[self.local_of[key] + slot])


class SmallSum:
    def __init__(self, place, dims, slots):
        self.place, self.slots, self.dims, self.base = place, slots, dims, {}
        count = 0
        for d in dims:
            self.base[d] = count
            count += place.size[d]

    def copies(self, d):
        slot = self.slots.at[self.base[d] + self.place.me[d]]
        for k in range(1, self.place.size[d]):
            yield self.place.send((self.dims, d, k), slot, slot, **{d: k})

    def start(self, d, value):
        self.slots[self.base[d] + self.place.me[d]] = value
        for copy in self.copies(d):
            copy.start()

    def finish(self, d):
        for copy in self.copies(d):
            copy.wait()
        total = self.slots[self.base[d]]
        for k in range(1, self.place.size[d]):
            total = total + self.slots[self.base[d] + k]
        return total


def scope(name):
    return jax.named_scope(name)


def start_all(copies):
    for copy in copies:
        copy.start()


def digits(text):
    return tuple(tuple(int(d) for d in word) for word in text.split())


UNITS = [digits(u) for u in ("00", "10 30", "01 03 20", "02 11 31", "13 33 21 23", "12 32 22")]
PAIR, ALL = 1, "all"
PIECES = [2 * len(u) for u in UNITS]
EXP_RATE = SOFT_CAP * math.log2(math.e)
BASE = [sum(PIECES[:i]) for i in range(len(UNITS))]


def front_kernel(
    dims,
    shard_hbm, tok_hbm, lab_hbm, w_hbm, h_hbm, g_hbm,
    et_out, xnt_out, xpar_out, gt_out, gpar_out, lt_out, dz_out, dzpar_out, x0_out, q5_out, u_hbm, gain_hbm, loss_hbm, tokc_hbm,
    shard_ref, tok_ref, lab_ref, w_ref, gain_out, loss_out, tokc_out, shard_t, chunk, tokr, hit_t, lhs, xp, xw, xr, xf, xg, xq, etb, xn, gl, z_even, z_odd, dzb,
    acc_e, acc_l, inv_s, labc, w_slots, s_slots, sends, recvs, local_sems,
):
    n, tok, vocab, width, vt = dims["n"], dims["tok"], dims["vocab"], dims["width"], dims["vt"]
    place = Place(n, sends, recvs, local_sems)
    x, z, y, c = place.x, place.z, place.y, place.c
    half_v = vocab // CORES
    n_tile = vocab // vt
    n_half = n_tile // CORES
    hh = n_half // 2
    cols = width // (n * n * CORES)
    quarter = tok // n
    row_start = x * vocab

    def ring1(h, k):
        return {"dy": k} if h == 0 else {"dz": k}

    def ring2(h, k):
        return {"dz": k} if h == 0 else {"dy": k}

    def coord(base, k, paired):
        every = slice(None)
        if k == ALL:
            return every, every
        return every if paired else (base + k) % n // 2, (base + k) % 2

    def loc(h, k1, k2, lo=0, size=n_half, pair1=False, pair2=False):
        first, second = coord((y, z)[h], k1, pair1), coord((z, y)[h], k2, pair2)
        return et_out.at[(pl.ds(c * n_half + lo, size), *((second, first)[h]), *((first, second)[h]), h)]

    knocks = place.knock()
    early_loads = [
        place.local(("in", i), src, dst, 0, 1)
        for i, (src, dst) in enumerate(((shard_hbm, shard_ref), (tok_hbm, tok_ref), (lab_hbm, lab_ref), (w_hbm, w_ref)))
    ]
    start_all(early_loads)
    load_g = place.local("g", g_hbm, xn)
    load_g.start()
    with scope("f_cast"):
        for copy in early_loads:
            copy.wait()
        for t in range(n_tile):
            shard_t[t] = shard_ref[:, pl.ds(t * vt, vt)].astype(BF16)
    with scope("f_enter"):
        place.enter(knocks)
    with scope("f_swap"):
        tokr[c] = jnp.broadcast_to(tok_ref[...], (SUB, tok))
        give_tok = place.send("tok", tokr.at[c], tokr.at[c], dc=1)
        give_chunk = place.send("chunk", shard_t.at[pl.ds((1 - c) * n_half, n_half)], chunk.at[c], dc=1)
        give_chunk.start()
        give_tok.start()
        chunk[c] = shard_t[pl.ds(c * n_half, n_half)]
        gain_sum = SmallSum(place, ("dc", "dy", "dz"), w_slots)
        own_w = jnp.concatenate([w_ref[...], jnp.zeros((1, width - cols), F32)], axis=1)
        gain_sum.start("dc", pltpu.roll(jnp.broadcast_to(own_w, (SUB, width)), place.f * cols, axis=1)[0:1])

    def p1_send(h, i):
        return place.send(("p1", h, i), chunk.at[h], loc(h, 0, 0), **ring1(h, WAYS[i]))

    def p1_fwd(h, i):
        ref = loc(h, FROM[i], 0, i * hh, hh)
        return place.send(("p1f", h, i), ref, ref, **ring1(h, WAYS[i]))

    def p2_send(h, k1, i):
        ref = loc(h, k1, 0, pair1=k1 == PAIR)
        return place.send(("p2", h, k1, i), chunk.at[h] if k1 == 0 else ref, ref, **ring2(h, WAYS[i]))

    def p2_fwd(h, k1, i):
        ref = loc(h, k1, FROM[i], i * hh, hh, pair1=k1 == PAIR)
        return place.send(("p2f", h, k1, i), ref, ref, **ring2(h, WAYS[i]))

    def keep(h):
        return place.local("keep", chunk.at[h], loc(h, 0, 0), h)

    def share(h, k2):
        ref = loc(h, ALL, k2, pair2=k2 == PAIR)
        return place.send(("share", h, k2), ref, ref, dc=1)

    def pass_first():
        with scope("f_p1"):
            for h in BOTH:
                for i in BOTH:
                    p1_send(h, i).wait_recv()
                    p1_fwd(h, i).start()
            for h in BOTH:
                start_all(p2_send(h, PAIR, i) for i in BOTH)

    def pass_first_far():
        with scope("f_p1f"):
            for h in BOTH:
                for i in BOTH:
                    p1_fwd(h, i).wait_recv()
                start_all(p2_send(h, FAR, j) for j in BOTH)

    def pass_second(k1):
        with scope("f_p2"):
            for h in BOTH:
                for i in BOTH:
                    p2_send(h, k1, i).wait_recv()
                    p2_fwd(h, k1, i).start()

    def end_second(k1):
        with scope("f_p2f"):
            for h in BOTH:
                for i in BOTH:
                    p2_fwd(h, k1, i).wait_recv()

    def share_group(k2):
        start_all(share(h, k2) for h in BOTH)

    with scope("f_chunk"):
        give_chunk.wait_recv()
        start_all(keep(h) for h in BOTH)
        gain_sum.start("dy", gain_sum.finish("dc"))
        for h in BOTH:
            start_all(p1_send(h, i) for i in BOTH)
        for h in BOTH:
            start_all(p2_send(h, 0, i) for i in BOTH)

    v_step = min(LANE, half_v)

    def hit_body(j, carry):
        off = j * v_step
        ids = lax.broadcasted_iota(I32, (v_step, tok), 0) + (row_start + c * half_v + off)
        for i, core in enumerate((c, 1 - c)):
            hit_t[span(off, v_step, v_step), pl.ds(i * tok, tok)] = jnp.where(ids == tokr[core, 0:1, :], 1.0, 0.0).astype(BF16)
        return carry

    def make_hits():
        with scope("f_hit"):
            give_tok.wait_recv()
            lax.fori_loop(0, half_v // v_step, hit_body, 0)

    most = max(PIECES)

    def whole(u):
        return pl.ds(BASE[u], PIECES[u])

    def unit_copies(u):
        slot = u % 2
        for p, (h, (k1, k2)) in enumerate((h, k) for h in BOTH for k in UNITS[u]):
            yield place.local("lhs", loc(h, k1, k2), lhs.at[slot, p], slot * most + p, 2 * most)

    def load_unit(u):
        start_all(unit_copies(u))

    def look(u):
        pieces = PIECES[u]
        with scope("f_look"):
            if u > 1:
                x_swap(u - 2).wait_send()
            left = lhs.at[u % 2]
            for copy in unit_copies(u):
                copy.wait()
            n_step = min(2 * vt if pieces > n else vt, tok)
            per_core = tok // n_step

            def body(j, carry):
                value = jnp.concatenate([left[pl.ds(0, pieces), t].reshape(pieces * cols, vt) for t in range(n_half)], axis=1)
                rows = jnp.dot(value, hit_t[:, span(j * n_step, n_step)], preferred_element_type=F32)
                rows = rows.reshape(pieces, cols, n_step).astype(BF16)
                xw[u % 2, j // per_core, pl.ds(0, pieces), :, span(j % per_core * n_step, n_step)] = rows
                return carry

            lax.fori_loop(0, CORES * per_core, body, 0)
            x_swap(u).start()

    def x_swap(u):
        return place.send(("swap", u), xw.at[u % 2, 1, pl.ds(0, PIECES[u])], xr.at[whole(u)], dc=1)

    def lanes_of(k):
        return span((x + k) % n * quarter, quarter, quarter)

    def side(u, i):
        return pl.ds(BASE[u] + i * len(UNITS[u]), len(UNITS[u]))

    def x_far(u, i):
        return place.send(("xf", u, i), xp.at[side(u, i), :, lanes_of(FAR)], xf.at[side(u, i)], dx=WAYS[i])

    def x_near(u, i):
        return place.send(("xn", u, i), xp.at[whole(u), :, lanes_of(WAYS[i])], xg.at[i, whole(u)], dx=WAYS[i])

    def x_goal(k, sel):
        return x0_out.at[(x + k) % n, sel]

    def x_put(u, i):
        return place.send(("xp", u, i), xq.at[whole(u)], x_goal(0, whole(u)), dx=WAYS[i])

    last_unit = len(UNITS) - 1

    def x_keep(u):
        goal = x_goal(0, whole(u)) if u < last_unit else q5_out
        return place.local("x0", xq.at[whole(u)], goal, u, len(UNITS))

    def x_pass(u, i):
        ref = x_goal(FROM[i], side(u, i))
        return place.send(("xs", u, i), ref, ref, dx=WAYS[i])

    def x_first(u):
        with scope("f_x1"):
            x_swap(u).wait_recv()
            def body(p, carry):
                xp[BASE[u] + p] = xw[u % 2, 0, p] + xr[BASE[u] + p]
                return carry

            lax.fori_loop(0, PIECES[u], body, 0)
            start_all(x_far(u, i) for i in BOTH)

    def x_second(u):
        with scope("f_x2"):
            for i in BOTH:
                x_far(u, i).wait_recv()
                sel, lanes = side(u, i), lanes_of(WAYS[i])
                xp[sel, :, lanes] = xp[sel, :, lanes] + xf[sel]
                x_near(u, i).start()

    def x_third(u):
        with scope("f_x3"):
            for i in BOTH:
                x_near(u, i).wait_recv()
            sel = whole(u)
            xq[sel] = xp[sel, :, lanes_of(0)] + xg[0, sel] + xg[1, sel]
            if u < last_unit:
                start_all(x_put(u, i) for i in BOTH)
            x_keep(u).start()

    def x_fourth(u):
        with scope("f_x4"):
            for i in BOTH:
                x_put(u, i).wait_recv()
                x_pass(u, i).start()

    n_part = n * n * CORES // 2

    def moves(key, part, whole_t, other):
        sel = pl.ds(part * n_part, n_part)
        yield place.local(key, gl.at[sel], whole_t.at[sel], part)
        yield place.send((key, part), gl.at[sel], other.at[sel], dc=1)

    def move_g(part):
        return moves("g", part, gt_out, gpar_out)

    def move_xn(part):
        return moves("xt", part, xnt_out, xpar_out)

    def transpose_part(part, copies):
        block = width // dims["n_block"]
        first = part * dims["n_block"] // 2
        turned = [xn[:, pl.ds((first + j) * block, block)].T for j in range(dims["n_block"] // 2)]
        gl[pl.ds(part * n_part, n_part)] = jnp.concatenate(turned, axis=0).reshape(n_part, cols, tok)
        start_all(copies)

    def columns(row):
        return jnp.broadcast_to(row.astype(F32), (LANE, tok)).T.astype(I32)

    r_step = min(LANE, tok)

    def xn_body(j, carry):
        sel = span(j * r_step, r_step, r_step)
        h_wide = xn[sel].astype(F32)
        inv_rms = lax.rsqrt(jnp.sum(h_wide * h_wide, axis=1, keepdims=True) * (1.0 / width) + NORM_EPS)
        xn[sel] = (h_wide * inv_rms * gain_out[0:1]).astype(BF16)
        return carry

    e_step = min(LANE, tok)

    def tile_of(j):
        return (c * n_half + j) % n_tile

    def load_tile(j):
        return place.local("et", et_out.at[tile_of(j)], etb.at[j % 4], j % 4, 4)

    def save_u(i, odd):
        return place.local(("u", odd), (z_even, z_odd)[odd].at[i % 2], u_hbm.at[tile_of(2 * i + odd)], i % 2)

    def lane_blocks():
        return [(b, pl.ds(b, LANE)) for b in range(0, vt, LANE)]

    def post_rows(i, odd, sel, size):
        base = tile_of(2 * i + odd) * vt
        buf, slot = (z_even, z_odd)[odd], i % 2
        ids = lax.broadcasted_iota(I32, (size, LANE), 1) + base
        sum_e, sum_l = acc_e[sel], acc_l[sel]
        for b, lanes in lane_blocks():
            tanh_z = jnp.tanh(buf[slot, sel, lanes] * (1.0 / SOFT_CAP))
            buf[slot, sel, lanes] = tanh_z
            sum_e = sum_e + jnp.exp2(EXP_RATE * tanh_z - EXP_RATE)
            sum_l = sum_l + jnp.where(ids + b == labc[sel], tanh_z, 0.0)
        acc_e[sel] = sum_e
        acc_l[sel] = sum_l

    def post_tile(i, odd):
        def body(e, carry):
            post_rows(i, odd, span(e * e_step, e_step, e_step), e_step)
            return carry

        lax.fori_loop(0, tok // e_step, body, 0)

    def dot_pair(i):
        for odd in BOTH:
            value = etb[(2 * i + odd) % 4].reshape(width, vt)
            (z_even, z_odd)[odd][i % 2] = jnp.dot(xn[...], value, preferred_element_type=F32)

    def load_pair(i):
        start_all(load_tile(2 * i + odd) for odd in BOTH)

    def pair(i, carry):
        for odd in BOTH:
            load_tile(2 * i + odd).wait()

        @pl.when(i > 1)
        def _():
            for odd in BOTH:
                save_u(i - 2, odd).wait()

        m_step = min(vt, tok)
        for m in range(0, tok, m_step):
            for odd in BOTH:
                for e in range(m, m + m_step, r_step):
                    post_rows(i - 1, odd, pl.ds(e, r_step), r_step)
            for odd in BOTH:
                rows = pl.ds(m, m_step)
                value = etb[(2 * i + odd) % 4].reshape(width, vt)
                (z_even, z_odd)[odd][i % 2, rows] = jnp.dot(xn[rows], value, preferred_element_type=F32)

        @pl.when(i < last)
        def _():
            start_all(save_u(i - 1, odd) for odd in BOTH)

        @pl.when(i + 2 < n_tile // 2)
        def _():
            load_pair(i + 2)

        for k, work in enumerate(during):
            @pl.when(i == k + 1)
            def _():
                if k == 0:
                    wait_shares()
                perform(work)
        return carry

    def wait_shares():
        with scope("f_share"):
            for h in BOTH:
                for k2 in (0, PAIR, FAR):
                    share(h, k2).wait_recv()

    def logits_first():
        acc_e[...] = jnp.zeros_like(acc_e)
        acc_l[...] = jnp.zeros_like(acc_l)
        with scope("f_logits0"):
            far_ends(1)
            for odd in BOTH:
                load_tile(odd).wait()
            dot_pair(0)
            if n_tile // 2 > 2:
                load_pair(2)

    def load_first():
        for i in BOTH:
            load_pair(i)

    def put_small(i):
        src, dst = ((gain_out, gain_hbm), (loss_out, loss_hbm), (tokc_out, tokc_hbm))[i]
        return place.local(("out", i), src, dst, 0, 1)

    def lay_columns():
        with scope("f_cols"):
            labc[...] = columns(lab_ref[...] - row_start)
            for i, core in enumerate((c, 1 - c)):
                tokc_out[i] = columns(tokr[core, 0:1, :])
            put_small(2).start()

    def turn_g():
        with scope("f_gt"):
            load_g.wait()
            for part in BOTH:
                transpose_part(part, move_g(part))
            load_h.start()

    def gain_next():
        with scope("f_gain2"):
            gain_sum.start("dz", gain_sum.finish("dy"))

    def normalize():
        with scope("f_xn"):
            gain_out[...] = 1.0 + gain_sum.finish("dz")
            put_small(0).start()
            load_h.wait()
            lax.fori_loop(0, tok // r_step, xn_body, 0)

    def turn_xn():
        with scope("f_xt"):
            for part in BOTH:
                transpose_part(part, move_xn(part))

    spare = BASE[3]
    own_rows, their_rows = (pl.ds(spare + i * 2 * n, 2 * n) for i in BOTH)

    def far_loads(h):
        for i, (src, rows) in enumerate(((gt_out, own_rows), (gpar_out, their_rows))):
            if h == 0:
                yield place.local("far", src.at[pl.ds((z + FAR) % n * 2 * n, 2 * n)], xp.at[rows], i * n, 2 * n)
            else:
                for q in range(n):
                    piece = src.at[pl.ds((q * n + (y + FAR) % n) * 2, 2)]
                    yield place.local("far", piece, xp.at[pl.ds(spare + i * 2 * n + 2 * q, 2)], i * n + q)

    def far_load(h):
        if h == 0:
            for part in BOTH:
                for copy in move_g(part):
                    copy.wait()
        start_all(far_loads(h))

    def put_far(h, j):
        rows = pl.ds(0, 2 * n * cols)
        return place.local("lt", z_even.at[j % 2, rows], lt_out.at[h, :, span(j * vt, vt)], j % 2)

    def far_ends(h):
        for j in range(hh - 2, hh):
            put_far(h, j).wait()

    def far_look(h):
        def body(j, carry):
            @pl.when(j > 1)
            def _():
                put_far(h, j - 2).wait()

            left = jnp.concatenate([xp[rows].reshape(2 * n * cols, tok) for rows in (own_rows, their_rows)], axis=1)
            right = hit_t[span((h * hh + j) * vt, vt)]
            value = lax.dot_general(left, right, (((1,), (1,)), ((), ())), preferred_element_type=F32)
            z_even[j % 2, pl.ds(0, 2 * n * cols)] = value * dims["scale"]
            put_far(h, j).start()
            return carry

        with scope("f_far"):
            for copy in far_loads(h):
                copy.wait()
            if h:
                far_ends(0)
            lax.fori_loop(0, hh, body, 0)

    def begin_unit(u):
        if u == 0:
            for h in BOTH:
                keep(h).wait()
        load_unit(u)

    load_h = place.local("h", h_hbm, xn)
    works = {
        "HIT": make_hits, "GT": turn_g, "COL": lay_columns, "G2": gain_next, "XN": normalize, "XT": turn_xn, "LP": load_first, "L0": logits_first,
        "PF": pass_first, "PFF": pass_first_far,
    }
    groups = {"0": 0, "P": PAIR, "F": FAR}
    families = {"LF": far_load, "FL": far_look, "LU": begin_unit, "LK": look, "X1": x_first, "X2": x_second, "X3": x_third, "X4": x_fourth}
    families_k = {"SH": share_group, "S": pass_second, "E": end_second}

    def perform(text):
        for word in text.split():
            if word in works:
                works[word]()
            elif word[:-1] in families:
                families[word[:-1]](int(word[-1]))
            else:
                families_k[word[:-1]](groups[word[-1]])

    during = (
        "X24",
        "X15 X33",
        "",
        "X34",
        "X42",
        "X43",
        "",
    )
    for text in (
        "HIT LU0 LK0 G2", "GT X10 PF LU1", "LK1 LF0 S0 X20", "X11 FL0 PFF X21", "LU2 LF1 X30 LK2",
        "FL1 XN SP SH0", "E0 LU3 X12 X31", "LK3 SF LU4 X22", "X40 SHP LK4 X13", "EP X32 X41 EF",
        "LU5 SHF LP XT", "COL L0 X14 LK5", "X23",
    ):
        perform(text)
    if n_half < 4:
        wait_shares()
        for text in during:
            perform(text)
        during = ()
    last = n_tile // 2 - 1
    with scope("f_logits"):
        lax.fori_loop(1, last + 1, pair, 0)
        for odd in BOTH:
            post_tile(last, odd)

    with scope("f_stats"):
        row = lax.broadcasted_iota(I32, (2, tok), 0)
        sum_e = jnp.sum(acc_e[...].T, axis=0, keepdims=True)
        sum_l = SOFT_CAP * jnp.sum(acc_l[...].T, axis=0, keepdims=True)
        stats = SmallSum(place, ("dx",), s_slots)
        stats.start("dx", jnp.where(row == 0, sum_e, sum_l))
    perform("X25 X44")
    with scope("f_stats2"):
        stat = stats.finish("dx")
        all_e, all_l = stat[0:1], stat[1:2]
        inv_s[...] = jnp.broadcast_to((1.0 / dims["total"]) / all_e, (LANE, tok)).T
        s_slots[0, 0:1, :] = jnp.log(all_e) + SOFT_CAP - all_l
        own = s_slots[0, 0:1, lanes_of(0)]
        part_w = min(LANE, quarter)
        folded = own[:, 0:part_w]
        for j in range(part_w, quarter, part_w):
            folded = folded + own[:, j:j + part_w]
        loss_out[...] = jnp.where(lax.broadcasted_iota(I32, (SUB, part_w), 0) == 0, folded, 0.0)
        put_small(1).start()

    def dz_tile(j):
        return ((1 - c) * n_half + j) % n_tile

    def load_u(i, odd):
        return place.local(("u", odd), u_hbm.at[dz_tile(2 * i + odd)], (z_even, z_odd)[odd].at[i % 2], i % 2)

    def put_dz(i, odd):
        return place.local(("dz", odd), dzb.at[odd, i % 2], dz_out.at[dz_tile(2 * i + odd)], i % 2)

    def give_dz(part):
        src = dz_out.at[pl.ds((1 - c) * n_half + part * hh, hh)]
        return place.send(("dz", part), src, dzpar_out.at[pl.ds(part * hh, hh)], dc=1)

    d_step = min(256, tok)

    def dz_rows(i, odd):
        base = dz_tile(2 * i + odd) * vt
        buf, slot = (z_even, z_odd)[odd], i % 2

        def body(e, carry):
            sel = span(e * d_step, d_step, d_step)
            ids = lax.broadcasted_iota(I32, (d_step, LANE), 1) + base
            for b, lanes in lane_blocks():
                tanh_z = buf[slot, sel, lanes]
                prob = jnp.exp2(EXP_RATE * tanh_z - EXP_RATE) * inv_s[sel]
                prob = jnp.where(ids + b == labc[sel], prob - 1.0 / dims["total"], prob)
                dzb[odd, slot, sel, lanes] = (prob * (1.0 - tanh_z * tanh_z)).astype(BF16)
            return carry

        lax.fori_loop(0, tok // d_step, body, 0)

    def dz_pair(i, loaded, follow):
        for odd in BOTH:
            if loaded:
                load_u(i, odd).wait()

            @pl.when(i > hh + 1)
            def _():
                put_dz(i - 2, odd).wait()

            dz_rows(i, odd)
            put_dz(i, odd).start()

            @pl.when(i + follow < n_tile // 2)
            def _():
                load_u(i + follow, odd).start()

    def dz_run(lo, hi, loaded, follow):
        def body(i, carry):
            dz_pair(i, loaded, follow)
            return carry

        lax.fori_loop(lo, hi, body, 0)

    with scope("f_dz"):
        half = hh // 2
        for part in (1, 0):
            dz_run(part * half, (part + 1) * half, not part, hh if part == 0 else -half)
            for i in range(part * half, (part + 1) * half):
                for odd in BOTH:
                    put_dz(i, odd).wait()
            give_dz(part).start()
        dz_run(hh, n_tile // 2, True, half)

    perform("X35")
    with scope("f_end"):
        for i in range(3):
            put_small(i).wait()
        for part in BOTH:
            give_dz(part).wait()
        for i in range(n_tile // 2 - 2, n_tile // 2):
            for odd in BOTH:
                put_dz(i, odd).wait()
        give_tok.wait_send()
        give_chunk.wait_send()
        for h in BOTH:
            for i in BOTH:
                p1_send(h, i).wait_send()
                p1_fwd(h, i).wait_send()
                for k in (0, PAIR, FAR):
                    p2_send(h, k, i).wait_send()
                    p2_fwd(h, k, i).wait_send()
            for k in (0, PAIR, FAR):
                share(h, k).wait_send()
        for part in BOTH:
            for copy in move_xn(part):
                copy.wait()
        for u in range(len(UNITS)):
            if u > len(UNITS) - 3:
                x_swap(u).wait_send()
            x_keep(u).wait()
            for i in BOTH:
                x_far(u, i).wait_send()
                x_near(u, i).wait_send()
                if u < last_unit:
                    x_put(u, i).wait_send()
                    x_pass(u, i).wait()
    assert (place.n_link, place.n_local) <= dims["front_sems"], (place.n_link, place.n_local)


def specs(n_vmem, n_any):
    return [pl.BlockSpec(memory_space=pltpu.VMEM)] * n_vmem + [pl.BlockSpec(memory_space=pl.ANY)] * n_any


def shapes(items):
    return tuple(jax.ShapeDtypeStruct(*item) for item in items)


def scratch(items, n_link, n_local):
    dma = pltpu.SemaphoreType.DMA
    return [pltpu.VMEM(*item) for item in items] + [dma((n_link,)), dma((n_link,)), dma((n_local,))]


def params(collective_id, limit):
    return pltpu.CompilerParams(collective_id=collective_id, has_side_effects=True, vmem_limit_bytes=limit)


def front(dims, limit, shard, tok_row, lab_row, w, h, g):
    n, tok, vocab, width, vt = dims["n"], dims["tok"], dims["vocab"], dims["width"], dims["vt"]
    cols = shard.shape[0]
    half_v = vocab // CORES
    quarter = tok // n
    n_tile, n_half, most = vocab // vt, half_v // vt, max(PIECES)
    pieces = n * n * CORES
    grid = (n // 2, 2, n // 2, 2)
    return pl.pallas_call(
        functools.partial(front_kernel, dims),
        name="front",
        out_shape=shapes([
            ((n_tile, *grid, CORES, cols, vt), BF16), *[((pieces, cols, tok), BF16)] * 4, ((2, 2 * n * cols, half_v // 2), F32), ((n_tile, tok, vt), BF16),
            ((n_half, tok, vt), BF16), ((n, BASE[-1], cols, quarter), BF16), ((PIECES[-1], cols, quarter), BF16), ((n_tile, tok, vt), F32),
            ((1, width), F32), ((SUB, min(LANE, quarter)), F32), ((CORES, tok, LANE), I32),
        ]),
        in_specs=specs(0, 6),
        out_specs=tuple(specs(0, 14)),
        scratch_shapes=scratch([
            (shard.shape, F32), (tok_row.shape, I32), (lab_row.shape, I32), (w.shape, F32), ((1, width), F32),
            ((SUB, min(LANE, quarter)), F32), ((CORES, tok, LANE), I32),
            ((n_tile, cols, vt), BF16), ((CORES, n_half, cols, vt), BF16), ((CORES, SUB, tok), I32), ((half_v, CORES * tok), BF16),
            ((2, most, n_half, cols, vt), BF16), ((pieces, cols, tok), BF16), ((2, CORES, most, cols, tok), BF16), ((pieces, cols, tok), BF16),
            ((pieces, cols, quarter), BF16), ((2, pieces, cols, quarter), BF16), ((pieces, cols, quarter), BF16),
            ((4, *grid, CORES, cols, vt), BF16), ((tok, width), BF16), ((pieces, cols, tok), BF16),
            ((2, tok, vt), F32), ((2, tok, vt), F32), ((2, 2, tok, vt), BF16), ((tok, LANE), F32), ((tok, LANE), F32), ((tok, LANE), F32),
            ((tok, LANE), I32), ((2 * n + CORES, 1, width), F32), ((n, 2, tok), F32),
        ], dims["front_sems"][0], dims["front_sems"][1]),
        compiler_params=params(0, limit),
    )(shard, tok_row, lab_row, w, h, g)


def back_kernel(
    dims,
    gain_hbm, loss_hbm, tokc_hbm, lt_hbm, dz_hbm, dzp_hbm, et_hbm, xnt_hbm, xpar_hbm, gt_hbm, gpar_hbm, h_hbm, q5_hbm,
    tail_hbm, dh_out, de_out, x0_out, ra_hbm, rx_hbm,
    gain_ref, loss_ref, tokc, tail_out, q5, dz_own, dz_par, et_buf, part, fx, acc, fa, f2, r2, xb, h_buf, dh_buf, dg_acc, slots,
    sends, recvs, local_sems,
):
    n, tok, vocab, width, tile, vt = (dims[k] for k in ("n", "tok", "vocab", "width", "tile", "vt"))
    place = Place(n, sends, recvs, local_sems)
    x, z, y, c = place.x, place.z, place.y, place.c
    half_v = vocab // CORES
    n_tile, n_half = vocab // vt, half_v // vt
    lanes = half_v // 2
    rows = width // (n * n)
    half_rows = rows // 2
    quarter = tok // n
    hq = quarter // 2
    tiles = dims["tiles"]
    chunks = len(tiles)
    edges = [sum(tiles[:d]) for d in range(chunks + 1)]
    per_half = n_half // 2

    knocks = place.knock()
    load_q5 = place.local("q5", q5_hbm, q5)
    load_q5.start()
    load_h = place.local("h", h_hbm.at[span(x * quarter, quarter, quarter)], h_buf)

    def load_et(t, slot):
        return place.local("et", et_hbm.at[:, span(t * tile, tile, tile)], et_buf.at[slot], slot)

    slot_of = {FAR: 0, 1: 1, 3: 2, 0: 0}
    stages = dims["stages"]

    def load_stage(m, i):
        half, k, kind = stages[m]
        src = ((gt_hbm, gpar_hbm), (xnt_hbm, xpar_hbm))[kind][i]
        src = src.at[(z + k) % n] if half == 0 else src.at[:, (y + k) % n]
        return place.local(("xb", i), src, xb.at[m % 2, i], m % 2)

    def start_stage(m):
        if m < len(stages):
            start_all(load_stage(m, i) for i in BOTH)

    loads = [place.local("dz", dz_hbm, dz_own), place.local("dzp", dzp_hbm, dz_par)]
    load_et(0, 0).start()
    start_all(loads)
    keep_q5 = place.local("q5", q5, x0_out.at[x], 1)

    def y_put(i):
        return place.send(("yp", i), q5, x0_out.at[x], dx=WAYS[i])

    def y_pass(i):
        size = q5.shape[0] // 2
        ref = x0_out.at[(x + FROM[i]) % n, pl.ds(i * size, size)]
        return place.send(("yq", i), ref, ref, dx=WAYS[i])

    def y_passes():
        for i in BOTH:
            y_put(i).wait_recv()
            y_pass(i).start()

    small_loads = [
        place.local(("in", i), src, dst, 0, 1)
        for i, (src, dst) in enumerate(((tokc_hbm, tokc), (gain_hbm, gain_ref), (loss_hbm, loss_ref)))
    ]
    fars = [place.local("lt", lt_hbm.at[half], acc.at[half, 0], half) for half in BOTH]
    start_all(fars + small_loads)
    for m in BOTH:
        start_stage(m)
    load_h.start()

    def columns(d):
        return pl.ds(edges[d] * tile, tiles[d] * tile)

    def dxn_chunk(d):
        def body(t, carry):
            slot = t % 2

            @pl.when(t + 1 < edges[chunks])
            def _():
                load_et(t + 1, 1 - slot).start()

            load_et(t, slot).wait()
            left = jnp.concatenate([dz_own[j] for j in range(n_tile)], axis=1)
            right = jnp.concatenate([et_buf[slot, j] for j in range(n_tile)], axis=1)
            part[:, span(t * tile, tile, tile)] = lax.dot_general(
                left, right, (((1,), (1,)), ((), ())), preferred_element_type=F32)
            return carry

        with scope("b_dxn"):
            lax.fori_loop(edges[d], edges[d + 1], body, 0)

    def qrow(k, lo=0, size=hq):
        return span((x + k) % n * quarter + lo, size, SUB)

    def x_far(d, i):
        return place.send(("xf", d, i), part.at[qrow(FAR, i * hq), columns(d)], fx.at[i, :, columns(d)], dx=WAYS[i])

    def x_near(d, i, j):
        src = part.at[qrow(WAYS[i], j * hq), columns(d)]
        return place.send(("xn", d, i, j), src, rx_hbm.at[i, pl.ds(j * hq, hq), columns(d)], dx=WAYS[i])

    def x_first(d):
        start_all(x_far(d, i) for i in BOTH)

    def x_second(d):
        with scope("b_x2"):
            for i in BOTH:
                x_far(d, i).wait_recv()
                sel = qrow(WAYS[i], i * hq)
                part[sel, columns(d)] = part[sel, columns(d)] + fx[i, :, columns(d)]
                start_all(x_near(d, i, j) for j in BOTH)

    def stage_x(d, j, i):
        return place.local("sx", rx_hbm.at[i, pl.ds(j * hq, hq), columns(d)], fx.at[i, :, columns(d)], i)

    def x_third(d, j):
        with scope("b_x3"):
            for i in BOTH:
                x_near(d, i, j).wait_recv()
                stage_x(d, j, i).start()
            for i in BOTH:
                stage_x(d, j, i).wait()
            sel = qrow(0, j * hq)
            part[sel, columns(d)] = part[sel, columns(d)] + fx[0, :, columns(d)] + fx[1, :, columns(d)]

    def de_stage(half, k, kind):
        m = stages.index((half, k, kind))
        slot = slot_of[k]

        wide = min(2, per_half) if kind and k else 1

        def right(i, t):
            if kind:
                return dz_par[t] if i else dz_own[c * n_half + t]
            ids = lax.broadcasted_iota(I32, (tok, LANE), 1) + (x * vocab + c * half_v + t * vt)
            hits = [jnp.where(tokc[i] == ids + b, dims["scale"], 0.0).astype(BF16) for b in range(0, vt, LANE)]
            return jnp.concatenate(hits, axis=1)

        def body(j, carry):
            t = half * per_half + j * wide
            sel = span(j * wide * vt, wide * vt)
            left = jnp.concatenate([xb[m % 2, i].reshape(n * rows, tok) for i in BOTH], axis=1)
            both_right = [jnp.concatenate([right(i, t + q) for i in BOTH], axis=0) for q in range(wide)]
            total = jnp.dot(left, jnp.concatenate(both_right, axis=1), preferred_element_type=F32)
            total = total.reshape(n, rows, wide * vt)
            acc[half, slot, :, :, sel] = acc[half, slot, :, :, sel] + total if kind else total
            return carry

        with scope("b_de" if kind else "b_look"):
            for i in BOTH:
                load_stage(m, i).wait()
            lax.fori_loop(0, per_half // wide, body, 0)
            start_stage(m + 2)

    def de_unit(half, k):
        if k == FAR:
            fars[half].wait()
        else:
            de_stage(half, k, 0)
        de_stage(half, k, 1)

    def ring(half, k):
        return {"dz": k} if half == 0 else {"dy": k}

    def cross(half, k):
        return {"dy": k} if half == 0 else {"dz": k}

    def a_far(half, i):
        return place.send(("af", half, i), acc.at[half, 0, pl.ds(2 * i, 2)], fa.at[half, i], **ring(half, WAYS[i]))

    def a_near(half, i, j):
        sel = pl.ds(2 * j, 2)
        return place.send(("an", half, i, j), acc.at[half, 1 + i, sel], ra_hbm.at[half, i, sel], **ring(half, WAYS[i]))

    def a_first(half):
        start_all(a_far(half, i) for i in BOTH)

    def a_second(half, i):
        with scope("b_a2"):
            a_far(half, i).wait_recv()
            sel = pl.ds(2 * i, 2)
            acc[half, 1 + i, sel] = acc[half, 1 + i, sel] + fa[half, i]
            start_all(a_near(half, i, j) for j in BOTH)

    def stage_a(half, j, i):
        return place.local(("sa", half), ra_hbm.at[half, i, pl.ds(2 * j, 2)], fa.at[half, i], i)

    def piece(half, k):
        return ((y if half == 0 else z) + k) % n

    def c_far(half, i):
        src = acc.at[half, 0, piece(half, FAR), pl.ds(i * half_rows, half_rows)]
        return place.send(("cf", half, i), src, f2.at[half, i], **cross(half, WAYS[i]))

    def c_near(half, i):
        return place.send(("cn", half, i), acc.at[half, 0, piece(half, WAYS[i])], r2.at[half, i], **cross(half, WAYS[i]))

    def a_third(half, j):
        with scope("b_a3"):
            for i in BOTH:
                a_near(half, i, j).wait_recv()
                stage_a(half, j, i).start()
            for i in BOTH:
                stage_a(half, j, i).wait()
            sel = pl.ds(2 * j, 2)
            acc[half, 0, sel] = acc[half, 0, sel] + fa[half, 0] + fa[half, 1]

    def c_first(half):
        start_all(c_far(half, i) for i in BOTH)

    def c_second(half):
        with scope("b_c2"):
            for i in BOTH:
                c_far(half, i).wait_recv()
                at = piece(half, WAYS[i])
                sel = pl.ds(i * half_rows, half_rows)
                acc[half, 0, at, sel] = acc[half, 0, at, sel] + f2[half, i]
                c_near(half, i).start()

    def out_copies(half):
        sel = span(c * half_v + half * lanes, lanes)
        mine = acc.at[half, 0, piece(half, 0)]
        yield place.local("de", mine.at[span(c * half_rows, half_rows, SUB)], de_out.at[:, sel], half)
        yield place.send(("de", half), mine.at[span((1 - c) * half_rows, half_rows, SUB)], de_out.at[:, sel], dc=1)

    def c_third(half):
        with scope("b_c3"):
            for i in BOTH:
                c_near(half, i).wait_recv()
            at = piece(half, 0)
            acc[half, 0, at] = acc[half, 0, at] + r2[half, 0] + r2[half, 1]
            start_all(out_copies(half))

    step = min(32, hq)

    def dh_body(i, carry):
        sel = span(i * step, step, step)
        row = span(x * quarter + i * step, step, step)
        d_x = part[row]
        h_wide = h_buf[sel].astype(F32)
        inv_rms = lax.rsqrt(jnp.sum(h_wide * h_wide, axis=1, keepdims=True) * (1.0 / width) + NORM_EPS)
        h_norm = h_wide * inv_rms
        g_dir = d_x * gain_ref[0:1]
        mean = jnp.sum(g_dir * h_norm, axis=1, keepdims=True) * (1.0 / width)
        dh_buf[sel] = (inv_rms * (g_dir - h_norm * mean)).astype(BF16)
        prod = d_x * h_norm
        total = prod[0:SUB]
        for j in range(SUB, step, SUB):
            total = total + prod[j:j + SUB]
        dg_acc[...] = dg_acc[...] + total
        return carry

    def h_first(i, j):
        return place.send(("hf", i, j), dh_buf.at[pl.ds(j * hq, hq)], dh_out.at[qrow(0, j * hq)], dx=WAYS[i])

    def h_second(i):
        ref = dh_out.at[qrow(FROM[i], i * hq)]
        return place.send(("hs", i), ref, ref, dx=WAYS[i])

    keep_dh = place.local("dh", dh_buf, dh_out.at[qrow(0, 0, quarter)])
    small = SmallSum(place, ("dc", "dx", "dy", "dz"), slots)
    per_j = hq // step

    def dh_part(j):
        with scope("b_dh"):
            if j == 0:
                load_h.wait()
            lax.fori_loop(j * per_j, (j + 1) * per_j, dh_body, 0)
            start_all(h_first(i, j) for i in BOTH)
            if j:
                keep_dh.start()

    def h_pass(i):
        with scope("b_h2"):
            h_first(i, i).wait_recv()
            h_second(i).start()

    put_tail = place.local("tail", tail_out, tail_hbm, 0, 1)

    def small_step(k):
        dims_of = small.dims
        with scope("b_s"):
            if k == 1:
                sums = [jnp.sum(part_sum, axis=0, keepdims=True) for part_sum in (dg_acc[...], loss_ref[...])]
                small.start(dims_of[0], jnp.concatenate(sums, axis=1))
            elif k <= len(dims_of):
                small.start(dims_of[k - 1], small.finish(dims_of[k - 2]))
            else:
                total = small.finish(dims_of[-1])
                loss = jnp.sum(total[:, width:], axis=1, keepdims=True) * (1.0 / dims["total"])
                tail_out[...] = jnp.concatenate([total[:, 0:width], jnp.broadcast_to(loss, (1, LANE))], axis=1)
                put_tail.start()

    def dxn(d):
        dxn_chunk(d)
        x_first(d)

    def unit(half, k):
        if k == 0:
            with scope("b_wait_far"):
                for i in BOTH:
                    a_far(half, i).wait_send()
        while len(loads) > 1:
            loads.pop().wait()
            for copy in small_loads:
                copy.wait()
        de_unit(half, k)
        if k == FAR:
            a_first(half)

    families = {
        "CH": dxn, "XS": x_second, "UN": unit, "AS": a_second, "XT": x_third, "AT": a_third, "CF": c_first, "CS": c_second,
        "CT": c_third, "DH": dh_part, "SM": small_step, "HP": h_pass, "YQ": y_passes,
    }

    def perform(text):
        for word in text.split():
            families[word[:2]](*(int(digit) for digit in word[2:]))

    with scope("b_enter"):
        place.enter(knocks)
    with scope("b_load"):
        load_q5.wait()
        start_all(y_put(i) for i in BOTH)
        keep_q5.start()
        loads[0].wait()
        dg_acc[...] = jnp.zeros_like(dg_acc)
    for text in (
        "CH0 UN02 YQ CH1", "UN12 CH2 UN03 XS1", "UN01 XS2 UN13 AS01", "AS00 UN11 AS11 AS10",
        "XS0 CH3 XT10 CH4", "UN00 XT00 XS3 XT01", "XS4 UN10 XT20 AT00", "XT30 XT21 XT11 XT40",
        "DH0 XT31 XT41 DH1", "AT01 AT10 CF0 SM1", "AT11 CF1 SM2 HP0", "CS0 CS1 SM3 HP1", "CT0 SM4 CT1 SM5",
    ):
        perform(text)

    with scope("b_end_x"):
        put_tail.wait()
        keep_dh.wait()
        keep_q5.wait()
        for i in BOTH:
            y_put(i).wait_send()
            y_pass(i).wait()
            for d in range(chunks):
                x_far(d, i).wait_send()
                for j in BOTH:
                    x_near(d, i, j).wait_send()
            h_first(i, i).wait_send()
            h_first(i, 1 - i).wait()
            h_second(i).wait()
    with scope("b_end_a"):
        for half in BOTH:
            for i in BOTH:
                for j in BOTH:
                    a_near(half, i, j).wait_send()
                c_far(half, i).wait_send()
                c_near(half, i).wait_send()
            for copy in out_copies(half):
                copy.wait()
    assert (place.n_link, place.n_local) <= dims["back_sems"], (place.n_link, place.n_local)


def back(dims, limit, gain, loss, tokc, far, dz, dzp, et, xnt, xpar, gt, gpar, h, q5):
    n, tok, vocab, width, tile = (dims[k] for k in ("n", "tok", "vocab", "width", "tile"))
    rows = width // (n * n)
    half_v = vocab // CORES
    lanes = half_v // 2
    quarter = tok // n
    hq = quarter // 2
    tail_w = width + loss.shape[1]
    n_tile, n_half, vt = dz.shape[0], dzp.shape[0], dims["vt"]
    turned = [a.reshape(n, n, rows, tok) for a in (xnt, xpar, gt, gpar)]
    return pl.pallas_call(
        functools.partial(back_kernel, dims),
        name="back",
        out_shape=shapes([
            ((1, width + LANE), F32), ((tok, width), BF16), ((rows // CORES, vocab), F32), ((n, *q5.shape), BF16),
            ((2, 2, n, rows, lanes), F32),
            ((2, quarter, width), F32),
        ]),
        in_specs=specs(0, 13),
        out_specs=tuple(specs(0, 6)),
        scratch_shapes=scratch([
            (gain.shape, F32), (loss.shape, F32), (tokc.shape, I32), ((1, width + LANE), F32),
            (q5.shape, BF16), ((n_tile, tok, vt), BF16), ((n_half, tok, vt), BF16), ((2, n_tile, tile, vt), BF16), ((tok, width), F32),
            ((2, hq, width), F32), ((2, 3, n, rows, lanes), F32), ((2, 2, 2, rows, lanes), F32),
            ((2, 2, rows // 2, lanes), F32), ((2, 2, rows, lanes), F32), ((2, CORES, n, rows, tok), BF16), ((quarter, width), BF16),
            ((quarter, width), BF16), ((SUB, width), F32), ((3 * n + CORES, 1, tail_w), F32),
        ], dims["back_sems"][0], dims["back_sems"][1]),
        compiler_params=params(1, limit),
    )(gain, loss, tokc, far.reshape(2, n, rows, lanes), dz, dzp, et.reshape(n_tile, width, vt), *turned, h, q5)[:4]


def finish_kernel(
    n, scale, table_ref, tail_hbm, x0_hbm, x5_hbm, dh_hbm, de_hbm, dg_hbm, loss_hbm, x0_out, dh_out, de_out,
    tail_ref, dg_out, loss_out, x0_in, x0_buf, rows_ref, dh_buf, de_buf, sems,
):
    place = Place(n, None, None, sems)
    quarter, cols, width = x0_in.shape[3], x0_in.shape[2], x0_buf.shape[2]

    def step(q):
        rows = span(q * quarter, quarter, quarter)
        return (
            place.local("x0", x0_hbm.at[q], x0_in.at[q, pl.ds(0, BASE[-1])], q, n),
            place.local("x5", x5_hbm.at[q], x0_in.at[q, pl.ds(BASE[-1], PIECES[-1])], q, n), place.local("x0o", x0_buf.at[q], x0_out.at[rows], q, n),
            place.local("dh", dh_hbm.at[rows], dh_buf.at[q], q, n), place.local("dho", dh_buf.at[q], dh_out.at[rows], q, n),
        )

    moves = [step(q) for q in range(n)]
    de_in, de_put = place.local("de", de_hbm, de_buf, 0), place.local("de", de_buf, de_out, 1)
    for x0_load, x5_load, _, dh_load, _ in moves:
        start_all((x0_load, x5_load, dh_load))
    de_in.start()
    tail_in = place.local("tail", tail_hbm, tail_ref)
    small_puts = [place.local("dg", dg_out, dg_hbm), place.local("loss", loss_out, loss_hbm)]
    tail_in.start()
    tail_in.wait()
    gain = jnp.broadcast_to(tail_ref[:, 0:width], (SUB, width))
    dg_out[...] = pltpu.roll(gain, width - place.f * cols, axis=1)[0:1, 0:cols]
    loss_out[...] = tail_ref[:, width:width + 1]
    start_all(small_puts)

    def body(q, carry):
        x0_load, x5_load, x0_put, dh_load, dh_put = step(q)
        x0_load.wait()
        x5_load.wait()
        for zi in range(n):
            for yi in range(n):
                for h in BOTH:
                    dz, dy = (zi - place.z) % n, (yi - place.y) % n
                    k1, k2 = (dy, dz) if h == 0 else (dz, dy)
                    piece = table_ref[(h * n + k1) * n + k2]
                    rows_ref[pl.ds(((zi * n + yi) * CORES + h) * cols, cols)] = x0_in[q, piece]
        x0_buf[q] = (rows_ref[...].T.astype(F32) * scale).astype(BF16)
        x0_put.start()
        dh_load.wait()
        dh_put.start()
        return carry

    lax.fori_loop(0, n, body, 0)
    de_in.wait()
    de_put.start()
    for _, _, x0_put, _, dh_put in moves:
        x0_put.wait()
        dh_put.wait()
    de_put.wait()
    for copy in small_puts:
        copy.wait()


def finish(n, scale, limit, tail, x0, x5, dh, de):
    cols, quarter = x0.shape[2:]
    pieces = n * n * CORES
    width = pieces * cols
    table = np.zeros((CORES, n, n), np.int32)
    for u, unit in enumerate(UNITS):
        for h in BOTH:
            for i, (k1, k2) in enumerate(unit):
                table[h, k1, k2] = BASE[u] + h * len(unit) + i
    return pl.pallas_call(
        functools.partial(finish_kernel, n, scale),
        name="finish",
        in_specs=[pl.BlockSpec(memory_space=pltpu.SMEM)] + specs(0, 5),
        out_specs=tuple(specs(0, 5)),
        out_shape=shapes([((1, cols), F32), ((1, 1), F32), (dh.shape, BF16), (dh.shape, BF16), (de.shape, F32)]),
        scratch_shapes=[
            pltpu.VMEM(tail.shape, F32), pltpu.VMEM((1, cols), F32), pltpu.VMEM((1, 1), F32),
            pltpu.VMEM((n, pieces, cols, quarter), BF16), pltpu.VMEM((n, quarter, width), BF16), pltpu.VMEM((width, quarter), BF16),
            pltpu.VMEM((n, quarter, width), BF16), pltpu.VMEM(de.shape, F32), pltpu.SemaphoreType.DMA((7 * n,)),
        ],
        compiler_params=pltpu.CompilerParams(vmem_limit_bytes=limit),
    )(jnp.asarray(table.reshape(-1)), tail, x0, x5, dh, de)


def solution(mesh):
    return build(mesh, mesh.shape["tp"], 256, digits("12222")[0], 256, 6, 67_000_000)


def build(mesh, n, tile, tiles, vt, n_block, limit):
    fsdp_size = mesh.shape["fsdp"]

    def device_step(emb_shard, tok_ids, lab_ids, h_last, g_embed, norm_w):
        vocab_rows, cols = emb_shard.shape
        batch_loc, seq_len, width = h_last.shape
        tok_count = batch_loc * seq_len
        fsdp_id = lax.axis_index("fsdp")
        scale = float(np.asarray(math.sqrt(width)).astype(jnp.bfloat16))
        dims = {
            "n": n, "tok": tok_count, "vocab": vocab_rows, "width": width, "total": tok_count * fsdp_size, "vt": vt,
            "tile": tile, "tiles": tiles, "scale": scale, "n_block": n_block,
            "stages": digits("021 121 030 031") + digits("010 011 130 131") + digits("110 111 000 001") + digits("100 101"),
            "front_sems": (106, 59), "back_sems": (72, 30),
        }
        h_flat = h_last.reshape(tok_count, width)
        placed = lax.dynamic_update_slice(jnp.zeros((SUB, width), F32), jnp.broadcast_to(norm_w, (SUB, cols)), (0, fsdp_id * cols))
        ids = [a.reshape(1, tok_count) for a in (tok_ids, lab_ids)]
        table, xn_t, xpar_t, g_t, gpar_t, far, dz, dzp, x0, q5, _, gain, loss_part, tokc = front(
            dims, limit, emb_shard.T, *ids, norm_w.reshape(1, cols), h_flat, g_embed.reshape(tok_count, width))
        tail, d_hidden, d_cols, x5 = back(dims, limit, gain, loss_part, tokc, far, dz, dzp, table, xn_t, xpar_t, g_t, gpar_t, h_flat, q5)
        d_norm_w, loss, x_emb, d_hidden, d_cols = finish(n, scale, limit, tail, x0, x5, d_hidden, d_cols)
        return (x_emb.reshape(h_last.shape), loss.reshape(()), d_hidden.reshape(h_last.shape), d_norm_w.reshape(cols), d_cols.T)

    spec_tok = P("fsdp", None)
    spec_act = P("fsdp", None, None)
    return jax.shard_map(device_step, mesh=mesh, in_specs=(P("tp", "fsdp"), spec_tok, spec_tok, spec_act, spec_act, P("fsdp")), out_specs=(spec_act, P(), spec_act, P("fsdp"), P("tp", "fsdp")), check_vma=False)
```

```python
import functools
import math
import jax
import numpy as np
import jax.numpy as jnp
from jax import lax
from jax.experimental import pallas as pl
from jax.experimental.pallas import tpu as pltpu
from jax.sharding import PartitionSpec as P

SOFT_CAP = 30.0
NORM_EPS = 1e-6
F32, BF16, I32 = jnp.float32, jnp.bfloat16, jnp.int32
LANE, SUB = 128, 8
BOTH = (0, 1)
FOUR = range(4)
WAYS = (1, 3)
FROM = (3, 1)
FAR = 2
CORES = 2


def span(start, size, unit=LANE):
    return pl.ds(pl.multiple_of(start, unit), size)


class Place:
    def __init__(self, n, sends, recvs, local_sems):
        self.n, self.sends, self.recvs, self.local_sems = n, sends, recvs, local_sems
        self.x = lax.axis_index("tp")
        f = lax.axis_index("fsdp")
        self.f = f
        self.c = f % CORES
        self.y = f // CORES % n
        self.z = f // CORES // n
        self.link_of, self.local_of, self.n_link, self.n_local = {}, {}, 0, 0
        self.size = {"dx": n, "dz": n, "dy": n, "dc": CORES}
        self.me = {"dx": self.x, "dz": self.z, "dy": self.y, "dc": self.c}

    def at(self, dx=0, dz=0, dy=0, dc=0):
        n = self.n
        z, y, c = (self.z + dz) % n, (self.y + dy) % n, (self.c + dc) % CORES
        return ((self.x + dx) % n, (z * n + y) * CORES + c)

    def knock(self):
        peers = [self.at(**{d: k}) for d in self.size for k in range(1, self.size[d])]
        for peer in peers:
            pl.semaphore_signal(pltpu.get_barrier_semaphore(), inc=1, device_id=peer, device_id_type=pl.DeviceIdType.MESH)
        return len(peers)

    def enter(self, knocks):
        pl.semaphore_wait(pltpu.get_barrier_semaphore(), knocks)

    def link(self, key, count=1):
        if key not in self.link_of:
            self.link_of[key] = self.n_link
            self.n_link += count
        return self.link_of[key]

    def send(self, key, src, dst, **step):
        i = self.link(key)
        return pltpu.make_async_remote_copy(
            src, dst, self.sends.at[i], self.recvs.at[i], device_id=self.at(**step), device_id_type=pl.DeviceIdType.MESH)

    def local(self, key, src, dst, slot=0, count=2):
        if key not in self.local_of:
            self.local_of[key] = self.n_local
            self.n_local += count
        return pltpu.make_async_copy(src, dst, self.local_sems.at[self.local_of[key] + slot])


class SmallSum:
    def __init__(self, place, dims, slots):
        self.place, self.slots, self.dims, self.base = place, slots, dims, {}
        count = 0
        for d in dims:
            self.base[d] = count
            count += place.size[d]

    def copies(self, d):
        slot = self.slots.at[self.base[d] + self.place.me[d]]
        for k in range(1, self.place.size[d]):
            yield self.place.send((self.dims, d, k), slot, slot, **{d: k})

    def start(self, d, value):
        self.slots[self.base[d] + self.place.me[d]] = value
        for copy in self.copies(d):
            copy.start()

    def finish(self, d):
        for copy in self.copies(d):
            copy.wait()
        total = self.slots[self.base[d]]
        for k in range(1, self.place.size[d]):
            total = total + self.slots[self.base[d] + k]
        return total


def scope(name):
    return jax.named_scope(name)


def start_all(copies):
    for copy in copies:
        copy.start()


def digits(text):
    return tuple(tuple(int(d) for d in word) for word in text.split())


UNITS = [digits(u) for u in ("00", "10 30", "01 03 20", "02 11 31", "13 33 21 23", "12 32 22")]
PAIR, ALL = 1, "all"
PIECES = [2 * len(u) for u in UNITS]
EXP_RATE = SOFT_CAP * math.log2(math.e)
BASE = [sum(PIECES[:i]) for i in range(len(UNITS))]


def front_kernel(
    dims,
    shard_hbm, tok_hbm, lab_hbm, w_hbm, h_hbm, g_hbm,
    et_out, xnt_out, xpar_out, gt_out, gpar_out, lt_out, dz_out, dzpar_out, x0_out, q5_out, u_hbm, gain_hbm, loss_hbm, tokc_hbm,
    shard_ref, tok_ref, lab_ref, w_ref, gain_out, loss_out, tokc_out, shard_t, chunk, tokr, hit_t, lhs, xp, xw, xr, xf, xg, xq, etb, xn, gl, z_even, z_odd, dzb,
    acc_e, acc_l, inv_s, labc, w_slots, s_slots, sends, recvs, local_sems,
):
    n, tok, vocab, width, vt = dims["n"], dims["tok"], dims["vocab"], dims["width"], dims["vt"]
    place = Place(n, sends, recvs, local_sems)
    x, z, y, c = place.x, place.z, place.y, place.c
    half_v = vocab // CORES
    n_tile = vocab // vt
    n_half = n_tile // CORES
    hh = n_half // 2
    cols = width // (n * n * CORES)
    quarter = tok // n
    row_start = x * vocab

    def ring1(h, k):
        return {"dy": k} if h == 0 else {"dz": k}

    def ring2(h, k):
        return {"dz": k} if h == 0 else {"dy": k}

    def coord(base, k, paired):
        every = slice(None)
        if k == ALL:
            return every, every
        return every if paired else (base + k) % n // 2, (base + k) % 2

    def loc(h, k1, k2, lo=0, size=n_half, pair1=False, pair2=False):
        first, second = coord((y, z)[h], k1, pair1), coord((z, y)[h], k2, pair2)
        return et_out.at[(pl.ds(c * n_half + lo, size), *((second, first)[h]), *((first, second)[h]), h)]

    knocks = place.knock()
    early_loads = [
        place.local(("in", i), src, dst, 0, 1)
        for i, (src, dst) in enumerate(((shard_hbm, shard_ref), (tok_hbm, tok_ref), (lab_hbm, lab_ref), (w_hbm, w_ref)))
    ]
    start_all(early_loads)
    load_g = place.local("g", g_hbm, xn)
    load_g.start()
    with scope("f_cast"):
        for copy in early_loads:
            copy.wait()
        for t in range(n_tile):
            shard_t[t] = shard_ref[:, pl.ds(t * vt, vt)].astype(BF16)
    with scope("f_enter"):
        place.enter(knocks)
    with scope("f_swap"):
        tokr[c] = jnp.broadcast_to(tok_ref[...], (SUB, tok))
        give_tok = place.send("tok", tokr.at[c], tokr.at[c], dc=1)
        give_chunk = place.send("chunk", shard_t.at[pl.ds((1 - c) * n_half, n_half)], chunk.at[c], dc=1)
        give_chunk.start()
        give_tok.start()
        chunk[c] = shard_t[pl.ds(c * n_half, n_half)]
        gain_sum = SmallSum(place, ("dc", "dy", "dz"), w_slots)
        own_w = jnp.concatenate([w_ref[...], jnp.zeros((1, width - cols), F32)], axis=1)
        gain_sum.start("dc", pltpu.roll(jnp.broadcast_to(own_w, (SUB, width)), place.f * cols, axis=1)[0:1])

    def p1_send(h, i):
        return place.send(("p1", h, i), chunk.at[h], loc(h, 0, 0), **ring1(h, WAYS[i]))

    def p1_fwd(h, i):
        ref = loc(h, FROM[i], 0, i * hh, hh)
        return place.send(("p1f", h, i), ref, ref, **ring1(h, WAYS[i]))

    def p2_send(h, k1, i):
        ref = loc(h, k1, 0, pair1=k1 == PAIR)
        return place.send(("p2", h, k1, i), chunk.at[h] if k1 == 0 else ref, ref, **ring2(h, WAYS[i]))

    def p2_fwd(h, k1, i):
        ref = loc(h, k1, FROM[i], i * hh, hh, pair1=k1 == PAIR)
        return place.send(("p2f", h, k1, i), ref, ref, **ring2(h, WAYS[i]))

    def keep(h):
        return place.local("keep", chunk.at[h], loc(h, 0, 0), h)

    def share(h, k2):
        ref = loc(h, ALL, k2, pair2=k2 == PAIR)
        return place.send(("share", h, k2), ref, ref, dc=1)

    def pass_first():
        with scope("f_p1"):
            for h in BOTH:
                for i in BOTH:
                    p1_send(h, i).wait_recv()
                    p1_fwd(h, i).start()
            for h in BOTH:
                start_all(p2_send(h, PAIR, i) for i in BOTH)

    def pass_first_far():
        with scope("f_p1f"):
            for h in BOTH:
                for i in BOTH:
                    p1_fwd(h, i).wait_recv()
                start_all(p2_send(h, FAR, j) for j in BOTH)

    def pass_second(k1):
        with scope("f_p2"):
            for h in BOTH:
                for i in BOTH:
                    p2_send(h, k1, i).wait_recv()
                    p2_fwd(h, k1, i).start()

    def end_second(k1):
        with scope("f_p2f"):
            for h in BOTH:
                for i in BOTH:
                    p2_fwd(h, k1, i).wait_recv()

    def share_group(k2):
        start_all(share(h, k2) for h in BOTH)

    with scope("f_chunk"):
        give_chunk.wait_recv()
        start_all(keep(h) for h in BOTH)
        gain_sum.start("dy", gain_sum.finish("dc"))
        for h in BOTH:
            start_all(p1_send(h, i) for i in BOTH)
        for h in BOTH:
            start_all(p2_send(h, 0, i) for i in BOTH)

    v_step = min(LANE, half_v)

    def hit_body(j, carry):
        off = j * v_step
        ids = lax.broadcasted_iota(I32, (v_step, tok), 0) + (row_start + c * half_v + off)
        for i, core in enumerate((c, 1 - c)):
            hit_t[span(off, v_step, v_step), pl.ds(i * tok, tok)] = jnp.where(ids == tokr[core, 0:1, :], 1.0, 0.0).astype(BF16)
        return carry

    def make_hits():
        with scope("f_hit"):
            give_tok.wait_recv()
            lax.fori_loop(0, half_v // v_step, hit_body, 0)

    most = max(PIECES)

    def whole(u):
        return pl.ds(BASE[u], PIECES[u])

    def unit_copies(u):
        slot = u % 2
        for p, (h, (k1, k2)) in enumerate((h, k) for h in BOTH for k in UNITS[u]):
            yield place.local("lhs", loc(h, k1, k2), lhs.at[slot, p], slot * most + p, 2 * most)

    def load_unit(u):
        start_all(unit_copies(u))

    def look(u):
        pieces = PIECES[u]
        with scope("f_look"):
            if u > 1:
                x_swap(u - 2).wait_send()
            left = lhs.at[u % 2]
            for copy in unit_copies(u):
                copy.wait()
            n_step = min(2 * vt if pieces > n else vt, tok)
            per_core = tok // n_step

            def body(j, carry):
                value = jnp.concatenate([left[pl.ds(0, pieces), t].reshape(pieces * cols, vt) for t in range(n_half)], axis=1)
                rows = jnp.dot(value, hit_t[:, span(j * n_step, n_step)], preferred_element_type=F32)
                rows = rows.reshape(pieces, cols, n_step).astype(BF16)
                xw[u % 2, j // per_core, pl.ds(0, pieces), :, span(j % per_core * n_step, n_step)] = rows
                return carry

            lax.fori_loop(0, CORES * per_core, body, 0)
            x_swap(u).start()

    def x_swap(u):
        return place.send(("swap", u), xw.at[u % 2, 1, pl.ds(0, PIECES[u])], xr.at[whole(u)], dc=1)

    def lanes_of(k):
        return span((x + k) % n * quarter, quarter, quarter)

    def side(u, i):
        return pl.ds(BASE[u] + i * len(UNITS[u]), len(UNITS[u]))

    def x_far(u, i):
        return place.send(("xf", u, i), xp.at[side(u, i), :, lanes_of(FAR)], xf.at[side(u, i)], dx=WAYS[i])

    def x_near(u, i):
        return place.send(("xn", u, i), xp.at[whole(u), :, lanes_of(WAYS[i])], xg.at[i, whole(u)], dx=WAYS[i])

    def x_goal(k, sel):
        return x0_out.at[(x + k) % n, sel]

    def x_put(u, i):
        return place.send(("xp", u, i), xq.at[whole(u)], x_goal(0, whole(u)), dx=WAYS[i])

    last_unit = len(UNITS) - 1

    def x_keep(u):
        goal = x_goal(0, whole(u)) if u < last_unit else q5_out
        return place.local("x0", xq.at[whole(u)], goal, u, len(UNITS))

    def x_pass(u, i):
        ref = x_goal(FROM[i], side(u, i))
        return place.send(("xs", u, i), ref, ref, dx=WAYS[i])

    def x_first(u):
        with scope("f_x1"):
            x_swap(u).wait_recv()
            def body(p, carry):
                xp[BASE[u] + p] = xw[u % 2, 0, p] + xr[BASE[u] + p]
                return carry

            lax.fori_loop(0, PIECES[u], body, 0)
            start_all(x_far(u, i) for i in BOTH)

    def x_second(u):
        with scope("f_x2"):
            for i in BOTH:
                x_far(u, i).wait_recv()
                sel, lanes = side(u, i), lanes_of(WAYS[i])
                xp[sel, :, lanes] = xp[sel, :, lanes] + xf[sel]
                x_near(u, i).start()

    def x_third(u):
        with scope("f_x3"):
            for i in BOTH:
                x_near(u, i).wait_recv()
            sel = whole(u)
            xq[sel] = xp[sel, :, lanes_of(0)] + xg[0, sel] + xg[1, sel]
            if u < last_unit:
                start_all(x_put(u, i) for i in BOTH)
            x_keep(u).start()

    def x_fourth(u):
        with scope("f_x4"):
            for i in BOTH:
                x_put(u, i).wait_recv()
                x_pass(u, i).start()

    n_part = n * n * CORES // 2

    def moves(key, part, whole_t, other):
        sel = pl.ds(part * n_part, n_part)
        yield place.local(key, gl.at[sel], whole_t.at[sel], part)
        yield place.send((key, part), gl.at[sel], other.at[sel], dc=1)

    def move_g(part):
        return moves("g", part, gt_out, gpar_out)

    def move_xn(part):
        return moves("xt", part, xnt_out, xpar_out)

    def transpose_part(part, copies):
        block = width // dims["n_block"]
        first = part * dims["n_block"] // 2
        turned = [xn[:, pl.ds((first + j) * block, block)].T for j in range(dims["n_block"] // 2)]
        gl[pl.ds(part * n_part, n_part)] = jnp.concatenate(turned, axis=0).reshape(n_part, cols, tok)
        start_all(copies)

    def columns(row):
        return jnp.broadcast_to(row.astype(F32), (LANE, tok)).T.astype(I32)

    r_step = min(LANE, tok)

    def xn_body(j, carry):
        sel = span(j * r_step, r_step, r_step)
        h_wide = xn[sel].astype(F32)
        inv_rms = lax.rsqrt(jnp.sum(h_wide * h_wide, axis=1, keepdims=True) * (1.0 / width) + NORM_EPS)
        xn[sel] = (h_wide * inv_rms * gain_out[0:1]).astype(BF16)
        return carry

    e_step = min(LANE, tok)

    def tile_of(j):
        return (c * n_half + j) % n_tile

    def load_tile(j):
        return place.local("et", et_out.at[tile_of(j)], etb.at[j % 4], j % 4, 4)

    def save_u(i, odd):
        return place.local(("u", odd), (z_even, z_odd)[odd].at[i % 2], u_hbm.at[tile_of(2 * i + odd)], i % 2)

    def lane_blocks():
        return [(b, pl.ds(b, LANE)) for b in range(0, vt, LANE)]

    def post_rows(i, odd, sel, size):
        base = tile_of(2 * i + odd) * vt
        buf, slot = (z_even, z_odd)[odd], i % 2
        ids = lax.broadcasted_iota(I32, (size, LANE), 1) + base
        sum_e, sum_l = acc_e[sel], acc_l[sel]
        for b, lanes in lane_blocks():
            tanh_z = jnp.tanh(buf[slot, sel, lanes] * (1.0 / SOFT_CAP))
            buf[slot, sel, lanes] = tanh_z
            sum_e = sum_e + jnp.exp2(EXP_RATE * tanh_z - EXP_RATE)
            sum_l = sum_l + jnp.where(ids + b == labc[sel], tanh_z, 0.0)
        acc_e[sel] = sum_e
        acc_l[sel] = sum_l

    def post_tile(i, odd):
        def body(e, carry):
            post_rows(i, odd, span(e * e_step, e_step, e_step), e_step)
            return carry

        lax.fori_loop(0, tok // e_step, body, 0)

    def dot_pair(i):
        for odd in BOTH:
            value = etb[(2 * i + odd) % 4].reshape(width, vt)
            (z_even, z_odd)[odd][i % 2] = jnp.dot(xn[...], value, preferred_element_type=F32)

    def load_pair(i):
        start_all(load_tile(2 * i + odd) for odd in BOTH)

    def pair(i, carry):
        for odd in BOTH:
            load_tile(2 * i + odd).wait()

        @pl.when(i > 1)
        def _():
            for odd in BOTH:
                save_u(i - 2, odd).wait()

        m_step = min(vt, tok)
        for m in range(0, tok, m_step):
            for odd in BOTH:
                for e in range(m, m + m_step, r_step):
                    post_rows(i - 1, odd, pl.ds(e, r_step), r_step)
            for odd in BOTH:
                rows = pl.ds(m, m_step)
                value = etb[(2 * i + odd) % 4].reshape(width, vt)
                (z_even, z_odd)[odd][i % 2, rows] = jnp.dot(xn[rows], value, preferred_element_type=F32)

        @pl.when(i < last)
        def _():
            start_all(save_u(i - 1, odd) for odd in BOTH)

        @pl.when(i + 2 < n_tile // 2)
        def _():
            load_pair(i + 2)

        for k, work in enumerate(during):
            @pl.when(i == k + 1)
            def _():
                if k == 0:
                    wait_shares()
                perform(work)
        return carry

    def wait_shares():
        with scope("f_share"):
            for h in BOTH:
                for k2 in (0, PAIR, FAR):
                    share(h, k2).wait_recv()

    def logits_first():
        acc_e[...] = jnp.zeros_like(acc_e)
        acc_l[...] = jnp.zeros_like(acc_l)
        with scope("f_logits0"):
            far_ends(1)
            for odd in BOTH:
                load_tile(odd).wait()
            dot_pair(0)
            if n_tile // 2 > 2:
                load_pair(2)

    def load_first():
        for i in BOTH:
            load_pair(i)

    def put_small(i):
        src, dst = ((gain_out, gain_hbm), (loss_out, loss_hbm), (tokc_out, tokc_hbm))[i]
        return place.local(("out", i), src, dst, 0, 1)

    def lay_columns():
        with scope("f_cols"):
            labc[...] = columns(lab_ref[...] - row_start)
            for i, core in enumerate((c, 1 - c)):
                tokc_out[i] = columns(tokr[core, 0:1, :])
            put_small(2).start()

    def turn_g():
        with scope("f_gt"):
            load_g.wait()
            for part in BOTH:
                transpose_part(part, move_g(part))
            load_h.start()

    def gain_next():
        with scope("f_gain2"):
            gain_sum.start("dz", gain_sum.finish("dy"))

    def normalize():
        with scope("f_xn"):
            gain_out[...] = 1.0 + gain_sum.finish("dz")
            put_small(0).start()
            load_h.wait()
            lax.fori_loop(0, tok // r_step, xn_body, 0)

    def turn_xn():
        with scope("f_xt"):
            for part in BOTH:
                transpose_part(part, move_xn(part))

    spare = BASE[3]
    own_rows, their_rows = (pl.ds(spare + i * 2 * n, 2 * n) for i in BOTH)

    def far_loads(h):
        for i, (src, rows) in enumerate(((gt_out, own_rows), (gpar_out, their_rows))):
            if h == 0:
                yield place.local("far", src.at[pl.ds((z + FAR) % n * 2 * n, 2 * n)], xp.at[rows], i * n, 2 * n)
            else:
                for q in range(n):
                    piece = src.at[pl.ds((q * n + (y + FAR) % n) * 2, 2)]
                    yield place.local("far", piece, xp.at[pl.ds(spare + i * 2 * n + 2 * q, 2)], i * n + q)

    def far_load(h):
        if h == 0:
            for part in BOTH:
                for copy in move_g(part):
                    copy.wait()
        start_all(far_loads(h))

    def put_far(h, j):
        rows = pl.ds(0, 2 * n * cols)
        return place.local("lt", z_even.at[j % 2, rows], lt_out.at[h, :, span(j * vt, vt)], j % 2)

    def far_ends(h):
        for j in range(hh - 2, hh):
            put_far(h, j).wait()

    def far_look(h):
        def body(j, carry):
            @pl.when(j > 1)
            def _():
                put_far(h, j - 2).wait()

            left = jnp.concatenate([xp[rows].reshape(2 * n * cols, tok) for rows in (own_rows, their_rows)], axis=1)
            right = hit_t[span((h * hh + j) * vt, vt)]
            value = lax.dot_general(left, right, (((1,), (1,)), ((), ())), preferred_element_type=F32)
            z_even[j % 2, pl.ds(0, 2 * n * cols)] = value * dims["scale"]
            put_far(h, j).start()
            return carry

        with scope("f_far"):
            for copy in far_loads(h):
                copy.wait()
            if h:
                far_ends(0)
            lax.fori_loop(0, hh, body, 0)

    def begin_unit(u):
        if u == 0:
            for h in BOTH:
                keep(h).wait()
        load_unit(u)

    load_h = place.local("h", h_hbm, xn)
    works = {
        "HIT": make_hits, "GT": turn_g, "COL": lay_columns, "G2": gain_next, "XN": normalize, "XT": turn_xn, "LP": load_first, "L0": logits_first,
        "PF": pass_first, "PFF": pass_first_far,
    }
    groups = {"0": 0, "P": PAIR, "F": FAR}
    families = {"LF": far_load, "FL": far_look, "LU": begin_unit, "LK": look, "X1": x_first, "X2": x_second, "X3": x_third, "X4": x_fourth}
    families_k = {"SH": share_group, "S": pass_second, "E": end_second}

    def perform(text):
        for word in text.split():
            if word in works:
                works[word]()
            elif word[:-1] in families:
                families[word[:-1]](int(word[-1]))
            else:
                families_k[word[:-1]](groups[word[-1]])

    during = (
        "",
        "X24",
        "X15 X33",
        "",
        "X34",
        "X42 X43",
        "",
    )
    for text in (
        "HIT LU0 LK0 G2", "GT X10 PF LU1", "LK1 LF0 S0 X20", "X11 FL0 PFF X21", "LU2 LF1 X30 LK2",
        "FL1 XN SP SH0", "E0 LU3 X12 X31", "LK3 SF LU4 X22", "X40 SHP LK4 X13", "EP X32 X41 EF",
        "LU5 SHF LP XT", "COL L0 X14 LK5", "X23",
    ):
        perform(text)
    if n_half < 4:
        wait_shares()
        for text in during:
            perform(text)
        during = ()
    last = n_tile // 2 - 1
    with scope("f_logits"):
        lax.fori_loop(1, last + 1, pair, 0)
        for odd in BOTH:
            post_tile(last, odd)

    with scope("f_stats"):
        row = lax.broadcasted_iota(I32, (2, tok), 0)
        sum_e = jnp.sum(acc_e[...].T, axis=0, keepdims=True)
        sum_l = SOFT_CAP * jnp.sum(acc_l[...].T, axis=0, keepdims=True)
        stats = SmallSum(place, ("dx",), s_slots)
        stats.start("dx", jnp.where(row == 0, sum_e, sum_l))
    perform("X25 X44")
    with scope("f_stats2"):
        stat = stats.finish("dx")
        all_e, all_l = stat[0:1], stat[1:2]
        inv_s[...] = jnp.broadcast_to((1.0 / dims["total"]) / all_e, (LANE, tok)).T
        s_slots[0, 0:1, :] = jnp.log(all_e) + SOFT_CAP - all_l
        own = s_slots[0, 0:1, lanes_of(0)]
        part_w = min(LANE, quarter)
        folded = own[:, 0:part_w]
        for j in range(part_w, quarter, part_w):
            folded = folded + own[:, j:j + part_w]
        loss_out[...] = jnp.where(lax.broadcasted_iota(I32, (SUB, part_w), 0) == 0, folded, 0.0)
        put_small(1).start()

    def dz_tile(j):
        return ((1 - c) * n_half + j) % n_tile

    def load_u(i, odd):
        return place.local(("u", odd), u_hbm.at[dz_tile(2 * i + odd)], (z_even, z_odd)[odd].at[i % 2], i % 2)

    def put_dz(i, odd):
        return place.local(("dz", odd), dzb.at[odd, i % 2], dz_out.at[dz_tile(2 * i + odd)], i % 2)

    def give_dz(part):
        src = dz_out.at[pl.ds((1 - c) * n_half + part * hh, hh)]
        return place.send(("dz", part), src, dzpar_out.at[pl.ds(part * hh, hh)], dc=1)

    d_step = min(256, tok)

    def dz_rows(i, odd):
        base = dz_tile(2 * i + odd) * vt
        buf, slot = (z_even, z_odd)[odd], i % 2

        def body(e, carry):
            sel = span(e * d_step, d_step, d_step)
            ids = lax.broadcasted_iota(I32, (d_step, LANE), 1) + base
            for b, lanes in lane_blocks():
                tanh_z = buf[slot, sel, lanes]
                prob = jnp.exp2(EXP_RATE * tanh_z - EXP_RATE) * inv_s[sel]
                prob = jnp.where(ids + b == labc[sel], prob - 1.0 / dims["total"], prob)
                dzb[odd, slot, sel, lanes] = (prob * (1.0 - tanh_z * tanh_z)).astype(BF16)
            return carry

        lax.fori_loop(0, tok // d_step, body, 0)

    def dz_pair(i, loaded, follow):
        for odd in BOTH:
            if loaded:
                load_u(i, odd).wait()

            @pl.when(i > hh + 1)
            def _():
                put_dz(i - 2, odd).wait()

            dz_rows(i, odd)
            put_dz(i, odd).start()

            @pl.when(i + follow < n_tile // 2)
            def _():
                load_u(i + follow, odd).start()

    def dz_run(lo, hi, loaded, follow):
        def body(i, carry):
            dz_pair(i, loaded, follow)
            return carry

        lax.fori_loop(lo, hi, body, 0)

    with scope("f_dz"):
        half = hh // 2
        for part in (1, 0):
            dz_run(part * half, (part + 1) * half, not part, hh if part == 0 else -half)
            for i in range(part * half, (part + 1) * half):
                for odd in BOTH:
                    put_dz(i, odd).wait()
            give_dz(part).start()
        dz_run(hh, n_tile // 2, True, half)

    perform("X35")
    with scope("f_end"):
        for i in range(3):
            put_small(i).wait()
        for part in BOTH:
            give_dz(part).wait()
        for i in range(n_tile // 2 - 2, n_tile // 2):
            for odd in BOTH:
                put_dz(i, odd).wait()
        give_tok.wait_send()
        give_chunk.wait_send()
        for h in BOTH:
            for i in BOTH:
                p1_send(h, i).wait_send()
                p1_fwd(h, i).wait_send()
                for k in (0, PAIR, FAR):
                    p2_send(h, k, i).wait_send()
                    p2_fwd(h, k, i).wait_send()
            for k in (0, PAIR, FAR):
                share(h, k).wait_send()
        for part in BOTH:
            for copy in move_xn(part):
                copy.wait()
        for u in range(len(UNITS)):
            if u > len(UNITS) - 3:
                x_swap(u).wait_send()
            x_keep(u).wait()
            for i in BOTH:
                x_far(u, i).wait_send()
                x_near(u, i).wait_send()
                if u < last_unit:
                    x_put(u, i).wait_send()
                    x_pass(u, i).wait()
    assert (place.n_link, place.n_local) <= dims["front_sems"], (place.n_link, place.n_local)


def specs(n_vmem, n_any):
    return [pl.BlockSpec(memory_space=pltpu.VMEM)] * n_vmem + [pl.BlockSpec(memory_space=pl.ANY)] * n_any


def shapes(items):
    return tuple(jax.ShapeDtypeStruct(*item) for item in items)


def scratch(items, n_link, n_local):
    dma = pltpu.SemaphoreType.DMA
    return [pltpu.VMEM(*item) for item in items] + [dma((n_link,)), dma((n_link,)), dma((n_local,))]


def params(collective_id, limit):
    return pltpu.CompilerParams(collective_id=collective_id, has_side_effects=True, vmem_limit_bytes=limit)


def front(dims, limit, shard, tok_row, lab_row, w, h, g):
    n, tok, vocab, width, vt = dims["n"], dims["tok"], dims["vocab"], dims["width"], dims["vt"]
    cols = shard.shape[0]
    half_v = vocab // CORES
    quarter = tok // n
    n_tile, n_half, most = vocab // vt, half_v // vt, max(PIECES)
    pieces = n * n * CORES
    grid = (n // 2, 2, n // 2, 2)
    return pl.pallas_call(
        functools.partial(front_kernel, dims),
        name="front",
        out_shape=shapes([
            ((n_tile, *grid, CORES, cols, vt), BF16), *[((pieces, cols, tok), BF16)] * 4, ((2, 2 * n * cols, half_v // 2), F32), ((n_tile, tok, vt), BF16),
            ((n_half, tok, vt), BF16), ((n, BASE[-1], cols, quarter), BF16), ((PIECES[-1], cols, quarter), BF16), ((n_tile, tok, vt), F32),
            ((1, width), F32), ((SUB, min(LANE, quarter)), F32), ((CORES, tok, LANE), I32),
        ]),
        in_specs=specs(0, 6),
        out_specs=tuple(specs(0, 14)),
        scratch_shapes=scratch([
            (shard.shape, F32), (tok_row.shape, I32), (lab_row.shape, I32), (w.shape, F32), ((1, width), F32),
            ((SUB, min(LANE, quarter)), F32), ((CORES, tok, LANE), I32),
            ((n_tile, cols, vt), BF16), ((CORES, n_half, cols, vt), BF16), ((CORES, SUB, tok), I32), ((half_v, CORES * tok), BF16),
            ((2, most, n_half, cols, vt), BF16), ((pieces, cols, tok), BF16), ((2, CORES, most, cols, tok), BF16), ((pieces, cols, tok), BF16),
            ((pieces, cols, quarter), BF16), ((2, pieces, cols, quarter), BF16), ((pieces, cols, quarter), BF16),
            ((4, *grid, CORES, cols, vt), BF16), ((tok, width), BF16), ((pieces, cols, tok), BF16),
            ((2, tok, vt), F32), ((2, tok, vt), F32), ((2, 2, tok, vt), BF16), ((tok, LANE), F32), ((tok, LANE), F32), ((tok, LANE), F32),
            ((tok, LANE), I32), ((2 * n + CORES, 1, width), F32), ((n, 2, tok), F32),
        ], dims["front_sems"][0], dims["front_sems"][1]),
        compiler_params=params(0, limit),
    )(shard, tok_row, lab_row, w, h, g)


def back_kernel(
    dims,
    gain_hbm, loss_hbm, tokc_hbm, lt_hbm, dz_hbm, dzp_hbm, et_hbm, xnt_hbm, xpar_hbm, gt_hbm, gpar_hbm, h_hbm, q5_hbm,
    tail_hbm, dh_out, de_out, x0_out, ra_hbm, rx_hbm,
    gain_ref, loss_ref, tokc, tail_out, q5, dz_own, dz_par, et_buf, part, fx, acc, fa, f2, r2, xb, h_buf, dh_buf, dg_acc, slots,
    sends, recvs, local_sems,
):
    n, tok, vocab, width, tile, vt = (dims[k] for k in ("n", "tok", "vocab", "width", "tile", "vt"))
    place = Place(n, sends, recvs, local_sems)
    x, z, y, c = place.x, place.z, place.y, place.c
    half_v = vocab // CORES
    n_tile, n_half = vocab // vt, half_v // vt
    lanes = half_v // 2
    rows = width // (n * n)
    half_rows = rows // 2
    quarter = tok // n
    hq = quarter // 2
    tiles = dims["tiles"]
    chunks = len(tiles)
    edges = [sum(tiles[:d]) for d in range(chunks + 1)]
    per_half = n_half // 2

    knocks = place.knock()
    load_q5 = place.local("q5", q5_hbm, q5)
    load_q5.start()
    load_h = place.local("h", h_hbm.at[span(x * quarter, quarter, quarter)], h_buf)

    def load_et(t, slot):
        return place.local("et", et_hbm.at[:, span(t * tile, tile, tile)], et_buf.at[slot], slot)

    slot_of = {FAR: 0, 1: 1, 3: 2, 0: 0}
    stages = dims["stages"]

    def load_stage(m, i):
        half, k, kind = stages[m]
        src = ((gt_hbm, gpar_hbm), (xnt_hbm, xpar_hbm))[kind][i]
        src = src.at[(z + k) % n] if half == 0 else src.at[:, (y + k) % n]
        return place.local(("xb", i), src, xb.at[m % 2, i], m % 2)

    def start_stage(m):
        if m < len(stages):
            start_all(load_stage(m, i) for i in BOTH)

    loads = [place.local("dz", dz_hbm, dz_own), place.local("dzp", dzp_hbm, dz_par)]
    load_et(0, 0).start()
    start_all(loads)
    keep_q5 = place.local("q5", q5, x0_out.at[x], 1)

    def y_put(i):
        return place.send(("yp", i), q5, x0_out.at[x], dx=WAYS[i])

    def y_pass(i):
        size = q5.shape[0] // 2
        ref = x0_out.at[(x + FROM[i]) % n, pl.ds(i * size, size)]
        return place.send(("yq", i), ref, ref, dx=WAYS[i])

    def y_passes():
        for i in BOTH:
            y_put(i).wait_recv()
            y_pass(i).start()

    small_loads = [
        place.local(("in", i), src, dst, 0, 1)
        for i, (src, dst) in enumerate(((tokc_hbm, tokc), (gain_hbm, gain_ref), (loss_hbm, loss_ref)))
    ]
    fars = [place.local("lt", lt_hbm.at[half], acc.at[half, 0], half) for half in BOTH]
    start_all(fars + small_loads)
    for m in BOTH:
        start_stage(m)
    load_h.start()

    def columns(d):
        return pl.ds(edges[d] * tile, tiles[d] * tile)

    def dxn_chunk(d):
        def body(t, carry):
            slot = t % 2

            @pl.when(t + 1 < edges[chunks])
            def _():
                load_et(t + 1, 1 - slot).start()

            load_et(t, slot).wait()
            left = jnp.concatenate([dz_own[j] for j in range(n_tile)], axis=1)
            right = jnp.concatenate([et_buf[slot, j] for j in range(n_tile)], axis=1)
            part[:, span(t * tile, tile, tile)] = lax.dot_general(
                left, right, (((1,), (1,)), ((), ())), preferred_element_type=F32)
            return carry

        with scope("b_dxn"):
            lax.fori_loop(edges[d], edges[d + 1], body, 0)

    def qrow(k, lo=0, size=hq):
        return span((x + k) % n * quarter + lo, size, SUB)

    def x_far(d, i):
        return place.send(("xf", d, i), part.at[qrow(FAR, i * hq), columns(d)], fx.at[i, :, columns(d)], dx=WAYS[i])

    def x_near(d, i, j):
        src = part.at[qrow(WAYS[i], j * hq), columns(d)]
        return place.send(("xn", d, i, j), src, rx_hbm.at[i, pl.ds(j * hq, hq), columns(d)], dx=WAYS[i])

    def x_first(d):
        start_all(x_far(d, i) for i in BOTH)

    def x_second(d):
        with scope("b_x2"):
            for i in BOTH:
                x_far(d, i).wait_recv()
                sel = qrow(WAYS[i], i * hq)
                part[sel, columns(d)] = part[sel, columns(d)] + fx[i, :, columns(d)]
                start_all(x_near(d, i, j) for j in BOTH)

    def stage_x(d, j, i):
        return place.local("sx", rx_hbm.at[i, pl.ds(j * hq, hq), columns(d)], fx.at[i, :, columns(d)], i)

    def x_third(d, j):
        with scope("b_x3"):
            for i in BOTH:
                x_near(d, i, j).wait_recv()
                stage_x(d, j, i).start()
            for i in BOTH:
                stage_x(d, j, i).wait()
            sel = qrow(0, j * hq)
            part[sel, columns(d)] = part[sel, columns(d)] + fx[0, :, columns(d)] + fx[1, :, columns(d)]

    def de_stage(half, k, kind):
        m = stages.index((half, k, kind))
        slot = slot_of[k]

        wide = min(2, per_half) if kind and k else 1

        def right(i, t):
            if kind:
                return dz_par[t] if i else dz_own[c * n_half + t]
            ids = lax.broadcasted_iota(I32, (tok, LANE), 1) + (x * vocab + c * half_v + t * vt)
            hits = [jnp.where(tokc[i] == ids + b, dims["scale"], 0.0).astype(BF16) for b in range(0, vt, LANE)]
            return jnp.concatenate(hits, axis=1)

        def body(j, carry):
            t = half * per_half + j * wide
            sel = span(j * wide * vt, wide * vt)
            left = jnp.concatenate([xb[m % 2, i].reshape(n * rows, tok) for i in BOTH], axis=1)
            both_right = [jnp.concatenate([right(i, t + q) for i in BOTH], axis=0) for q in range(wide)]
            total = jnp.dot(left, jnp.concatenate(both_right, axis=1), preferred_element_type=F32)
            total = total.reshape(n, rows, wide * vt)
            acc[half, slot, :, :, sel] = acc[half, slot, :, :, sel] + total if kind else total
            return carry

        with scope("b_de" if kind else "b_look"):
            for i in BOTH:
                load_stage(m, i).wait()
            lax.fori_loop(0, per_half // wide, body, 0)
            start_stage(m + 2)

    def de_unit(half, k):
        if k == FAR:
            fars[half].wait()
        else:
            de_stage(half, k, 0)
        de_stage(half, k, 1)

    def ring(half, k):
        return {"dz": k} if half == 0 else {"dy": k}

    def cross(half, k):
        return {"dy": k} if half == 0 else {"dz": k}

    def a_far(half, i):
        return place.send(("af", half, i), acc.at[half, 0, pl.ds(2 * i, 2)], fa.at[half, i], **ring(half, WAYS[i]))

    def a_near(half, i, j):
        sel = pl.ds(2 * j, 2)
        return place.send(("an", half, i, j), acc.at[half, 1 + i, sel], ra_hbm.at[half, i, sel], **ring(half, WAYS[i]))

    def a_first(half):
        start_all(a_far(half, i) for i in BOTH)

    def a_second(half, i):
        with scope("b_a2"):
            a_far(half, i).wait_recv()
            sel = pl.ds(2 * i, 2)
            acc[half, 1 + i, sel] = acc[half, 1 + i, sel] + fa[half, i]
            start_all(a_near(half, i, j) for j in BOTH)

    def stage_a(half, j, i):
        return place.local(("sa", half), ra_hbm.at[half, i, pl.ds(2 * j, 2)], fa.at[half, i], i)

    def piece(half, k):
        return ((y if half == 0 else z) + k) % n

    def c_far(half, i):
        src = acc.at[half, 0, piece(half, FAR), pl.ds(i * half_rows, half_rows)]
        return place.send(("cf", half, i), src, f2.at[half, i], **cross(half, WAYS[i]))

    def c_near(half, i):
        return place.send(("cn", half, i), acc.at[half, 0, piece(half, WAYS[i])], r2.at[half, i], **cross(half, WAYS[i]))

    def a_third(half, j):
        with scope("b_a3"):
            for i in BOTH:
                a_near(half, i, j).wait_recv()
                stage_a(half, j, i).start()
            for i in BOTH:
                stage_a(half, j, i).wait()
            sel = pl.ds(2 * j, 2)
            acc[half, 0, sel] = acc[half, 0, sel] + fa[half, 0] + fa[half, 1]

    def c_first(half):
        start_all(c_far(half, i) for i in BOTH)

    def c_second(half):
        with scope("b_c2"):
            for i in BOTH:
                c_far(half, i).wait_recv()
                at = piece(half, WAYS[i])
                sel = pl.ds(i * half_rows, half_rows)
                acc[half, 0, at, sel] = acc[half, 0, at, sel] + f2[half, i]
                c_near(half, i).start()

    def out_copies(half):
        sel = span(c * half_v + half * lanes, lanes)
        mine = acc.at[half, 0, piece(half, 0)]
        yield place.local("de", mine.at[span(c * half_rows, half_rows, SUB)], de_out.at[:, sel], half)
        yield place.send(("de", half), mine.at[span((1 - c) * half_rows, half_rows, SUB)], de_out.at[:, sel], dc=1)

    def c_third(half):
        with scope("b_c3"):
            for i in BOTH:
                c_near(half, i).wait_recv()
            at = piece(half, 0)
            acc[half, 0, at] = acc[half, 0, at] + r2[half, 0] + r2[half, 1]
            start_all(out_copies(half))

    step = min(32, hq)

    def dh_body(i, carry):
        sel = span(i * step, step, step)
        row = span(x * quarter + i * step, step, step)
        d_x = part[row]
        h_wide = h_buf[sel].astype(F32)
        inv_rms = lax.rsqrt(jnp.sum(h_wide * h_wide, axis=1, keepdims=True) * (1.0 / width) + NORM_EPS)
        h_norm = h_wide * inv_rms
        g_dir = d_x * gain_ref[0:1]
        mean = jnp.sum(g_dir * h_norm, axis=1, keepdims=True) * (1.0 / width)
        dh_buf[sel] = (inv_rms * (g_dir - h_norm * mean)).astype(BF16)
        prod = d_x * h_norm
        total = prod[0:SUB]
        for j in range(SUB, step, SUB):
            total = total + prod[j:j + SUB]
        dg_acc[...] = dg_acc[...] + total
        return carry

    def h_first(i, j):
        return place.send(("hf", i, j), dh_buf.at[pl.ds(j * hq, hq)], dh_out.at[qrow(0, j * hq)], dx=WAYS[i])

    def h_second(i):
        ref = dh_out.at[qrow(FROM[i], i * hq)]
        return place.send(("hs", i), ref, ref, dx=WAYS[i])

    keep_dh = place.local("dh", dh_buf, dh_out.at[qrow(0, 0, quarter)])
    small = SmallSum(place, ("dc", "dx", "dy", "dz"), slots)
    per_j = hq // step

    def dh_part(j):
        with scope("b_dh"):
            if j == 0:
                load_h.wait()
            lax.fori_loop(j * per_j, (j + 1) * per_j, dh_body, 0)
            start_all(h_first(i, j) for i in BOTH)
            if j:
                keep_dh.start()

    def h_pass(i):
        with scope("b_h2"):
            h_first(i, i).wait_recv()
            h_second(i).start()

    put_tail = place.local("tail", tail_out, tail_hbm, 0, 1)

    def small_step(k):
        dims_of = small.dims
        with scope("b_s"):
            if k == 1:
                sums = [jnp.sum(part_sum, axis=0, keepdims=True) for part_sum in (dg_acc[...], loss_ref[...])]
                small.start(dims_of[0], jnp.concatenate(sums, axis=1))
            elif k <= len(dims_of):
                small.start(dims_of[k - 1], small.finish(dims_of[k - 2]))
            else:
                total = small.finish(dims_of[-1])
                loss = jnp.sum(total[:, width:], axis=1, keepdims=True) * (1.0 / dims["total"])
                tail_out[...] = jnp.concatenate([total[:, 0:width], jnp.broadcast_to(loss, (1, LANE))], axis=1)
                put_tail.start()

    def dxn(d):
        dxn_chunk(d)
        x_first(d)

    def unit(half, k):
        if k == 0:
            with scope("b_wait_far"):
                for i in BOTH:
                    a_far(half, i).wait_send()
        while len(loads) > 1:
            loads.pop().wait()
            for copy in small_loads:
                copy.wait()
        de_unit(half, k)
        if k == FAR:
            a_first(half)

    families = {
        "CH": dxn, "XS": x_second, "UN": unit, "AS": a_second, "XT": x_third, "AT": a_third, "CF": c_first, "CS": c_second,
        "CT": c_third, "DH": dh_part, "SM": small_step, "HP": h_pass, "YQ": y_passes,
    }

    def perform(text):
        for word in text.split():
            families[word[:2]](*(int(digit) for digit in word[2:]))

    with scope("b_enter"):
        place.enter(knocks)
    with scope("b_load"):
        load_q5.wait()
        start_all(y_put(i) for i in BOTH)
        keep_q5.start()
        loads[0].wait()
        dg_acc[...] = jnp.zeros_like(dg_acc)
    for text in (
        "CH0 UN02 YQ CH1", "UN12 CH2 UN03 XS1", "UN01 XS2 UN13 AS01", "AS00 UN11 AS11 AS10",
        "XS0 CH3 XT10 CH4", "UN00 XT00 XS3 XT01", "XS4 UN10 XT20 AT00", "XT30 XT21 XT11 XT40",
        "DH0 XT31 XT41 DH1", "AT01 AT10 CF0 SM1", "AT11 CF1 SM2 HP0", "CS0 CS1 SM3 HP1", "CT0 SM4 CT1 SM5",
    ):
        perform(text)

    with scope("b_end_x"):
        put_tail.wait()
        keep_dh.wait()
        keep_q5.wait()
        for i in BOTH:
            y_put(i).wait_send()
            y_pass(i).wait()
            for d in range(chunks):
                x_far(d, i).wait_send()
                for j in BOTH:
                    x_near(d, i, j).wait_send()
            h_first(i, i).wait_send()
            h_first(i, 1 - i).wait()
            h_second(i).wait()
    with scope("b_end_a"):
        for half in BOTH:
            for i in BOTH:
                for j in BOTH:
                    a_near(half, i, j).wait_send()
                c_far(half, i).wait_send()
                c_near(half, i).wait_send()
            for copy in out_copies(half):
                copy.wait()
    assert (place.n_link, place.n_local) <= dims["back_sems"], (place.n_link, place.n_local)


def back(dims, limit, gain, loss, tokc, far, dz, dzp, et, xnt, xpar, gt, gpar, h, q5):
    n, tok, vocab, width, tile = (dims[k] for k in ("n", "tok", "vocab", "width", "tile"))
    rows = width // (n * n)
    half_v = vocab // CORES
    lanes = half_v // 2
    quarter = tok // n
    hq = quarter // 2
    tail_w = width + loss.shape[1]
    n_tile, n_half, vt = dz.shape[0], dzp.shape[0], dims["vt"]
    turned = [a.reshape(n, n, rows, tok) for a in (xnt, xpar, gt, gpar)]
    return pl.pallas_call(
        functools.partial(back_kernel, dims),
        name="back",
        out_shape=shapes([
            ((1, width + LANE), F32), ((tok, width), BF16), ((rows // CORES, vocab), F32), ((n, *q5.shape), BF16),
            ((2, 2, n, rows, lanes), F32),
            ((2, quarter, width), F32),
        ]),
        in_specs=specs(0, 13),
        out_specs=tuple(specs(0, 6)),
        scratch_shapes=scratch([
            (gain.shape, F32), (loss.shape, F32), (tokc.shape, I32), ((1, width + LANE), F32),
            (q5.shape, BF16), ((n_tile, tok, vt), BF16), ((n_half, tok, vt), BF16), ((2, n_tile, tile, vt), BF16), ((tok, width), F32),
            ((2, hq, width), F32), ((2, 3, n, rows, lanes), F32), ((2, 2, 2, rows, lanes), F32),
            ((2, 2, rows // 2, lanes), F32), ((2, 2, rows, lanes), F32), ((2, CORES, n, rows, tok), BF16), ((quarter, width), BF16),
            ((quarter, width), BF16), ((SUB, width), F32), ((3 * n + CORES, 1, tail_w), F32),
        ], dims["back_sems"][0], dims["back_sems"][1]),
        compiler_params=params(1, limit),
    )(gain, loss, tokc, far.reshape(2, n, rows, lanes), dz, dzp, et.reshape(n_tile, width, vt), *turned, h, q5)[:4]


def finish_kernel(
    n, scale, table_ref, tail_hbm, x0_hbm, x5_hbm, dh_hbm, de_hbm, dg_hbm, loss_hbm, x0_out, dh_out, de_out,
    tail_ref, dg_out, loss_out, x0_in, x0_buf, rows_ref, dh_buf, de_buf, sems,
):
    place = Place(n, None, None, sems)
    quarter, cols, width = x0_in.shape[3], x0_in.shape[2], x0_buf.shape[2]

    def step(q):
        rows = span(q * quarter, quarter, quarter)
        return (
            place.local("x0", x0_hbm.at[q], x0_in.at[q, pl.ds(0, BASE[-1])], q, n),
            place.local("x5", x5_hbm.at[q], x0_in.at[q, pl.ds(BASE[-1], PIECES[-1])], q, n), place.local("x0o", x0_buf.at[q], x0_out.at[rows], q, n),
            place.local("dh", dh_hbm.at[rows], dh_buf.at[q], q, n), place.local("dho", dh_buf.at[q], dh_out.at[rows], q, n),
        )

    moves = [step(q) for q in range(n)]
    de_in, de_put = place.local("de", de_hbm, de_buf, 0), place.local("de", de_buf, de_out, 1)
    for x0_load, x5_load, _, dh_load, _ in moves:
        start_all((x0_load, x5_load, dh_load))
    de_in.start()
    tail_in = place.local("tail", tail_hbm, tail_ref)
    small_puts = [place.local("dg", dg_out, dg_hbm), place.local("loss", loss_out, loss_hbm)]
    tail_in.start()
    tail_in.wait()
    gain = jnp.broadcast_to(tail_ref[:, 0:width], (SUB, width))
    dg_out[...] = pltpu.roll(gain, width - place.f * cols, axis=1)[0:1, 0:cols]
    loss_out[...] = tail_ref[:, width:width + 1]
    start_all(small_puts)

    def body(q, carry):
        x0_load, x5_load, x0_put, dh_load, dh_put = step(q)
        x0_load.wait()
        x5_load.wait()
        for zi in range(n):
            for yi in range(n):
                for h in BOTH:
                    dz, dy = (zi - place.z) % n, (yi - place.y) % n
                    k1, k2 = (dy, dz) if h == 0 else (dz, dy)
                    piece = table_ref[(h * n + k1) * n + k2]
                    rows_ref[pl.ds(((zi * n + yi) * CORES + h) * cols, cols)] = x0_in[q, piece]
        x0_buf[q] = (rows_ref[...].T.astype(F32) * scale).astype(BF16)
        x0_put.start()
        dh_load.wait()
        dh_put.start()
        return carry

    lax.fori_loop(0, n, body, 0)
    de_in.wait()
    de_put.start()
    for _, _, x0_put, _, dh_put in moves:
        x0_put.wait()
        dh_put.wait()
    de_put.wait()
    for copy in small_puts:
        copy.wait()


def finish(n, scale, limit, tail, x0, x5, dh, de):
    cols, quarter = x0.shape[2:]
    pieces = n * n * CORES
    width = pieces * cols
    table = np.zeros((CORES, n, n), np.int32)
    for u, unit in enumerate(UNITS):
        for h in BOTH:
            for i, (k1, k2) in enumerate(unit):
                table[h, k1, k2] = BASE[u] + h * len(unit) + i
    return pl.pallas_call(
        functools.partial(finish_kernel, n, scale),
        name="finish",
        in_specs=[pl.BlockSpec(memory_space=pltpu.SMEM)] + specs(0, 5),
        out_specs=tuple(specs(0, 5)),
        out_shape=shapes([((1, cols), F32), ((1, 1), F32), (dh.shape, BF16), (dh.shape, BF16), (de.shape, F32)]),
        scratch_shapes=[
            pltpu.VMEM(tail.shape, F32), pltpu.VMEM((1, cols), F32), pltpu.VMEM((1, 1), F32),
            pltpu.VMEM((n, pieces, cols, quarter), BF16), pltpu.VMEM((n, quarter, width), BF16), pltpu.VMEM((width, quarter), BF16),
            pltpu.VMEM((n, quarter, width), BF16), pltpu.VMEM(de.shape, F32), pltpu.SemaphoreType.DMA((7 * n,)),
        ],
        compiler_params=pltpu.CompilerParams(vmem_limit_bytes=limit),
    )(jnp.asarray(table.reshape(-1)), tail, x0, x5, dh, de)


def solution(mesh):
    return build(mesh, mesh.shape["tp"], 256, digits("12222")[0], 256, 6, 67_000_000)


def build(mesh, n, tile, tiles, vt, n_block, limit):
    fsdp_size = mesh.shape["fsdp"]

    def device_step(emb_shard, tok_ids, lab_ids, h_last, g_embed, norm_w):
        vocab_rows, cols = emb_shard.shape
        batch_loc, seq_len, width = h_last.shape
        tok_count = batch_loc * seq_len
        fsdp_id = lax.axis_index("fsdp")
        scale = float(np.asarray(math.sqrt(width)).astype(jnp.bfloat16))
        dims = {
            "n": n, "tok": tok_count, "vocab": vocab_rows, "width": width, "total": tok_count * fsdp_size, "vt": vt,
            "tile": tile, "tiles": tiles, "scale": scale, "n_block": n_block,
            "stages": digits("021 121 030 031") + digits("010 011 130 131") + digits("110 111 000 001") + digits("100 101"),
            "front_sems": (106, 59), "back_sems": (72, 30),
        }
        h_flat = h_last.reshape(tok_count, width)
        placed = lax.dynamic_update_slice(jnp.zeros((SUB, width), F32), jnp.broadcast_to(norm_w, (SUB, cols)), (0, fsdp_id * cols))
        ids = [a.reshape(1, tok_count) for a in (tok_ids, lab_ids)]
        table, xn_t, xpar_t, g_t, gpar_t, far, dz, dzp, x0, q5, _, gain, loss_part, tokc = front(
            dims, limit, emb_shard.T, *ids, norm_w.reshape(1, cols), h_flat, g_embed.reshape(tok_count, width))
        tail, d_hidden, d_cols, x5 = back(dims, limit, gain, loss_part, tokc, far, dz, dzp, table, xn_t, xpar_t, g_t, gpar_t, h_flat, q5)
        d_norm_w, loss, x_emb, d_hidden, d_cols = finish(n, scale, limit, tail, x0, x5, d_hidden, d_cols)
        return (x_emb.reshape(h_last.shape), loss.reshape(()), d_hidden.reshape(h_last.shape), d_norm_w.reshape(cols), d_cols.T)

    spec_tok = P("fsdp", None)
    spec_act = P("fsdp", None, None)
    return jax.shard_map(device_step, mesh=mesh, in_specs=(P("tp", "fsdp"), spec_tok, spec_tok, spec_act, spec_act, P("fsdp")), out_specs=(spec_act, P(), spec_act, P("fsdp"), P("tp", "fsdp")), check_vma=False)
```
